32 devices in a mesh: rep: 2 (over x), shard: 16 (over z, y, core).
Axes of the slice: x: 2, y: 2, z: 4, core: 2. Of those that a mesh axis runs over, the one named last changes fastest.
Arguments:
- tokens: bfloat16 [4096, 2048], P(('rep', 'shard')), may hold values from -6 to 6
- segment_ids: int32 [4096], P(('rep', 'shard')), may hold values from -1 to 31, as said below
- cotangent: bfloat16 [4096, 2048], P(('rep', 'shard')), may hold values from -6 to 6
- w_qkv: bfloat16 [2048, 6144], P('shard'), may hold values from -0.125 to 0.125
- w_out: bfloat16 [2048, 2048], P('shard'), may hold values from -0.125 to 0.125
- w_gate_up: bfloat16 [2048, 16384], P('shard'), may hold values from -0.125 to 0.125
- w_down: bfloat16 [8192, 2048], P('shard'), may hold values from -0.0625 to 0.0625
- q_gain: bfloat16 [2048], P('shard'), may hold values from 0.5 to 1.5
- k_gain: bfloat16 [2048], P('shard'), may hold values from 0.5 to 1.5
- attn_gain: bfloat16 [2048], P('shard'), may hold values from 0.5 to 1.5
- mlp_gain: bfloat16 [2048], P('shard'), may hold values from 0.5 to 1.5
Outputs:
- output: bfloat16 [4096, 2048], P(('rep', 'shard'))
- grad_tokens: float32 [4096, 2048], P(('rep', 'shard'))
- grad_qkv: float32 [2048, 6144], P('shard')
- grad_out: float32 [2048, 2048], P('shard')
- grad_gate_up: float32 [2048, 16384], P('shard')
- grad_down: float32 [8192, 2048], P('shard')
- grad_q_gain: float32 [2048], P('shard')
- grad_k_gain: float32 [2048], P('shard')
- grad_attn_gain: float32 [2048], P('shard')
- grad_mlp_gain: float32 [2048], P('shard')
The draws below stay inside these ranges and needn't reach their ends.
Inputs may be any that keep to these rules, and one draw needn't show every extreme that they name: `segment_ids`: within each block of 128 slots, live slots come first in runs of equal ids numbered upwards from 0 (one packed sequence each), each run starting at a slot whose index within the block is a multiple of 4, then padding slots with id -1; at least one block has no padding and starts a run at every multiple of 4.
All inputs are finite; a program needn't handle non-finite values.
Results may differ from the reference program's by a relative error of at most 0.02.
Values may be sent and summed in bfloat16 or wider, within the bound.
A program may use at most 384 MiB of HBM per device.

```python
import jax
import jax.numpy as jnp
from jax import lax

D = 2048
H = 16
FF = 8192
TOK_DEV = 128
TOKENS = 4096
N_REP = 2
N_SHARD = 16


def draw_segment_ids(key, part):
    device_count = TOKENS // TOK_DEV
    key_fill, key_full, key_start = jax.random.split(key, 3)
    filled = jax.random.randint(key_fill, (device_count,), TOK_DEV // 2, TOK_DEV + 1)
    fullest = jax.random.randint(key_full, (), 0, device_count)
    is_fullest = jnp.arange(device_count) == fullest
    filled = jnp.where(is_fullest, TOK_DEV, filled)
    slots = jnp.arange(TOK_DEV)
    aligned = slots % 4 == 0
    chance = jax.random.randint(key_start, (device_count, TOK_DEV), 0, max(TOK_DEV // 16, 2)) == 0
    starts = aligned[None, :] & (chance | is_fullest[:, None])
    starts = starts.at[:, 0].set(True)
    numbers = jnp.cumsum(starts.astype(jnp.int32), axis=1) - 1
    numbers = jnp.where(slots[None, :] < filled[:, None], numbers, -1)
    return numbers.reshape(-1).astype(jnp.int32)


def steps_of(rng, dims, pieces, low, largest):
    factor_of, own = 1.0, jax.random.fold_in(rng, 6)
    for position, shards_of in pieces:
        heights = jnp.exp(jax.random.uniform(jax.random.fold_in(own, position), (shards_of,), jnp.float32, low / len(pieces), largest / len(pieces)))
        factor_of = factor_of * jnp.repeat(heights, dims[position] // shards_of).reshape([-1 if axis == position else 1 for axis in range(len(dims))])
    return factor_of


def centred(key, extent, deviation, most, cuts=(), kind=jnp.bfloat16):
    values = jax.random.normal(key, extent, jnp.float32) * deviation
    if len(cuts) > 0:
        values = steps_of(key, extent, cuts, -0.22, 0.18) * values
    return jnp.clip(values, min=-most, max=most).astype(kind)


def setup_inputs(seed: int = 0) -> dict:
    key_of = jax.random.split(jax.random.key(seed), 12)
    tokens = centred(key_of[0], (TOKENS, D), 1.0, 6.0, ((0, 32),))
    segment_ids = draw_segment_ids(jax.random.fold_in(key_of[11], 71), 0)
    cotangent = centred(key_of[2], (TOKENS, D), 1.0, 6.0, ((0, 32),))
    w_qkv = centred(key_of[3], (D, 3 * D), D ** -0.5, 0.125, ((0, 16),))
    w_out = centred(key_of[4], (D, D), D ** -0.5, 0.125, ((0, 16),))
    w_gate_up = centred(key_of[5], (D, 2 * FF), D ** -0.5, 0.125, ((0, 16),))
    w_down = centred(key_of[6], (FF, D), FF ** -0.5, 0.0625, ((0, 16),))
    q_gain = jnp.clip(1.0 + 0.1 * jax.random.normal(key_of[7], (D,), jnp.float32), 0.5, 1.5).astype(jnp.bfloat16)
    k_gain = jnp.clip(1.0 + 0.1 * jax.random.normal(key_of[8], (D,), jnp.float32), 0.5, 1.5).astype(jnp.bfloat16)
    attn_gain = jnp.clip(1.0 + 0.1 * jax.random.normal(key_of[9], (D,), jnp.float32), 0.5, 1.5).astype(jnp.bfloat16)
    mlp_gain = jnp.clip(1.0 + 0.1 * jax.random.normal(key_of[10], (D,), jnp.float32), 0.5, 1.5).astype(jnp.bfloat16)
    return {"tokens": tokens, "segment_ids": segment_ids, "cotangent": cotangent, "w_qkv": w_qkv, "w_out": w_out, "w_gate_up": w_gate_up, "w_down": w_down, "q_gain": q_gain, "k_gain": k_gain, "attn_gain": attn_gain, "mlp_gain": mlp_gain}


EPSILON = 1e-06
THETA = 500000.0

def positions(seg_row):
    count = seg_row.shape[0]
    slots = jnp.arange(count, dtype=jnp.int32)
    starts = jnp.concatenate([jnp.ones((1,), jnp.bool_), seg_row[1:] != seg_row[:-1]])
    first = lax.cummax(jnp.where(starts, slots, 0).astype(jnp.int32), axis=0)
    return (slots - first).astype(jnp.int32)

def rope_tables(seg_row, head_width):
    half_width = head_width // 2
    spots = positions(seg_row).astype(jnp.float32)
    inverse = THETA ** (-(2.0 * jnp.arange(half_width, dtype=jnp.float32)) / head_width)
    angle = spots[:, None] * inverse[None, :]
    return (jnp.cos(angle), jnp.sin(angle))

def rotate(matrix, cosine, sine, num_heads):
    count, width = matrix.shape
    shaped = matrix.reshape(count, num_heads, width // num_heads)
    half_width = shaped.shape[2] // 2
    first_half = shaped[..., :half_width]
    second_half = shaped[..., half_width:]
    cos_head = cosine[:, None, :]
    sin_head = sine[:, None, :]
    joined = jnp.concatenate([first_half * cos_head - second_half * sin_head, second_half * cos_head + first_half * sin_head], axis=-1)
    return joined.reshape(count, width)

def allowed(seg_row):
    count = seg_row.shape[0]
    slots = jnp.arange(count)
    return (seg_row[:, None] == seg_row[None, :]) & (slots[None, :] <= slots[:, None])

def norm_forward(vector, gain):
    rscale = lax.rsqrt(lax.optimization_barrier(jnp.mean(vector * vector, axis=-1, keepdims=True)) + EPSILON)
    normed = vector * rscale
    return (normed * gain, normed, rscale)

def norm_backward(upstream, normed, rscale, gain):
    scaled = upstream * gain
    inner = lax.optimization_barrier(jnp.mean(scaled * normed, axis=-1, keepdims=True))
    return (rscale * (scaled - normed * inner), lax.optimization_barrier(jnp.sum(upstream * normed, axis=0)))

def head_split(matrix, num_heads):
    return matrix.reshape(matrix.shape[0], num_heads, -1).astype(jnp.float32)

def attention_scores(query_rot, keys_rot, seg_row, num_heads):
    head_width = query_rot.shape[1] // num_heads
    scores = jnp.einsum('thd,shd->hts', head_split(query_rot, num_heads), head_split(keys_rot, num_heads)) * head_width ** (-0.5)
    return jnp.where(allowed(seg_row)[None], scores, -1e+30)

def attention_forward(query_rot, keys_rot, values_b, seg_row, num_heads):
    scores = attention_scores(query_rot, keys_rot, seg_row, num_heads)
    top = lax.optimization_barrier(jnp.max(scores, axis=-1, keepdims=True))
    log_total = top[..., 0] + jnp.log(lax.optimization_barrier(jnp.sum(jnp.exp(scores - top), axis=-1)))
    probs_b = jnp.exp(scores - log_total[..., None]).astype(jnp.bfloat16)
    context = jnp.einsum('hts,shd->thd', probs_b.astype(jnp.float32), head_split(values_b, num_heads))
    return (context.reshape(query_rot.shape), log_total)

def attention_backward(query_rot, keys_rot, values_b, seg_row, log_total, context, d_context_b, num_heads):
    count, width = query_rot.shape
    head_width = width // num_heads
    scores = attention_scores(query_rot, keys_rot, seg_row, num_heads)
    probs = jnp.exp(scores - log_total[..., None])
    probs_b = probs.astype(jnp.bfloat16)
    d_heads = head_split(d_context_b, num_heads)
    d_values = jnp.einsum('hts,thd->shd', probs_b.astype(jnp.float32), d_heads)
    d_probs = jnp.einsum('thd,shd->hts', d_heads, head_split(values_b, num_heads))
    delta = lax.optimization_barrier(jnp.sum(d_heads * context.reshape(count, num_heads, head_width), axis=-1)).T
    d_scores_b = (probs * (d_probs - delta[..., None]) * head_width ** (-0.5)).astype(jnp.bfloat16)
    d_scores_f = d_scores_b.astype(jnp.float32)
    d_query = jnp.einsum('hts,shd->thd', d_scores_f, head_split(keys_rot, num_heads))
    d_keys = jnp.einsum('hts,thd->shd', d_scores_f, head_split(query_rot, num_heads))
    return (d_query.reshape(count, width), d_keys.reshape(count, width), d_values.reshape(count, width))

def device_pass(tokens_dev, seg_row, cot_dev, w_qkv, w_out, w_gate_up, w_down, q_gain, k_gain, attn_gain, mlp_gain):
    count, width = tokens_dev.shape
    num_heads = H
    ff_width = w_down.shape[0]
    gain_query = q_gain.astype(jnp.float32)
    gain_keys = k_gain.astype(jnp.float32)
    gain_attn = attn_gain.astype(jnp.float32)
    gain_mlp = mlp_gain.astype(jnp.float32)
    cosine, sine = rope_tables(seg_row, width // num_heads)
    qkv = jnp.dot(tokens_dev, w_qkv, preferred_element_type=jnp.float32)
    query_norm, query_hat, query_scale = norm_forward(qkv[:, :width], gain_query)
    keys_norm, keys_hat, keys_scale = norm_forward(qkv[:, width:2 * width], gain_keys)
    query_rot = rotate(query_norm, cosine, sine, num_heads).astype(jnp.bfloat16)
    keys_rot = rotate(keys_norm, cosine, sine, num_heads).astype(jnp.bfloat16)
    values_b = qkv[:, 2 * width:].astype(jnp.bfloat16)
    context, log_total = attention_forward(query_rot, keys_rot, values_b, seg_row, num_heads)
    context_b = context.astype(jnp.bfloat16)
    attn_raw = jnp.dot(context_b, w_out, preferred_element_type=jnp.float32)
    attn_norm, attn_hat, attn_scale = norm_forward(attn_raw, gain_attn)
    resid = tokens_dev.astype(jnp.float32) + attn_norm
    resid_b = resid.astype(jnp.bfloat16)
    gate_up = jnp.dot(resid_b, w_gate_up, preferred_element_type=jnp.float32)
    gate_raw = gate_up[:, :ff_width]
    up_raw = gate_up[:, ff_width:]
    sigma = jax.nn.sigmoid(gate_raw)
    activated = gate_raw * sigma
    mixed_b = (activated * up_raw).astype(jnp.bfloat16)
    down_raw = jnp.dot(mixed_b, w_down, preferred_element_type=jnp.float32)
    down_norm, down_hat, down_scale = norm_forward(down_raw, gain_mlp)
    output = (resid + down_norm).astype(jnp.bfloat16)
    valid = (seg_row >= 0).astype(jnp.float32)[:, None]
    d_out = cot_dev.astype(jnp.float32) * valid
    d_down, grad_mlp = norm_backward(d_out, down_hat, down_scale, gain_mlp)
    d_down_b = d_down.astype(jnp.bfloat16)
    grad_down = jnp.dot(mixed_b.T, d_down_b, preferred_element_type=jnp.float32)
    d_mixed = jnp.dot(d_down_b, w_down.T, preferred_element_type=jnp.float32)
    d_gate = d_mixed * up_raw * sigma * (1.0 + gate_raw * (1.0 - sigma))
    d_up = d_mixed * activated
    d_gu_b = jnp.concatenate([d_gate, d_up], axis=1).astype(jnp.bfloat16)
    grad_gate_up = jnp.dot(resid_b.T, d_gu_b, preferred_element_type=jnp.float32)
    d_resid = d_out + jnp.dot(d_gu_b, w_gate_up.T, preferred_element_type=jnp.float32)
    d_attn, grad_attn = norm_backward(d_resid, attn_hat, attn_scale, gain_attn)
    d_attn_b = d_attn.astype(jnp.bfloat16)
    grad_out = jnp.dot(context_b.T, d_attn_b, preferred_element_type=jnp.float32)
    d_context_b = jnp.dot(d_attn_b, w_out.T, preferred_element_type=jnp.float32).astype(jnp.bfloat16)
    d_query_rot, d_keys_rot, d_values = attention_backward(query_rot, keys_rot, values_b, seg_row, log_total, context, d_context_b, num_heads)
    d_query_norm = rotate(d_query_rot, cosine, -sine, num_heads)
    d_keys_norm = rotate(d_keys_rot, cosine, -sine, num_heads)
    d_query, grad_query = norm_backward(d_query_norm, query_hat, query_scale, gain_query)
    d_keys, grad_keys = norm_backward(d_keys_norm, keys_hat, keys_scale, gain_keys)
    d_qkv_b = jnp.concatenate([d_query, d_keys, d_values], axis=1).astype(jnp.bfloat16)
    grad_qkv = jnp.dot(tokens_dev.T, d_qkv_b, preferred_element_type=jnp.float32)
    grad_tokens = d_resid + jnp.dot(d_qkv_b, w_qkv.T, preferred_element_type=jnp.float32)
    return (output, grad_tokens, (grad_qkv, grad_out, grad_gate_up, grad_down, grad_query, grad_keys, grad_attn, grad_mlp))

def reference(tokens, segment_ids, cotangent, w_qkv, w_out, w_gate_up, w_down, q_gain, k_gain, attn_gain, mlp_gain):
    device_count = N_REP * N_SHARD
    width = tokens.shape[1]
    token_blocks = tokens.reshape(device_count, -1, width)
    seg_blocks = segment_ids.reshape(device_count, -1)
    cot_blocks = cotangent.reshape(device_count, -1, width)
    weights = (w_qkv, w_out, w_gate_up, w_down, q_gain, k_gain, attn_gain, mlp_gain)
    zeros = tuple((jnp.zeros(weight.shape, jnp.float32) for weight in weights))

    def step_block(totals, items):
        tokens_dev, seg_row, cot_dev = items
        output, grad_tokens, grads = device_pass(tokens_dev, seg_row, cot_dev, *weights)
        return (tuple((total + grad for total, grad in zip(totals, grads))), (output, grad_tokens))
    totals, (outputs, grad_rows) = lax.scan(step_block, zeros, (token_blocks, seg_blocks, cot_blocks))
    return (outputs.reshape(-1, width), grad_rows.reshape(-1, width), totals[0], totals[1], totals[2], totals[3], totals[4], totals[5], totals[6], totals[7])
```

```python
import jax
import jax.numpy as jnp
from jax import lax
from jax.sharding import PartitionSpec as P

H = 16
EPSILON = 1e-06
THETA = 500000.0
BF = jnp.bfloat16
F32 = jnp.float32


def positions(seg):
    slots = lax.broadcasted_iota(jnp.int32, seg.shape, 1)
    starts = jnp.concatenate(
        [jnp.ones((seg.shape[0], 1), jnp.bool_), seg[:, 1:] != seg[:, :-1]], axis=1
    )
    first = lax.cummax(jnp.where(starts, slots, 0), axis=1)
    return slots - first


def rope_tables(seg, head_width):
    half_width = head_width // 2
    spots = positions(seg).astype(F32).reshape(-1)
    inverse = THETA ** (-(2.0 * jnp.arange(half_width, dtype=F32)) / head_width)
    angle = spots[:, None] * inverse[None, :]
    return jnp.cos(angle), jnp.sin(angle)


def rotate(matrix, cosine, sine):
    half = matrix.shape[-1] // 2
    a, b = matrix[..., :half], matrix[..., half:]
    return jnp.concatenate([a * cosine - b * sine, b * cosine + a * sine], axis=-1)


def mm(left, right):
    return jnp.dot(left, right, preferred_element_type=F32)


def mm_nt(left, right):
    return lax.dot_general(left, right, (((1,), (1,)), ((), ())), preferred_element_type=F32)


def mm_tn(left, right):
    return lax.dot_general(left, right, (((0,), (0,)), ((), ())), preferred_element_type=F32)


def norm_scale(vector):
    return lax.rsqrt(jnp.mean(vector * vector, axis=-1, keepdims=True) + EPSILON)


def norm_back(upstream, normed, rscale, gain):
    scaled = upstream * gain
    inner = jnp.mean(scaled * normed, axis=-1, keepdims=True)
    return rscale * (scaled - normed * inner), jnp.sum(upstream * normed, axis=0)


def gather(piece):
    return lax.all_gather(piece, "shard", axis=0, tiled=True)


def scatter(partial):
    return lax.psum_scatter(partial.astype(BF), "shard", scatter_dimension=0, tiled=True).astype(F32)


def make(n_rep, n_shard):
    def rep_scatter(x):
        if n_rep == 2:
            me = lax.axis_index("rep")
            mine = lax.dynamic_index_in_dim(x, me, 0, keepdims=False)
            other = lax.dynamic_index_in_dim(x, 1 - me, 0, keepdims=False)
            got = lax.ppermute(other.astype(BF), "rep", [(0, 1), (1, 0)])
            return (mine + got.astype(F32)).astype(BF)
        return lax.psum_scatter(x.astype(BF), "rep", scatter_dimension=0, tiled=False)

    def rep_gather(x):
        if n_rep == 2:
            me = lax.axis_index("rep")
            got = lax.ppermute(x, "rep", [(0, 1), (1, 0)])
            first = jnp.where(me == 0, x, got)
            second = jnp.where(me == 0, got, x)
            return jnp.stack([first, second])
        return lax.all_gather(x, "rep", axis=0, tiled=False)

    def rep_sum(x):
        rows = x.shape[0]
        part = rep_scatter(x.reshape(n_rep, rows // n_rep, x.shape[1]))
        return rep_gather(part).reshape(x.shape).astype(F32)

    def grad_back(x, groups):
        rows, cols = x.shape
        own = rows // n_shard
        width = cols // groups
        split = x.reshape(n_shard, n_rep, own // n_rep, cols).transpose(1, 0, 2, 3)
        part = rep_scatter(split)
        part = lax.all_to_all(part, "shard", split_axis=0, concat_axis=0, tiled=True)
        whole = rep_gather(part)
        whole = whole.reshape(n_rep, n_shard, own // n_rep, groups, width)
        return whole.transpose(0, 2, 3, 1, 4).reshape(own, groups * n_shard * width).astype(F32)

    def columns(w, groups):
        rows, cols = w.shape
        w = w.reshape(rows, groups, n_shard, cols // (groups * n_shard))
        w = lax.all_to_all(w, "shard", split_axis=2, concat_axis=0, tiled=True)
        return w.reshape(rows * n_shard, cols // n_shard)

    def shards(
        tokens, segment_ids, cotangent, w_qkv, w_out, w_gate_up, w_down,
        q_gain, k_gain, attn_gain, mlp_gain,
    ):
        count, width = tokens.shape
        heads = H // n_shard
        hw = width // H
        own = width // n_shard
        ff = w_down.shape[0]
        total = count * n_shard

        small = gather(jnp.stack([segment_ids.astype(BF), attn_gain, mlp_gain])[None])
        tokens_g = gather(tokens)
        wq = columns(w_qkv, 3)
        wg = columns(w_gate_up, 2)
        seg = small[:, 0].astype(jnp.int32)
        gain_attn = small[:, 1].reshape(-1).astype(F32)
        gain_mlp = small[:, 2].reshape(-1).astype(F32)
        gain_query = q_gain.astype(F32)
        gain_keys = k_gain.astype(F32)
        cosine, sine = rope_tables(seg, hw)
        cos3 = cosine[:, None, :]
        sin3 = sine[:, None, :]

        qkv = mm(tokens_g, wq)
        query, keys, values_b = qkv[:, :own], qkv[:, own : 2 * own], qkv[:, 2 * own :].astype(BF)
        squares = jnp.stack([jnp.sum(query * query, axis=-1), jnp.sum(keys * keys, axis=-1)])
        squares = lax.psum(squares, "shard")
        scales = lax.rsqrt(squares / width + EPSILON)
        query_scale, keys_scale = scales[0][:, None], scales[1][:, None]
        query_hat, keys_hat = query * query_scale, keys * keys_scale

        def rot(x, sign):
            return rotate(x.reshape(total, heads, hw), cos3, sign * sin3).reshape(total, own)

        query_rot = rot(query_hat * gain_query, 1.0).astype(BF)
        keys_rot = rot(keys_hat * gain_keys, 1.0).astype(BF)

        slots = jnp.arange(count)
        ok = (seg[:, :, None] == seg[:, None, :]) & (slots[None, :] <= slots[:, None])[None]
        ok = ok[:, None]

        def blocks(x):
            return x.reshape(n_shard, count, heads, hw)

        root = hw ** (-0.5)
        qb, kb, vb = blocks(query_rot), blocks(keys_rot), blocks(values_b)
        scores = jnp.einsum("bthd,bshd->bhts", qb, kb, preferred_element_type=F32) * root
        scores = jnp.where(ok, scores, -1e30)
        top = jnp.max(scores, axis=-1, keepdims=True)
        lse = top + jnp.log(jnp.sum(jnp.exp(scores - top), axis=-1, keepdims=True))
        probs = jnp.exp(scores - lse)
        probs_b = probs.astype(BF)
        context = jnp.einsum("bhts,bshd->bthd", probs_b, vb, preferred_element_type=F32)
        context_b = context.astype(BF).reshape(total, own)

        attn_raw = scatter(mm(context_b, w_out))
        attn_scale = norm_scale(attn_raw)
        attn_hat = attn_raw * attn_scale
        resid = tokens.astype(F32) + attn_hat * gain_attn
        resid_g = gather(resid.astype(BF))

        gate_up = mm(resid_g, wg)
        gate, up = gate_up[:, :ff], gate_up[:, ff:]
        sigma = jax.nn.sigmoid(gate)
        activated = gate * sigma
        mixed_b = (activated * up).astype(BF)
        down_raw = scatter(mm(mixed_b, w_down))
        down_scale = norm_scale(down_raw)
        down_hat = down_raw * down_scale
        output = (resid + down_hat * gain_mlp).astype(BF)

        valid = (segment_ids >= 0).astype(F32)[:, None]
        d_out = cotangent.astype(F32) * valid
        d_down, grad_mlp = norm_back(d_out, down_hat, down_scale, gain_mlp)
        d_down_g = gather(d_down.astype(BF))
        d_mixed = mm_nt(d_down_g, w_down)
        d_gate = d_mixed * up * sigma * (1.0 + gate * (1.0 - sigma))
        d_up = d_mixed * activated
        d_gu_b = jnp.concatenate([d_gate, d_up], axis=1).astype(BF)
        d_resid = d_out + scatter(mm_nt(d_gu_b, wg))
        grad_down = rep_sum(mm_tn(mixed_b, d_down_g))
        grad_gu = grad_back(mm_tn(resid_g, d_gu_b), 2)

        d_attn, grad_attn = norm_back(d_resid, attn_hat, attn_scale, gain_attn)
        d_attn_g = gather(d_attn.astype(BF))
        d_context_b = mm_nt(d_attn_g, w_out).astype(BF)
        grad_out = rep_sum(mm_tn(context_b, d_attn_g))

        db = blocks(d_context_b)
        d_values = jnp.einsum("bhts,bthd->bshd", probs_b, db, preferred_element_type=F32)
        d_probs = jnp.einsum("bthd,bshd->bhts", db, vb, preferred_element_type=F32)
        delta = jnp.sum(db.astype(F32) * context, axis=-1).transpose(0, 2, 1)[..., None]
        d_scores_b = (probs * (d_probs - delta) * root).astype(BF)
        d_query_rot = jnp.einsum("bhts,bshd->bthd", d_scores_b, kb, preferred_element_type=F32)
        d_keys_rot = jnp.einsum("bhts,bthd->bshd", d_scores_b, qb, preferred_element_type=F32)
        d_query_norm = rot(d_query_rot, -1.0)
        d_keys_norm = rot(d_keys_rot, -1.0)
        grad_query = jnp.sum(d_query_norm * query_hat, axis=0)
        grad_keys = jnp.sum(d_keys_norm * keys_hat, axis=0)
        query_up = d_query_norm * gain_query
        keys_up = d_keys_norm * gain_keys
        inner = jnp.stack(
            [jnp.sum(query_up * query_hat, axis=-1), jnp.sum(keys_up * keys_hat, axis=-1)]
        )
        inner = lax.psum(inner, "shard") / width
        d_query = query_scale * (query_up - query_hat * inner[0][:, None])
        d_keys = keys_scale * (keys_up - keys_hat * inner[1][:, None])
        d_qkv_b = jnp.concatenate(
            [d_query, d_keys, d_values.reshape(total, own)], axis=1
        ).astype(BF)
        grad_tokens = d_resid + scatter(mm_nt(d_qkv_b, wq))
        grad_qkv = grad_back(mm_tn(tokens_g, d_qkv_b), 3)

        gains_local = lax.psum_scatter(
            jnp.stack([grad_attn, grad_mlp]), "shard", scatter_dimension=1, tiled=True
        )
        gains = lax.psum(
            jnp.concatenate([gains_local, jnp.stack([grad_query, grad_keys])]), "rep"
        )
        return (
            output, grad_tokens, grad_qkv, grad_out, grad_gu, grad_down,
            gains[2], gains[3], gains[0], gains[1],
        )

    return shards


def solution(mesh):
    rows = P(("rep", "shard"), None)
    return jax.shard_map(
        make(mesh.shape["rep"], mesh.shape["shard"]),
        mesh=mesh,
        in_specs=(rows, P(("rep", "shard")), rows)
        + (P("shard", None),) * 4
        + (P("shard"),) * 4,
        out_specs=(rows, rows) + (P("shard", None),) * 4 + (P("shard"),) * 4,
        check_vma=False,
    )
```

```python
import functools

import jax
import jax.numpy as jnp
from jax import lax
from jax.experimental import pallas as pl
from jax.experimental.pallas import tpu as pltpu
from jax.sharding import PartitionSpec as P

H = 16
EPSILON = 1e-06
THETA = 500000.0
BF = jnp.bfloat16
F32 = jnp.float32
MESH = pl.DeviceIdType.MESH
DMA = pltpu.SemaphoreType.DMA
ANY = pl.BlockSpec(memory_space=pl.ANY)
VM = pl.BlockSpec(memory_space=pltpu.VMEM)
CHUNKS = 2
VMEM_LIMIT = 62 << 20


def position(n_shard):
    s = lax.axis_index("shard")
    return s // 4, (s // 2) % 2, s % 2, n_shard // 4


def index(a, b, c):
    return (a * 2 + b) * 2 + c


def line_order(t, a, na):
    m = jnp.minimum(a, na - 1 - a)
    near = jnp.where(t % 2 == 1, a - (t + 1) // 2, a + (t + 1) // 2)
    far = jnp.where(m == a, t, na - 1 - t)
    return jnp.where(t <= 2 * m, near, far)


def rows_of(i, size):
    return pl.ds(pl.multiple_of(i * size, size), size)


def send(src, dst, ssem, rsem, **target):
    return pltpu.make_async_remote_copy(
        src_ref=src, dst_ref=dst, send_sem=ssem, recv_sem=rsem,
        device_id=target, device_id_type=MESH,
    )


def signal(sem, **target):
    pl.semaphore_signal(sem, inc=1, device_id=target, device_id_type=MESH)


def greet(pos):
    barrier = pltpu.get_barrier_semaphore()
    a, b, c, na = pos

    @pl.when(a > 0)
    def _():
        signal(barrier, shard=index(a - 1, b, c))

    @pl.when(a < na - 1)
    def _():
        signal(barrier, shard=index(a + 1, b, c))

    signal(barrier, shard=index(a, 1 - b, c))
    signal(barrier, shard=index(a, b, 1 - c))
    pl.semaphore_wait(barrier, 2 + (a > 0).astype(jnp.int32) + (a < na - 1).astype(jnp.int32))


def greet_all(n_shard, n_rep):
    barrier = pltpu.get_barrier_semaphore()
    s, r = lax.axis_index("shard"), lax.axis_index("rep")

    def one(k, _):
        signal(barrier, shard=lax.rem(s + k, n_shard))
        return 0

    lax.fori_loop(1, n_shard, one, 0)
    for k in range(1, n_rep):
        signal(barrier, rep=lax.rem(r + k, n_rep))
    pl.semaphore_wait(barrier, n_shard - 1 + n_rep - 1)


def gather_sems(n_shard):
    na = n_shard // 4
    return [
        DMA((n_shard * CHUNKS,)), DMA((na * CHUNKS,)), DMA((na * CHUNKS,)),
        DMA((na * CHUNKS,)), DMA((2 * na * CHUNKS,)),
    ]


def gather_loop(pos, count, buf, sems, on_chip, hook=None):
    recv, up, down, ysend, csend = sems
    a, b, c, na = pos
    rows = count // CHUNKS

    def desc(i, ch, ssem, target):
        piece = buf.at[pl.ds(pl.multiple_of(i * count + ch * rows, rows), rows)]
        return send(piece, piece, ssem, recv.at[i * CHUNKS + ch], shard=target)

    def sends(j, ch):
        i = index(j, b, c)

        @pl.when((j <= a) & (a < na - 1))
        def _():
            desc(i, ch, up.at[j * CHUNKS + ch], index(a + 1, b, c)).start()

        @pl.when((j >= a) & (a > 0))
        def _():
            desc(i, ch, down.at[j * CHUNKS + ch], index(a - 1, b, c)).start()

        desc(i, ch, ysend.at[j * CHUNKS + ch], index(a, 1 - b, c)).start()
        desc(i, ch, csend.at[(j * 2 + b) * CHUNKS + ch], index(a, b, 1 - c)).start()

    def arrived(i, ch):
        desc(i, ch, csend.at[0], index(a, b, 1 - c)).wait_recv()

    def pair_step(j):
        i = index(j, 1 - b, c)
        for ch in range(CHUNKS):
            arrived(i, ch)
            desc(i, ch, csend.at[(j * 2 + 1 - b) * CHUNKS + ch], index(a, b, 1 - c)).start()
        for ch in range(CHUNKS):
            arrived(index(j, 1 - b, 1 - c), ch)
        on_chip(j * 2 + 1 - b)

    def step(t, _):
        j = line_order(t, a, na)
        for ch in range(CHUNKS):

            @pl.when(t > 0)
            def _():
                arrived(index(j, b, c), ch)

            sends(j, ch)
        if hook is not None:
            hook(t)
        for ch in range(CHUNKS):
            arrived(index(j, b, 1 - c), ch)
        on_chip(j * 2 + b)

        @pl.when(t > 0)
        def _():
            pair_step(line_order(t - 1, a, na))

        return 0

    lax.fori_loop(0, na, step, 0)
    pair_step(line_order(na - 1, a, na))

    def finish(j, _):
        i = index(j, b, c)
        for ch in range(CHUNKS):

            @pl.when((j <= a) & (a < na - 1))
            def _():
                desc(i, ch, up.at[j * CHUNKS + ch], index(a, b, 1 - c)).wait_send()

            @pl.when((j >= a) & (a > 0))
            def _():
                desc(i, ch, down.at[j * CHUNKS + ch], index(a, b, 1 - c)).wait_send()

            desc(i, ch, ysend.at[j * CHUNKS + ch], index(a, 1 - b, c)).wait_send()
            for bb in range(2):
                slot = (j * 2 + bb) * CHUNKS + ch
                desc(index(j, bb, c), ch, csend.at[slot], index(a, b, 1 - c)).wait_send()
        return 0

    lax.fori_loop(0, na, finish, 0)


def scatter_sems(n_shard):
    na = n_shard // 4
    return [DMA((2 * na,)), DMA((2 * na,)), DMA((na,)), DMA((na,)), DMA((na,)), DMA((na + 1,))]


def scatter_bufs(n_shard, count, width):
    na = n_shard // 4
    return [
        pltpu.VMEM((n_shard * count, width), BF), pltpu.VMEM((2 * na * count, width), BF),
        pltpu.VMEM((na * count, width), BF), pltpu.VMEM(((na + 1) * count, width), BF),
    ]


def scatter_loop(pos, count, bufs, sems, partial, out, hook=None):
    p, cgot, ygot, zgot = bufs
    csend, crecv, ysend, yrecv, zsend, zrecv = sems
    a, b, c, na = pos
    tile = 32

    def to_core(q):
        return send(
            p.at[rows_of(q * 2 + 1 - c, count)], cgot.at[rows_of(q, count)],
            csend.at[q], crecv.at[q], shard=index(a, b, 1 - c),
        )

    def to_pair(j):
        return send(
            p.at[rows_of(index(j, 1 - b, c), count)], ygot.at[rows_of(j, count)],
            ysend.at[j], yrecv.at[j], shard=index(a, 1 - b, c),
        )

    def along(j, slot, target):
        return send(
            p.at[rows_of(index(j, b, c), count)], zgot.at[rows_of(slot, count)],
            zsend.at[j], zrecv.at[slot], shard=target,
        )

    def add(i, others, into=None):
        def one(k, _):
            def at(slot):
                return pl.ds(pl.multiple_of(slot * count + k * tile, tile), tile)

            total = p[at(i), :].astype(F32)
            for ref, slot in others:
                total = total + ref[at(slot), :].astype(F32)
            if into is None:
                p[at(i), :] = total.astype(BF)
            else:
                into[at(0), :] = total
            return 0

        lax.fori_loop(0, count // tile, one, 0)

    def first(t, _):
        j = line_order(na - 1 - t, a, na)
        far, near = j * 2 + 1 - b, j * 2 + b
        partial(far)
        to_core(far).start()
        partial(near)
        to_core(near).start()
        to_core(far).wait_recv()
        add(index(j, 1 - b, c), [(cgot, far)])
        to_pair(j).start()
        return 0

    lax.fori_loop(0, na, first, 0)

    def second(t, _):
        j = line_order(na - 1 - t, a, na)
        near = j * 2 + b
        i = index(j, b, c)
        if hook is not None:
            hook(t)
        to_core(near).wait_recv()
        to_pair(j).wait_recv()
        inner = ((j < a) & (a < na - 1)) | ((j > a) & (a > 0))

        @pl.when(inner)
        def _():
            along(j, j, index(a, b, 1 - c)).wait_recv()
            add(i, [(cgot, near), (ygot, j), (zgot, j)])

        @pl.when(jnp.logical_not(inner))
        def _():
            add(i, [(cgot, near), (ygot, j)])

        @pl.when(j > a)
        def _():
            along(j, j, index(a + 1, b, c)).start()

        @pl.when(j < a)
        def _():
            along(j, jnp.where(j == a - 1, na, j), index(a - 1, b, c)).start()

        return 0

    lax.fori_loop(0, na - 1, second, 0)
    near = a * 2 + b
    to_core(near).wait_recv()
    to_pair(a).wait_recv()
    add(index(a, b, c), [(cgot, near), (ygot, a)], out)

    def more(slot):
        along(a, slot, index(a, b, 1 - c)).wait_recv()

        def one(k, _):
            got = zgot[pl.ds(pl.multiple_of(slot * count + k * tile, tile), tile), :]
            out[rows_of(k, tile), :] += got.astype(F32)
            return 0

        lax.fori_loop(0, count // tile, one, 0)

    @pl.when(a > 0)
    def _():
        more(a)

    @pl.when(a < na - 1)
    def _():
        more(na)

    def finish(j, _):
        for bb in range(2):
            to_core(j * 2 + bb).wait_send()
        to_pair(j).wait_send()

        @pl.when(j != a)
        def _():
            along(j, j, index(a, b, 1 - c)).wait_send()

        return 0

    lax.fori_loop(0, na, finish, 0)


def columns_sems(n_shard, n_rep, groups):
    return [
        DMA((n_shard * groups,)), DMA((n_shard * groups,)),
        DMA((n_shard * n_rep,)), DMA((n_shard * n_rep,)), DMA((groups + 1,)),
    ]


class Columns:
    def __init__(self, w, out, stage, sems, groups, n_shard, n_rep):
        self.w, self.out, self.stage, self.groups = w, out, stage, groups
        self.ssem, self.rsem, self.fsend, self.frecv, self.lsem = sems
        self.n_shard, self.n_rep = n_shard, n_rep
        self.own = w.shape[0]
        self.share = self.own // n_rep
        self.total = w.shape[1] // groups
        self.width = self.total // n_shard
        self.s, self.r = lax.axis_index("shard"), lax.axis_index("rep")

    def move(self, source, target, g):
        cols = pl.ds(pl.multiple_of(g * self.total + target * self.width, 128), self.width)
        src = self.w.at[rows_of(self.r, self.share), cols]
        at = pl.ds(pl.multiple_of(source * self.own + self.r * self.share, self.share), self.share)
        dst = self.out.at[at, pl.ds(g * self.width, self.width)]
        return send(
            src, dst, self.ssem.at[target * self.groups + g],
            self.rsem.at[source * self.groups + g], shard=target,
        )

    def pass_on(self, source, k, replica):
        at = pl.ds(
            pl.multiple_of(source * self.own + replica * self.share, self.share), self.share
        )
        piece = self.out.at[at]
        return send(
            piece, piece, self.fsend.at[source * self.n_rep + k],
            self.frecv.at[source * self.n_rep + replica],
            rep=lax.rem(self.r + k, self.n_rep),
        )

    def local_in(self, g):
        cols = pl.ds(pl.multiple_of(g * self.total + self.s * self.width, 128), self.width)
        return pltpu.make_async_copy(
            self.w.at[:, cols], self.stage.at[:, pl.ds(g * self.width, self.width)], self.lsem.at[g]
        )

    def local_out(self):
        return pltpu.make_async_copy(
            self.stage, self.out.at[rows_of(self.s, self.own)], self.lsem.at[self.groups]
        )

    def start(self):
        for g in range(self.groups):
            self.local_in(g).start()

        def one(k, _):
            target = lax.rem(self.s + k, self.n_shard)
            for g in range(self.groups):
                self.move(self.s, target, g).start()
            return 0

        lax.fori_loop(1, self.n_shard, one, 0)
        for g in range(self.groups):
            self.local_in(g).wait()
        self.local_out().start()

    def forward(self, low, high):
        def one(k, _):
            source = lax.rem(self.s + self.n_shard - k, self.n_shard)
            for g in range(self.groups):
                self.move(source, self.s, g).wait_recv()
            for m in range(1, self.n_rep):
                self.pass_on(source, m, self.r).start()
            return 0

        lax.fori_loop(low, high, one, 0)

    def finish(self):
        def one(k, _):
            source = lax.rem(self.s + self.n_shard - k, self.n_shard)
            for g in range(self.groups):
                self.move(self.s, source, g).wait_send()
            for m in range(1, self.n_rep):
                self.pass_on(source, m, self.r).wait_send()
                self.pass_on(source, m, lax.rem(self.r + m, self.n_rep)).wait_recv()
            return 0

        lax.fori_loop(1, self.n_shard, one, 0)
        self.local_out().wait()

    def spread(self, t, steps):
        each = -(-(self.n_shard - 1) // steps)
        low = 1 + t * each
        self.forward(low, jnp.minimum(low + each, self.n_shard))


def mm(left, right):
    return jnp.dot(left, right, preferred_element_type=F32)


def mm_nt(left, right):
    return lax.dot_general(left, right, (((1,), (1,)), ((), ())), preferred_element_type=F32)


def mm_tn(left, right):
    return lax.dot_general(left, right, (((0,), (0,)), ((), ())), preferred_element_type=F32)


def call(kernel, name, cid, outs, ins, scratch, *args, flops=0, moved=0):
    return pl.pallas_call(
        kernel,
        name=name,
        out_shape=[jax.ShapeDtypeStruct(shape, dtype) for shape, dtype, _ in outs],
        in_specs=ins,
        out_specs=[spec for _, _, spec in outs],
        scratch_shapes=scratch,
        compiler_params=pltpu.CompilerParams(
            collective_id=cid, has_side_effects=True, vmem_limit_bytes=VMEM_LIMIT
        ),
        cost_estimate=pl.CostEstimate(flops=flops, bytes_accessed=moved, transcendentals=0),
    )(*args)


def load(src, dst, sem):
    cp = pltpu.make_async_copy(src, dst, sem)
    cp.start()
    return cp


def own_rows(pos, count):
    a, b, c, _ = pos
    return rows_of(index(a, b, c), count)


class Out:
    def __init__(self, src, dst, sem, size):
        self.src, self.dst, self.sem, self.size = src, dst, sem, size

    def desc(self, q):
        r = rows_of(q, self.size)
        return pltpu.make_async_copy(self.src.at[r], self.dst.at[r], self.sem.at[q])

    def start(self, q):
        self.desc(q).start()

    def wait(self, q):
        self.desc(q).wait()


def wait_all(outs, chips):
    def one(q, _):
        for o in outs:
            o.wait(q)
        return 0

    lax.fori_loop(0, chips, one, 0)


def qkv_kernel(
    n_shard, n_rep, x_ref, w_ref, g_ref, qkv_ref, cols_ref, sums_ref,
    buf, wq, stage, qkv, stats, got, lsem, osem, vsem, xs, xr, *sems,
):
    pos = position(n_shard)
    count = x_ref.shape[0]
    chips = n_shard // 2
    big = 2 * count
    own = stage.shape[1] // 3
    na = pos[3]
    s = lax.axis_index("shard")
    mine = load(x_ref, buf.at[own_rows(pos, count)], lsem.at[0])
    weights = Columns(w_ref, cols_ref, stage, sems[5:], 3, n_shard, n_rep)
    greet_all(n_shard, n_rep)
    mine.wait()
    out_x = Out(buf, g_ref, osem, big)

    def hook(t):
        @pl.when(t == 0)
        def _():
            weights.start()

        @pl.when(t > 0)
        def _():
            weights.spread(t - 1, na - 1)

    gather_loop(pos, count, buf, sems[:5], out_x.start, hook)
    weights.finish()
    pltpu.sync_copy(cols_ref, wq)
    out_v = Out(qkv, qkv_ref, vsem, big)
    ones = jnp.ones((8, own), F32)

    def one(q, _):
        r = rows_of(q, big)
        v = mm(buf[r, :], wq[...])
        qkv[r, :] = v
        for g in range(2):
            x = v[:, g * own : (g + 1) * own]
            total = lax.dot_general(
                ones, x * x, (((1,), (1,)), ((), ())),
                preferred_element_type=F32, precision=lax.Precision.HIGHEST,
            )
            stats[pl.ds(g, 1), pl.ds(pl.multiple_of(q * big, big), big)] = total[:1]
        out_v.start(q)
        return 0

    lax.fori_loop(0, chips, one, 0)
    exchange(n_shard, stats, got, xs, xr, sums_ref)
    wait_all([out_x, out_v], chips)


def exchange(n_shard, stats, got, xs, xr, sums_ref):
    s = lax.axis_index("shard")

    def desc(k):
        target = lax.rem(s + k, n_shard)
        return send(stats, got.at[k - 1], xs.at[k - 1], xr.at[k - 1], shard=target)

    def start(k, _):
        desc(k).start()
        return 0

    lax.fori_loop(1, n_shard, start, 0)
    sums_ref[...] = stats[...]

    def take(k, _):
        desc(k).wait_recv()
        sums_ref[...] += got[k - 1]
        return 0

    lax.fori_loop(1, n_shard, take, 0)

    def done(k, _):
        desc(k).wait_send()
        return 0

    lax.fori_loop(1, n_shard, done, 0)


def sum_kernel(n_shard, x_ref, sums_ref, stats, got, xs, xr):
    barrier = pltpu.get_barrier_semaphore()
    s = lax.axis_index("shard")

    def one(k, _):
        signal(barrier, shard=lax.rem(s + k, n_shard))
        return 0

    lax.fori_loop(1, n_shard, one, 0)
    stats[...] = x_ref[...]
    pl.semaphore_wait(barrier, n_shard - 1)
    exchange(n_shard, stats, got, xs, xr, sums_ref)


def attn_out_kernel(
    n_shard, n_rep, ctx_ref, wo_ref, w_ref, out_ref, cols_ref, stage, *rest,
):
    pos = position(n_shard)
    na = pos[3]
    bufs, sems, csems = rest[:4], rest[4:10], rest[10:]
    p = bufs[0]
    count = out_ref.shape[0]
    big = 2 * count
    width = out_ref.shape[1]
    weights = Columns(w_ref, cols_ref, stage, csems, 2, n_shard, n_rep)
    greet_all(n_shard, n_rep)

    def partial(q):
        r = rows_of(q, big)
        p[r, :] = mm(ctx_ref[r, :], wo_ref[...]).astype(BF)

    def hook(t):
        @pl.when(t == 0)
        def _():
            weights.start()

        @pl.when(t > 0)
        def _():
            weights.spread(t - 1, na - 1)

    scatter_loop(pos, count, bufs, sems, partial, out_ref, hook)
    weights.spread(na - 2, na - 1)
    weights.finish()


def mlp_kernel(
    n_shard, x_ref, wg_ref, wd_ref, g_ref, gu_ref, mixed_ref, out_ref,
    buf, wg, wd, gu, mixed, lsem, osem, gsem, msem, *rest,
):
    pos = position(n_shard)
    bufs, ssems, gsems = rest[:4], rest[4:10], rest[10:]
    p = bufs[0]
    count, width = out_ref.shape
    big = 2 * count
    chips = n_shard // 2
    ff = wd.shape[0]
    mine = load(x_ref, buf.at[own_rows(pos, count)], lsem.at[0])
    w1 = load(wg_ref, wg, lsem.at[1])
    w2 = load(wd_ref, wd, lsem.at[2])
    greet(pos)
    mine.wait()
    out_x, out_g = Out(buf, g_ref, osem, big), Out(gu, gu_ref, gsem, big)
    out_m = Out(mixed, mixed_ref, msem, big)
    w1.wait()

    def on_chip(q):
        r = rows_of(q, big)
        out_x.start(q)

        def one(k, _):
            lo = pl.ds(pl.multiple_of(k * 256, 256), 256)
            hi = pl.ds(pl.multiple_of(ff + k * 256, 256), 256)
            gate = mm(buf[r, :], wg[:, lo])
            up = mm(buf[r, :], wg[:, hi])
            gu[r, lo] = gate
            gu[r, hi] = up
            mixed[r, lo] = (gate * jax.nn.sigmoid(gate) * up).astype(BF)
            return 0

        lax.fori_loop(0, ff // 256, one, 0)
        out_g.start(q)
        out_m.start(q)

    gather_loop(pos, count, buf, gsems, on_chip)
    w2.wait()

    def partial(q):
        r = rows_of(q, big)

        def one(k, _):
            lo = rows_of(k, 512)
            p[r, lo] = mm(mixed[r, :], wd[:, lo]).astype(BF)
            return 0

        lax.fori_loop(0, width // 512, one, 0)

    scatter_loop(pos, count, bufs, ssems, partial, out_ref)
    wait_all([out_x, out_g, out_m], chips)


def mlp_back_kernel(
    n_shard, x_ref, gu_ref, wg_ref, wd_ref, g_ref, dgu_ref, out_ref,
    buf, wg, wd, gu, dgu, lsem, isem, osem, dsem, *rest,
):
    pos = position(n_shard)
    bufs, ssems, gsems = rest[:4], rest[4:10], rest[10:]
    p = bufs[0]
    count, width = out_ref.shape
    big = 2 * count
    chips = n_shard // 2
    ff = wd.shape[0]
    mine = load(x_ref, buf.at[own_rows(pos, count)], lsem.at[0])
    w2 = load(wd_ref, wd, lsem.at[2])
    saved = Out(gu_ref, gu, isem, big)

    def fetch(q, _):
        saved.start(q)
        return 0

    lax.fori_loop(0, chips, fetch, 0)
    w1 = load(wg_ref, wg, lsem.at[1])
    greet(pos)
    mine.wait()
    out_x, out_d = Out(buf, g_ref, osem, big), Out(dgu, dgu_ref, dsem, big)
    w2.wait()

    def on_chip(q):
        r = rows_of(q, big)
        out_x.start(q)
        saved.wait(q)

        def one(k, _):
            lo = pl.ds(pl.multiple_of(k * 256, 256), 256)
            hi = pl.ds(pl.multiple_of(ff + k * 256, 256), 256)
            d_mixed = mm_nt(buf[r, :], wd[lo, :])
            gate, up = gu[r, lo], gu[r, hi]
            sigma = jax.nn.sigmoid(gate)
            d_gate = d_mixed * up * sigma * (1.0 + gate * (1.0 - sigma))
            dgu[r, lo] = d_gate.astype(BF)
            dgu[r, hi] = (d_mixed * gate * sigma).astype(BF)
            return 0

        lax.fori_loop(0, ff // 256, one, 0)
        out_d.start(q)

    gather_loop(pos, count, buf, gsems, on_chip)
    w1.wait()

    def partial(q):
        r = rows_of(q, big)

        def one(k, _):
            lo = rows_of(k, 256)
            p[r, lo] = mm_nt(dgu[r, :], wg[lo, :]).astype(BF)
            return 0

        lax.fori_loop(0, width // 256, one, 0)

    scatter_loop(pos, count, bufs, ssems, partial, out_ref)
    wait_all([out_x, out_d], chips)


def context_back_kernel(n_shard, x_ref, wo_ref, g_ref, ctx_ref, buf, lsem, osem, *gsems):
    pos = position(n_shard)
    count = x_ref.shape[0]
    big = 2 * count
    mine = load(x_ref, buf.at[own_rows(pos, count)], lsem.at[0])
    greet(pos)
    mine.wait()
    out_x = Out(buf, g_ref, osem, big)

    def on_chip(q):
        r = rows_of(q, big)
        out_x.start(q)
        ctx_ref[r, :] = mm_nt(buf[r, :], wo_ref[...]).astype(BF)

    gather_loop(pos, count, buf, gsems, on_chip)
    wait_all([out_x], n_shard // 2)


def tokens_back_kernel(n_shard, d_ref, wq_ref, out_ref, *rest):
    pos = position(n_shard)
    bufs, sems = rest[:4], rest[4:]
    p = bufs[0]
    count, width = out_ref.shape
    big = 2 * count
    greet(pos)

    def partial(q):
        r = rows_of(q, big)

        def one(k, _):
            lo = rows_of(k, 512)
            p[r, lo] = mm_nt(d_ref[r, :], wq_ref[lo, :]).astype(BF)
            return 0

        lax.fori_loop(0, width // 512, one, 0)

    scatter_loop(pos, count, bufs, sems, partial, out_ref)


def positions(seg):
    slots = lax.broadcasted_iota(jnp.int32, seg.shape, 1)
    starts = jnp.concatenate(
        [jnp.ones((seg.shape[0], 1), jnp.bool_), seg[:, 1:] != seg[:, :-1]], axis=1
    )
    first = lax.cummax(jnp.where(starts, slots, 0), axis=1)
    return slots - first


def rope_tables(seg, head_width):
    half_width = head_width // 2
    spots = positions(seg).astype(F32).reshape(-1)
    inverse = THETA ** (-(2.0 * jnp.arange(half_width, dtype=F32)) / head_width)
    angle = spots[:, None] * inverse[None, :]
    return jnp.cos(angle), jnp.sin(angle)


def rotate(matrix, cosine, sine):
    half = matrix.shape[-1] // 2
    a, b = matrix[..., :half], matrix[..., half:]
    return jnp.concatenate([a * cosine - b * sine, b * cosine + a * sine], axis=-1)


def norm_scale(vector):
    return lax.rsqrt(jnp.mean(vector * vector, axis=-1, keepdims=True) + EPSILON)


def norm_back(upstream, normed, rscale, gain):
    scaled = upstream * gain
    inner = jnp.mean(scaled * normed, axis=-1, keepdims=True)
    return rscale * (scaled - normed * inner), jnp.sum(upstream * normed, axis=0)


def make(n_rep, n_shard):
    chips = n_shard // 2

    def rep_scatter(x):
        if n_rep == 2:
            me = lax.axis_index("rep")
            mine = lax.dynamic_index_in_dim(x, me, 0, keepdims=False)
            other = lax.dynamic_index_in_dim(x, 1 - me, 0, keepdims=False)
            got = lax.ppermute(other.astype(BF), "rep", [(0, 1), (1, 0)])
            return (mine + got.astype(F32)).astype(BF)
        return lax.psum_scatter(x.astype(BF), "rep", scatter_dimension=0, tiled=False)

    def rep_gather(x):
        if n_rep == 2:
            me = lax.axis_index("rep")
            got = lax.ppermute(x, "rep", [(0, 1), (1, 0)])
            first = jnp.where(me == 0, x, got)
            second = jnp.where(me == 0, got, x)
            return jnp.stack([first, second])
        return lax.all_gather(x, "rep", axis=0, tiled=False)

    def rep_sum(x):
        rows = x.shape[0]
        part = rep_scatter(x.reshape(n_rep, rows // n_rep, x.shape[1]))
        return rep_gather(part).reshape(x.shape).astype(F32)

    def grad_back(x, groups):
        rows, cols = x.shape
        own = rows // n_shard
        width = cols // groups
        split = x.reshape(n_shard, n_rep, own // n_rep, cols).transpose(1, 0, 2, 3)
        part = rep_scatter(split)
        part = lax.all_to_all(part, "shard", split_axis=0, concat_axis=0, tiled=True)
        whole = rep_gather(part)
        whole = whole.reshape(n_rep, n_shard, own // n_rep, groups, width)
        return whole.transpose(0, 2, 3, 1, 4).reshape(own, groups * n_shard * width).astype(F32)

    def group_sum(x):
        return call(
            functools.partial(sum_kernel, n_shard), "group_sum", 11,
            [(x.shape, F32, VM)], [VM],
            [
                pltpu.VMEM(x.shape, F32), pltpu.VMEM((n_shard - 1,) + x.shape, F32),
                DMA((n_shard - 1,)), DMA((n_shard - 1,)),
            ],
            x,
        )[0]

    def shards(
        tokens, segment_ids, cotangent, w_qkv, w_out, w_gate_up, w_down,
        q_gain, k_gain, attn_gain, mlp_gain,
    ):
        count, width = tokens.shape
        heads = H // n_shard
        hw = width // H
        own = width // n_shard
        ff = w_down.shape[0]
        total = count * n_shard
        gathered = pltpu.VMEM((total, width), BF)

        small = lax.all_gather(
            jnp.stack([segment_ids.astype(BF), attn_gain, mlp_gain])[None], "shard", axis=0, tiled=True
        )
        seg = small[:, 0].astype(jnp.int32)
        gain_attn = small[:, 1].reshape(-1).astype(F32)
        gain_mlp = small[:, 2].reshape(-1).astype(F32)
        gain_query = q_gain.astype(F32)
        gain_keys = k_gain.astype(F32)
        cosine, sine = rope_tables(seg, hw)
        cos3 = cosine[:, None, :]
        sin3 = sine[:, None, :]

        tokens_g, qkv, wq, squares = call(
            functools.partial(qkv_kernel, n_shard, n_rep), "qkv", 1,
            [
                ((total, width), BF, ANY), ((total, 3 * own), F32, ANY),
                ((width, 3 * own), BF, ANY), ((2, total), F32, VM),
            ],
            [ANY, ANY],
            [
                gathered, pltpu.VMEM((width, 3 * own), BF), pltpu.VMEM((own, 3 * own), BF),
                pltpu.VMEM((total, 3 * own), F32), pltpu.VMEM((2, total), F32),
                pltpu.VMEM((n_shard - 1, 2, total), F32),
                DMA((1,)), DMA((chips,)), DMA((chips,)), DMA((n_shard - 1,)), DMA((n_shard - 1,)),
            ] + gather_sems(n_shard) + columns_sems(n_shard, n_rep, 3),
            tokens, w_qkv,
        )
        query, keys, values_b = qkv[:, :own], qkv[:, own : 2 * own], qkv[:, 2 * own :].astype(BF)
        scales = lax.rsqrt(squares / width + EPSILON)
        query_scale, keys_scale = scales[0][:, None], scales[1][:, None]
        query_hat, keys_hat = query * query_scale, keys * keys_scale

        def rot(x, sign):
            return rotate(x.reshape(total, heads, hw), cos3, sign * sin3).reshape(total, own)

        query_rot = rot(query_hat * gain_query, 1.0).astype(BF)
        keys_rot = rot(keys_hat * gain_keys, 1.0).astype(BF)

        slots = jnp.arange(count)
        ok = (seg[:, :, None] == seg[:, None, :]) & (slots[None, :] <= slots[:, None])[None]
        ok = ok[:, None]

        def blocks(x):
            return x.reshape(n_shard, count, heads, hw)

        root = hw ** (-0.5)
        qb, kb, vb = blocks(query_rot), blocks(keys_rot), blocks(values_b)
        scores = jnp.einsum("bthd,bshd->bhts", qb, kb, preferred_element_type=F32) * root
        scores = jnp.where(ok, scores, -1e30)
        top = jnp.max(scores, axis=-1, keepdims=True)
        lse = top + jnp.log(jnp.sum(jnp.exp(scores - top), axis=-1, keepdims=True))
        probs = jnp.exp(scores - lse)
        probs_b = probs.astype(BF)
        context = jnp.einsum("bhts,bshd->bthd", probs_b, vb, preferred_element_type=F32)
        context_b = context.astype(BF).reshape(total, own)

        attn_raw, wg = call(
            functools.partial(attn_out_kernel, n_shard, n_rep), "attn_out", 2,
            [((count, width), F32, VM), ((width, 2 * ff), BF, ANY)],
            [VM, VM, ANY],
            [pltpu.VMEM((own, 2 * ff), BF)] + scatter_bufs(n_shard, count, width)
            + scatter_sems(n_shard) + columns_sems(n_shard, n_rep, 2),
            context_b, w_out, w_gate_up,
        )
        attn_scale = norm_scale(attn_raw)
        attn_hat = attn_raw * attn_scale
        resid = tokens.astype(F32) + attn_hat * gain_attn

        resid_g, gate_up, mixed_b, down_raw = call(
            functools.partial(mlp_kernel, n_shard), "mlp", 3,
            [
                ((total, width), BF, ANY), ((total, 2 * ff), F32, ANY),
                ((total, ff), BF, ANY), ((count, width), F32, VM),
            ],
            [ANY, ANY, ANY],
            [
                gathered, pltpu.VMEM((width, 2 * ff), BF), pltpu.VMEM((ff, width), BF),
                pltpu.VMEM((total, 2 * ff), F32), pltpu.VMEM((total, ff), BF),
                DMA((3,)), DMA((chips,)), DMA((chips,)), DMA((chips,)),
            ] + scatter_bufs(n_shard, count, width) + scatter_sems(n_shard) + gather_sems(n_shard),
            resid.astype(BF), wg, w_down,
        )
        down_scale = norm_scale(down_raw)
        down_hat = down_raw * down_scale
        output = (resid + down_hat * gain_mlp).astype(BF)

        valid = (segment_ids >= 0).astype(F32)[:, None]
        d_out = cotangent.astype(F32) * valid
        d_down, grad_mlp = norm_back(d_out, down_hat, down_scale, gain_mlp)
        d_down_g, d_gu_b, d_resid_sum = call(
            functools.partial(mlp_back_kernel, n_shard), "mlp_back", 4,
            [((total, width), BF, ANY), ((total, 2 * ff), BF, ANY), ((count, width), F32, VM)],
            [ANY, ANY, ANY, ANY],
            [
                gathered, pltpu.VMEM((width, 2 * ff), BF), pltpu.VMEM((ff, width), BF),
                pltpu.VMEM((total, 2 * ff), F32), pltpu.VMEM((total, 2 * ff), BF),
                DMA((3,)), DMA((chips,)), DMA((chips,)), DMA((chips,)),
            ] + scatter_bufs(n_shard, count, width) + scatter_sems(n_shard) + gather_sems(n_shard),
            d_down.astype(BF), gate_up, wg, w_down,
        )
        d_resid = d_out + d_resid_sum
        grad_down = rep_sum(mm_tn(mixed_b, d_down_g))
        grad_gu = grad_back(mm_tn(resid_g, d_gu_b), 2)

        d_attn, grad_attn = norm_back(d_resid, attn_hat, attn_scale, gain_attn)
        d_attn_g, d_context_b = call(
            functools.partial(context_back_kernel, n_shard), "context_back", 5,
            [((total, width), BF, ANY), ((total, own), BF, VM)],
            [ANY, VM],
            [gathered, DMA((1,)), DMA((chips,))] + gather_sems(n_shard),
            d_attn.astype(BF), w_out,
        )
        grad_out = rep_sum(mm_tn(context_b, d_attn_g))

        db = blocks(d_context_b)
        d_values = jnp.einsum("bhts,bthd->bshd", probs_b, db, preferred_element_type=F32)
        d_probs = jnp.einsum("bthd,bshd->bhts", db, vb, preferred_element_type=F32)
        delta = jnp.sum(db.astype(F32) * context, axis=-1).transpose(0, 2, 1)[..., None]
        d_scores_b = (probs * (d_probs - delta) * root).astype(BF)
        d_query_rot = jnp.einsum("bhts,bshd->bthd", d_scores_b, kb, preferred_element_type=F32)
        d_keys_rot = jnp.einsum("bhts,bthd->bshd", d_scores_b, qb, preferred_element_type=F32)
        d_query_norm = rot(d_query_rot, -1.0)
        d_keys_norm = rot(d_keys_rot, -1.0)
        grad_query = jnp.sum(d_query_norm * query_hat, axis=0)
        grad_keys = jnp.sum(d_keys_norm * keys_hat, axis=0)
        query_up = d_query_norm * gain_query
        keys_up = d_keys_norm * gain_keys
        inner = group_sum(
            jnp.stack([jnp.sum(query_up * query_hat, axis=-1), jnp.sum(keys_up * keys_hat, axis=-1)])
        ) / width
        d_query = query_scale * (query_up - query_hat * inner[0][:, None])
        d_keys = keys_scale * (keys_up - keys_hat * inner[1][:, None])
        d_qkv_b = jnp.concatenate(
            [d_query, d_keys, d_values.reshape(total, own)], axis=1
        ).astype(BF)
        d_tokens_sum = call(
            functools.partial(tokens_back_kernel, n_shard), "tokens_back", 6,
            [((count, width), F32, VM)], [VM, VM],
            scatter_bufs(n_shard, count, width) + scatter_sems(n_shard),
            d_qkv_b, wq,
        )[0]
        grad_tokens = d_resid + d_tokens_sum
        grad_qkv = grad_back(mm_tn(tokens_g, d_qkv_b), 3)

        gains_local = lax.psum_scatter(
            jnp.stack([grad_attn, grad_mlp]), "shard", scatter_dimension=1, tiled=True
        )
        gains = lax.psum(
            jnp.concatenate([gains_local, jnp.stack([grad_query, grad_keys])]), "rep"
        )
        return (
            output, grad_tokens, grad_qkv, grad_out, grad_gu, grad_down,
            gains[2], gains[3], gains[0], gains[1],
        )

    return shards


def solution(mesh):
    rows = P(("rep", "shard"), None)
    return jax.shard_map(
        make(mesh.shape["rep"], mesh.shape["shard"]),
        mesh=mesh,
        in_specs=(rows, P(("rep", "shard")), rows)
        + (P("shard", None),) * 4
        + (P("shard"),) * 4,
        out_specs=(rows, rows) + (P("shard", None),) * 4 + (P("shard"),) * 4,
        check_vma=False,
    )
```

```python
import functools

import jax
import jax.numpy as jnp
from jax import lax
from jax.experimental import pallas as pl
from jax.experimental.pallas import tpu as pltpu
from jax.sharding import PartitionSpec as P

H = 16
EPSILON = 1e-06
THETA = 500000.0
BF = jnp.bfloat16
F32 = jnp.float32
MESH = pl.DeviceIdType.MESH
DMA = pltpu.SemaphoreType.DMA
ANY = pl.BlockSpec(memory_space=pl.ANY)
VM = pl.BlockSpec(memory_space=pltpu.VMEM)
CHUNKS = 2
VMEM_LIMIT = 62 << 20


def position(n_shard):
    s = lax.axis_index("shard")
    return s // 4, (s // 2) % 2, s % 2, n_shard // 4


def index(a, b, c):
    return (a * 2 + b) * 2 + c


def line_order(t, a, na):
    m = jnp.minimum(a, na - 1 - a)
    near = jnp.where(t % 2 == 1, a - (t + 1) // 2, a + (t + 1) // 2)
    far = jnp.where(m == a, t, na - 1 - t)
    return jnp.where(t <= 2 * m, near, far)


def rows_of(i, size):
    return pl.ds(pl.multiple_of(i * size, size), size)


def send(src, dst, ssem, rsem, **target):
    return pltpu.make_async_remote_copy(
        src_ref=src, dst_ref=dst, send_sem=ssem, recv_sem=rsem,
        device_id=target, device_id_type=MESH,
    )


def signal(sem, **target):
    pl.semaphore_signal(sem, inc=1, device_id=target, device_id_type=MESH)


def greet(pos):
    barrier = pltpu.get_barrier_semaphore()
    a, b, c, na = pos

    @pl.when(a > 0)
    def _():
        signal(barrier, shard=index(a - 1, b, c))

    @pl.when(a < na - 1)
    def _():
        signal(barrier, shard=index(a + 1, b, c))

    signal(barrier, shard=index(a, 1 - b, c))
    signal(barrier, shard=index(a, b, 1 - c))
    pl.semaphore_wait(barrier, 2 + (a > 0).astype(jnp.int32) + (a < na - 1).astype(jnp.int32))


def greet_all(n_shard, n_rep):
    barrier = pltpu.get_barrier_semaphore()
    s, r = lax.axis_index("shard"), lax.axis_index("rep")

    def one(k, _):
        signal(barrier, shard=lax.rem(s + k, n_shard))
        return 0

    lax.fori_loop(1, n_shard, one, 0)
    for k in range(1, n_rep):
        signal(barrier, rep=lax.rem(r + k, n_rep))
    pl.semaphore_wait(barrier, n_shard - 1 + n_rep - 1)


def gather_sems(n_shard):
    na = n_shard // 4
    return [
        DMA((n_shard * CHUNKS,)), DMA((na * CHUNKS,)), DMA((na * CHUNKS,)),
        DMA((na * CHUNKS,)), DMA((2 * na * CHUNKS,)),
    ]


def gather_loop(pos, count, buf, sems, on_chip, hook=None):
    recv, up, down, ysend, csend = sems
    a, b, c, na = pos
    rows = count // CHUNKS

    def desc(i, ch, ssem, target):
        piece = buf.at[pl.ds(pl.multiple_of(i * count + ch * rows, rows), rows)]
        return send(piece, piece, ssem, recv.at[i * CHUNKS + ch], shard=target)

    def sends(j, ch):
        i = index(j, b, c)

        @pl.when((j <= a) & (a < na - 1))
        def _():
            desc(i, ch, up.at[j * CHUNKS + ch], index(a + 1, b, c)).start()

        @pl.when((j >= a) & (a > 0))
        def _():
            desc(i, ch, down.at[j * CHUNKS + ch], index(a - 1, b, c)).start()

        desc(i, ch, ysend.at[j * CHUNKS + ch], index(a, 1 - b, c)).start()
        desc(i, ch, csend.at[(j * 2 + b) * CHUNKS + ch], index(a, b, 1 - c)).start()

    def arrived(i, ch):
        desc(i, ch, csend.at[0], index(a, b, 1 - c)).wait_recv()

    def pair_step(j):
        i = index(j, 1 - b, c)
        for ch in range(CHUNKS):
            arrived(i, ch)
            desc(i, ch, csend.at[(j * 2 + 1 - b) * CHUNKS + ch], index(a, b, 1 - c)).start()
        for ch in range(CHUNKS):
            arrived(index(j, 1 - b, 1 - c), ch)
        on_chip(j * 2 + 1 - b)

    def step(t, _):
        j = line_order(t, a, na)
        for ch in range(CHUNKS):

            @pl.when(t > 0)
            def _():
                arrived(index(j, b, c), ch)

            sends(j, ch)
        if hook is not None:
            hook(t)
        for ch in range(CHUNKS):
            arrived(index(j, b, 1 - c), ch)
        on_chip(j * 2 + b)

        @pl.when(t > 0)
        def _():
            pair_step(line_order(t - 1, a, na))

        return 0

    lax.fori_loop(0, na, step, 0)
    pair_step(line_order(na - 1, a, na))

    def finish(j, _):
        i = index(j, b, c)
        for ch in range(CHUNKS):

            @pl.when((j <= a) & (a < na - 1))
            def _():
                desc(i, ch, up.at[j * CHUNKS + ch], index(a, b, 1 - c)).wait_send()

            @pl.when((j >= a) & (a > 0))
            def _():
                desc(i, ch, down.at[j * CHUNKS + ch], index(a, b, 1 - c)).wait_send()

            desc(i, ch, ysend.at[j * CHUNKS + ch], index(a, 1 - b, c)).wait_send()
            for bb in range(2):
                slot = (j * 2 + bb) * CHUNKS + ch
                desc(index(j, bb, c), ch, csend.at[slot], index(a, b, 1 - c)).wait_send()
        return 0

    lax.fori_loop(0, na, finish, 0)


def scatter_sems(n_shard):
    na = n_shard // 4
    return [DMA((2 * na,)), DMA((2 * na,)), DMA((na,)), DMA((na,)), DMA((na,)), DMA((na + 1,))]


def scatter_bufs(n_shard, count, width):
    na = n_shard // 4
    return [
        pltpu.VMEM((n_shard * count, width), BF), pltpu.VMEM((2 * na * count, width), BF),
        pltpu.VMEM((na * count, width), BF), pltpu.VMEM(((na + 1) * count, width), BF),
    ]


def scatter_loop(pos, count, bufs, sems, partial, out, hook=None, final=None):
    p, cgot, ygot, zgot = bufs
    csend, crecv, ysend, yrecv, zsend, zrecv = sems
    a, b, c, na = pos
    tile = 32

    def to_core(q):
        return send(
            p.at[rows_of(q * 2 + 1 - c, count)], cgot.at[rows_of(q, count)],
            csend.at[q], crecv.at[q], shard=index(a, b, 1 - c),
        )

    def to_pair(j):
        return send(
            p.at[rows_of(index(j, 1 - b, c), count)], ygot.at[rows_of(j, count)],
            ysend.at[j], yrecv.at[j], shard=index(a, 1 - b, c),
        )

    def along(j, slot, target):
        return send(
            p.at[rows_of(index(j, b, c), count)], zgot.at[rows_of(slot, count)],
            zsend.at[j], zrecv.at[slot], shard=target,
        )

    def add(i, others, into=None):
        def one(k, _):
            def at(slot):
                return pl.ds(pl.multiple_of(slot * count + k * tile, tile), tile)

            total = p[at(i), :].astype(F32)
            for ref, slot in others:
                total = total + ref[at(slot), :].astype(F32)
            if into is None:
                p[at(i), :] = total.astype(BF)
            else:
                into[at(0), :] = total
            return 0

        lax.fori_loop(0, count // tile, one, 0)

    def first(t, _):
        j = line_order(na - 1 - t, a, na)
        far, near = j * 2 + 1 - b, j * 2 + b
        partial(far)
        to_core(far).start()
        partial(near)
        to_core(near).start()
        to_core(far).wait_recv()
        add(index(j, 1 - b, c), [(cgot, far)])
        to_pair(j).start()
        return 0

    lax.fori_loop(0, na, first, 0)

    def second(t, _):
        j = line_order(na - 1 - t, a, na)
        near = j * 2 + b
        i = index(j, b, c)
        if hook is not None:
            hook(t)
        to_core(near).wait_recv()
        to_pair(j).wait_recv()
        inner = ((j < a) & (a < na - 1)) | ((j > a) & (a > 0))

        @pl.when(inner)
        def _():
            along(j, j, index(a, b, 1 - c)).wait_recv()
            add(i, [(cgot, near), (ygot, j), (zgot, j)])

        @pl.when(jnp.logical_not(inner))
        def _():
            add(i, [(cgot, near), (ygot, j)])

        @pl.when(j > a)
        def _():
            along(j, j, index(a + 1, b, c)).start()

        @pl.when(j < a)
        def _():
            along(j, jnp.where(j == a - 1, na, j), index(a - 1, b, c)).start()

        return 0

    lax.fori_loop(0, na - 1, second, 0)
    if final is not None:
        final()
    near = a * 2 + b
    to_core(near).wait_recv()
    to_pair(a).wait_recv()
    add(index(a, b, c), [(cgot, near), (ygot, a)], out)

    def more(slot):
        along(a, slot, index(a, b, 1 - c)).wait_recv()

        def one(k, _):
            got = zgot[pl.ds(pl.multiple_of(slot * count + k * tile, tile), tile), :]
            out[rows_of(k, tile), :] += got.astype(F32)
            return 0

        lax.fori_loop(0, count // tile, one, 0)

    @pl.when(a > 0)
    def _():
        more(a)

    @pl.when(a < na - 1)
    def _():
        more(na)

    def finish(j, _):
        for bb in range(2):
            to_core(j * 2 + bb).wait_send()
        to_pair(j).wait_send()

        @pl.when(j != a)
        def _():
            along(j, j, index(a, b, 1 - c)).wait_send()

        return 0

    lax.fori_loop(0, na, finish, 0)


def columns_sems(n_shard, n_rep, groups):
    return [
        DMA((n_shard * groups,)), DMA((n_shard * groups,)),
        DMA((n_shard * n_rep,)), DMA((n_shard * n_rep,)), DMA((groups + 1,)),
    ]


class Columns:
    def __init__(self, w, out, stage, sems, groups, n_shard, n_rep):
        self.w, self.out, self.stage, self.groups = w, out, stage, groups
        self.ssem, self.rsem, self.fsend, self.frecv, self.lsem = sems
        self.n_shard, self.n_rep = n_shard, n_rep
        self.own = w.shape[0]
        self.share = self.own // n_rep
        self.total = w.shape[1] // groups
        self.width = self.total // n_shard
        self.s, self.r = lax.axis_index("shard"), lax.axis_index("rep")

    def move(self, source, target, g):
        cols = pl.ds(pl.multiple_of(g * self.total + target * self.width, 128), self.width)
        src = self.w.at[rows_of(self.r, self.share), cols]
        at = pl.ds(pl.multiple_of(source * self.own + self.r * self.share, self.share), self.share)
        dst = self.out.at[at, pl.ds(g * self.width, self.width)]
        return send(
            src, dst, self.ssem.at[target * self.groups + g],
            self.rsem.at[source * self.groups + g], shard=target,
        )

    def pass_on(self, source, k, replica):
        at = pl.ds(
            pl.multiple_of(source * self.own + replica * self.share, self.share), self.share
        )
        piece = self.out.at[at]
        return send(
            piece, piece, self.fsend.at[source * self.n_rep + k],
            self.frecv.at[source * self.n_rep + replica],
            rep=lax.rem(self.r + k, self.n_rep),
        )

    def local_in(self, g):
        cols = pl.ds(pl.multiple_of(g * self.total + self.s * self.width, 128), self.width)
        into = pl.ds(g * self.width, self.width)
        if self.stage is None:
            dst = self.out.at[rows_of(self.s, self.own), into]
        else:
            dst = self.stage.at[:, into]
        return pltpu.make_async_copy(self.w.at[:, cols], dst, self.lsem.at[g])

    def local_out(self):
        return pltpu.make_async_copy(
            self.stage, self.out.at[rows_of(self.s, self.own)], self.lsem.at[self.groups]
        )

    def start(self):
        for g in range(self.groups):
            self.local_in(g).start()

        def one(k, _):
            target = lax.rem(self.s + k, self.n_shard)
            for g in range(self.groups):
                self.move(self.s, target, g).start()
            return 0

        lax.fori_loop(1, self.n_shard, one, 0)
        if self.stage is not None:
            for g in range(self.groups):
                self.local_in(g).wait()
            self.local_out().start()

    def forward(self, low, high):
        def one(k, _):
            source = lax.rem(self.s + self.n_shard - k, self.n_shard)
            for g in range(self.groups):
                self.move(source, self.s, g).wait_recv()
            for m in range(1, self.n_rep):
                self.pass_on(source, m, self.r).start()
            return 0

        lax.fori_loop(low, high, one, 0)

    def finish(self):
        def one(k, _):
            source = lax.rem(self.s + self.n_shard - k, self.n_shard)
            for g in range(self.groups):
                self.move(self.s, source, g).wait_send()
            for m in range(1, self.n_rep):
                self.pass_on(source, m, self.r).wait_send()
                self.pass_on(source, m, lax.rem(self.r + m, self.n_rep)).wait_recv()
            return 0

        lax.fori_loop(1, self.n_shard, one, 0)
        if self.stage is not None:
            self.local_out().wait()
        else:
            for g in range(self.groups):
                self.local_in(g).wait()

    def spread(self, t, steps):
        each = -(-(self.n_shard - 1) // steps)
        low = 1 + t * each
        self.forward(low, jnp.minimum(low + each, self.n_shard))


class ShareSum:
    def __init__(self, acc, got, sems, blocks, n_rep):
        self.acc, self.got, self.blocks, self.n_rep = acc, got, blocks, n_rep
        self.ssem, self.rsem = sems
        self.share = acc.shape[0] // (blocks * n_rep)
        self.r = lax.axis_index("rep")

    def part(self, block, replica):
        return rows_of(block * self.n_rep + replica, self.share)

    def desc(self, block, m):
        target = lax.rem(self.r + m, self.n_rep)
        slot = (m - 1) * self.blocks + block
        return send(
            self.acc.at[self.part(block, target)], self.got.at[rows_of(slot, self.share)],
            self.ssem.at[slot], self.rsem.at[slot], rep=target,
        )

    def start(self, block):
        for m in range(1, self.n_rep):
            self.desc(block, m).start()

    def add(self, block):
        for m in range(1, self.n_rep):
            self.desc(block, m).wait_recv()
        tile = min(self.share, 32)

        def one(k, _):
            at = pl.ds(
                pl.multiple_of((block * self.n_rep + self.r) * self.share + k * tile, tile), tile
            )
            total = self.acc[at, :].astype(F32)
            for m in range(1, self.n_rep):
                slot = (m - 1) * self.blocks + block
                total = total + self.got[
                    pl.ds(pl.multiple_of(slot * self.share + k * tile, tile), tile), :
                ].astype(F32)
            self.acc[at, :] = total.astype(BF)
            return 0

        lax.fori_loop(0, self.share // tile, one, 0)

    def sent(self, block):
        for m in range(1, self.n_rep):
            self.desc(block, m).wait_send()


def share_scratch(rows, cols, blocks, n_rep):
    return [
        pltpu.VMEM((rows, cols), BF), pltpu.VMEM(((n_rep - 1) * rows // n_rep, cols), BF),
        DMA(((n_rep - 1) * blocks,)), DMA(((n_rep - 1) * blocks,)),
    ]


class ShareGather:
    def __init__(self, src, out, sems, n_rep):
        self.src, self.out, self.n_rep = src, out, n_rep
        self.ssem, self.rsem, self.lsem = sems
        self.r = lax.axis_index("rep")
        self.share = out.shape[0] // n_rep

    def local(self):
        return pltpu.make_async_copy(self.src, self.out.at[rows_of(self.r, self.share)], self.lsem)

    def desc(self, m, replica):
        return send(
            self.src, self.out.at[rows_of(replica, self.share)],
            self.ssem.at[m - 1], self.rsem.at[replica], rep=lax.rem(self.r + m, self.n_rep),
        )

    def start(self):
        self.local().start()
        for m in range(1, self.n_rep):
            self.desc(m, self.r).start()

    def finish(self):
        self.local().wait()
        for m in range(1, self.n_rep):
            self.desc(m, self.r).wait_send()
            self.desc(m, lax.rem(self.r + m, self.n_rep)).wait_recv()


def share_gather_sems(n_rep):
    return [DMA((n_rep - 1,)), DMA((n_rep,)), DMA(())]


class RowsBack:
    def __init__(self, src, out, sems, groups, n_shard, n_rep):
        self.src, self.out, self.groups = src, out, groups
        self.ssem, self.rsem, self.fsend, self.frecv, self.lsem = sems
        self.n_shard, self.n_rep = n_shard, n_rep
        self.share = out.shape[0] // n_rep
        self.total = out.shape[1] // groups
        self.width = self.total // n_shard
        self.s, self.r = lax.axis_index("shard"), lax.axis_index("rep")

    def place(self, source, replica, g):
        cols = pl.ds(pl.multiple_of(g * self.total + source * self.width, 128), self.width)
        return self.out.at[rows_of(replica, self.share), cols]

    def piece(self, target, g):
        return self.src(target).at[:, pl.ds(g * self.width, self.width)]

    def move(self, source, target, g):
        return send(
            self.piece(target, g), self.place(source, self.r, g),
            self.ssem.at[target * self.groups + g], self.rsem.at[source * self.groups + g],
            shard=target,
        )

    def local(self, g):
        return pltpu.make_async_copy(
            self.piece(self.s, g), self.place(self.s, self.r, g), self.lsem.at[g]
        )

    def pass_on(self, source, m, replica, g):
        at = self.place(source, replica, g)
        return send(
            at, at, self.fsend.at[(source * self.n_rep + m) * self.groups + g],
            self.frecv.at[(source * self.n_rep + replica) * self.groups + g],
            rep=lax.rem(self.r + m, self.n_rep),
        )

    def start(self):
        for g in range(self.groups):
            self.local(g).start()

        def one(k, _):
            for g in range(self.groups):
                self.move(self.s, lax.rem(self.s + k, self.n_shard), g).start()
            return 0

        lax.fori_loop(1, self.n_shard, one, 0)

    def relay(self, source):
        for g in range(self.groups):
            for m in range(1, self.n_rep):
                self.pass_on(source, m, self.r, g).start()

    def forward_own(self):
        for g in range(self.groups):
            self.local(g).wait()
        self.relay(self.s)

    def forward(self, low, high):
        def one(k, _):
            source = lax.rem(self.s + self.n_shard - k, self.n_shard)
            for g in range(self.groups):
                self.move(source, self.s, g).wait_recv()
            self.relay(source)
            return 0

        lax.fori_loop(low, high, one, 0)

    def spread(self, t, steps):
        @pl.when(t == 0)
        def _():
            self.forward_own()

        each = -(-(self.n_shard - 1) // steps)
        low = 1 + t * each
        self.forward(low, jnp.minimum(low + each, self.n_shard))

    def finish(self):
        def one(k, _):
            source = lax.rem(self.s + self.n_shard - k, self.n_shard)
            for g in range(self.groups):

                @pl.when(k > 0)
                def _():
                    self.move(self.s, source, g).wait_send()

                for m in range(1, self.n_rep):
                    self.pass_on(source, m, self.r, g).wait_send()
                    self.pass_on(source, m, lax.rem(self.r + m, self.n_rep), g).wait_recv()
            return 0

        lax.fori_loop(0, self.n_shard, one, 0)


def rows_back_sems(n_shard, n_rep, groups):
    return [
        DMA((n_shard * groups,)), DMA((n_shard * groups,)),
        DMA((n_shard * n_rep * groups,)), DMA((n_shard * n_rep * groups,)), DMA((groups,)),
    ]


def mm(left, right):
    return jnp.dot(left, right, preferred_element_type=F32)


def mm_nt(left, right):
    return lax.dot_general(left, right, (((1,), (1,)), ((), ())), preferred_element_type=F32)


def mm_tn(left, right):
    return lax.dot_general(left, right, (((0,), (0,)), ((), ())), preferred_element_type=F32)


def call(kernel, name, cid, outs, ins, scratch, *args, flops=0, moved=0):
    return pl.pallas_call(
        kernel,
        name=name,
        out_shape=[jax.ShapeDtypeStruct(shape, dtype) for shape, dtype, _ in outs],
        in_specs=ins,
        out_specs=[spec for _, _, spec in outs],
        scratch_shapes=scratch,
        compiler_params=pltpu.CompilerParams(
            collective_id=cid, has_side_effects=True, vmem_limit_bytes=VMEM_LIMIT
        ),
        cost_estimate=pl.CostEstimate(flops=flops, bytes_accessed=moved, transcendentals=0),
    )(*args)


def load(src, dst, sem):
    cp = pltpu.make_async_copy(src, dst, sem)
    cp.start()
    return cp


def own_rows(pos, count):
    a, b, c, _ = pos
    return rows_of(index(a, b, c), count)


class Out:
    def __init__(self, src, dst, sem, size):
        self.src, self.dst, self.sem, self.size = src, dst, sem, size

    def desc(self, q):
        r = rows_of(q, self.size)
        return pltpu.make_async_copy(self.src.at[r], self.dst.at[r], self.sem.at[q])

    def start(self, q):
        self.desc(q).start()

    def wait(self, q):
        self.desc(q).wait()


def wait_all(outs, chips):
    def one(q, _):
        for o in outs:
            o.wait(q)
        return 0

    lax.fori_loop(0, chips, one, 0)


def turned(row, count):
    return jnp.transpose(jnp.broadcast_to(row, (count, count)))


def swap_halves(x):
    return pltpu.roll(x, x.shape[1] // 2, 1)


def rope_of(spots, table):
    count = spots.shape[0]
    lane = lax.broadcasted_iota(jnp.int32, (count, count), 1)
    pick = jnp.where(lane.astype(F32) == spots, 1.0, 0.0).astype(F32)
    both = jnp.dot(pick, table, preferred_element_type=F32, precision=lax.Precision.HIGHEST)
    half = both.shape[1] // 2
    return both[:, :half], both[:, half:]


def row_sums(x):
    ones = jnp.ones((8, x.shape[1]), F32)
    return lax.dot_general(
        ones, x, (((1,), (1,)), ((), ())),
        preferred_element_type=F32, precision=lax.Precision.HIGHEST,
    )[:1]


def attn_kernel(
    n_shard, n_rep, heads,
    x_ref, aux_ref, wqkv_ref, wo_ref, wgu_ref, table_ref, qg_ref, kg_ref,
    g_ref, wq_ref, wg_ref, auxg_ref, sums_ref, hats_ref, rot_ref, prob_ref, ctx_ref, out_ref,
    buf, wq, stage, qkv, stats, got, lsem, osem, xs, xr, as_, ar, *rest,
):
    pos = position(n_shard)
    gsems, c3, c2, bufs, ssems = rest[:5], rest[5:10], rest[10:15], rest[15:19], rest[19:]
    p = bufs[0]
    count, width = out_ref.shape
    chips = n_shard // 2
    big = 2 * count
    own = wo_ref.shape[0]
    hw = own // heads
    na = pos[3]
    s = lax.axis_index("shard")
    mine = load(x_ref, buf.at[own_rows(pos, count)], lsem.at[0])
    qkv_w = Columns(wqkv_ref, wq, None, c3, 3, n_shard, n_rep)
    gu_w = Columns(wgu_ref, wg_ref, stage, c2, 2, n_shard, n_rep)
    auxg_ref[s] = aux_ref[...]
    greet_all(n_shard, n_rep)
    mine.wait()
    out_x = Out(buf, g_ref, osem, big)

    def aux_desc(k):
        target = lax.rem(s + k, n_shard)
        return send(aux_ref, auxg_ref.at[s], as_.at[k - 1], ar.at[k - 1], shard=target)

    def hook(t):
        @pl.when(t == 0)
        def _():
            qkv_w.start()

            def one(k, _):
                aux_desc(k).start()
                return 0

            lax.fori_loop(1, n_shard, one, 0)

        @pl.when(t > 0)
        def _():
            qkv_w.spread(t - 1, na - 1)

    gather_loop(pos, count, buf, gsems, out_x.start, hook)
    qkv_w.finish()
    gu_w.start()
    keep = load(wq, wq_ref, lsem.at[1])

    def project(q, _):
        r = rows_of(q, big)
        v = mm(buf[r, :], wq[...])
        qkv[r, :] = v
        for g in range(2):
            x = v[:, g * own : (g + 1) * own]
            stats[pl.ds(g, 1), pl.ds(pl.multiple_of(q * big, big), big)] = row_sums(x * x)
        return 0

    lax.fori_loop(0, chips, project, 0)
    exchange_start(n_shard, stats, got, xs, xr)
    exchange_finish(n_shard, stats, got, xs, xr, sums_ref)

    def aux_done(k, _):
        aux_desc(k).wait_recv()
        aux_desc(k).wait_send()
        return 0

    lax.fori_loop(1, n_shard, aux_done, 0)
    root = hw ** (-0.5)
    lane = lax.broadcasted_iota(jnp.int32, (count, count), 1)
    slot = lax.broadcasted_iota(jnp.int32, (count, count), 0)

    def attend(i, _):
        r = rows_of(i, count)
        at = pl.ds(pl.multiple_of(i * count, count), count)
        spots = turned(auxg_ref[i, 1:2, :], count)
        cos, sin = rope_of(spots, table_ref[...])
        ok = (lane <= slot) & (lane >= slot - spots.astype(jnp.int32))
        scale = lax.rsqrt(sums_ref[:, at] / width + EPSILON)
        q_scale = turned(scale[0:1], count)[:, :1]
        k_scale = turned(scale[1:2], count)[:, :1]
        for h in range(heads):
            def part(g):
                lo = g * own + h * hw
                return slice(lo, lo + hw)

            cols = slice(h * hw, (h + 1) * hw)

            def turn(g, scale, gain):
                hat = qkv[r, part(g)] * scale
                hats_ref[r, part(g)] = hat
                x = hat * gain
                x = (x * cos + swap_halves(x) * sin).astype(BF)
                rot_ref[r, part(g)] = x
                return x

            query = turn(0, q_scale, qg_ref[:, cols])
            keys = turn(1, k_scale, kg_ref[:, cols])
            values = qkv[r, part(2)].astype(BF)
            rot_ref[r, part(2)] = values
            scores = jnp.where(ok, mm_nt(query, keys) * root, -1e30)
            e = jnp.exp(scores - jnp.max(scores, axis=-1, keepdims=True))
            probs = e / jnp.sum(e, axis=-1, keepdims=True)
            prob_ref[r, h * count : (h + 1) * count] = probs
            ctx_ref[r, cols] = mm(probs.astype(BF), values).astype(BF)
        return 0

    lax.fori_loop(0, n_shard, attend, 0)

    def partial(q):
        r = rows_of(q, big)
        p[r, :] = mm(ctx_ref[r, :], wo_ref[...]).astype(BF)

    scatter_loop(pos, count, bufs, ssems, partial, out_ref, lambda t: gu_w.spread(t, na))
    gu_w.spread(na - 1, na)
    gu_w.finish()
    keep.wait()
    wait_all([out_x], chips)


def exchange_desc(n_shard, stats, got, xs, xr, k):
    target = lax.rem(lax.axis_index("shard") + k, n_shard)
    return send(stats, got.at[k - 1], xs.at[k - 1], xr.at[k - 1], shard=target)


def exchange_start(n_shard, stats, got, xs, xr):
    def start(k, _):
        exchange_desc(n_shard, stats, got, xs, xr, k).start()
        return 0

    lax.fori_loop(1, n_shard, start, 0)


def exchange_finish(n_shard, stats, got, xs, xr, sums):
    sums[...] = stats[...]

    def take(k, _):
        exchange_desc(n_shard, stats, got, xs, xr, k).wait_recv()
        sums[...] += got[k - 1]
        return 0

    lax.fori_loop(1, n_shard, take, 0)

    def done(k, _):
        exchange_desc(n_shard, stats, got, xs, xr, k).wait_send()
        return 0

    lax.fori_loop(1, n_shard, done, 0)


def mlp_kernel(
    n_shard, x_ref, wg_ref, wd_ref, g_ref, gu_ref, mixed_ref, out_ref,
    buf, wg, wd, gu, mixed, lsem, osem, gsem, msem, *rest,
):
    pos = position(n_shard)
    bufs, ssems, gsems = rest[:4], rest[4:10], rest[10:]
    p = bufs[0]
    count, width = out_ref.shape
    big = 2 * count
    chips = n_shard // 2
    ff = wd.shape[0]
    mine = load(x_ref, buf.at[own_rows(pos, count)], lsem.at[0])
    w1 = load(wg_ref, wg, lsem.at[1])
    w2 = load(wd_ref, wd, lsem.at[2])
    greet(pos)
    mine.wait()
    out_x, out_g = Out(buf, g_ref, osem, big), Out(gu, gu_ref, gsem, big)
    out_m = Out(mixed, mixed_ref, msem, big)
    w1.wait()

    def on_chip(q):
        r = rows_of(q, big)
        out_x.start(q)

        def one(k, _):
            lo = pl.ds(pl.multiple_of(k * 256, 256), 256)
            hi = pl.ds(pl.multiple_of(ff + k * 256, 256), 256)
            gate = mm(buf[r, :], wg[:, lo])
            up = mm(buf[r, :], wg[:, hi])
            gu[r, lo] = gate.astype(BF)
            gu[r, hi] = up.astype(BF)
            mixed[r, lo] = (gate * jax.nn.sigmoid(gate) * up).astype(BF)
            return 0

        lax.fori_loop(0, ff // 256, one, 0)
        out_g.start(q)
        out_m.start(q)

    gather_loop(pos, count, buf, gsems, on_chip)
    w2.wait()

    def partial(q):
        r = rows_of(q, big)

        def one(k, _):
            lo = rows_of(k, 512)
            p[r, lo] = mm(mixed[r, :], wd[:, lo]).astype(BF)
            return 0

        lax.fori_loop(0, width // 512, one, 0)

    scatter_loop(pos, count, bufs, ssems, partial, out_ref)
    wait_all([out_x, out_g, out_m], chips)


def flip(src, cols, flipped):
    step = 256

    def one(k, _):
        at = rows_of(k, step)
        flipped[:, at] = jnp.transpose(src[at, cols])
        return 0

    lax.fori_loop(0, src.shape[0] // step, one, 0)


def mlp_back_kernel(
    n_shard, n_rep, x_ref, gu_ref, wg_ref, wd_ref, resid_ref, mixed_ref,
    gsum_ref, down_ref, out_ref,
    buf, wg, wd, gu, dgu, resid, mixed, flipped, down, lsem, isem, osem, acc, got, xs, xr, *rest,
):
    pos = position(n_shard)
    na = pos[3]
    bufs, ssems, gsems = rest[:4], rest[4:10], rest[10:]
    p = bufs[0]
    count, width = out_ref.shape
    big = 2 * count
    chips = n_shard // 2
    ff = wd.shape[0]
    own = width // n_shard
    share = own // n_rep
    mine = load(x_ref, buf.at[own_rows(pos, count)], lsem.at[0])
    w2 = load(wd_ref, wd, lsem.at[2])
    saved = Out(gu_ref, gu, isem, big)

    def fetch(q, _):
        saved.start(q)
        return 0

    lax.fori_loop(0, chips, fetch, 0)
    w1 = load(wg_ref, wg, lsem.at[1])
    in_r = load(resid_ref, resid, lsem.at[3])
    in_m = load(mixed_ref, mixed, lsem.at[4])
    greet_all(n_shard, n_rep)
    mine.wait()
    w2.wait()

    def on_chip(q):
        r = rows_of(q, big)
        saved.wait(q)

        def one(k, _):
            lo = pl.ds(pl.multiple_of(k * 256, 256), 256)
            hi = pl.ds(pl.multiple_of(ff + k * 256, 256), 256)
            d_mixed = mm_nt(buf[r, :], wd[lo, :])
            gate, up = gu[r, lo].astype(F32), gu[r, hi].astype(F32)
            sigma = jax.nn.sigmoid(gate)
            d_gate = d_mixed * up * sigma * (1.0 + gate * (1.0 - sigma))
            dgu[r, lo] = d_gate.astype(BF)
            dgu[r, hi] = (d_mixed * gate * sigma).astype(BF)
            return 0

        lax.fori_loop(0, ff // 256, one, 0)

    gather_loop(pos, count, buf, gsems, on_chip)
    w1.wait()
    in_r.wait()
    in_m.wait()

    def partial(q):
        r = rows_of(q, big)

        def one(k, _):
            lo = rows_of(k, 256)
            p[r, lo] = mm_nt(dgu[r, :], wg[lo, :]).astype(BF)
            return 0

        lax.fori_loop(0, width // 256, one, 0)

    shares = ShareSum(acc, got, (xs, xr), n_shard, n_rep)
    most = flipped.shape[0]
    owners = most // own
    parts = width // most

    def grad_rows(k):
        flip(resid, pl.ds(pl.multiple_of(k * most, most), most), flipped)

        def one(n, _):
            lo = rows_of(n, 256)
            acc[rows_of(k, most), lo] = mm(flipped[...], dgu[:, lo]).astype(BF)
            return 0

        lax.fori_loop(0, 2 * ff // 256, one, 0)
        for d in range(owners):
            shares.start(k * owners + d)

    def hook(t):
        def one(k, _):
            grad_rows(k)
            return 0

        lax.fori_loop(parts * t // (na - 1), parts * (t + 1) // (na - 1), one, 0)

    def grad_down():
        def rows(m, _):
            flip(mixed, pl.ds(pl.multiple_of(m * most, most), most), flipped)

            def one(n, _):
                lo = rows_of(n, 256)
                down[rows_of(m, most), lo] = mm(flipped[...], buf[:, lo]).astype(BF)
                return 0

            lax.fori_loop(0, width // 256, one, 0)
            return 0

        lax.fori_loop(0, ff // most, rows, 0)
        load(down, down_ref, lsem.at[3])

    scatter_loop(pos, count, bufs, ssems, partial, out_ref, hook, grad_down)

    def collect(d, _):
        shares.add(d)
        pltpu.make_async_copy(
            acc.at[shares.part(d, shares.r)], gsum_ref.at[rows_of(d, share)], osem.at[d]
        ).start()
        return 0

    lax.fori_loop(0, n_shard, collect, 0)

    def end(d, _):
        shares.sent(d)
        pltpu.make_async_copy(
            acc.at[shares.part(d, shares.r)], gsum_ref.at[rows_of(d, share)], osem.at[d]
        ).wait()
        return 0

    lax.fori_loop(0, n_shard, end, 0)
    pltpu.make_async_copy(down, down_ref, lsem.at[3]).wait()


def attn_back_kernel(
    n_shard, n_rep, heads,
    x_ref, tok_ref, wo_ref, wq_ref, hats_ref, rot_ref, prob_ref, ctx_ref, aux_ref, sums_ref,
    table_ref, qg_ref, kg_ref, gsum_ref, down_ref,
    gu_ref, dn_ref, go_ref, gq_ref, gains_ref, out_ref,
    buf, tok, wq, dctx, ups, dqkv, flipped, stats, inner, got, lsem, xs, xr, *rest,
):
    rest = list(rest)

    def take(n):
        out = rest[:n]
        del rest[:n]
        return out

    pos = position(n_shard)
    na = pos[3]
    gsems, bufs, ssems = take(5), take(4), take(6)
    dacc, dgot, *dsems = take(4)
    oacc, ogot, *osems = take(4)
    qacc, qgot, *qsems = take(4)
    dgsems, ogsems, gusems, qksems = take(3), take(3), take(5), take(5)
    p = bufs[0]
    count, width = out_ref.shape
    big = 2 * count
    own = wo_ref.shape[0]
    hw = own // heads
    r_me = lax.axis_index("rep")
    mine = load(x_ref, buf.at[own_rows(pos, count)], lsem.at[0])
    in_d = load(down_ref, dacc, lsem.at[1])
    in_t = load(tok_ref, tok, lsem.at[2])
    in_w = load(wq_ref, wq, lsem.at[3])
    share = own // n_rep
    gu_rows = RowsBack(lambda d: gsum_ref.at[rows_of(d, share)], gu_ref, gusems, 2, n_shard, n_rep)
    down = ShareSum(dacc, dgot, dsems, 1, n_rep)
    down_all = ShareGather(dacc.at[down.part(0, r_me)], dn_ref, dgsems, n_rep)
    wout = ShareSum(oacc, ogot, osems, 1, n_rep)
    wout_all = ShareGather(oacc.at[wout.part(0, r_me)], go_ref, ogsems, n_rep)
    wqkv = ShareSum(qacc, qgot, qsems, n_shard, n_rep)
    wqkv_rows = RowsBack(
        lambda d: qacc.at[wqkv.part(d, r_me)], gq_ref, qksems, 3, n_shard, n_rep
    )
    greet_all(n_shard, n_rep)
    mine.wait()

    def hook(t):
        @pl.when(t == 0)
        def _():
            gu_rows.start()
            in_d.wait()
            down.start(0)

        @pl.when(t > 0)
        def _():
            gu_rows.spread(t - 1, na - 1)

    def on_chip(q):
        r = rows_of(q, big)
        dctx[r, :] = mm_nt(buf[r, :], wo_ref[...]).astype(BF)

    gather_loop(pos, count, buf, gsems, on_chip, hook)
    down.add(0)
    down_all.start()
    root = hw ** (-0.5)
    gains_ref[...] = jnp.zeros_like(gains_ref)

    def scale_of(i):
        at = pl.ds(pl.multiple_of(i * count, count), count)
        return lax.rsqrt(sums_ref[:, at] / width + EPSILON)

    def attend(i, _):
        r = rows_of(i, count)
        at = pl.ds(pl.multiple_of(i * count, count), count)
        cos, sin = rope_of(turned(aux_ref[i, 1:2, :], count), table_ref[...])
        totals = [jnp.zeros((1, count), F32), jnp.zeros((1, count), F32)]
        for h in range(heads):
            def part(g):
                lo = g * own + h * hw
                return slice(lo, lo + hw)

            cols = slice(h * hw, (h + 1) * hw)
            query, keys, values = rot_ref[r, part(0)], rot_ref[r, part(1)], rot_ref[r, part(2)]
            probs = prob_ref[r, h * count : (h + 1) * count]
            probs_b = probs.astype(BF)
            d_ctx = dctx[r, cols]
            d_values = mm_tn(probs_b, d_ctx)
            d_probs = mm_nt(d_ctx, values)
            delta = jnp.sum(probs_b.astype(F32) * d_probs, axis=-1, keepdims=True)
            d_scores = (probs * (d_probs - delta) * root).astype(BF)
            d_query = mm(d_scores, keys)
            d_keys = mm_tn(d_scores, query)
            dqkv[r, part(2)] = d_values.astype(BF)
            for g, (x, gain) in enumerate(((d_query, qg_ref), (d_keys, kg_ref))):
                x = x * cos - swap_halves(x) * sin
                hat = hats_ref[r, part(g)]
                gains_ref[g : g + 1, cols] += jnp.sum(x * hat, axis=0, keepdims=True)
                up = x * gain[:, cols]
                ups[r, part(g)] = up
                totals[g] = totals[g] + row_sums(up * hat)
        for g in range(2):
            stats[pl.ds(g, 1), at] = totals[g]
        return 0

    lax.fori_loop(0, n_shard, attend, 0)
    exchange_start(n_shard, stats, got, xs, xr)

    fo = flipped.at[pl.ds(0, own)]
    flip(ctx_ref, slice(0, own), fo)

    def out_cols(n, _):
        lo = rows_of(n, 256)
        oacc[:, lo] = mm(fo[...], buf[:, lo]).astype(BF)
        return 0

    lax.fori_loop(0, width // 256, out_cols, 0)
    wout.start(0)
    exchange_finish(n_shard, stats, got, xs, xr, inner)

    def settle(i, _):
        r = rows_of(i, count)
        at = pl.ds(pl.multiple_of(i * count, count), count)
        scale = scale_of(i)
        mean = inner[:, at] / width
        for g in range(2):
            lo = slice(g * own, (g + 1) * own)
            column = turned(scale[g : g + 1], count)[:, :1]
            down_by = turned(mean[g : g + 1], count)[:, :1]
            dqkv[r, lo] = (column * (ups[r, lo] - hats_ref[r, lo] * down_by)).astype(BF)
        return 0

    lax.fori_loop(0, n_shard, settle, 0)
    in_w.wait()
    in_t.wait()

    def partial(q):
        r = rows_of(q, big)

        def one(k, _):
            lo = rows_of(k, 512)
            p[r, lo] = mm_nt(dqkv[r, :], wq[lo, :]).astype(BF)
            return 0

        lax.fori_loop(0, width // 512, one, 0)

    most = flipped.shape[0]
    owners = most // own

    def grad_rows(k, _):
        flip(tok, pl.ds(pl.multiple_of(k * most, most), most), flipped)
        qacc[rows_of(k, most), :] = mm(flipped[...], dqkv[...]).astype(BF)
        for d in range(owners):
            wqkv.start(k * owners + d)
        return 0

    def sum_up(d, _):
        wqkv.add(d)
        return 0

    def hook2(t):
        @pl.when(t == 0)
        def _():
            lax.fori_loop(0, width // most, grad_rows, 0)

        @pl.when(t == 1)
        def _():
            lax.fori_loop(0, n_shard, sum_up, 0)
            wqkv_rows.start()
            wout.add(0)
            wout_all.start()

    scatter_loop(
        pos, count, bufs, ssems, partial, out_ref, hook2, lambda: wqkv_rows.spread(0, 1)
    )

    def end(d, _):
        wqkv.sent(d)
        return 0

    lax.fori_loop(0, n_shard, end, 0)
    down.sent(0)
    wout.sent(0)
    wqkv_rows.finish()
    gu_rows.finish()
    down_all.finish()
    wout_all.finish()


def positions(seg):
    slots = lax.broadcasted_iota(jnp.int32, seg.shape, 1)
    starts = jnp.concatenate(
        [jnp.ones((seg.shape[0], 1), jnp.bool_), seg[:, 1:] != seg[:, :-1]], axis=1
    )
    first = lax.cummax(jnp.where(starts, slots, 0), axis=1)
    return slots - first


def rope_table(count, head_width):
    half_width = head_width // 2
    inverse = THETA ** (-(2.0 * jnp.arange(half_width, dtype=F32)) / head_width)
    angle = jnp.arange(count, dtype=F32)[:, None] * inverse[None, :]
    cosine, sine = jnp.cos(angle), jnp.sin(angle)
    return jnp.concatenate([cosine, cosine, -sine, sine], axis=1)


def norm_scale(vector):
    return lax.rsqrt(jnp.mean(vector * vector, axis=-1, keepdims=True) + EPSILON)


def norm_back(upstream, normed, rscale, gain):
    scaled = upstream * gain
    inner = jnp.mean(scaled * normed, axis=-1, keepdims=True)
    return rscale * (scaled - normed * inner), jnp.sum(upstream * normed, axis=0)


def make(n_rep, n_shard):
    chips = n_shard // 2

    def shards(
        tokens, segment_ids, cotangent, w_qkv, w_out, w_gate_up, w_down,
        q_gain, k_gain, attn_gain, mlp_gain,
    ):
        count, width = tokens.shape
        heads = H // n_shard
        hw = width // H
        own = width // n_shard
        ff = w_down.shape[0]
        total = count * n_shard
        gathered = pltpu.VMEM((total, width), BF)

        gain_query = q_gain.astype(F32)
        gain_keys = k_gain.astype(F32)
        spots = positions(segment_ids[None]).astype(F32)
        aux = jnp.concatenate(
            [
                segment_ids.astype(F32)[None], spots, attn_gain.astype(F32)[None],
                mlp_gain.astype(F32)[None], jnp.zeros((4, count), F32),
            ]
        )
        table = rope_table(count, hw)
        chunk = n_shard - 1
        tokens_g, wq, wg, auxg, squares, hats, rots, probs, context_b, attn_raw = call(
            functools.partial(attn_kernel, n_shard, n_rep, heads), "attn", 1,
            [
                ((total, width), BF, ANY), ((width, 3 * own), BF, ANY), ((width, 2 * ff), BF, ANY),
                ((n_shard, 8, count), F32, VM), ((2, total), F32, VM), ((total, 2 * own), F32, VM),
                ((total, 3 * own), BF, VM), ((total, heads * count), F32, VM),
                ((total, own), BF, VM), ((count, width), F32, VM),
            ],
            [ANY, VM, ANY, VM, ANY, VM, VM, VM],
            [
                gathered, pltpu.VMEM((width, 3 * own), BF), pltpu.VMEM((own, 2 * ff), BF),
                pltpu.VMEM((total, 3 * own), F32), pltpu.VMEM((2, total), F32),
                pltpu.VMEM((chunk, 2, total), F32),
                DMA((2,)), DMA((chips,)), DMA((chunk,)), DMA((chunk,)), DMA((chunk,)), DMA((chunk,)),
            ] + gather_sems(n_shard) + columns_sems(n_shard, n_rep, 3)
            + columns_sems(n_shard, n_rep, 2)
            + scatter_bufs(n_shard, count, width) + scatter_sems(n_shard),
            tokens, aux, w_qkv, w_out, w_gate_up, table, gain_query[None], gain_keys[None],
        )
        gain_attn = auxg[:, 2].reshape(-1)
        gain_mlp = auxg[:, 3].reshape(-1)
        attn_scale = norm_scale(attn_raw)
        attn_hat = attn_raw * attn_scale
        resid = tokens.astype(F32) + attn_hat * gain_attn

        resid_g, gate_up, mixed_b, down_raw = call(
            functools.partial(mlp_kernel, n_shard), "mlp", 3,
            [
                ((total, width), BF, ANY), ((total, 2 * ff), BF, ANY),
                ((total, ff), BF, ANY), ((count, width), F32, VM),
            ],
            [ANY, ANY, ANY],
            [
                gathered, pltpu.VMEM((width, 2 * ff), BF), pltpu.VMEM((ff, width), BF),
                pltpu.VMEM((total, 2 * ff), BF), pltpu.VMEM((total, ff), BF),
                DMA((3,)), DMA((chips,)), DMA((chips,)), DMA((chips,)),
            ] + scatter_bufs(n_shard, count, width) + scatter_sems(n_shard) + gather_sems(n_shard),
            resid.astype(BF), wg, w_down,
        )
        down_scale = norm_scale(down_raw)
        down_hat = down_raw * down_scale
        output = (resid + down_hat * gain_mlp).astype(BF)

        valid = (segment_ids >= 0).astype(F32)[:, None]
        d_out = cotangent.astype(F32) * valid
        d_down, grad_mlp = norm_back(d_out, down_hat, down_scale, gain_mlp)
        most = 4 * own
        gu_sum, down_acc, d_resid_sum = call(
            functools.partial(mlp_back_kernel, n_shard, n_rep), "mlp_back", 4,
            [
                ((width // n_rep, 2 * ff), BF, ANY), ((ff, width), BF, ANY),
                ((count, width), F32, VM),
            ],
            [ANY] * 6,
            [
                gathered, pltpu.VMEM((width, 2 * ff), BF), pltpu.VMEM((ff, width), BF),
                pltpu.VMEM((total, 2 * ff), BF), pltpu.VMEM((total, 2 * ff), BF),
                gathered, pltpu.VMEM((total, ff), BF), pltpu.VMEM((most, total), BF),
                pltpu.VMEM((ff, width), BF), DMA((5,)), DMA((chips,)), DMA((n_shard,)),
            ] + share_scratch(width, 2 * ff, n_shard, n_rep)
            + scatter_bufs(n_shard, count, width) + scatter_sems(n_shard) + gather_sems(n_shard),
            d_down.astype(BF), gate_up, wg, w_down, resid_g, mixed_b,
        )
        d_resid = d_out + d_resid_sum
        d_attn, grad_attn = norm_back(d_resid, attn_hat, attn_scale, gain_attn)

        gu_rows, down_rows, out_rows, qkv_rows, gains_qk, d_tokens_sum = call(
            functools.partial(attn_back_kernel, n_shard, n_rep, heads), "attn_back", 5,
            [
                ((own, n_shard * 2 * ff), BF, ANY), ((ff, width), BF, ANY), ((own, width), BF, ANY),
                ((own, 3 * width), BF, ANY), ((2, own), F32, VM), ((count, width), F32, VM),
            ],
            [ANY, ANY, VM, ANY, VM, VM, VM, VM, VM, VM, VM, VM, VM, ANY, ANY],
            [
                gathered, gathered, pltpu.VMEM((width, 3 * own), BF), pltpu.VMEM((total, own), BF),
                pltpu.VMEM((total, 2 * own), F32), pltpu.VMEM((total, 3 * own), BF),
                pltpu.VMEM((most, total), BF), pltpu.VMEM((2, total), F32),
                pltpu.VMEM((2, total), F32), pltpu.VMEM((chunk, 2, total), F32),
                DMA((4,)), DMA((chunk,)), DMA((chunk,)),
            ] + gather_sems(n_shard) + scatter_bufs(n_shard, count, width) + scatter_sems(n_shard)
            + share_scratch(ff, width, 1, n_rep) + share_scratch(own, width, 1, n_rep)
            + share_scratch(width, 3 * own, n_shard, n_rep)
            + share_gather_sems(n_rep) * 2
            + rows_back_sems(n_shard, n_rep, 2) + rows_back_sems(n_shard, n_rep, 3),
            d_attn.astype(BF), tokens_g, w_out, wq, hats, rots, probs, context_b, auxg, squares,
            table, gain_query[None], gain_keys[None], gu_sum, down_acc,
        )
        grad_tokens = d_resid + d_tokens_sum
        gains_local = lax.psum_scatter(
            jnp.stack([grad_attn, grad_mlp]), "shard", scatter_dimension=1, tiled=True
        )
        gains = lax.psum(jnp.concatenate([gains_local, gains_qk]), "rep")
        return (
            output, grad_tokens, qkv_rows.astype(F32), out_rows.astype(F32), gu_rows.astype(F32),
            down_rows.astype(F32), gains[2], gains[3], gains[0], gains[1],
        )

    return shards


def solution(mesh):
    rows = P(("rep", "shard"), None)
    return jax.shard_map(
        make(mesh.shape["rep"], mesh.shape["shard"]),
        mesh=mesh,
        in_specs=(rows, P(("rep", "shard")), rows)
        + (P("shard", None),) * 4
        + (P("shard"),) * 4,
        out_specs=(rows, rows) + (P("shard", None),) * 4 + (P("shard"),) * 4,
        check_vma=False,
    )
```

```python
import functools

import jax
import jax.numpy as jnp
from jax import lax
from jax.experimental import pallas as pl
from jax.experimental.pallas import tpu as pltpu
from jax.sharding import PartitionSpec as P

H = 16
EPSILON = 1e-06
THETA = 500000.0
BF = jnp.bfloat16
F32 = jnp.float32
MESH = pl.DeviceIdType.MESH
DMA = pltpu.SemaphoreType.DMA
ANY = pl.BlockSpec(memory_space=pl.ANY)
VM = pl.BlockSpec(memory_space=pltpu.VMEM)
CHUNKS = 2
UNROLL = 2
VMEM_LIMIT = 62 << 20


def position(n_shard):
    s = lax.axis_index("shard")
    return s // 4, (s // 2) % 2, s % 2, n_shard // 4


def index(a, b, c):
    return (a * 2 + b) * 2 + c


def line_order(t, a, na):
    m = jnp.minimum(a, na - 1 - a)
    near = jnp.where(t % 2 == 1, a - (t + 1) // 2, a + (t + 1) // 2)
    far = jnp.where(m == a, t, na - 1 - t)
    return jnp.where(t <= 2 * m, near, far)


def peer(k, flip, sign):
    s = lax.axis_index("shard")
    na = lax.axis_size("shard") // 4
    a, b, c = s // 4, (s // 2) % 2, s % 2
    return index(lax.rem(a + na + sign * (k // 2), na), (b + flip) % 2, (c + k) % 2)


def rows_of(i, size):
    return pl.ds(pl.multiple_of(i * size, size), size)


def send(src, dst, ssem, rsem, **target):
    return pltpu.make_async_remote_copy(
        src_ref=src, dst_ref=dst, send_sem=ssem, recv_sem=rsem,
        device_id=target, device_id_type=MESH,
    )


def signal(sem, **target):
    pl.semaphore_signal(sem, inc=1, device_id=target, device_id_type=MESH)


def greet(pos):
    barrier = pltpu.get_barrier_semaphore()
    a, b, c, na = pos

    @pl.when(a > 0)
    def _():
        signal(barrier, shard=index(a - 1, b, c))

    @pl.when(a < na - 1)
    def _():
        signal(barrier, shard=index(a + 1, b, c))

    signal(barrier, shard=index(a, 1 - b, c))
    signal(barrier, shard=index(a, b, 1 - c))
    pl.semaphore_wait(barrier, 2 + (a > 0).astype(jnp.int32) + (a < na - 1).astype(jnp.int32))


def greet_all(n_shard, n_rep):
    barrier = pltpu.get_barrier_semaphore()
    s, r = lax.axis_index("shard"), lax.axis_index("rep")

    def one(k, _):
        signal(barrier, shard=lax.rem(s + k, n_shard))
        return 0

    lax.fori_loop(1, n_shard, one, 0)
    for k in range(1, n_rep):
        signal(barrier, rep=lax.rem(r + k, n_rep))
    pl.semaphore_wait(barrier, n_shard - 1 + n_rep - 1)


def gather_sems(n_shard):
    na = n_shard // 4
    return [
        DMA((n_shard * CHUNKS,)), DMA((na * CHUNKS,)), DMA((na * CHUNKS,)),
        DMA((na * CHUNKS,)), DMA((2 * na * CHUNKS,)),
    ]


def gather_loop(pos, count, buf, sems, on_chip, hook=None):
    recv, up, down, ysend, csend = sems
    a, b, c, na = pos
    rows = count // CHUNKS

    def desc(i, ch, ssem, target):
        piece = buf.at[pl.ds(pl.multiple_of(i * count + ch * rows, rows), rows)]
        return send(piece, piece, ssem, recv.at[i * CHUNKS + ch], shard=target)

    def sends(j, ch):
        i = index(j, b, c)

        @pl.when((j <= a) & (a < na - 1))
        def _():
            desc(i, ch, up.at[j * CHUNKS + ch], index(a + 1, b, c)).start()

        @pl.when((j >= a) & (a > 0))
        def _():
            desc(i, ch, down.at[j * CHUNKS + ch], index(a - 1, b, c)).start()

        desc(i, ch, ysend.at[j * CHUNKS + ch], index(a, 1 - b, c)).start()
        desc(i, ch, csend.at[(j * 2 + b) * CHUNKS + ch], index(a, b, 1 - c)).start()

    def arrived(i, ch):
        desc(i, ch, csend.at[0], index(a, b, 1 - c)).wait_recv()

    def pair_step(j):
        i = index(j, 1 - b, c)
        for ch in range(CHUNKS):
            arrived(i, ch)
            desc(i, ch, csend.at[(j * 2 + 1 - b) * CHUNKS + ch], index(a, b, 1 - c)).start()
        for ch in range(CHUNKS):
            arrived(index(j, 1 - b, 1 - c), ch)
        on_chip(j * 2 + 1 - b)

    def step(t, _):
        j = line_order(t, a, na)
        for ch in range(CHUNKS):

            @pl.when(t > 0)
            def _():
                arrived(index(j, b, c), ch)

            sends(j, ch)
        if hook is not None:
            hook(t)
        for ch in range(CHUNKS):
            arrived(index(j, b, 1 - c), ch)
        on_chip(j * 2 + b)

        @pl.when(t > 0)
        def _():
            pair_step(line_order(t - 1, a, na))

        return 0

    lax.fori_loop(0, na, step, 0)
    pair_step(line_order(na - 1, a, na))

    def finish(j, _):
        i = index(j, b, c)
        for ch in range(CHUNKS):

            @pl.when((j <= a) & (a < na - 1))
            def _():
                desc(i, ch, up.at[j * CHUNKS + ch], index(a, b, 1 - c)).wait_send()

            @pl.when((j >= a) & (a > 0))
            def _():
                desc(i, ch, down.at[j * CHUNKS + ch], index(a, b, 1 - c)).wait_send()

            desc(i, ch, ysend.at[j * CHUNKS + ch], index(a, 1 - b, c)).wait_send()
            for bb in range(2):
                slot = (j * 2 + bb) * CHUNKS + ch
                desc(index(j, bb, c), ch, csend.at[slot], index(a, b, 1 - c)).wait_send()
        return 0

    lax.fori_loop(0, na, finish, 0)


def scatter_sems(n_shard):
    na = n_shard // 4
    return [DMA((2 * na,)), DMA((2 * na,)), DMA((na,)), DMA((na,)), DMA((na,)), DMA((na + 1,))]


def scatter_bufs(n_shard, count, width):
    na = n_shard // 4
    return [
        pltpu.VMEM((n_shard * count, width), BF), pltpu.VMEM((2 * na * count, width), BF),
        pltpu.VMEM((na * count, width), BF), pltpu.VMEM(((na + 1) * count, width), BF),
    ]


def scatter_loop(pos, count, bufs, sems, partial, out, hook=None, final=None):
    p, cgot, ygot, zgot = bufs
    csend, crecv, ysend, yrecv, zsend, zrecv = sems
    a, b, c, na = pos
    tile = 32

    def to_core(q):
        return send(
            p.at[rows_of(q * 2 + 1 - c, count)], cgot.at[rows_of(q, count)],
            csend.at[q], crecv.at[q], shard=index(a, b, 1 - c),
        )

    def to_pair(j):
        return send(
            p.at[rows_of(index(j, 1 - b, c), count)], ygot.at[rows_of(j, count)],
            ysend.at[j], yrecv.at[j], shard=index(a, 1 - b, c),
        )

    def along(j, slot, target):
        return send(
            p.at[rows_of(index(j, b, c), count)], zgot.at[rows_of(slot, count)],
            zsend.at[j], zrecv.at[slot], shard=target,
        )

    def add(i, others, into=None):
        def one(k, _):
            def at(slot):
                return pl.ds(pl.multiple_of(slot * count + k * tile, tile), tile)

            total = p[at(i), :].astype(F32)
            for ref, slot in others:
                total = total + ref[at(slot), :].astype(F32)
            if into is None:
                p[at(i), :] = total.astype(BF)
            else:
                into[at(0), :] = total
            return 0

        lax.fori_loop(0, count // tile, one, 0)

    def first(t, _):
        j = line_order(na - 1 - t, a, na)
        far, near = j * 2 + 1 - b, j * 2 + b
        partial(far)
        to_core(far).start()
        partial(near)
        to_core(near).start()
        to_core(far).wait_recv()
        add(index(j, 1 - b, c), [(cgot, far)])
        to_pair(j).start()
        return 0

    lax.fori_loop(0, na, first, 0)

    def second(t, _):
        j = line_order(na - 1 - t, a, na)
        near = j * 2 + b
        i = index(j, b, c)
        if hook is not None:
            hook(t)
        to_core(near).wait_recv()
        to_pair(j).wait_recv()
        inner = ((j < a) & (a < na - 1)) | ((j > a) & (a > 0))

        @pl.when(inner)
        def _():
            along(j, j, index(a, b, 1 - c)).wait_recv()
            add(i, [(cgot, near), (ygot, j), (zgot, j)])

        @pl.when(jnp.logical_not(inner))
        def _():
            add(i, [(cgot, near), (ygot, j)])

        @pl.when(j > a)
        def _():
            along(j, j, index(a + 1, b, c)).start()

        @pl.when(j < a)
        def _():
            along(j, jnp.where(j == a - 1, na, j), index(a - 1, b, c)).start()

        return 0

    lax.fori_loop(0, na - 1, second, 0)
    if final is not None:
        final()
    near = a * 2 + b
    to_core(near).wait_recv()
    to_pair(a).wait_recv()
    add(index(a, b, c), [(cgot, near), (ygot, a)], out)

    def more(slot):
        along(a, slot, index(a, b, 1 - c)).wait_recv()

        def one(k, _):
            got = zgot[pl.ds(pl.multiple_of(slot * count + k * tile, tile), tile), :]
            out[rows_of(k, tile), :] += got.astype(F32)
            return 0

        lax.fori_loop(0, count // tile, one, 0)

    @pl.when(a > 0)
    def _():
        more(a)

    @pl.when(a < na - 1)
    def _():
        more(na)

    def finish(j, _):
        for bb in range(2):
            to_core(j * 2 + bb).wait_send()
        to_pair(j).wait_send()

        @pl.when(j != a)
        def _():
            along(j, j, index(a, b, 1 - c)).wait_send()

        return 0

    lax.fori_loop(0, na, finish, 0)


def columns_sems(n_shard, n_rep, groups):
    return [
        DMA((n_shard * groups,)), DMA((n_shard * groups,)),
        DMA((n_shard * n_rep,)), DMA((n_shard * n_rep,)), DMA((groups + 1,)),
    ]


class Columns:
    def __init__(self, w, out, stage, sems, groups, n_shard, n_rep):
        self.w, self.out, self.stage, self.groups = w, out, stage, groups
        self.ssem, self.rsem, self.fsend, self.frecv, self.lsem = sems
        self.n_shard, self.n_rep = n_shard, n_rep
        self.own = w.shape[0]
        self.share = self.own // n_rep
        self.total = w.shape[1] // groups
        self.width = self.total // n_shard
        self.s, self.r = lax.axis_index("shard"), lax.axis_index("rep")

    def move(self, source, target, g):
        cols = pl.ds(pl.multiple_of(g * self.total + target * self.width, 128), self.width)
        src = self.w.at[rows_of(self.r, self.share), cols]
        at = pl.ds(pl.multiple_of(source * self.own + self.r * self.share, self.share), self.share)
        dst = self.out.at[at, pl.ds(g * self.width, self.width)]
        return send(
            src, dst, self.ssem.at[target * self.groups + g],
            self.rsem.at[source * self.groups + g], shard=target,
        )

    def pass_on(self, source, k, replica):
        at = pl.ds(
            pl.multiple_of(source * self.own + replica * self.share, self.share), self.share
        )
        piece = self.out.at[at]
        return send(
            piece, piece, self.fsend.at[source * self.n_rep + k],
            self.frecv.at[source * self.n_rep + replica],
            rep=lax.rem(self.r + k, self.n_rep),
        )

    def local_in(self, g):
        cols = pl.ds(pl.multiple_of(g * self.total + self.s * self.width, 128), self.width)
        into = pl.ds(g * self.width, self.width)
        if self.stage is None:
            dst = self.out.at[rows_of(self.s, self.own), into]
        else:
            dst = self.stage.at[:, into]
        return pltpu.make_async_copy(self.w.at[:, cols], dst, self.lsem.at[g])

    def local_out(self):
        return pltpu.make_async_copy(
            self.stage, self.out.at[rows_of(self.s, self.own)], self.lsem.at[self.groups]
        )

    def start(self, flip, low, high):
        def one(k, _):
            for g in range(self.groups):
                self.move(self.s, peer(k, flip, 1), g).start()
            return 0

        lax.fori_loop(low, high, one, 0)

    def start_own(self):
        for g in range(self.groups):
            self.local_in(g).start()
        if self.stage is not None:
            for g in range(self.groups):
                self.local_in(g).wait()
            self.local_out().start()

    def forward(self, flip, low, high):
        def one(k, _):
            source = peer(k, flip, -1)
            for g in range(self.groups):
                self.move(source, self.s, g).wait_recv()
            for m in range(1, self.n_rep):
                self.pass_on(source, m, self.r).start()
            return 0

        lax.fori_loop(low, high, one, 0)

    def finish(self):
        def one(k, _):
            source = lax.rem(self.s + self.n_shard - k, self.n_shard)
            for g in range(self.groups):
                self.move(self.s, source, g).wait_send()
            for m in range(1, self.n_rep):
                self.pass_on(source, m, self.r).wait_send()
                self.pass_on(source, m, lax.rem(self.r + m, self.n_rep)).wait_recv()
            return 0

        lax.fori_loop(1, self.n_shard, one, 0)
        if self.stage is not None:
            self.local_out().wait()
        else:
            for g in range(self.groups):
                self.local_in(g).wait()


class ShareSum:
    def __init__(self, acc, got, sems, blocks, n_rep):
        self.acc, self.got, self.blocks, self.n_rep = acc, got, blocks, n_rep
        self.ssem, self.rsem = sems
        self.share = acc.shape[0] // (blocks * n_rep)
        self.r = lax.axis_index("rep")

    def part(self, block, replica):
        return rows_of(block * self.n_rep + replica, self.share)

    def desc(self, block, m):
        target = lax.rem(self.r + m, self.n_rep)
        slot = (m - 1) * self.blocks + block
        return send(
            self.acc.at[self.part(block, target)], self.got.at[rows_of(slot, self.share)],
            self.ssem.at[slot], self.rsem.at[slot], rep=target,
        )

    def start(self, block):
        for m in range(1, self.n_rep):
            self.desc(block, m).start()

    def add(self, block):
        for m in range(1, self.n_rep):
            self.desc(block, m).wait_recv()
        tile = min(self.share, 32)

        def one(k, _):
            at = pl.ds(
                pl.multiple_of((block * self.n_rep + self.r) * self.share + k * tile, tile), tile
            )
            total = self.acc[at, :].astype(F32)
            for m in range(1, self.n_rep):
                slot = (m - 1) * self.blocks + block
                total = total + self.got[
                    pl.ds(pl.multiple_of(slot * self.share + k * tile, tile), tile), :
                ].astype(F32)
            self.acc[at, :] = total.astype(BF)
            return 0

        lax.fori_loop(0, self.share // tile, one, 0)

    def sent(self, block):
        for m in range(1, self.n_rep):
            self.desc(block, m).wait_send()


def share_scratch(rows, cols, blocks, n_rep):
    return [
        pltpu.VMEM((rows, cols), BF), pltpu.VMEM(((n_rep - 1) * rows // n_rep, cols), BF),
        DMA(((n_rep - 1) * blocks,)), DMA(((n_rep - 1) * blocks,)),
    ]


class ShareGather:
    def __init__(self, src, out, sems, n_rep):
        self.src, self.out, self.n_rep = src, out, n_rep
        self.ssem, self.rsem, self.lsem = sems
        self.r = lax.axis_index("rep")
        self.share = out.shape[0] // n_rep

    def local(self):
        return pltpu.make_async_copy(self.src, self.out.at[rows_of(self.r, self.share)], self.lsem)

    def desc(self, m, replica):
        return send(
            self.src, self.out.at[rows_of(replica, self.share)],
            self.ssem.at[m - 1], self.rsem.at[replica], rep=lax.rem(self.r + m, self.n_rep),
        )

    def start(self):
        self.local().start()
        for m in range(1, self.n_rep):
            self.desc(m, self.r).start()

    def finish(self):
        self.local().wait()
        for m in range(1, self.n_rep):
            self.desc(m, self.r).wait_send()
            self.desc(m, lax.rem(self.r + m, self.n_rep)).wait_recv()


def share_gather_sems(n_rep):
    return [DMA((n_rep - 1,)), DMA((n_rep,)), DMA(())]


class RowsBack:
    def __init__(self, src, out, sems, groups, n_shard, n_rep):
        self.src, self.out, self.groups = src, out, groups
        self.ssem, self.rsem, self.fsend, self.frecv, self.lsem = sems
        self.n_shard, self.n_rep = n_shard, n_rep
        self.share = out.shape[0] // n_rep
        self.total = out.shape[1] // groups
        self.width = self.total // n_shard
        self.s, self.r = lax.axis_index("shard"), lax.axis_index("rep")

    def place(self, source, replica, g):
        cols = pl.ds(pl.multiple_of(g * self.total + source * self.width, 128), self.width)
        return self.out.at[rows_of(replica, self.share), cols]

    def piece(self, target, g):
        return self.src(target).at[:, pl.ds(g * self.width, self.width)]

    def move(self, source, target, g):
        return send(
            self.piece(target, g), self.place(source, self.r, g),
            self.ssem.at[target * self.groups + g], self.rsem.at[source * self.groups + g],
            shard=target,
        )

    def local(self, g):
        return pltpu.make_async_copy(
            self.piece(self.s, g), self.place(self.s, self.r, g), self.lsem.at[g]
        )

    def pass_on(self, source, m, replica, g):
        at = self.place(source, replica, g)
        return send(
            at, at, self.fsend.at[(source * self.n_rep + m) * self.groups + g],
            self.frecv.at[(source * self.n_rep + replica) * self.groups + g],
            rep=lax.rem(self.r + m, self.n_rep),
        )

    def start(self, flip, low, high):
        def one(k, _):
            for g in range(self.groups):
                self.move(self.s, peer(k, flip, 1), g).start()
            return 0

        lax.fori_loop(low, high, one, 0)

    def start_own(self):
        for g in range(self.groups):
            self.local(g).start()

    def relay(self, source):
        for g in range(self.groups):
            for m in range(1, self.n_rep):
                self.pass_on(source, m, self.r, g).start()

    def forward_own(self):
        for g in range(self.groups):
            self.local(g).wait()
        self.relay(self.s)

    def forward(self, flip, low, high):
        def one(k, _):
            source = peer(k, flip, -1)
            for g in range(self.groups):
                self.move(source, self.s, g).wait_recv()
            self.relay(source)
            return 0

        lax.fori_loop(low, high, one, 0)

    def finish(self):
        def one(k, _):
            source = lax.rem(self.s + self.n_shard - k, self.n_shard)
            for g in range(self.groups):

                @pl.when(k > 0)
                def _():
                    self.move(self.s, source, g).wait_send()

                for m in range(1, self.n_rep):
                    self.pass_on(source, m, self.r, g).wait_send()
                    self.pass_on(source, m, lax.rem(self.r + m, self.n_rep), g).wait_recv()
            return 0

        lax.fori_loop(0, self.n_shard, one, 0)


def rows_back_sems(n_shard, n_rep, groups):
    return [
        DMA((n_shard * groups,)), DMA((n_shard * groups,)),
        DMA((n_shard * n_rep * groups,)), DMA((n_shard * n_rep * groups,)), DMA((groups,)),
    ]


def mm(left, right):
    return jnp.dot(left, right, preferred_element_type=F32)


def mm_nt(left, right):
    return lax.dot_general(left, right, (((1,), (1,)), ((), ())), preferred_element_type=F32)


def mm_tn(left, right):
    return lax.dot_general(left, right, (((0,), (0,)), ((), ())), preferred_element_type=F32)


def call(kernel, name, cid, outs, ins, scratch, *args, flops=0, moved=0):
    return pl.pallas_call(
        kernel,
        name=name,
        out_shape=[jax.ShapeDtypeStruct(shape, dtype) for shape, dtype, _ in outs],
        in_specs=ins,
        out_specs=[spec for _, _, spec in outs],
        scratch_shapes=scratch,
        compiler_params=pltpu.CompilerParams(
            collective_id=cid, has_side_effects=True, vmem_limit_bytes=VMEM_LIMIT
        ),
        cost_estimate=pl.CostEstimate(flops=flops, bytes_accessed=moved, transcendentals=0),
    )(*args)


def load(src, dst, sem):
    cp = pltpu.make_async_copy(src, dst, sem)
    cp.start()
    return cp


def own_rows(pos, count):
    a, b, c, _ = pos
    return rows_of(index(a, b, c), count)


class Out:
    def __init__(self, src, dst, sem, size):
        self.src, self.dst, self.sem, self.size = src, dst, sem, size

    def desc(self, q):
        r = rows_of(q, self.size)
        return pltpu.make_async_copy(self.src.at[r], self.dst.at[r], self.sem.at[q])

    def start(self, q):
        self.desc(q).start()

    def wait(self, q):
        self.desc(q).wait()


def wait_all(outs, chips):
    def one(q, _):
        for o in outs:
            o.wait(q)
        return 0

    lax.fori_loop(0, chips, one, 0)


def turned(row, count):
    return jnp.transpose(jnp.broadcast_to(row, (count, count)))


def swap_halves(x):
    return pltpu.roll(x, x.shape[1] // 2, 1)


def rope_of(spots, table):
    count = spots.shape[0]
    lane = lax.broadcasted_iota(jnp.int32, (count, count), 1)
    pick = jnp.where(lane.astype(F32) == spots, 1.0, 0.0).astype(F32)
    both = jnp.dot(pick, table, preferred_element_type=F32, precision=lax.Precision.HIGHEST)
    half = both.shape[1] // 2
    return both[:, :half], both[:, half:]


def row_sums(x):
    ones = jnp.ones((8, x.shape[1]), F32)
    return lax.dot_general(
        ones, x, (((1,), (1,)), ((), ())),
        preferred_element_type=F32, precision=lax.Precision.HIGHEST,
    )[:1]


def attn_kernel(
    n_shard, n_rep, heads,
    x_ref, aux_ref, wqkv_ref, wo_ref, wgu_ref, table_ref, qg_ref, kg_ref,
    g_ref, wq_ref, wg_ref, auxg_ref, sums_ref, hats_ref, rot_ref, prob_ref, ctx_ref, out_ref,
    buf, wq, stage, qkv, stats, got, lsem, osem, xs, xr, as_, ar, *rest,
):
    pos = position(n_shard)
    gsems, c3, c2, bufs, ssems = rest[:5], rest[5:10], rest[10:15], rest[15:19], rest[19:]
    p = bufs[0]
    count, width = out_ref.shape
    chips = n_shard // 2
    big = 2 * count
    own = wo_ref.shape[0]
    hw = own // heads
    na = pos[3]
    s = lax.axis_index("shard")
    mine = load(x_ref, buf.at[own_rows(pos, count)], lsem.at[0])
    qkv_w = Columns(wqkv_ref, wq, None, c3, 3, n_shard, n_rep)
    gu_w = Columns(wgu_ref, wg_ref, stage, c2, 2, n_shard, n_rep)
    auxg_ref[s] = aux_ref[...]
    greet_all(n_shard, n_rep)
    mine.wait()
    out_x = Out(buf, g_ref, osem, big)

    def aux_desc(k):
        target = lax.rem(s + k, n_shard)
        return send(aux_ref, auxg_ref.at[s], as_.at[k - 1], ar.at[k - 1], shard=target)

    def hook(t):
        @pl.when(t == 0)
        def _():
            qkv_w.start_own()
            gu_w.start_own()
            qkv_w.start(0, 1, half)
            qkv_w.start(1, 0, half)

            def one(k, _):
                aux_desc(k).start()
                return 0

            lax.fori_loop(1, n_shard, one, 0)

        @pl.when(t == na - 1)
        def _():
            gu_w.start(0, 1, half)
            qkv_w.forward(0, 1, half)
            qkv_w.forward(1, 0, half)

    half = n_shard // 2

    gather_loop(pos, count, buf, gsems, out_x.start, hook)
    early = half * 3 // 8
    gu_w.start(1, 0, early)
    qkv_w.finish()
    keep = load(wq, wq_ref, lsem.at[1])

    def project(q, _):
        r = rows_of(q, big)
        v = mm(buf[r, :], wq[...])
        qkv[r, :] = v
        for g in range(2):
            x = v[:, g * own : (g + 1) * own]
            stats[pl.ds(g, 1), pl.ds(pl.multiple_of(q * big, big), big)] = row_sums(x * x)
        return 0

    lax.fori_loop(0, chips, project, 0)
    exchange_start(n_shard, stats, got, xs, xr)
    gu_w.start(1, early, half)
    exchange_finish(n_shard, stats, got, xs, xr, sums_ref)

    def aux_done(k, _):
        aux_desc(k).wait_recv()
        aux_desc(k).wait_send()
        return 0

    lax.fori_loop(1, n_shard, aux_done, 0)
    root = hw ** (-0.5)
    lane = lax.broadcasted_iota(jnp.int32, (count, count), 1)
    slot = lax.broadcasted_iota(jnp.int32, (count, count), 0)

    def attend(i, _):
        r = rows_of(i, count)
        at = pl.ds(pl.multiple_of(i * count, count), count)
        spots = turned(auxg_ref[i, 1:2, :], count)
        cos, sin = rope_of(spots, table_ref[...])
        ok = (lane <= slot) & (lane >= slot - spots.astype(jnp.int32))
        scale = lax.rsqrt(sums_ref[:, at] / width + EPSILON)
        q_scale = turned(scale[0:1], count)[:, :1]
        k_scale = turned(scale[1:2], count)[:, :1]
        for h in range(heads):
            def part(g):
                lo = g * own + h * hw
                return slice(lo, lo + hw)

            cols = slice(h * hw, (h + 1) * hw)

            def turn(g, scale, gain):
                hat = qkv[r, part(g)] * scale
                hats_ref[r, part(g)] = hat
                x = hat * gain
                x = (x * cos + swap_halves(x) * sin).astype(BF)
                rot_ref[r, part(g)] = x
                return x

            query = turn(0, q_scale, qg_ref[:, cols])
            keys = turn(1, k_scale, kg_ref[:, cols])
            values = qkv[r, part(2)].astype(BF)
            rot_ref[r, part(2)] = values
            scores = jnp.where(ok, mm_nt(query, keys) * root, -1e30)
            e = jnp.exp(scores - jnp.max(scores, axis=-1, keepdims=True))
            probs = e / jnp.sum(e, axis=-1, keepdims=True)
            prob_ref[r, h * count : (h + 1) * count] = probs
            ctx_ref[r, cols] = mm(probs.astype(BF), values).astype(BF)

        @pl.when(i >= half + 1)
        def _():
            gu_w.forward(0, i - half, i - half + 1)

        return 0

    lax.fori_loop(0, n_shard, attend, 0, unroll=UNROLL)

    def partial(q):
        r = rows_of(q, big)
        p[r, :] = mm(ctx_ref[r, :], wo_ref[...]).astype(BF)

    def hook2(t):
        gu_w.forward(1, half * t // (na - 1), half * (t + 1) // (na - 1))

    scatter_loop(pos, count, bufs, ssems, partial, out_ref, hook2)
    gu_w.finish()
    keep.wait()
    wait_all([out_x], chips)


def exchange_desc(n_shard, stats, got, xs, xr, k):
    target = lax.rem(lax.axis_index("shard") + k, n_shard)
    return send(stats, got.at[k - 1], xs.at[k - 1], xr.at[k - 1], shard=target)


def exchange_start(n_shard, stats, got, xs, xr):
    def start(k, _):
        exchange_desc(n_shard, stats, got, xs, xr, k).start()
        return 0

    lax.fori_loop(1, n_shard, start, 0)


def exchange_finish(n_shard, stats, got, xs, xr, sums):
    sums[...] = stats[...]

    def take(k, _):
        exchange_desc(n_shard, stats, got, xs, xr, k).wait_recv()
        sums[...] += got[k - 1]
        return 0

    lax.fori_loop(1, n_shard, take, 0)

    def done(k, _):
        exchange_desc(n_shard, stats, got, xs, xr, k).wait_send()
        return 0

    lax.fori_loop(1, n_shard, done, 0)


def mlp_kernel(
    n_shard, x_ref, wg_ref, wd_ref, g_ref, gu_ref, mixed_ref, out_ref,
    buf, wg, wd, gu, mixed, lsem, osem, gsem, msem, *rest,
):
    pos = position(n_shard)
    bufs, ssems, gsems = rest[:4], rest[4:10], rest[10:]
    p = bufs[0]
    count, width = out_ref.shape
    big = 2 * count
    chips = n_shard // 2
    ff = wd.shape[0]
    mine = load(x_ref, buf.at[own_rows(pos, count)], lsem.at[0])
    w1 = load(wg_ref, wg, lsem.at[1])
    w2 = load(wd_ref, wd, lsem.at[2])
    greet(pos)
    mine.wait()
    out_x, out_g = Out(buf, g_ref, osem, big), Out(gu, gu_ref, gsem, big)
    out_m = Out(mixed, mixed_ref, msem, big)
    w1.wait()

    def on_chip(q):
        r = rows_of(q, big)
        out_x.start(q)

        def one(k, _):
            lo = pl.ds(pl.multiple_of(k * 256, 256), 256)
            hi = pl.ds(pl.multiple_of(ff + k * 256, 256), 256)
            gate = mm(buf[r, :], wg[:, lo])
            up = mm(buf[r, :], wg[:, hi])
            gu[r, lo] = gate.astype(BF)
            gu[r, hi] = up.astype(BF)
            mixed[r, lo] = (gate * jax.nn.sigmoid(gate) * up).astype(BF)
            return 0

        lax.fori_loop(0, ff // 256, one, 0)
        out_g.start(q)
        out_m.start(q)

    gather_loop(pos, count, buf, gsems, on_chip)
    w2.wait()

    def partial(q):
        r = rows_of(q, big)

        def one(k, _):
            lo = rows_of(k, 512)
            p[r, lo] = mm(mixed[r, :], wd[:, lo]).astype(BF)
            return 0

        lax.fori_loop(0, width // 512, one, 0)

    scatter_loop(pos, count, bufs, ssems, partial, out_ref)
    wait_all([out_x, out_g, out_m], chips)


def mlp_back_kernel(
    n_shard, n_rep, x_ref, gu_ref, wg_ref, wd_ref, resid_ref, mixed_ref,
    gsum_ref, down_ref, out_ref,
    buf, wg, wd, gu, dgu, resid, mixed, down, lsem, isem, osem, acc, got, xs, xr, *rest,
):
    pos = position(n_shard)
    na = pos[3]
    bufs, ssems, gsems = rest[:4], rest[4:10], rest[10:]
    p = bufs[0]
    count, width = out_ref.shape
    big = 2 * count
    chips = n_shard // 2
    ff = wd.shape[0]
    own = width // n_shard
    share = own // n_rep
    mine = load(x_ref, buf.at[own_rows(pos, count)], lsem.at[0])
    w2 = load(wd_ref, wd, lsem.at[2])
    saved = Out(gu_ref, gu, isem, big)

    def fetch(q, _):
        saved.start(q)
        return 0

    lax.fori_loop(0, chips, fetch, 0)
    w1 = load(wg_ref, wg, lsem.at[1])
    in_r = load(resid_ref, resid, lsem.at[3])
    in_m = load(mixed_ref, mixed, lsem.at[4])
    greet_all(n_shard, n_rep)
    mine.wait()
    w2.wait()

    def on_chip(q):
        r = rows_of(q, big)
        saved.wait(q)

        def one(k, _):
            lo = pl.ds(pl.multiple_of(k * 256, 256), 256)
            hi = pl.ds(pl.multiple_of(ff + k * 256, 256), 256)
            d_mixed = mm_nt(buf[r, :], wd[lo, :])
            gate, up = gu[r, lo].astype(F32), gu[r, hi].astype(F32)
            sigma = jax.nn.sigmoid(gate)
            d_gate = d_mixed * up * sigma * (1.0 + gate * (1.0 - sigma))
            dgu[r, lo] = d_gate.astype(BF)
            dgu[r, hi] = (d_mixed * gate * sigma).astype(BF)
            return 0

        lax.fori_loop(0, ff // 256, one, 0)

    gather_loop(pos, count, buf, gsems, on_chip)
    w1.wait()
    in_r.wait()
    in_m.wait()

    def partial(q):
        r = rows_of(q, big)

        def one(k, _):
            lo = rows_of(k, 256)
            p[r, lo] = mm_nt(dgu[r, :], wg[lo, :]).astype(BF)
            return 0

        lax.fori_loop(0, width // 256, one, 0)

    shares = ShareSum(acc, got, (xs, xr), n_shard, n_rep)
    owners = 4
    most = owners * own
    parts = width // most

    def grad_rows(k):
        at = rows_of(k, most)

        def one(n, _):
            lo = rows_of(n, 256)
            acc[at, lo] = mm_tn(resid[:, at], dgu[:, lo]).astype(BF)
            return 0

        lax.fori_loop(0, 2 * ff // 256, one, 0)
        for d in range(owners):
            shares.start(k * owners + d)

    def hook(t):
        def one(k, _):
            grad_rows(k)
            return 0

        lax.fori_loop(
            (parts * t + na - 2) // (na - 1), (parts * (t + 1) + na - 2) // (na - 1), one, 0
        )

    def grad_down():
        def rows(m, _):
            at = rows_of(m, most)

            def one(n, _):
                lo = rows_of(n, 256)
                down[at, lo] = mm_tn(mixed[:, at], buf[:, lo]).astype(BF)
                return 0

            lax.fori_loop(0, width // 256, one, 0)
            return 0

        lax.fori_loop(0, ff // most, rows, 0)
        load(down, down_ref, lsem.at[3])

    scatter_loop(pos, count, bufs, ssems, partial, out_ref, hook, grad_down)

    def collect(d, _):
        shares.add(d)
        pltpu.make_async_copy(
            acc.at[shares.part(d, shares.r)], gsum_ref.at[rows_of(d, share)], osem.at[d]
        ).start()
        return 0

    lax.fori_loop(0, n_shard, collect, 0)

    def end(d, _):
        shares.sent(d)
        pltpu.make_async_copy(
            acc.at[shares.part(d, shares.r)], gsum_ref.at[rows_of(d, share)], osem.at[d]
        ).wait()
        return 0

    lax.fori_loop(0, n_shard, end, 0)
    pltpu.make_async_copy(down, down_ref, lsem.at[3]).wait()


def attn_back_kernel(
    n_shard, n_rep, heads,
    x_ref, tok_ref, wo_ref, wq_ref, hats_ref, rot_ref, prob_ref, ctx_ref, aux_ref, sums_ref,
    table_ref, qg_ref, kg_ref, gsum_ref, down_ref,
    gu_ref, dn_ref, go_ref, gq_ref, gains_ref, out_ref,
    buf, tok, wq, dctx, ups, dqkv, stats, inner, got, lsem, xs, xr, *rest,
):
    rest = list(rest)

    def take(n):
        out = rest[:n]
        del rest[:n]
        return out

    pos = position(n_shard)
    na = pos[3]
    gsems, bufs, ssems = take(5), take(4), take(6)
    dacc, dgot, *dsems = take(4)
    oacc, ogot, *osems = take(4)
    qacc, qgot, *qsems = take(4)
    dgsems, ogsems, gusems, qksems = take(3), take(3), take(5), take(5)
    p = bufs[0]
    count, width = out_ref.shape
    big = 2 * count
    own = wo_ref.shape[0]
    hw = own // heads
    r_me = lax.axis_index("rep")
    mine = load(x_ref, buf.at[own_rows(pos, count)], lsem.at[0])
    in_d = load(down_ref, dacc, lsem.at[1])
    in_t = load(tok_ref, tok, lsem.at[2])
    in_w = load(wq_ref, wq, lsem.at[3])
    share = own // n_rep
    gu_rows = RowsBack(lambda d: gsum_ref.at[rows_of(d, share)], gu_ref, gusems, 2, n_shard, n_rep)
    down = ShareSum(dacc, dgot, dsems, 1, n_rep)
    down_all = ShareGather(dacc.at[down.part(0, r_me)], dn_ref, dgsems, n_rep)
    wout = ShareSum(oacc, ogot, osems, 1, n_rep)
    wout_all = ShareGather(oacc.at[wout.part(0, r_me)], go_ref, ogsems, n_rep)
    wqkv = ShareSum(qacc, qgot, qsems, n_shard, n_rep)
    wqkv_rows = RowsBack(
        lambda d: qacc.at[wqkv.part(d, r_me)], gq_ref, qksems, 3, n_shard, n_rep
    )
    greet_all(n_shard, n_rep)
    mine.wait()

    def hook(t):
        @pl.when(t == 0)
        def _():
            gu_rows.start_own()
            in_d.wait()
            down.start(0)

        @pl.when(t == na - 1)
        def _():
            gu_rows.start(0, 1, half)
            gu_rows.forward_own()
            down.add(0)
            down_all.start()

    half = n_shard // 2

    def on_chip(q):
        r = rows_of(q, big)
        dctx[r, :] = mm_nt(buf[r, :], wo_ref[...]).astype(BF)

    gather_loop(pos, count, buf, gsems, on_chip, hook)
    early = half * 5 // 8
    gu_rows.start(1, 0, early)
    root = hw ** (-0.5)
    gains_ref[...] = jnp.zeros_like(gains_ref)

    def scale_of(i):
        at = pl.ds(pl.multiple_of(i * count, count), count)
        return lax.rsqrt(sums_ref[:, at] / width + EPSILON)

    def attend(i, _):
        r = rows_of(i, count)
        at = pl.ds(pl.multiple_of(i * count, count), count)
        cos, sin = rope_of(turned(aux_ref[i, 1:2, :], count), table_ref[...])
        totals = [jnp.zeros((1, count), F32), jnp.zeros((1, count), F32)]
        for h in range(heads):
            def part(g):
                lo = g * own + h * hw
                return slice(lo, lo + hw)

            cols = slice(h * hw, (h + 1) * hw)
            query, keys, values = rot_ref[r, part(0)], rot_ref[r, part(1)], rot_ref[r, part(2)]
            probs = prob_ref[r, h * count : (h + 1) * count]
            probs_b = probs.astype(BF)
            d_ctx = dctx[r, cols]
            d_values = mm_tn(probs_b, d_ctx)
            d_probs = mm_nt(d_ctx, values)
            delta = jnp.sum(probs_b.astype(F32) * d_probs, axis=-1, keepdims=True)
            d_scores = (probs * (d_probs - delta) * root).astype(BF)
            d_query = mm(d_scores, keys)
            d_keys = mm_tn(d_scores, query)
            dqkv[r, part(2)] = d_values.astype(BF)
            for g, (x, gain) in enumerate(((d_query, qg_ref), (d_keys, kg_ref))):
                x = x * cos - swap_halves(x) * sin
                hat = hats_ref[r, part(g)]
                gains_ref[g : g + 1, cols] += jnp.sum(x * hat, axis=0, keepdims=True)
                up = x * gain[:, cols]
                ups[r, part(g)] = up
                totals[g] = totals[g] + row_sums(up * hat)
        for g in range(2):
            stats[pl.ds(g, 1), at] = totals[g]

        @pl.when(i >= half + 1)
        def _():
            gu_rows.forward(0, i - half, i - half + 1)

        return 0

    lax.fori_loop(0, n_shard, attend, 0, unroll=UNROLL)
    exchange_start(n_shard, stats, got, xs, xr)
    gu_rows.start(1, early, half)

    def out_cols(n, _):
        lo = rows_of(n, 256)
        oacc[:, lo] = mm_tn(ctx_ref[...], buf[:, lo]).astype(BF)
        return 0

    lax.fori_loop(0, width // 256, out_cols, 0)
    wout.start(0)
    exchange_finish(n_shard, stats, got, xs, xr, inner)

    def settle(i, _):
        r = rows_of(i, count)
        at = pl.ds(pl.multiple_of(i * count, count), count)
        scale = scale_of(i)
        mean = inner[:, at] / width
        for g in range(2):
            lo = slice(g * own, (g + 1) * own)
            column = turned(scale[g : g + 1], count)[:, :1]
            down_by = turned(mean[g : g + 1], count)[:, :1]
            dqkv[r, lo] = (column * (ups[r, lo] - hats_ref[r, lo] * down_by)).astype(BF)
        return 0

    lax.fori_loop(0, n_shard, settle, 0)
    in_w.wait()
    in_t.wait()

    def partial(q):
        r = rows_of(q, big)

        def one(k, _):
            lo = rows_of(k, 512)
            p[r, lo] = mm_nt(dqkv[r, :], wq[lo, :]).astype(BF)
            return 0

        lax.fori_loop(0, width // 512, one, 0)

    most = 4 * own

    def grad_rows(k, _):
        at = rows_of(k, most)
        qacc[at, :] = mm_tn(tok[:, at], dqkv[...]).astype(BF)
        return 0

    def near_far(do, flip):
        def one(k, _):
            do(peer(k, flip, 1))
            return 0

        lax.fori_loop(0, half, one, 0)

    def hook2(t):
        @pl.when(t == 0)
        def _():
            lax.fori_loop(0, width // most, grad_rows, 0)
            near_far(wqkv.start, 0)
            near_far(wqkv.start, 1)
            wout.add(0)
            wout_all.start()
            gu_rows.forward(1, 0, half)

        @pl.when(t == 1)
        def _():
            near_far(wqkv.add, 0)
            wqkv_rows.start_own()
            wqkv_rows.start(0, 1, half)

        @pl.when(t == 2)
        def _():
            near_far(wqkv.add, 1)
            wqkv_rows.start(1, 0, half)

    def final():
        wqkv_rows.forward_own()
        wqkv_rows.forward(0, 1, half)

    scatter_loop(pos, count, bufs, ssems, partial, out_ref, hook2, final)
    wqkv_rows.forward(1, 0, half)

    def end(d, _):
        wqkv.sent(d)
        return 0

    lax.fori_loop(0, n_shard, end, 0)
    down.sent(0)
    wout.sent(0)
    wqkv_rows.finish()
    gu_rows.finish()
    down_all.finish()
    wout_all.finish()


def positions(seg):
    slots = lax.broadcasted_iota(jnp.int32, seg.shape, 1)
    starts = jnp.concatenate(
        [jnp.ones((seg.shape[0], 1), jnp.bool_), seg[:, 1:] != seg[:, :-1]], axis=1
    )
    first = lax.cummax(jnp.where(starts, slots, 0), axis=1)
    return slots - first


def rope_table(count, head_width):
    half_width = head_width // 2
    inverse = THETA ** (-(2.0 * jnp.arange(half_width, dtype=F32)) / head_width)
    angle = jnp.arange(count, dtype=F32)[:, None] * inverse[None, :]
    cosine, sine = jnp.cos(angle), jnp.sin(angle)
    return jnp.concatenate([cosine, cosine, -sine, sine], axis=1)


def norm_scale(vector):
    return lax.rsqrt(jnp.mean(vector * vector, axis=-1, keepdims=True) + EPSILON)


def norm_back(upstream, normed, rscale, gain):
    scaled = upstream * gain
    inner = jnp.mean(scaled * normed, axis=-1, keepdims=True)
    return rscale * (scaled - normed * inner), jnp.sum(upstream * normed, axis=0)


def make(n_rep, n_shard):
    chips = n_shard // 2

    def shards(
        tokens, segment_ids, cotangent, w_qkv, w_out, w_gate_up, w_down,
        q_gain, k_gain, attn_gain, mlp_gain,
    ):
        count, width = tokens.shape
        heads = H // n_shard
        hw = width // H
        own = width // n_shard
        ff = w_down.shape[0]
        total = count * n_shard
        gathered = pltpu.VMEM((total, width), BF)

        gain_query = q_gain.astype(F32)
        gain_keys = k_gain.astype(F32)
        spots = positions(segment_ids[None]).astype(F32)
        aux = jnp.concatenate(
            [
                segment_ids.astype(F32)[None], spots, attn_gain.astype(F32)[None],
                mlp_gain.astype(F32)[None], jnp.zeros((4, count), F32),
            ]
        )
        table = rope_table(count, hw)
        chunk = n_shard - 1
        tokens_g, wq, wg, auxg, squares, hats, rots, probs, context_b, attn_raw = call(
            functools.partial(attn_kernel, n_shard, n_rep, heads), "attn", 1,
            [
                ((total, width), BF, ANY), ((width, 3 * own), BF, ANY), ((width, 2 * ff), BF, ANY),
                ((n_shard, 8, count), F32, VM), ((2, total), F32, VM), ((total, 2 * own), F32, VM),
                ((total, 3 * own), BF, VM), ((total, heads * count), F32, VM),
                ((total, own), BF, VM), ((count, width), F32, VM),
            ],
            [ANY, VM, ANY, VM, ANY, VM, VM, VM],
            [
                gathered, pltpu.VMEM((width, 3 * own), BF), pltpu.VMEM((own, 2 * ff), BF),
                pltpu.VMEM((total, 3 * own), F32), pltpu.VMEM((2, total), F32),
                pltpu.VMEM((chunk, 2, total), F32),
                DMA((2,)), DMA((chips,)), DMA((chunk,)), DMA((chunk,)), DMA((chunk,)), DMA((chunk,)),
            ] + gather_sems(n_shard) + columns_sems(n_shard, n_rep, 3)
            + columns_sems(n_shard, n_rep, 2)
            + scatter_bufs(n_shard, count, width) + scatter_sems(n_shard),
            tokens, aux, w_qkv, w_out, w_gate_up, table, gain_query[None], gain_keys[None],
        )
        gain_attn = auxg[:, 2].reshape(-1)
        gain_mlp = auxg[:, 3].reshape(-1)
        attn_scale = norm_scale(attn_raw)
        attn_hat = attn_raw * attn_scale
        resid = tokens.astype(F32) + attn_hat * gain_attn

        resid_g, gate_up, mixed_b, down_raw = call(
            functools.partial(mlp_kernel, n_shard), "mlp", 3,
            [
                ((total, width), BF, ANY), ((total, 2 * ff), BF, ANY),
                ((total, ff), BF, ANY), ((count, width), F32, VM),
            ],
            [ANY, ANY, ANY],
            [
                gathered, pltpu.VMEM((width, 2 * ff), BF), pltpu.VMEM((ff, width), BF),
                pltpu.VMEM((total, 2 * ff), BF), pltpu.VMEM((total, ff), BF),
                DMA((3,)), DMA((chips,)), DMA((chips,)), DMA((chips,)),
            ] + scatter_bufs(n_shard, count, width) + scatter_sems(n_shard) + gather_sems(n_shard),
            resid.astype(BF), wg, w_down,
        )
        down_scale = norm_scale(down_raw)
        down_hat = down_raw * down_scale
        output = (resid + down_hat * gain_mlp).astype(BF)

        valid = (segment_ids >= 0).astype(F32)[:, None]
        d_out = cotangent.astype(F32) * valid
        d_down, grad_mlp = norm_back(d_out, down_hat, down_scale, gain_mlp)
        gu_sum, down_acc, d_resid_sum = call(
            functools.partial(mlp_back_kernel, n_shard, n_rep), "mlp_back", 4,
            [
                ((width // n_rep, 2 * ff), BF, ANY), ((ff, width), BF, ANY),
                ((count, width), F32, VM),
            ],
            [ANY] * 6,
            [
                gathered, pltpu.VMEM((width, 2 * ff), BF), pltpu.VMEM((ff, width), BF),
                pltpu.VMEM((total, 2 * ff), BF), pltpu.VMEM((total, 2 * ff), BF),
                gathered, pltpu.VMEM((total, ff), BF),
                pltpu.VMEM((ff, width), BF), DMA((5,)), DMA((chips,)), DMA((n_shard,)),
            ] + share_scratch(width, 2 * ff, n_shard, n_rep)
            + scatter_bufs(n_shard, count, width) + scatter_sems(n_shard) + gather_sems(n_shard),
            d_down.astype(BF), gate_up, wg, w_down, resid_g, mixed_b,
        )
        d_resid = d_out + d_resid_sum
        d_attn, grad_attn = norm_back(d_resid, attn_hat, attn_scale, gain_attn)

        gu_rows, down_rows, out_rows, qkv_rows, gains_qk, d_tokens_sum = call(
            functools.partial(attn_back_kernel, n_shard, n_rep, heads), "attn_back", 5,
            [
                ((own, n_shard * 2 * ff), BF, ANY), ((ff, width), BF, ANY), ((own, width), BF, ANY),
                ((own, 3 * width), BF, ANY), ((2, own), F32, VM), ((count, width), F32, VM),
            ],
            [ANY, ANY, VM, ANY, VM, VM, VM, VM, VM, VM, VM, VM, VM, ANY, ANY],
            [
                gathered, gathered, pltpu.VMEM((width, 3 * own), BF), pltpu.VMEM((total, own), BF),
                pltpu.VMEM((total, 2 * own), F32), pltpu.VMEM((total, 3 * own), BF),
                pltpu.VMEM((2, total), F32),
                pltpu.VMEM((2, total), F32), pltpu.VMEM((chunk, 2, total), F32),
                DMA((4,)), DMA((chunk,)), DMA((chunk,)),
            ] + gather_sems(n_shard) + scatter_bufs(n_shard, count, width) + scatter_sems(n_shard)
            + share_scratch(ff, width, 1, n_rep) + share_scratch(own, width, 1, n_rep)
            + share_scratch(width, 3 * own, n_shard, n_rep)
            + share_gather_sems(n_rep) * 2
            + rows_back_sems(n_shard, n_rep, 2) + rows_back_sems(n_shard, n_rep, 3),
            d_attn.astype(BF), tokens_g, w_out, wq, hats, rots, probs, context_b, auxg, squares,
            table, gain_query[None], gain_keys[None], gu_sum, down_acc,
        )
        grad_tokens = d_resid + d_tokens_sum
        gains_local = lax.psum_scatter(
            jnp.stack([grad_attn, grad_mlp]), "shard", scatter_dimension=1, tiled=True
        )
        gains = lax.psum(jnp.concatenate([gains_local, gains_qk]), "rep")
        return (
            output, grad_tokens, qkv_rows.astype(F32), out_rows.astype(F32), gu_rows.astype(F32),
            down_rows.astype(F32), gains[2], gains[3], gains[0], gains[1],
        )

    return shards


def solution(mesh):
    rows = P(("rep", "shard"), None)
    return jax.shard_map(
        make(mesh.shape["rep"], mesh.shape["shard"]),
        mesh=mesh,
        in_specs=(rows, P(("rep", "shard")), rows)
        + (P("shard", None),) * 4
        + (P("shard"),) * 4,
        out_specs=(rows, rows) + (P("shard", None),) * 4 + (P("shard"),) * 4,
        check_vma=False,
    )
```

```python
import functools

import jax
import jax.numpy as jnp
from jax import lax
from jax.experimental import pallas as pl
from jax.experimental.pallas import tpu as pltpu
from jax.sharding import PartitionSpec as P

H = 16
EPSILON = 1e-06
THETA = 500000.0
BF = jnp.bfloat16
F32 = jnp.float32
MESH = pl.DeviceIdType.MESH
DMA = pltpu.SemaphoreType.DMA
ANY = pl.BlockSpec(memory_space=pl.ANY)
VM = pl.BlockSpec(memory_space=pltpu.VMEM)
CHUNKS = 2
UNROLL = 2
VMEM_LIMIT = 62 << 20


def position(n_shard):
    s = lax.axis_index("shard")
    return s // 4, (s // 2) % 2, s % 2, n_shard // 4


def index(a, b, c):
    return (a * 2 + b) * 2 + c


def line_order(t, a, na):
    m = jnp.minimum(a, na - 1 - a)
    near = jnp.where(t % 2 == 1, a - (t + 1) // 2, a + (t + 1) // 2)
    far = jnp.where(m == a, t, na - 1 - t)
    return jnp.where(t <= 2 * m, near, far)


def peer(k, flip, sign):
    s = lax.axis_index("shard")
    na = lax.axis_size("shard") // 4
    a, b, c = s // 4, (s // 2) % 2, s % 2
    return index(lax.rem(a + na + sign * (k // 2), na), (b + flip) % 2, (c + k) % 2)


def rows_of(i, size):
    return pl.ds(pl.multiple_of(i * size, size), size)


def send(src, dst, ssem, rsem, **target):
    return pltpu.make_async_remote_copy(
        src_ref=src, dst_ref=dst, send_sem=ssem, recv_sem=rsem,
        device_id=target, device_id_type=MESH,
    )


def signal(sem, **target):
    pl.semaphore_signal(sem, inc=1, device_id=target, device_id_type=MESH)


def greet(pos):
    barrier = pltpu.get_barrier_semaphore()
    a, b, c, na = pos

    @pl.when(a > 0)
    def _():
        signal(barrier, shard=index(a - 1, b, c))

    @pl.when(a < na - 1)
    def _():
        signal(barrier, shard=index(a + 1, b, c))

    signal(barrier, shard=index(a, 1 - b, c))
    signal(barrier, shard=index(a, b, 1 - c))
    pl.semaphore_wait(barrier, 2 + (a > 0).astype(jnp.int32) + (a < na - 1).astype(jnp.int32))


def greet_all(n_shard, n_rep):
    barrier = pltpu.get_barrier_semaphore()
    s, r = lax.axis_index("shard"), lax.axis_index("rep")

    def one(k, _):
        signal(barrier, shard=lax.rem(s + k, n_shard))
        return 0

    lax.fori_loop(1, n_shard, one, 0)
    for k in range(1, n_rep):
        signal(barrier, rep=lax.rem(r + k, n_rep))
    pl.semaphore_wait(barrier, n_shard - 1 + n_rep - 1)


def gather_sems(n_shard):
    na = n_shard // 4
    return [
        DMA((n_shard * CHUNKS,)), DMA((na * CHUNKS,)), DMA((na * CHUNKS,)),
        DMA((na * CHUNKS,)), DMA((2 * na * CHUNKS,)),
    ]


def gather_loop(pos, count, buf, sems, on_chip, hook=None):
    recv, up, down, ysend, csend = sems
    a, b, c, na = pos
    rows = count // CHUNKS

    def desc(i, ch, ssem, target):
        piece = buf.at[pl.ds(pl.multiple_of(i * count + ch * rows, rows), rows)]
        return send(piece, piece, ssem, recv.at[i * CHUNKS + ch], shard=target)

    def sends(j, ch):
        i = index(j, b, c)

        @pl.when((j <= a) & (a < na - 1))
        def _():
            desc(i, ch, up.at[j * CHUNKS + ch], index(a + 1, b, c)).start()

        @pl.when((j >= a) & (a > 0))
        def _():
            desc(i, ch, down.at[j * CHUNKS + ch], index(a - 1, b, c)).start()

        desc(i, ch, ysend.at[j * CHUNKS + ch], index(a, 1 - b, c)).start()
        desc(i, ch, csend.at[(j * 2 + b) * CHUNKS + ch], index(a, b, 1 - c)).start()

    def arrived(i, ch):
        desc(i, ch, csend.at[0], index(a, b, 1 - c)).wait_recv()

    def pair_step(j, t):
        i = index(j, 1 - b, c)
        for ch in range(CHUNKS):
            arrived(i, ch)
            desc(i, ch, csend.at[(j * 2 + 1 - b) * CHUNKS + ch], index(a, b, 1 - c)).start()
        for ch in range(CHUNKS):
            arrived(index(j, 1 - b, 1 - c), ch)
        on_chip(j * 2 + 1 - b, t)

    def step(t, _):
        j = line_order(t, a, na)
        for ch in range(CHUNKS):

            @pl.when(t > 0)
            def _():
                arrived(index(j, b, c), ch)

            sends(j, ch)
        if hook is not None:
            hook(t)
        for ch in range(CHUNKS):
            arrived(index(j, b, 1 - c), ch)
        on_chip(j * 2 + b, t)

        @pl.when(t > 0)
        def _():
            pair_step(line_order(t - 1, a, na), t)

        return 0

    lax.fori_loop(0, na, step, 0)
    pair_step(line_order(na - 1, a, na), na)

    def finish(j, _):
        i = index(j, b, c)
        for ch in range(CHUNKS):

            @pl.when((j <= a) & (a < na - 1))
            def _():
                desc(i, ch, up.at[j * CHUNKS + ch], index(a, b, 1 - c)).wait_send()

            @pl.when((j >= a) & (a > 0))
            def _():
                desc(i, ch, down.at[j * CHUNKS + ch], index(a, b, 1 - c)).wait_send()

            desc(i, ch, ysend.at[j * CHUNKS + ch], index(a, 1 - b, c)).wait_send()
            for bb in range(2):
                slot = (j * 2 + bb) * CHUNKS + ch
                desc(index(j, bb, c), ch, csend.at[slot], index(a, b, 1 - c)).wait_send()
        return 0

    lax.fori_loop(0, na, finish, 0)


def scatter_sems(n_shard):
    na = n_shard // 4
    return [DMA((2 * na,)), DMA((2 * na,)), DMA((na,)), DMA((na,)), DMA((na,)), DMA((na + 1,))]


def scatter_bufs(n_shard, count, width):
    na = n_shard // 4
    return [
        pltpu.VMEM((n_shard * count, width), BF), pltpu.VMEM((2 * na * count, width), BF),
        pltpu.VMEM((na * count, width), BF), pltpu.VMEM(((na + 1) * count, width), BF),
    ]


def scatter_loop(pos, count, bufs, sems, partial, out, works=(), order=None):
    p, cgot, ygot, zgot = bufs
    csend, crecv, ysend, yrecv, zsend, zrecv = sems
    a, b, c, na = pos
    tile = 32

    def to_core(q):
        return send(
            p.at[rows_of(q * 2 + 1 - c, count)], cgot.at[rows_of(q, count)],
            csend.at[q], crecv.at[q], shard=index(a, b, 1 - c),
        )

    def to_pair(j):
        return send(
            p.at[rows_of(index(j, 1 - b, c), count)], ygot.at[rows_of(j, count)],
            ysend.at[j], yrecv.at[j], shard=index(a, 1 - b, c),
        )

    def along(j, slot, target):
        return send(
            p.at[rows_of(index(j, b, c), count)], zgot.at[rows_of(slot, count)],
            zsend.at[j], zrecv.at[slot], shard=target,
        )

    def add(i, others, into=None):
        def one(k, _):
            def at(slot):
                return pl.ds(pl.multiple_of(slot * count + k * tile, tile), tile)

            total = p[at(i), :].astype(F32)
            for ref, slot in others:
                total = total + ref[at(slot), :].astype(F32)
            if into is None:
                p[at(i), :] = total.astype(BF)
            else:
                into[at(0), :] = total
            return 0

        lax.fori_loop(0, count // tile, one, 0)

    def first(t, _):
        j = line_order(na - 1 - t, a, na)
        far, near = j * 2 + 1 - b, j * 2 + b
        partial(far)
        to_core(far).start()
        partial(near)
        to_core(near).start()
        to_core(far).wait_recv()
        add(index(j, 1 - b, c), [(cgot, far)])
        to_pair(j).start()
        return 0

    def second(t, _):
        j = line_order(na - 1 - t, a, na)
        near = j * 2 + b
        i = index(j, b, c)
        to_core(near).wait_recv()
        to_pair(j).wait_recv()
        inner = ((j < a) & (a < na - 1)) | ((j > a) & (a > 0))

        @pl.when(inner)
        def _():
            along(j, j, index(a, b, 1 - c)).wait_recv()
            add(i, [(cgot, near), (ygot, j), (zgot, j)])

        @pl.when(jnp.logical_not(inner))
        def _():
            add(i, [(cgot, near), (ygot, j)])

        @pl.when(j > a)
        def _():
            along(j, j, index(a + 1, b, c)).start()

        @pl.when(j < a)
        def _():
            along(j, jnp.where(j == a - 1, na, j), index(a - 1, b, c)).start()

        return 0

    if order is None:
        lax.fori_loop(0, na, first, 0)
        lax.fori_loop(0, na - 1, second, 0)
    else:
        done_first = done_second = 0
        for token in order:
            if token == "f":
                first(done_first, 0)
                done_first += 1
            elif token == "s":
                second(done_second, 0)
                done_second += 1
            else:
                works[int(token)]()
        assert done_first == na and done_second == na - 1
    near = a * 2 + b
    to_core(near).wait_recv()
    to_pair(a).wait_recv()
    add(index(a, b, c), [(cgot, near), (ygot, a)], out)

    def more(slot):
        along(a, slot, index(a, b, 1 - c)).wait_recv()

        def one(k, _):
            got = zgot[pl.ds(pl.multiple_of(slot * count + k * tile, tile), tile), :]
            out[rows_of(k, tile), :] += got.astype(F32)
            return 0

        lax.fori_loop(0, count // tile, one, 0)

    @pl.when(a > 0)
    def _():
        more(a)

    @pl.when(a < na - 1)
    def _():
        more(na)

    def finish(j, _):
        for bb in range(2):
            to_core(j * 2 + bb).wait_send()
        to_pair(j).wait_send()

        @pl.when(j != a)
        def _():
            along(j, j, index(a, b, 1 - c)).wait_send()

        return 0

    lax.fori_loop(0, na, finish, 0)


def columns_sems(n_shard, n_rep, groups):
    return [
        DMA((n_shard * groups,)), DMA((n_shard * groups,)),
        DMA((n_shard * n_rep,)), DMA((n_shard * n_rep,)), DMA((groups + 1,)),
    ]


class Columns:
    def __init__(self, w, out, stage, sems, groups, n_shard, n_rep):
        self.w, self.out, self.stage, self.groups = w, out, stage, groups
        self.ssem, self.rsem, self.fsend, self.frecv, self.lsem = sems
        self.n_shard, self.n_rep = n_shard, n_rep
        self.own = w.shape[0]
        self.share = self.own // n_rep
        self.total = w.shape[1] // groups
        self.width = self.total // n_shard
        self.s, self.r = lax.axis_index("shard"), lax.axis_index("rep")

    def move(self, source, target, g):
        cols = pl.ds(pl.multiple_of(g * self.total + target * self.width, 128), self.width)
        src = self.w.at[rows_of(self.r, self.share), cols]
        at = pl.ds(pl.multiple_of(source * self.own + self.r * self.share, self.share), self.share)
        dst = self.out.at[at, pl.ds(g * self.width, self.width)]
        return send(
            src, dst, self.ssem.at[target * self.groups + g],
            self.rsem.at[source * self.groups + g], shard=target,
        )

    def pass_on(self, source, k, replica):
        at = pl.ds(
            pl.multiple_of(source * self.own + replica * self.share, self.share), self.share
        )
        piece = self.out.at[at]
        return send(
            piece, piece, self.fsend.at[source * self.n_rep + k],
            self.frecv.at[source * self.n_rep + replica],
            rep=lax.rem(self.r + k, self.n_rep),
        )

    def local_in(self, g):
        cols = pl.ds(pl.multiple_of(g * self.total + self.s * self.width, 128), self.width)
        into = pl.ds(g * self.width, self.width)
        if self.stage is None:
            dst = self.out.at[rows_of(self.s, self.own), into]
        else:
            dst = self.stage.at[:, into]
        return pltpu.make_async_copy(self.w.at[:, cols], dst, self.lsem.at[g])

    def local_out(self):
        return pltpu.make_async_copy(
            self.stage, self.out.at[rows_of(self.s, self.own)], self.lsem.at[self.groups]
        )

    def start(self, flip, low, high):
        def one(k, _):
            for g in range(self.groups):
                self.move(self.s, peer(k, flip, 1), g).start()
            return 0

        lax.fori_loop(low, high, one, 0)

    def start_own(self):
        for g in range(self.groups):
            self.local_in(g).start()
        if self.stage is not None:
            for g in range(self.groups):
                self.local_in(g).wait()
            self.local_out().start()

    def forward(self, flip, low, high):
        def one(k, _):
            source = peer(k, flip, -1)
            for g in range(self.groups):
                self.move(source, self.s, g).wait_recv()
            for m in range(1, self.n_rep):
                self.pass_on(source, m, self.r).start()
            return 0

        lax.fori_loop(low, high, one, 0)

    def finish(self):
        def one(k, _):
            source = lax.rem(self.s + self.n_shard - k, self.n_shard)
            for g in range(self.groups):
                self.move(self.s, source, g).wait_send()
            for m in range(1, self.n_rep):
                self.pass_on(source, m, self.r).wait_send()
                self.pass_on(source, m, lax.rem(self.r + m, self.n_rep)).wait_recv()
            return 0

        lax.fori_loop(1, self.n_shard, one, 0)
        if self.stage is not None:
            self.local_out().wait()
        else:
            for g in range(self.groups):
                self.local_in(g).wait()


class ShareSum:
    def __init__(self, acc, got, sems, blocks, n_rep):
        self.acc, self.got, self.blocks, self.n_rep = acc, got, blocks, n_rep
        self.ssem, self.rsem = sems
        self.share = acc.shape[0] // (blocks * n_rep)
        self.r = lax.axis_index("rep")

    def part(self, block, replica):
        return rows_of(block * self.n_rep + replica, self.share)

    def desc(self, block, m):
        target = lax.rem(self.r + m, self.n_rep)
        slot = (m - 1) * self.blocks + block
        return send(
            self.acc.at[self.part(block, target)], self.got.at[rows_of(slot, self.share)],
            self.ssem.at[slot], self.rsem.at[slot], rep=target,
        )

    def start(self, block):
        for m in range(1, self.n_rep):
            self.desc(block, m).start()

    def add(self, block):
        for m in range(1, self.n_rep):
            self.desc(block, m).wait_recv()
        tile = min(self.share, 32)

        def one(k, _):
            at = pl.ds(
                pl.multiple_of((block * self.n_rep + self.r) * self.share + k * tile, tile), tile
            )
            total = self.acc[at, :].astype(F32)
            for m in range(1, self.n_rep):
                slot = (m - 1) * self.blocks + block
                total = total + self.got[
                    pl.ds(pl.multiple_of(slot * self.share + k * tile, tile), tile), :
                ].astype(F32)
            self.acc[at, :] = total.astype(BF)
            return 0

        lax.fori_loop(0, self.share // tile, one, 0)

    def sent(self, block):
        for m in range(1, self.n_rep):
            self.desc(block, m).wait_send()


def share_scratch(rows, cols, blocks, n_rep):
    return [
        pltpu.VMEM((rows, cols), BF), pltpu.VMEM(((n_rep - 1) * rows // n_rep, cols), BF),
        DMA(((n_rep - 1) * blocks,)), DMA(((n_rep - 1) * blocks,)),
    ]


class ShareGather:
    def __init__(self, src, out, sems, n_rep):
        self.src, self.out, self.n_rep = src, out, n_rep
        self.ssem, self.rsem, self.lsem = sems
        self.r = lax.axis_index("rep")
        self.share = out.shape[0] // n_rep

    def local(self):
        return pltpu.make_async_copy(self.src, self.out.at[rows_of(self.r, self.share)], self.lsem)

    def desc(self, m, replica):
        return send(
            self.src, self.out.at[rows_of(replica, self.share)],
            self.ssem.at[m - 1], self.rsem.at[replica], rep=lax.rem(self.r + m, self.n_rep),
        )

    def start(self):
        self.local().start()
        for m in range(1, self.n_rep):
            self.desc(m, self.r).start()

    def finish(self):
        self.local().wait()
        for m in range(1, self.n_rep):
            self.desc(m, self.r).wait_send()
            self.desc(m, lax.rem(self.r + m, self.n_rep)).wait_recv()


def share_gather_sems(n_rep):
    return [DMA((n_rep - 1,)), DMA((n_rep,)), DMA(())]


class RowsBack:
    def __init__(self, src, out, sems, groups, n_shard, n_rep):
        self.src, self.out, self.groups = src, out, groups
        self.ssem, self.rsem, self.fsend, self.frecv, self.lsem = sems
        self.n_shard, self.n_rep = n_shard, n_rep
        self.share = out.shape[0] // n_rep
        self.total = out.shape[1] // groups
        self.width = self.total // n_shard
        self.s, self.r = lax.axis_index("shard"), lax.axis_index("rep")

    def place(self, source, replica, g):
        cols = pl.ds(pl.multiple_of(g * self.total + source * self.width, 128), self.width)
        return self.out.at[rows_of(replica, self.share), cols]

    def piece(self, target, g):
        return self.src(target).at[:, pl.ds(g * self.width, self.width)]

    def move(self, source, target, g):
        return send(
            self.piece(target, g), self.place(source, self.r, g),
            self.ssem.at[target * self.groups + g], self.rsem.at[source * self.groups + g],
            shard=target,
        )

    def local(self, g):
        return pltpu.make_async_copy(
            self.piece(self.s, g), self.place(self.s, self.r, g), self.lsem.at[g]
        )

    def pass_on(self, source, m, replica, g):
        at = self.place(source, replica, g)
        return send(
            at, at, self.fsend.at[(source * self.n_rep + m) * self.groups + g],
            self.frecv.at[(source * self.n_rep + replica) * self.groups + g],
            rep=lax.rem(self.r + m, self.n_rep),
        )

    def start(self, flip, low, high):
        def one(k, _):
            for g in range(self.groups):
                self.move(self.s, peer(k, flip, 1), g).start()
            return 0

        lax.fori_loop(low, high, one, 0)

    def start_own(self):
        for g in range(self.groups):
            self.local(g).start()

    def relay(self, source):
        for g in range(self.groups):
            for m in range(1, self.n_rep):
                self.pass_on(source, m, self.r, g).start()

    def forward_own(self):
        for g in range(self.groups):
            self.local(g).wait()
        self.relay(self.s)

    def forward(self, flip, low, high):
        def one(k, _):
            source = peer(k, flip, -1)
            for g in range(self.groups):
                self.move(source, self.s, g).wait_recv()
            self.relay(source)
            return 0

        lax.fori_loop(low, high, one, 0)

    def finish(self):
        def one(k, _):
            source = lax.rem(self.s + self.n_shard - k, self.n_shard)
            for g in range(self.groups):

                @pl.when(k > 0)
                def _():
                    self.move(self.s, source, g).wait_send()

                for m in range(1, self.n_rep):
                    self.pass_on(source, m, self.r, g).wait_send()
                    self.pass_on(source, m, lax.rem(self.r + m, self.n_rep), g).wait_recv()
            return 0

        lax.fori_loop(0, self.n_shard, one, 0)


def rows_back_sems(n_shard, n_rep, groups):
    return [
        DMA((n_shard * groups,)), DMA((n_shard * groups,)),
        DMA((n_shard * n_rep * groups,)), DMA((n_shard * n_rep * groups,)), DMA((groups,)),
    ]


def mm(left, right):
    return jnp.dot(left, right, preferred_element_type=F32)


def mm_nt(left, right):
    return lax.dot_general(left, right, (((1,), (1,)), ((), ())), preferred_element_type=F32)


def mm_tn(left, right):
    return lax.dot_general(left, right, (((0,), (0,)), ((), ())), preferred_element_type=F32)


def call(kernel, name, cid, outs, ins, scratch, *args, flops=0, moved=0):
    return pl.pallas_call(
        kernel,
        name=name,
        out_shape=[jax.ShapeDtypeStruct(shape, dtype) for shape, dtype, _ in outs],
        in_specs=ins,
        out_specs=[spec for _, _, spec in outs],
        scratch_shapes=scratch,
        compiler_params=pltpu.CompilerParams(
            collective_id=cid, has_side_effects=True, vmem_limit_bytes=VMEM_LIMIT
        ),
        cost_estimate=pl.CostEstimate(flops=flops, bytes_accessed=moved, transcendentals=0),
    )(*args)


def load(src, dst, sem):
    cp = pltpu.make_async_copy(src, dst, sem)
    cp.start()
    return cp


def own_rows(pos, count):
    a, b, c, _ = pos
    return rows_of(index(a, b, c), count)


class Out:
    def __init__(self, src, dst, sem, size):
        self.src, self.dst, self.sem, self.size = src, dst, sem, size

    def desc(self, q):
        r = rows_of(q, self.size)
        return pltpu.make_async_copy(self.src.at[r], self.dst.at[r], self.sem.at[q])

    def start(self, q):
        self.desc(q).start()

    def wait(self, q):
        self.desc(q).wait()


def wait_all(outs, chips):
    def one(q, _):
        for o in outs:
            o.wait(q)
        return 0

    lax.fori_loop(0, chips, one, 0)


def turned(row, count):
    return jnp.transpose(jnp.broadcast_to(row, (count, count)))


def swap_halves(x):
    return pltpu.roll(x, x.shape[1] // 2, 1)


def rope_of(spots, table):
    count = spots.shape[0]
    lane = lax.broadcasted_iota(jnp.int32, (count, count), 1)
    pick = jnp.where(lane.astype(F32) == spots, 1.0, 0.0).astype(F32)
    both = jnp.dot(pick, table, preferred_element_type=F32, precision=lax.Precision.HIGHEST)
    half = both.shape[1] // 2
    return both[:, :half], both[:, half:]


def row_sums(x):
    ones = jnp.ones((8, x.shape[1]), F32)
    return lax.dot_general(
        ones, x, (((1,), (1,)), ((), ())),
        preferred_element_type=F32, precision=lax.Precision.HIGHEST,
    )[:1]


def attn_kernel(
    n_shard, n_rep, heads,
    x_ref, aux_ref, wqkv_ref, wo_ref, wgu_ref, table_ref, qg_ref, kg_ref,
    g_ref, wq_ref, wg_ref, auxg_ref, sums_ref, hats_ref, rot_ref, prob_ref, ctx_ref, out_ref,
    buf, wq, stage, qkv, stats, got, lsem, osem, xs, xr, as_, ar, *rest,
):
    pos = position(n_shard)
    gsems, c3, c2, bufs, ssems = rest[:5], rest[5:10], rest[10:15], rest[15:19], rest[19:]
    p = bufs[0]
    count, width = out_ref.shape
    chips = n_shard // 2
    big = 2 * count
    own = wo_ref.shape[0]
    hw = own // heads
    na = pos[3]
    s = lax.axis_index("shard")
    mine = load(x_ref, buf.at[own_rows(pos, count)], lsem.at[0])
    qkv_w = Columns(wqkv_ref, wq, None, c3, 3, n_shard, n_rep)
    gu_w = Columns(wgu_ref, wg_ref, stage, c2, 2, n_shard, n_rep)
    auxg_ref[s] = aux_ref[...]
    greet_all(n_shard, n_rep)
    mine.wait()
    out_x = Out(buf, g_ref, osem, big)

    def aux_desc(k):
        target = lax.rem(s + k, n_shard)
        return send(aux_ref, auxg_ref.at[s], as_.at[k - 1], ar.at[k - 1], shard=target)

    def hook(t):
        @pl.when(t == 0)
        def _():
            qkv_w.start_own()
            gu_w.start_own()
            qkv_w.start(0, 1, half)
            qkv_w.start(1, 0, half)

            def one(k, _):
                aux_desc(k).start()
                return 0

            lax.fori_loop(1, n_shard, one, 0)

        @pl.when(t == na - 1)
        def _():
            gu_w.start(0, 1, half)
            qkv_w.forward(0, 1, half)
            qkv_w.forward(1, 0, half)

    half = n_shard // 2

    def project(q, _):
        r = rows_of(q, big)
        v = mm(buf[r, :], wq[...])
        qkv[r, :] = v
        for g in range(2):
            x = v[:, g * own : (g + 1) * own]
            stats[pl.ds(g, 1), pl.ds(pl.multiple_of(q * big, big), big)] = row_sums(x * x)
        return 0

    gather_loop(pos, count, buf, gsems, lambda q, t: out_x.start(q), hook)
    early = half * 3 // 8
    gu_w.start(1, 0, early)
    qkv_w.finish()
    keep = load(wq, wq_ref, lsem.at[1])
    lax.fori_loop(0, chips, project, 0)
    exchange_start(n_shard, stats, got, xs, xr)
    gu_w.start(1, early, half)
    exchange_finish(n_shard, stats, got, xs, xr, sums_ref)

    def aux_done(k, _):
        aux_desc(k).wait_recv()
        aux_desc(k).wait_send()
        return 0

    lax.fori_loop(1, n_shard, aux_done, 0)
    root = hw ** (-0.5)
    lane = lax.broadcasted_iota(jnp.int32, (count, count), 1)
    slot = lax.broadcasted_iota(jnp.int32, (count, count), 0)

    def attend(i, _):
        r = rows_of(i, count)
        at = pl.ds(pl.multiple_of(i * count, count), count)
        spots = turned(auxg_ref[i, 1:2, :], count)
        cos, sin = rope_of(spots, table_ref[...])
        ok = (lane <= slot) & (lane >= slot - spots.astype(jnp.int32))
        scale = lax.rsqrt(sums_ref[:, at] / width + EPSILON)
        q_scale = turned(scale[0:1], count)[:, :1]
        k_scale = turned(scale[1:2], count)[:, :1]
        for h in range(heads):
            def part(g):
                lo = g * own + h * hw
                return slice(lo, lo + hw)

            cols = slice(h * hw, (h + 1) * hw)

            def turn(g, scale, gain):
                hat = qkv[r, part(g)] * scale
                hats_ref[r, part(g)] = hat
                x = hat * gain
                x = (x * cos + swap_halves(x) * sin).astype(BF)
                rot_ref[r, part(g)] = x
                return x

            query = turn(0, q_scale, qg_ref[:, cols])
            keys = turn(1, k_scale, kg_ref[:, cols])
            values = qkv[r, part(2)].astype(BF)
            rot_ref[r, part(2)] = values
            scores = jnp.where(ok, mm_nt(query, keys) * root, -1e30)
            e = jnp.exp(scores - jnp.max(scores, axis=-1, keepdims=True))
            probs = e / jnp.sum(e, axis=-1, keepdims=True)
            prob_ref[r, h * count : (h + 1) * count] = probs
            ctx_ref[r, cols] = mm(probs.astype(BF), values).astype(BF)

        @pl.when(i >= half + 1)
        def _():
            gu_w.forward(0, i - half, i - half + 1)

        return 0

    lax.fori_loop(0, n_shard, attend, 0, unroll=UNROLL)

    def partial(q):
        r = rows_of(q, big)
        p[r, :] = mm(ctx_ref[r, :], wo_ref[...]).astype(BF)

    def pass_far(t):
        return lambda: gu_w.forward(1, half * t // 3, half * (t + 1) // 3)

    scatter_loop(
        pos, count, bufs, ssems, partial, out_ref, [pass_far(t) for t in range(3)],
        "f" * na + "0s1s2" + "s" * (na - 3),
    )
    gu_w.finish()
    keep.wait()
    wait_all([out_x], chips)


def exchange_desc(n_shard, stats, got, xs, xr, k):
    target = lax.rem(lax.axis_index("shard") + k, n_shard)
    return send(stats, got.at[k - 1], xs.at[k - 1], xr.at[k - 1], shard=target)


def exchange_start(n_shard, stats, got, xs, xr):
    def start(k, _):
        exchange_desc(n_shard, stats, got, xs, xr, k).start()
        return 0

    lax.fori_loop(1, n_shard, start, 0)


def exchange_finish(n_shard, stats, got, xs, xr, sums):
    sums[...] = stats[...]

    def take(k, _):
        exchange_desc(n_shard, stats, got, xs, xr, k).wait_recv()
        sums[...] += got[k - 1]
        return 0

    lax.fori_loop(1, n_shard, take, 0)

    def done(k, _):
        exchange_desc(n_shard, stats, got, xs, xr, k).wait_send()
        return 0

    lax.fori_loop(1, n_shard, done, 0)


def mlp_kernel(
    n_shard, x_ref, wg_ref, wd_ref, g_ref, gu_ref, mixed_ref, out_ref,
    buf, wg, wd, gu, mixed, lsem, osem, gsem, msem, *rest,
):
    pos = position(n_shard)
    bufs, ssems, gsems = rest[:4], rest[4:10], rest[10:]
    p = bufs[0]
    count, width = out_ref.shape
    big = 2 * count
    chips = n_shard // 2
    ff = wd.shape[0]
    mine = load(x_ref, buf.at[own_rows(pos, count)], lsem.at[0])
    w1 = load(wg_ref, wg, lsem.at[1])
    w2 = load(wd_ref, wd, lsem.at[2])
    greet(pos)
    mine.wait()
    out_x, out_g = Out(buf, g_ref, osem, big), Out(gu, gu_ref, gsem, big)
    out_m = Out(mixed, mixed_ref, msem, big)
    w1.wait()

    def on_chip(q, t):
        r = rows_of(q, big)
        out_x.start(q)

        def one(k, _):
            lo = pl.ds(pl.multiple_of(k * 256, 256), 256)
            hi = pl.ds(pl.multiple_of(ff + k * 256, 256), 256)
            gate = mm(buf[r, :], wg[:, lo])
            up = mm(buf[r, :], wg[:, hi])
            gu[r, lo] = gate.astype(BF)
            gu[r, hi] = up.astype(BF)
            mixed[r, lo] = (gate * jax.nn.sigmoid(gate) * up).astype(BF)
            return 0

        lax.fori_loop(0, ff // 256, one, 0)
        out_g.start(q)
        out_m.start(q)

    gather_loop(pos, count, buf, gsems, on_chip)
    w2.wait()

    def partial(q):
        r = rows_of(q, big)

        def one(k, _):
            lo = rows_of(k, 512)
            p[r, lo] = mm(mixed[r, :], wd[:, lo]).astype(BF)
            return 0

        lax.fori_loop(0, width // 512, one, 0)

    scatter_loop(pos, count, bufs, ssems, partial, out_ref)
    wait_all([out_x, out_g, out_m], chips)


def mlp_back_kernel(
    n_shard, n_rep, x_ref, gu_ref, wg_ref, wd_ref, resid_ref, mixed_ref,
    gsum_ref, down_ref, out_ref,
    buf, wg, wd, gu, dgu, resid, mixed, down, lsem, isem, osem, acc, got, xs, xr, *rest,
):
    pos = position(n_shard)
    na = pos[3]
    bufs, ssems, gsems = rest[:4], rest[4:10], rest[10:]
    p = bufs[0]
    count, width = out_ref.shape
    big = 2 * count
    chips = n_shard // 2
    ff = wd.shape[0]
    own = width // n_shard
    share = own // n_rep
    mine = load(x_ref, buf.at[own_rows(pos, count)], lsem.at[0])
    w2 = load(wd_ref, wd, lsem.at[2])
    saved = Out(gu_ref, gu, isem, big)

    def fetch(q, _):
        saved.start(q)
        return 0

    lax.fori_loop(0, chips, fetch, 0)
    w1 = load(wg_ref, wg, lsem.at[1])
    in_r = load(resid_ref, resid, lsem.at[3])
    in_m = load(mixed_ref, mixed, lsem.at[4])
    greet_all(n_shard, n_rep)
    mine.wait()
    w2.wait()

    def on_chip(q, t):
        r = rows_of(q, big)
        saved.wait(q)

        def one(k, _):
            lo = pl.ds(pl.multiple_of(k * 256, 256), 256)
            hi = pl.ds(pl.multiple_of(ff + k * 256, 256), 256)
            d_mixed = mm_nt(buf[r, :], wd[lo, :])
            gate, up = gu[r, lo].astype(F32), gu[r, hi].astype(F32)
            sigma = jax.nn.sigmoid(gate)
            d_gate = d_mixed * up * sigma * (1.0 + gate * (1.0 - sigma))
            dgu[r, lo] = d_gate.astype(BF)
            dgu[r, hi] = (d_mixed * gate * sigma).astype(BF)
            return 0

        lax.fori_loop(0, ff // 256, one, 0)

    gather_loop(pos, count, buf, gsems, on_chip)
    w1.wait()
    in_r.wait()
    in_m.wait()

    def partial(q):
        r = rows_of(q, big)

        def one(k, _):
            lo = rows_of(k, 512)
            p[r, lo] = mm_nt(dgu[r, :], wg[lo, :]).astype(BF)
            return 0

        lax.fori_loop(0, width // 512, one, 0)

    shares = ShareSum(acc, got, (xs, xr), n_shard, n_rep)
    owners = 4
    most = owners * own
    parts = width // most

    def grad_rows(k):
        at = rows_of(k, most)

        def one(n, _):
            lo = rows_of(n, 256)
            acc[at, lo] = mm_tn(resid[:, at], dgu[:, lo]).astype(BF)
            return 0

        lax.fori_loop(0, 2 * ff // 256, one, 0)
        for d in range(owners):
            shares.start(k * owners + d)

    def grad_down():
        def rows(m, _):
            at = rows_of(m, most)

            def one(n, _):
                lo = rows_of(n, 256)
                down[at, lo] = mm_tn(mixed[:, at], buf[:, lo]).astype(BF)
                return 0

            lax.fori_loop(0, width // 256, one, 0)
            return 0

        lax.fori_loop(0, ff // most, rows, 0)
        load(down, down_ref, lsem.at[3])

    def chunk(t):
        def run():
            def one(k, _):
                grad_rows(k)
                return 0

            lax.fori_loop(parts * t // 4, parts * (t + 1) // 4, one, 0)

        return run

    scatter_loop(
        pos, count, bufs, ssems, partial, out_ref, [chunk(t) for t in range(4)] + [grad_down],
        "0ff1" + "f" * (na - 2) + "s2s3" + "s" * (na - 3) + "4",
    )

    def collect(d, _):
        shares.add(d)
        pltpu.make_async_copy(
            acc.at[shares.part(d, shares.r)], gsum_ref.at[rows_of(d, share)], osem.at[d]
        ).start()
        return 0

    lax.fori_loop(0, n_shard, collect, 0)

    def end(d, _):
        shares.sent(d)
        pltpu.make_async_copy(
            acc.at[shares.part(d, shares.r)], gsum_ref.at[rows_of(d, share)], osem.at[d]
        ).wait()
        return 0

    lax.fori_loop(0, n_shard, end, 0)
    pltpu.make_async_copy(down, down_ref, lsem.at[3]).wait()


def attn_back_kernel(
    n_shard, n_rep, heads,
    x_ref, tok_ref, wo_ref, wq_ref, hats_ref, rot_ref, prob_ref, ctx_ref, aux_ref, sums_ref,
    table_ref, qg_ref, kg_ref, gain_ref, gsum_ref, down_ref,
    gu_ref, dn_ref, go_ref, gq_ref, gains_ref, out_ref,
    buf, tok, wq, dctx, ups, dqkv, stats, inner, got, ggot, mine_g, rgot, lsem, xs, xr, gs, gr, rs, rr, *rest,
):
    rest = list(rest)

    def take(n):
        out = rest[:n]
        del rest[:n]
        return out

    pos = position(n_shard)
    na = pos[3]
    gsems, bufs, ssems = take(5), take(4), take(6)
    dacc, dgot, *dsems = take(4)
    oacc, ogot, *osems = take(4)
    qacc, qgot, *qsems = take(4)
    dgsems, ogsems, gusems, qksems = take(3), take(3), take(5), take(5)
    p = bufs[0]
    count, width = out_ref.shape
    big = 2 * count
    own = wo_ref.shape[0]
    hw = own // heads
    r_me = lax.axis_index("rep")
    mine = load(x_ref, buf.at[own_rows(pos, count)], lsem.at[0])
    in_d = load(down_ref, dacc, lsem.at[1])
    in_t = load(tok_ref, tok, lsem.at[2])
    in_w = load(wq_ref, wq, lsem.at[3])
    share = own // n_rep
    gu_rows = RowsBack(lambda d: gsum_ref.at[rows_of(d, share)], gu_ref, gusems, 2, n_shard, n_rep)
    down = ShareSum(dacc, dgot, dsems, 1, n_rep)
    down_all = ShareGather(dacc.at[down.part(0, r_me)], dn_ref, dgsems, n_rep)
    wout = ShareSum(oacc, ogot, osems, 1, n_rep)
    wout_all = ShareGather(oacc.at[wout.part(0, r_me)], go_ref, ogsems, n_rep)
    wqkv = ShareSum(qacc, qgot, qsems, n_shard, n_rep)
    wqkv_rows = RowsBack(
        lambda d: qacc.at[wqkv.part(d, r_me)], gq_ref, qksems, 3, n_shard, n_rep
    )
    greet_all(n_shard, n_rep)
    mine.wait()

    def hook(t):
        @pl.when(t == 0)
        def _():
            gu_rows.start_own()
            in_d.wait()
            down.start(0)

            def one(k, _):
                gain_desc(k).start()
                return 0

            lax.fori_loop(1, n_shard, one, 0)

        @pl.when(t == na - 2)
        def _():
            down.add(0)
            down_all.start()

        @pl.when(t == na - 1)
        def _():
            gu_rows.start(0, 1, half)
            gu_rows.forward_own()

    half = n_shard // 2

    def gain_desc(k):
        target = lax.rem(lax.axis_index("shard") + k, n_shard)
        return send(gain_ref.at[target], ggot.at[k - 1], gs.at[k - 1], gr.at[k - 1], shard=target)

    def gain_rep(m):
        target = lax.rem(r_me + m, n_rep)
        return send(mine_g, rgot.at[m - 1], rs.at[m - 1], rr.at[m - 1], rep=target)

    def on_chip(q, t):
        r = rows_of(q, big)
        dctx[r, :] = mm_nt(buf[r, :], wo_ref[...]).astype(BF)

    gather_loop(pos, count, buf, gsems, on_chip, hook)
    early = half * 5 // 8
    gu_rows.start(1, 0, early)
    root = hw ** (-0.5)
    mine_g[...] = gain_ref[lax.axis_index("shard")]

    def scale_of(i):
        at = pl.ds(pl.multiple_of(i * count, count), count)
        return lax.rsqrt(sums_ref[:, at] / width + EPSILON)

    def attend(i, _):
        r = rows_of(i, count)
        at = pl.ds(pl.multiple_of(i * count, count), count)
        cos, sin = rope_of(turned(aux_ref[i, 1:2, :], count), table_ref[...])
        totals = [jnp.zeros((1, count), F32), jnp.zeros((1, count), F32)]
        for h in range(heads):
            def part(g):
                lo = g * own + h * hw
                return slice(lo, lo + hw)

            cols = slice(h * hw, (h + 1) * hw)
            query, keys, values = rot_ref[r, part(0)], rot_ref[r, part(1)], rot_ref[r, part(2)]
            probs = prob_ref[r, h * count : (h + 1) * count]
            probs_b = probs.astype(BF)
            d_ctx = dctx[r, cols]
            d_values = mm_tn(probs_b, d_ctx)
            d_probs = mm_nt(d_ctx, values)
            delta = jnp.sum(probs_b.astype(F32) * d_probs, axis=-1, keepdims=True)
            d_scores = (probs * (d_probs - delta) * root).astype(BF)
            d_query = mm(d_scores, keys)
            d_keys = mm_tn(d_scores, query)
            dqkv[r, part(2)] = d_values.astype(BF)
            for g, (x, gain) in enumerate(((d_query, qg_ref), (d_keys, kg_ref))):
                x = x * cos - swap_halves(x) * sin
                hat = hats_ref[r, part(g)]
                mine_g[2 + g : 3 + g, cols] += jnp.sum(x * hat, axis=0, keepdims=True)
                up = x * gain[:, cols]
                ups[r, part(g)] = up
                totals[g] = totals[g] + row_sums(up * hat)
        for g in range(2):
            stats[pl.ds(g, 1), at] = totals[g]

        @pl.when((i > 0) & (i < half))
        def _():
            gu_rows.forward(0, i, i + 1)

        return 0

    lax.fori_loop(0, n_shard, attend, 0, unroll=UNROLL)
    exchange_start(n_shard, stats, got, xs, xr)
    gu_rows.start(1, early, half)

    def out_cols(n, _):
        lo = rows_of(n, 256)
        oacc[:, lo] = mm_tn(ctx_ref[...], buf[:, lo]).astype(BF)
        return 0

    lax.fori_loop(0, width // 256, out_cols, 0)
    wout.start(0)

    def gain_take(k, _):
        gain_desc(k).wait_recv()
        mine_g[...] += ggot[k - 1]
        return 0

    lax.fori_loop(1, n_shard, gain_take, 0)
    for m in range(1, n_rep):
        gain_rep(m).start()
    exchange_finish(n_shard, stats, got, xs, xr, inner)

    def settle(i, _):
        r = rows_of(i, count)
        at = pl.ds(pl.multiple_of(i * count, count), count)
        scale = scale_of(i)
        mean = inner[:, at] / width
        for g in range(2):
            lo = slice(g * own, (g + 1) * own)
            column = turned(scale[g : g + 1], count)[:, :1]
            down_by = turned(mean[g : g + 1], count)[:, :1]
            dqkv[r, lo] = (column * (ups[r, lo] - hats_ref[r, lo] * down_by)).astype(BF)
        return 0

    lax.fori_loop(0, n_shard, settle, 0)
    in_w.wait()
    in_t.wait()

    def partial(q):
        r = rows_of(q, big)

        def one(k, _):
            lo = rows_of(k, 512)
            p[r, lo] = mm_nt(dqkv[r, :], wq[lo, :]).astype(BF)
            return 0

        lax.fori_loop(0, width // 512, one, 0)

    most = 4 * own

    def grad_rows(k, _):
        at = rows_of(k, most)
        qacc[at, :] = mm_tn(tok[:, at], dqkv[...]).astype(BF)
        return 0

    def near_far(do, flip):
        def one(k, _):
            do(peer(k, flip, 1))
            return 0

        lax.fori_loop(0, half, one, 0)

    def work0():
        lax.fori_loop(0, width // most, grad_rows, 0)
        near_far(wqkv.start, 0)
        near_far(wqkv.start, 1)

    def work1():
        gu_rows.forward(1, 0, half)

    def work2():
        wout.add(0)
        wout_all.start()

    def work3():
        near_far(wqkv.add, 0)
        wqkv_rows.start_own()
        wqkv_rows.start(0, 1, half)

    def work4():
        near_far(wqkv.add, 1)
        wqkv_rows.start(1, 0, half)

    def work5():
        wqkv_rows.forward_own()
        wqkv_rows.forward(0, 1, half)

    def work6():
        wqkv_rows.forward(1, 0, half)

    scatter_loop(
        pos, count, bufs, ssems, partial, out_ref, [work0, work1, work2, work3, work4, work5, work6],
        "0" + "f" * na + "12s3s45" + "s" * (na - 3) + "6",
    )

    def end(d, _):
        wqkv.sent(d)
        return 0

    lax.fori_loop(0, n_shard, end, 0)
    down.sent(0)
    wout.sent(0)

    def gain_sent(k, _):
        gain_desc(k).wait_send()
        return 0

    lax.fori_loop(1, n_shard, gain_sent, 0)
    gains_ref[...] = mine_g[...]
    for m in range(1, n_rep):
        gain_rep(m).wait_recv()
        gains_ref[...] += rgot[m - 1]
    for m in range(1, n_rep):
        gain_rep(m).wait_send()
    wqkv_rows.finish()
    gu_rows.finish()
    down_all.finish()
    wout_all.finish()


def positions(seg):
    slots = lax.broadcasted_iota(jnp.int32, seg.shape, 1)
    starts = jnp.concatenate(
        [jnp.ones((seg.shape[0], 1), jnp.bool_), seg[:, 1:] != seg[:, :-1]], axis=1
    )
    first = lax.cummax(jnp.where(starts, slots, 0), axis=1)
    return slots - first


def rope_table(count, head_width):
    half_width = head_width // 2
    inverse = THETA ** (-(2.0 * jnp.arange(half_width, dtype=F32)) / head_width)
    angle = jnp.arange(count, dtype=F32)[:, None] * inverse[None, :]
    cosine, sine = jnp.cos(angle), jnp.sin(angle)
    return jnp.concatenate([cosine, cosine, -sine, sine], axis=1)


def norm_scale(vector):
    return lax.rsqrt(jnp.mean(vector * vector, axis=-1, keepdims=True) + EPSILON)


def norm_back(upstream, normed, rscale, gain):
    scaled = upstream * gain
    inner = jnp.mean(scaled * normed, axis=-1, keepdims=True)
    return rscale * (scaled - normed * inner), jnp.sum(upstream * normed, axis=0)


def make(n_rep, n_shard):
    chips = n_shard // 2

    def shards(
        tokens, segment_ids, cotangent, w_qkv, w_out, w_gate_up, w_down,
        q_gain, k_gain, attn_gain, mlp_gain,
    ):
        count, width = tokens.shape
        heads = H // n_shard
        hw = width // H
        own = width // n_shard
        ff = w_down.shape[0]
        total = count * n_shard
        gathered = pltpu.VMEM((total, width), BF)

        gain_query = q_gain.astype(F32)
        gain_keys = k_gain.astype(F32)
        spots = positions(segment_ids[None]).astype(F32)
        aux = jnp.concatenate(
            [
                segment_ids.astype(F32)[None], spots, attn_gain.astype(F32)[None],
                mlp_gain.astype(F32)[None], jnp.zeros((4, count), F32),
            ]
        )
        table = rope_table(count, hw)
        chunk = n_shard - 1
        tokens_g, wq, wg, auxg, squares, hats, rots, probs, context_b, attn_raw = call(
            functools.partial(attn_kernel, n_shard, n_rep, heads), "attn", 1,
            [
                ((total, width), BF, ANY), ((width, 3 * own), BF, ANY), ((width, 2 * ff), BF, ANY),
                ((n_shard, 8, count), F32, VM), ((2, total), F32, VM), ((total, 2 * own), F32, VM),
                ((total, 3 * own), BF, VM), ((total, heads * count), F32, VM),
                ((total, own), BF, VM), ((count, width), F32, VM),
            ],
            [ANY, VM, ANY, VM, ANY, VM, VM, VM],
            [
                gathered, pltpu.VMEM((width, 3 * own), BF), pltpu.VMEM((own, 2 * ff), BF),
                pltpu.VMEM((total, 3 * own), F32), pltpu.VMEM((2, total), F32),
                pltpu.VMEM((chunk, 2, total), F32),
                DMA((2,)), DMA((chips,)), DMA((chunk,)), DMA((chunk,)), DMA((chunk,)), DMA((chunk,)),
            ] + gather_sems(n_shard) + columns_sems(n_shard, n_rep, 3)
            + columns_sems(n_shard, n_rep, 2)
            + scatter_bufs(n_shard, count, width) + scatter_sems(n_shard),
            tokens, aux, w_qkv, w_out, w_gate_up, table, gain_query[None], gain_keys[None],
        )
        gain_attn = auxg[:, 2].reshape(-1)
        gain_mlp = auxg[:, 3].reshape(-1)
        attn_scale = norm_scale(attn_raw)
        attn_hat = attn_raw * attn_scale
        resid = tokens.astype(F32) + attn_hat * gain_attn

        resid_g, gate_up, mixed_b, down_raw = call(
            functools.partial(mlp_kernel, n_shard), "mlp", 3,
            [
                ((total, width), BF, ANY), ((total, 2 * ff), BF, ANY),
                ((total, ff), BF, ANY), ((count, width), F32, VM),
            ],
            [ANY, ANY, ANY],
            [
                gathered, pltpu.VMEM((width, 2 * ff), BF), pltpu.VMEM((ff, width), BF),
                pltpu.VMEM((total, 2 * ff), BF), pltpu.VMEM((total, ff), BF),
                DMA((3,)), DMA((chips,)), DMA((chips,)), DMA((chips,)),
            ] + scatter_bufs(n_shard, count, width) + scatter_sems(n_shard) + gather_sems(n_shard),
            resid.astype(BF), wg, w_down,
        )
        down_scale = norm_scale(down_raw)
        down_hat = down_raw * down_scale
        output = (resid + down_hat * gain_mlp).astype(BF)

        valid = (segment_ids >= 0).astype(F32)[:, None]
        d_out = cotangent.astype(F32) * valid
        d_down, grad_mlp = norm_back(d_out, down_hat, down_scale, gain_mlp)
        gu_sum, down_acc, d_resid_sum = call(
            functools.partial(mlp_back_kernel, n_shard, n_rep), "mlp_back", 4,
            [
                ((width // n_rep, 2 * ff), BF, ANY), ((ff, width), BF, ANY),
                ((count, width), F32, VM),
            ],
            [ANY] * 6,
            [
                gathered, pltpu.VMEM((width, 2 * ff), BF), pltpu.VMEM((ff, width), BF),
                pltpu.VMEM((total, 2 * ff), BF), pltpu.VMEM((total, 2 * ff), BF),
                gathered, pltpu.VMEM((total, ff), BF),
                pltpu.VMEM((ff, width), BF), DMA((5,)), DMA((chips,)), DMA((n_shard,)),
            ] + share_scratch(width, 2 * ff, n_shard, n_rep)
            + scatter_bufs(n_shard, count, width) + scatter_sems(n_shard) + gather_sems(n_shard),
            d_down.astype(BF), gate_up, wg, w_down, resid_g, mixed_b,
        )
        d_resid = d_out + d_resid_sum
        d_attn, grad_attn = norm_back(d_resid, attn_hat, attn_scale, gain_attn)

        norm_gains = jnp.stack([grad_attn.reshape(n_shard, own), grad_mlp.reshape(n_shard, own)], axis=1)
        norm_gains = jnp.pad(norm_gains, ((0, 0), (0, 6), (0, 0)))
        gu_rows, down_rows, out_rows, qkv_rows, gains, d_tokens_sum = call(
            functools.partial(attn_back_kernel, n_shard, n_rep, heads), "attn_back", 5,
            [
                ((own, n_shard * 2 * ff), BF, ANY), ((ff, width), BF, ANY), ((own, width), BF, ANY),
                ((own, 3 * width), BF, ANY), ((8, own), F32, VM), ((count, width), F32, VM),
            ],
            [ANY, ANY, VM, ANY, VM, VM, VM, VM, VM, VM, VM, VM, VM, VM, ANY, ANY],
            [
                gathered, gathered, pltpu.VMEM((width, 3 * own), BF), pltpu.VMEM((total, own), BF),
                pltpu.VMEM((total, 2 * own), F32), pltpu.VMEM((total, 3 * own), BF),
                pltpu.VMEM((2, total), F32),
                pltpu.VMEM((2, total), F32), pltpu.VMEM((chunk, 2, total), F32),
                pltpu.VMEM((chunk, 8, own), F32), pltpu.VMEM((8, own), F32),
                pltpu.VMEM((n_rep - 1, 8, own), F32),
                DMA((4,)), DMA((chunk,)), DMA((chunk,)), DMA((chunk,)), DMA((chunk,)),
                DMA((n_rep - 1,)), DMA((n_rep - 1,)),
            ] + gather_sems(n_shard) + scatter_bufs(n_shard, count, width) + scatter_sems(n_shard)
            + share_scratch(ff, width, 1, n_rep) + share_scratch(own, width, 1, n_rep)
            + share_scratch(width, 3 * own, n_shard, n_rep)
            + share_gather_sems(n_rep) * 2
            + rows_back_sems(n_shard, n_rep, 2) + rows_back_sems(n_shard, n_rep, 3),
            d_attn.astype(BF), tokens_g, w_out, wq, hats, rots, probs, context_b, auxg, squares,
            table, gain_query[None], gain_keys[None], norm_gains, gu_sum, down_acc,
        )
        grad_tokens = d_resid + d_tokens_sum
        return (
            output, grad_tokens, qkv_rows.astype(F32), out_rows.astype(F32), gu_rows.astype(F32),
            down_rows.astype(F32), gains[2], gains[3], gains[0], gains[1],
        )

    return shards


def solution(mesh):
    rows = P(("rep", "shard"), None)
    return jax.shard_map(
        make(mesh.shape["rep"], mesh.shape["shard"]),
        mesh=mesh,
        in_specs=(rows, P(("rep", "shard")), rows)
        + (P("shard", None),) * 4
        + (P("shard"),) * 4,
        out_specs=(rows, rows) + (P("shard", None),) * 4 + (P("shard"),) * 4,
        check_vma=False,
    )
```

```python
import functools

import jax
import jax.numpy as jnp
import numpy as np
from jax import lax
from jax.experimental import pallas as pl
from jax.experimental.pallas import tpu as pltpu
from jax.sharding import PartitionSpec as P

H = 16
EPSILON = 1e-06
THETA = 500000.0
BF = jnp.bfloat16
F32 = jnp.float32
MESH = pl.DeviceIdType.MESH
DMA = pltpu.SemaphoreType.DMA
ANY = pl.BlockSpec(memory_space=pl.ANY)
VM = pl.BlockSpec(memory_space=pltpu.VMEM)
CHUNKS = 2
UNROLL = 2
VMEM_LIMIT = 62 << 20


def position(n_shard):
    s = lax.axis_index("shard")
    return s // 4, (s // 2) % 2, s % 2, n_shard // 4


def index(a, b, c):
    return (a * 2 + b) * 2 + c


def line_order(t, a, na):
    m = jnp.minimum(a, na - 1 - a)
    near = jnp.where(t % 2 == 1, a - (t + 1) // 2, a + (t + 1) // 2)
    far = jnp.where(m == a, t, na - 1 - t)
    return jnp.where(t <= 2 * m, near, far)


def peer(k, flip, sign):
    s = lax.axis_index("shard")
    na = lax.axis_size("shard") // 4
    a, b, c = s // 4, (s // 2) % 2, s % 2
    return index(lax.rem(a + na + sign * (k // 2), na), (b + flip) % 2, (c + k) % 2)


def rows_of(i, size):
    return pl.ds(pl.multiple_of(i * size, size), size)


def send(src, dst, ssem, rsem, **target):
    return pltpu.make_async_remote_copy(
        src_ref=src, dst_ref=dst, send_sem=ssem, recv_sem=rsem,
        device_id=target, device_id_type=MESH,
    )


def signal(sem, **target):
    pl.semaphore_signal(sem, inc=1, device_id=target, device_id_type=MESH)


def greet(pos):
    barrier = pltpu.get_barrier_semaphore()
    a, b, c, na = pos

    @pl.when(a > 0)
    def _():
        signal(barrier, shard=index(a - 1, b, c))

    @pl.when(a < na - 1)
    def _():
        signal(barrier, shard=index(a + 1, b, c))

    signal(barrier, shard=index(a, 1 - b, c))
    signal(barrier, shard=index(a, b, 1 - c))
    pl.semaphore_wait(barrier, 2 + (a > 0).astype(jnp.int32) + (a < na - 1).astype(jnp.int32))


def greet_all(n_shard, n_rep):
    barrier = pltpu.get_barrier_semaphore()
    s, r = lax.axis_index("shard"), lax.axis_index("rep")

    def one(k, _):
        signal(barrier, shard=lax.rem(s + k, n_shard))
        return 0

    lax.fori_loop(1, n_shard, one, 0)
    for k in range(1, n_rep):
        signal(barrier, rep=lax.rem(r + k, n_rep))
    pl.semaphore_wait(barrier, n_shard - 1 + n_rep - 1)


def gather_sems(n_shard):
    na = n_shard // 4
    return [
        DMA((n_shard * CHUNKS,)), DMA((na * CHUNKS,)), DMA((na * CHUNKS,)),
        DMA((na * CHUNKS,)), DMA((2 * na * CHUNKS,)),
    ]


def gather_loop(pos, count, buf, sems, on_chip, hook=None):
    recv, up, down, ysend, csend = sems
    a, b, c, na = pos
    rows = count // CHUNKS

    def desc(i, ch, ssem, target):
        piece = buf.at[pl.ds(pl.multiple_of(i * count + ch * rows, rows), rows)]
        return send(piece, piece, ssem, recv.at[i * CHUNKS + ch], shard=target)

    def sends(j, ch):
        i = index(j, b, c)

        @pl.when((j <= a) & (a < na - 1))
        def _():
            desc(i, ch, up.at[j * CHUNKS + ch], index(a + 1, b, c)).start()

        @pl.when((j >= a) & (a > 0))
        def _():
            desc(i, ch, down.at[j * CHUNKS + ch], index(a - 1, b, c)).start()

        desc(i, ch, ysend.at[j * CHUNKS + ch], index(a, 1 - b, c)).start()
        desc(i, ch, csend.at[(j * 2 + b) * CHUNKS + ch], index(a, b, 1 - c)).start()

    def arrived(i, ch):
        desc(i, ch, csend.at[0], index(a, b, 1 - c)).wait_recv()

    def pair_step(j, t):
        i = index(j, 1 - b, c)
        for ch in range(CHUNKS):
            arrived(i, ch)
            desc(i, ch, csend.at[(j * 2 + 1 - b) * CHUNKS + ch], index(a, b, 1 - c)).start()
        for ch in range(CHUNKS):
            arrived(index(j, 1 - b, 1 - c), ch)
        on_chip(j * 2 + 1 - b, t)

    def step(t, _):
        j = line_order(t, a, na)
        for ch in range(CHUNKS):

            @pl.when(t > 0)
            def _():
                arrived(index(j, b, c), ch)

            sends(j, ch)
        if hook is not None:
            hook(t)
        for ch in range(CHUNKS):
            arrived(index(j, b, 1 - c), ch)
        on_chip(j * 2 + b, t)

        @pl.when(t > 0)
        def _():
            pair_step(line_order(t - 1, a, na), t)

        return 0

    lax.fori_loop(0, na, step, 0)
    pair_step(line_order(na - 1, a, na), na)

    def finish(j, _):
        i = index(j, b, c)
        for ch in range(CHUNKS):

            @pl.when((j <= a) & (a < na - 1))
            def _():
                desc(i, ch, up.at[j * CHUNKS + ch], index(a, b, 1 - c)).wait_send()

            @pl.when((j >= a) & (a > 0))
            def _():
                desc(i, ch, down.at[j * CHUNKS + ch], index(a, b, 1 - c)).wait_send()

            desc(i, ch, ysend.at[j * CHUNKS + ch], index(a, 1 - b, c)).wait_send()
            for bb in range(2):
                slot = (j * 2 + bb) * CHUNKS + ch
                desc(index(j, bb, c), ch, csend.at[slot], index(a, b, 1 - c)).wait_send()
        return 0

    lax.fori_loop(0, na, finish, 0)


def scatter_sems(n_shard):
    na = n_shard // 4
    return [DMA((2 * na,)), DMA((2 * na,)), DMA((na,)), DMA((na,)), DMA((na,)), DMA((na + 1,))]


def scatter_bufs(n_shard, count, width):
    na = n_shard // 4
    return [
        pltpu.VMEM((n_shard * count, width), BF), pltpu.VMEM((2 * na * count, width), BF),
        pltpu.VMEM((na * count, width), BF), pltpu.VMEM(((na + 1) * count, width), BF),
    ]


def scatter_loop(pos, count, bufs, sems, partial, out, works=(), order=None):
    p, cgot, ygot, zgot = bufs
    csend, crecv, ysend, yrecv, zsend, zrecv = sems
    a, b, c, na = pos
    tile = 32

    def to_core(q):
        return send(
            p.at[rows_of(q * 2 + 1 - c, count)], cgot.at[rows_of(q, count)],
            csend.at[q], crecv.at[q], shard=index(a, b, 1 - c),
        )

    def to_pair(j):
        return send(
            p.at[rows_of(index(j, 1 - b, c), count)], ygot.at[rows_of(j, count)],
            ysend.at[j], yrecv.at[j], shard=index(a, 1 - b, c),
        )

    def along(j, slot, target):
        return send(
            p.at[rows_of(index(j, b, c), count)], zgot.at[rows_of(slot, count)],
            zsend.at[j], zrecv.at[slot], shard=target,
        )

    def add(i, others, into=None):
        def one(k, _):
            def at(slot):
                return pl.ds(pl.multiple_of(slot * count + k * tile, tile), tile)

            total = p[at(i), :].astype(F32)
            for ref, slot in others:
                total = total + ref[at(slot), :].astype(F32)
            if into is None:
                p[at(i), :] = total.astype(BF)
            else:
                into[at(0), :] = total
            return 0

        lax.fori_loop(0, count // tile, one, 0)

    def first(t, _):
        j = line_order(na - 1 - t, a, na)
        far, near = j * 2 + 1 - b, j * 2 + b
        partial(far)
        to_core(far).start()
        partial(near)
        to_core(near).start()
        to_core(far).wait_recv()
        add(index(j, 1 - b, c), [(cgot, far)])
        to_pair(j).start()
        return 0

    def second(t, _):
        j = line_order(na - 1 - t, a, na)
        near = j * 2 + b
        i = index(j, b, c)
        to_core(near).wait_recv()
        to_pair(j).wait_recv()
        inner = ((j < a) & (a < na - 1)) | ((j > a) & (a > 0))

        @pl.when(inner)
        def _():
            along(j, j, index(a, b, 1 - c)).wait_recv()
            add(i, [(cgot, near), (ygot, j), (zgot, j)])

        @pl.when(jnp.logical_not(inner))
        def _():
            add(i, [(cgot, near), (ygot, j)])

        @pl.when(j > a)
        def _():
            along(j, j, index(a + 1, b, c)).start()

        @pl.when(j < a)
        def _():
            along(j, jnp.where(j == a - 1, na, j), index(a - 1, b, c)).start()

        return 0

    if order is None:
        lax.fori_loop(0, na, first, 0)
        lax.fori_loop(0, na - 1, second, 0)
    else:
        done_first = done_second = 0
        for token in order:
            if token == "f":
                first(done_first, 0)
                done_first += 1
            elif token == "s":
                second(done_second, 0)
                done_second += 1
            else:
                works[int(token)]()
        assert done_first == na and done_second == na - 1
    near = a * 2 + b
    to_core(near).wait_recv()
    to_pair(a).wait_recv()
    add(index(a, b, c), [(cgot, near), (ygot, a)], out)

    def more(slot):
        along(a, slot, index(a, b, 1 - c)).wait_recv()

        def one(k, _):
            got = zgot[pl.ds(pl.multiple_of(slot * count + k * tile, tile), tile), :]
            out[rows_of(k, tile), :] += got.astype(F32)
            return 0

        lax.fori_loop(0, count // tile, one, 0)

    @pl.when(a > 0)
    def _():
        more(a)

    @pl.when(a < na - 1)
    def _():
        more(na)

    def finish(j, _):
        for bb in range(2):
            to_core(j * 2 + bb).wait_send()
        to_pair(j).wait_send()

        @pl.when(j != a)
        def _():
            along(j, j, index(a, b, 1 - c)).wait_send()

        return 0

    lax.fori_loop(0, na, finish, 0)


def columns_sems(n_shard, n_rep, groups):
    return [
        DMA((n_shard * groups,)), DMA((n_shard * groups,)),
        DMA((n_shard * n_rep,)), DMA((n_shard * n_rep,)), DMA((groups + 1,)),
    ]


class Columns:
    def __init__(self, w, out, stage, sems, groups, n_shard, n_rep):
        self.w, self.out, self.stage, self.groups = w, out, stage, groups
        self.ssem, self.rsem, self.fsend, self.frecv, self.lsem = sems
        self.n_shard, self.n_rep = n_shard, n_rep
        self.own = w.shape[0]
        self.share = self.own // n_rep
        self.total = w.shape[1] // groups
        self.width = self.total // n_shard
        self.s, self.r = lax.axis_index("shard"), lax.axis_index("rep")

    def move(self, source, target, g):
        cols = pl.ds(pl.multiple_of(g * self.total + target * self.width, 128), self.width)
        src = self.w.at[rows_of(self.r, self.share), cols]
        at = pl.ds(pl.multiple_of(source * self.own + self.r * self.share, self.share), self.share)
        dst = self.out.at[at, pl.ds(g * self.width, self.width)]
        return send(
            src, dst, self.ssem.at[target * self.groups + g],
            self.rsem.at[source * self.groups + g], shard=target,
        )

    def pass_on(self, source, k, replica):
        at = pl.ds(
            pl.multiple_of(source * self.own + replica * self.share, self.share), self.share
        )
        piece = self.out.at[at]
        return send(
            piece, piece, self.fsend.at[source * self.n_rep + k],
            self.frecv.at[source * self.n_rep + replica],
            rep=lax.rem(self.r + k, self.n_rep),
        )

    def local_in(self, g):
        cols = pl.ds(pl.multiple_of(g * self.total + self.s * self.width, 128), self.width)
        into = pl.ds(g * self.width, self.width)
        if self.stage is None:
            dst = self.out.at[rows_of(self.s, self.own), into]
        else:
            dst = self.stage.at[:, into]
        return pltpu.make_async_copy(self.w.at[:, cols], dst, self.lsem.at[g])

    def local_out(self):
        return pltpu.make_async_copy(
            self.stage, self.out.at[rows_of(self.s, self.own)], self.lsem.at[self.groups]
        )

    def start(self, flip, low, high):
        def one(k, _):
            for g in range(self.groups):
                self.move(self.s, peer(k, flip, 1), g).start()
            return 0

        lax.fori_loop(low, high, one, 0)

    def start_own(self):
        for g in range(self.groups):
            self.local_in(g).start()
        if self.stage is not None:
            for g in range(self.groups):
                self.local_in(g).wait()
            self.local_out().start()

    def forward(self, flip, low, high):
        def one(k, _):
            source = peer(k, flip, -1)
            for g in range(self.groups):
                self.move(source, self.s, g).wait_recv()
            for m in range(1, self.n_rep):
                self.pass_on(source, m, self.r).start()
            return 0

        lax.fori_loop(low, high, one, 0)

    def finish(self):
        def one(k, _):
            source = lax.rem(self.s + self.n_shard - k, self.n_shard)
            for g in range(self.groups):
                self.move(self.s, source, g).wait_send()
            for m in range(1, self.n_rep):
                self.pass_on(source, m, self.r).wait_send()
                self.pass_on(source, m, lax.rem(self.r + m, self.n_rep)).wait_recv()
            return 0

        lax.fori_loop(1, self.n_shard, one, 0)
        if self.stage is not None:
            self.local_out().wait()
        else:
            for g in range(self.groups):
                self.local_in(g).wait()


class ShareSum:
    def __init__(self, acc, got, sems, blocks, n_rep):
        self.acc, self.got, self.blocks, self.n_rep = acc, got, blocks, n_rep
        self.ssem, self.rsem = sems
        self.share = acc.shape[0] // (blocks * n_rep)
        self.r = lax.axis_index("rep")

    def part(self, block, replica):
        return rows_of(block * self.n_rep + replica, self.share)

    def desc(self, block, m):
        target = lax.rem(self.r + m, self.n_rep)
        slot = (m - 1) * self.blocks + block
        return send(
            self.acc.at[self.part(block, target)], self.got.at[rows_of(slot, self.share)],
            self.ssem.at[slot], self.rsem.at[slot], rep=target,
        )

    def start(self, block):
        for m in range(1, self.n_rep):
            self.desc(block, m).start()

    def add(self, block):
        for m in range(1, self.n_rep):
            self.desc(block, m).wait_recv()
        tile = min(self.share, 32)

        def one(k, _):
            at = pl.ds(
                pl.multiple_of((block * self.n_rep + self.r) * self.share + k * tile, tile), tile
            )
            total = self.acc[at, :].astype(F32)
            for m in range(1, self.n_rep):
                slot = (m - 1) * self.blocks + block
                total = total + self.got[
                    pl.ds(pl.multiple_of(slot * self.share + k * tile, tile), tile), :
                ].astype(F32)
            self.acc[at, :] = total.astype(BF)
            return 0

        lax.fori_loop(0, self.share // tile, one, 0)

    def sent(self, block):
        for m in range(1, self.n_rep):
            self.desc(block, m).wait_send()


def share_scratch(rows, cols, blocks, n_rep):
    return [
        pltpu.VMEM((rows, cols), BF), pltpu.VMEM(((n_rep - 1) * rows // n_rep, cols), BF),
        DMA(((n_rep - 1) * blocks,)), DMA(((n_rep - 1) * blocks,)),
    ]


class ShareGather:
    def __init__(self, src, out, sems, n_rep):
        self.src, self.out, self.n_rep = src, out, n_rep
        self.ssem, self.rsem, self.lsem = sems
        self.r = lax.axis_index("rep")
        self.share = out.shape[0] // n_rep

    def local(self):
        return pltpu.make_async_copy(self.src, self.out.at[rows_of(self.r, self.share)], self.lsem)

    def desc(self, m, replica):
        return send(
            self.src, self.out.at[rows_of(replica, self.share)],
            self.ssem.at[m - 1], self.rsem.at[replica], rep=lax.rem(self.r + m, self.n_rep),
        )

    def start(self):
        self.local().start()
        for m in range(1, self.n_rep):
            self.desc(m, self.r).start()

    def finish(self):
        self.local().wait()
        for m in range(1, self.n_rep):
            self.desc(m, self.r).wait_send()
            self.desc(m, lax.rem(self.r + m, self.n_rep)).wait_recv()


def share_gather_sems(n_rep):
    return [DMA((n_rep - 1,)), DMA((n_rep,)), DMA(())]


class RowsBack:
    def __init__(self, src, out, sems, groups, n_shard, n_rep):
        self.src, self.out, self.groups = src, out, groups
        self.ssem, self.rsem, self.fsend, self.frecv, self.lsem = sems
        self.n_shard, self.n_rep = n_shard, n_rep
        self.share = out.shape[0] // n_rep
        self.total = out.shape[1] // groups
        self.width = self.total // n_shard
        self.s, self.r = lax.axis_index("shard"), lax.axis_index("rep")

    def place(self, source, replica, g):
        cols = pl.ds(pl.multiple_of(g * self.total + source * self.width, 128), self.width)
        return self.out.at[rows_of(replica, self.share), cols]

    def piece(self, target, g):
        return self.src(target).at[:, pl.ds(g * self.width, self.width)]

    def move(self, source, target, g):
        return send(
            self.piece(target, g), self.place(source, self.r, g),
            self.ssem.at[target * self.groups + g], self.rsem.at[source * self.groups + g],
            shard=target,
        )

    def local(self, g):
        return pltpu.make_async_copy(
            self.piece(self.s, g), self.place(self.s, self.r, g), self.lsem.at[g]
        )

    def pass_on(self, source, m, replica, g):
        at = self.place(source, replica, g)
        return send(
            at, at, self.fsend.at[(source * self.n_rep + m) * self.groups + g],
            self.frecv.at[(source * self.n_rep + replica) * self.groups + g],
            rep=lax.rem(self.r + m, self.n_rep),
        )

    def start(self, flip, low, high):
        def one(k, _):
            for g in range(self.groups):
                self.move(self.s, peer(k, flip, 1), g).start()
            return 0

        lax.fori_loop(low, high, one, 0)

    def start_own(self):
        for g in range(self.groups):
            self.local(g).start()

    def relay(self, source):
        for g in range(self.groups):
            for m in range(1, self.n_rep):
                self.pass_on(source, m, self.r, g).start()

    def forward_own(self):
        for g in range(self.groups):
            self.local(g).wait()
        self.relay(self.s)

    def forward(self, flip, low, high):
        def one(k, _):
            source = peer(k, flip, -1)
            for g in range(self.groups):
                self.move(source, self.s, g).wait_recv()
            self.relay(source)
            return 0

        lax.fori_loop(low, high, one, 0)

    def finish(self):
        def one(k, _):
            source = lax.rem(self.s + self.n_shard - k, self.n_shard)
            for g in range(self.groups):

                @pl.when(k > 0)
                def _():
                    self.move(self.s, source, g).wait_send()

                for m in range(1, self.n_rep):
                    self.pass_on(source, m, self.r, g).wait_send()
                    self.pass_on(source, m, lax.rem(self.r + m, self.n_rep), g).wait_recv()
            return 0

        lax.fori_loop(0, self.n_shard, one, 0)


def rows_back_sems(n_shard, n_rep, groups):
    return [
        DMA((n_shard * groups,)), DMA((n_shard * groups,)),
        DMA((n_shard * n_rep * groups,)), DMA((n_shard * n_rep * groups,)), DMA((groups,)),
    ]


def mm(left, right):
    return jnp.dot(left, right, preferred_element_type=F32)


def mm_nt(left, right):
    return lax.dot_general(left, right, (((1,), (1,)), ((), ())), preferred_element_type=F32)


def mm_tn(left, right):
    return lax.dot_general(left, right, (((0,), (0,)), ((), ())), preferred_element_type=F32)


def call(kernel, name, cid, outs, ins, scratch, *args, flops=0, moved=0):
    return pl.pallas_call(
        kernel,
        name=name,
        out_shape=[jax.ShapeDtypeStruct(shape, dtype) for shape, dtype, _ in outs],
        in_specs=ins,
        out_specs=[spec for _, _, spec in outs],
        scratch_shapes=scratch,
        compiler_params=pltpu.CompilerParams(
            collective_id=cid, has_side_effects=True, vmem_limit_bytes=VMEM_LIMIT
        ),
        cost_estimate=pl.CostEstimate(flops=flops, bytes_accessed=moved, transcendentals=0),
    )(*args)


def load(src, dst, sem):
    cp = pltpu.make_async_copy(src, dst, sem)
    cp.start()
    return cp


def own_rows(pos, count):
    a, b, c, _ = pos
    return rows_of(index(a, b, c), count)


class Out:
    def __init__(self, src, dst, sem, size):
        self.src, self.dst, self.sem, self.size = src, dst, sem, size

    def desc(self, q):
        r = rows_of(q, self.size)
        return pltpu.make_async_copy(self.src.at[r], self.dst.at[r], self.sem.at[q])

    def start(self, q):
        self.desc(q).start()

    def wait(self, q):
        self.desc(q).wait()


def wait_all(outs, chips):
    def one(q, _):
        for o in outs:
            o.wait(q)
        return 0

    lax.fori_loop(0, chips, one, 0)


def turned(row, count):
    return jnp.transpose(jnp.broadcast_to(row, (count, count)))


def spots_of(seg_row, count):
    lane = lax.broadcasted_iota(jnp.int32, (count, count), 1).astype(F32)
    slot = lax.broadcasted_iota(jnp.int32, (count, count), 0).astype(F32)
    same = turned(seg_row, count) == seg_row
    first = jnp.min(jnp.where(same, lane, float(count)), axis=-1, keepdims=True)
    return same & (lane <= slot), slot[:, :1] - first


def swap_halves(x):
    return pltpu.roll(x, x.shape[1] // 2, 1)


def rope_of(spots, table):
    count = spots.shape[0]
    lane = lax.broadcasted_iota(jnp.int32, (count, count), 1)
    pick = jnp.where(lane.astype(F32) == spots, 1.0, 0.0).astype(F32)
    both = jnp.dot(pick, table, preferred_element_type=F32, precision=lax.Precision.HIGHEST)
    half = both.shape[1] // 2
    return both[:, :half], both[:, half:]


def row_sums(x):
    ones = jnp.ones((8, x.shape[1]), F32)
    return lax.dot_general(
        ones, x, (((1,), (1,)), ((), ())),
        preferred_element_type=F32, precision=lax.Precision.HIGHEST,
    )[:1]


def gain_rows(aux_ref, k, row):
    own = aux_ref.shape[2]
    for d in range(aux_ref.shape[0]):
        row[:, d * own : (d + 1) * own] = aux_ref[d, k : k + 1, :]


def norm_rows(rows, do):
    tile = 32

    def one(k, _):
        do(rows_of(k, tile))
        return 0

    lax.fori_loop(0, rows // tile, one, 0)


def row_scale(v):
    return lax.rsqrt(jnp.mean(v * v, axis=-1, keepdims=True) + EPSILON)


def norm_back(upstream, normed, rscale, gain):
    scaled = upstream * gain
    inner = jnp.mean(scaled * normed, axis=-1, keepdims=True)
    return rscale * (scaled - normed * inner)


def attn_kernel(
    n_shard, n_rep, heads,
    x_ref, aux_ref, wqkv_ref, wo_ref, wgu_ref, table_ref,
    g_ref, wq_ref, wg_ref, auxg_ref, sums_ref, hats_ref, rot_ref, prob_ref, ctx_ref,
    out_ref, scale_ref, resid_ref, residb_ref,
    row, buf, wq, stage, qkv, stats, got, lsem, osem, xs, xr, as_, ar, *rest,
):
    pos = position(n_shard)
    gsems, c3, c2, bufs, ssems = rest[:5], rest[5:10], rest[10:15], rest[15:19], rest[19:]
    p = bufs[0]
    count, width = out_ref.shape
    chips = n_shard // 2
    big = 2 * count
    own = wo_ref.shape[0]
    hw = own // heads
    na = pos[3]
    s = lax.axis_index("shard")
    mine = load(x_ref, buf.at[own_rows(pos, count)], lsem.at[0])
    qkv_w = Columns(wqkv_ref, wq, None, c3, 3, n_shard, n_rep)
    gu_w = Columns(wgu_ref, wg_ref, stage, c2, 2, n_shard, n_rep)
    auxg_ref[s] = aux_ref[...]
    greet_all(n_shard, n_rep)
    mine.wait()
    out_x = Out(buf, g_ref, osem, big)

    def aux_desc(k):
        target = lax.rem(s + k, n_shard)
        return send(aux_ref, auxg_ref.at[s], as_.at[k - 1], ar.at[k - 1], shard=target)

    def hook(t):
        @pl.when(t == 0)
        def _():
            qkv_w.start_own()
            gu_w.start_own()
            qkv_w.start(0, 1, half)
            qkv_w.start(1, 0, half)

            def one(k, _):
                aux_desc(k).start()
                return 0

            lax.fori_loop(1, n_shard, one, 0)

        @pl.when(t == na - 1)
        def _():
            gu_w.start(0, 1, half)
            qkv_w.forward(0, 1, half)
            qkv_w.forward(1, 0, half)

    half = n_shard // 2

    def project(q, _):
        r = rows_of(q, big)
        v = mm(buf[r, :], wq[...])
        qkv[r, :] = v
        for g in range(2):
            x = v[:, g * own : (g + 1) * own]
            stats[pl.ds(g, 1), pl.ds(pl.multiple_of(q * big, big), big)] = row_sums(x * x)

        @pl.when(q > 0)
        def _():
            gu_w.forward(0, q, q + 1)

        return 0

    gather_loop(pos, count, buf, gsems, lambda q, t: out_x.start(q), hook)
    qkv_w.finish()
    keep = load(wq, wq_ref, lsem.at[1])
    lax.fori_loop(0, chips, project, 0)
    exchange_start(n_shard, stats, got, xs, xr)
    gu_w.start(1, 0, half)
    exchange_finish(n_shard, stats, got, xs, xr, sums_ref)

    def aux_done(k, _):
        aux_desc(k).wait_recv()
        aux_desc(k).wait_send()
        return 0

    lax.fori_loop(1, n_shard, aux_done, 0)
    root = hw ** (-0.5)

    def attend(i, _):
        r = rows_of(i, count)
        at = pl.ds(pl.multiple_of(i * count, count), count)
        ok, spots = spots_of(auxg_ref[i, 0:1, :], count)
        cos, sin = rope_of(spots, table_ref[...])
        scale = lax.rsqrt(sums_ref[:, at] / width + EPSILON)
        q_scale = turned(scale[0:1], count)[:, :1]
        k_scale = turned(scale[1:2], count)[:, :1]
        for h in range(heads):
            def part(g):
                lo = g * own + h * hw
                return slice(lo, lo + hw)

            cols = slice(h * hw, (h + 1) * hw)

            def turn(g, scale, gain):
                hat = qkv[r, part(g)] * scale
                hats_ref[r, part(g)] = hat
                x = hat * gain
                x = (x * cos + swap_halves(x) * sin).astype(BF)
                rot_ref[r, part(g)] = x
                return x

            query = turn(0, q_scale, aux_ref[3:4, cols])
            keys = turn(1, k_scale, aux_ref[4:5, cols])
            values = qkv[r, part(2)].astype(BF)
            rot_ref[r, part(2)] = values
            scores = jnp.where(ok, mm_nt(query, keys) * root, -1e30)
            e = jnp.exp(scores - jnp.max(scores, axis=-1, keepdims=True))
            probs = e / jnp.sum(e, axis=-1, keepdims=True)
            prob_ref[r, h * count : (h + 1) * count] = probs
            ctx_ref[r, cols] = mm(probs.astype(BF), values).astype(BF)

        return 0

    lax.fori_loop(0, n_shard, attend, 0, unroll=UNROLL)

    def partial(q):
        r = rows_of(q, big)
        p[r, :] = mm(ctx_ref[r, :], wo_ref[...]).astype(BF)

    def pass_far(t):
        return lambda: gu_w.forward(1, half * t // 3, half * (t + 1) // 3)

    scatter_loop(
        pos, count, bufs, ssems, partial, out_ref, [pass_far(t) for t in range(3)],
        "f" * na + "0s1s2" + "s" * (na - 3),
    )
    gain_rows(auxg_ref, 1, row)

    def close(at):
        v = out_ref[at, :]
        scale = row_scale(v)
        hat = v * scale
        out_ref[at, :] = hat
        scale_ref[at, :] = jnp.broadcast_to(scale, (scale.shape[0], scale_ref.shape[1]))
        mine_at = pl.ds(pl.multiple_of(s * count + at.start, at.size), at.size)
        resid = buf[mine_at, :].astype(F32) + hat * row[...]
        resid_ref[at, :] = resid
        residb_ref[at, :] = resid.astype(BF)

    norm_rows(count, close)
    gu_w.finish()
    keep.wait()
    wait_all([out_x], chips)


def exchange_desc(n_shard, stats, got, xs, xr, k):
    target = lax.rem(lax.axis_index("shard") + k, n_shard)
    return send(stats, got.at[k - 1], xs.at[k - 1], xr.at[k - 1], shard=target)


def exchange_start(n_shard, stats, got, xs, xr):
    def start(k, _):
        exchange_desc(n_shard, stats, got, xs, xr, k).start()
        return 0

    lax.fori_loop(1, n_shard, start, 0)


def exchange_finish(n_shard, stats, got, xs, xr, sums):
    sums[...] = stats[...]

    def take(k, _):
        exchange_desc(n_shard, stats, got, xs, xr, k).wait_recv()
        sums[...] += got[k - 1]
        return 0

    lax.fori_loop(1, n_shard, take, 0)

    def done(k, _):
        exchange_desc(n_shard, stats, got, xs, xr, k).wait_send()
        return 0

    lax.fori_loop(1, n_shard, done, 0)


def live_rows(aux_ref, pos, mask):
    a, b, c, _ = pos
    segs = turned(aux_ref[index(a, b, c), 0:1, :], mask.shape[0])
    mask[...] = jnp.where(segs >= 0.0, 1.0, 0.0).astype(F32)


def mlp_kernel(
    n_shard, x_ref, wg_ref, wd_ref, aux_ref, resid_ref, cot_ref,
    g_ref, gu_ref, mixed_ref, y_ref, d_ref, gain_ref,
    out_ref, row, mask, buf, wg, wd, gu, mixed, lsem, osem, gsem, msem, *rest,
):
    pos = position(n_shard)
    bufs, ssems, gsems = rest[:4], rest[4:10], rest[10:]
    p = bufs[0]
    count, width = out_ref.shape
    big = 2 * count
    chips = n_shard // 2
    ff = wd.shape[0]
    mine = load(x_ref, buf.at[own_rows(pos, count)], lsem.at[0])
    w1 = load(wg_ref, wg, lsem.at[1])
    w2 = load(wd_ref, wd, lsem.at[2])
    greet(pos)
    mine.wait()
    out_x, out_g = Out(buf, g_ref, osem, big), Out(gu, gu_ref, gsem, big)
    out_m = Out(mixed, mixed_ref, msem, big)
    w1.wait()

    def on_chip(q, t):
        r = rows_of(q, big)
        out_x.start(q)

        def one(k, _):
            lo = pl.ds(pl.multiple_of(k * 256, 256), 256)
            hi = pl.ds(pl.multiple_of(ff + k * 256, 256), 256)
            gate = mm(buf[r, :], wg[:, lo])
            up = mm(buf[r, :], wg[:, hi])
            gu[r, lo] = gate.astype(BF)
            gu[r, hi] = up.astype(BF)
            mixed[r, lo] = (gate * jax.nn.sigmoid(gate) * up).astype(BF)
            return 0

        lax.fori_loop(0, ff // 256, one, 0)
        out_g.start(q)
        out_m.start(q)

    gather_loop(pos, count, buf, gsems, on_chip)
    w2.wait()

    def partial(q):
        r = rows_of(q, big)

        def one(k, _):
            lo = rows_of(k, 512)
            p[r, lo] = mm(mixed[r, :], wd[:, lo]).astype(BF)
            return 0

        lax.fori_loop(0, width // 512, one, 0)

    gain_rows(aux_ref, 2, row)
    live_rows(aux_ref, pos, mask)
    scatter_loop(pos, count, bufs, ssems, partial, out_ref)
    gain_ref[...] = jnp.zeros_like(gain_ref)

    def close(at):
        v = out_ref[at, :]
        scale = row_scale(v)
        hat = v * scale
        y_ref[at, :] = (resid_ref[at, :] + hat * row[...]).astype(BF)
        d_out = cot_ref[at, :].astype(F32) * mask[at, :1]
        gain_ref[...] += jnp.sum(d_out * hat, axis=0, keepdims=True)
        d_ref[at, :] = norm_back(d_out, hat, scale, row[...]).astype(BF)

    norm_rows(count, close)
    wait_all([out_x, out_g, out_m], chips)


def mlp_back_kernel(
    n_shard, n_rep, x_ref, gu_ref, wg_ref, wd_ref, resid_ref, mixed_ref,
    aux_ref, cot_ref, hat_ref, scale_ref, mlp_gain_ref,
    gsum_ref, down_ref, out_ref, d_ref, gain_ref,
    row, sums, mask, buf, wg, wd, gu, dgu, resid, mixed, down, lsem, isem, osem, acc, got, xs, xr, *rest,
):
    pos = position(n_shard)
    na = pos[3]
    bufs, ssems, gsems = rest[:4], rest[4:10], rest[10:]
    p = bufs[0]
    count, width = out_ref.shape
    big = 2 * count
    chips = n_shard // 2
    ff = wd.shape[0]
    own = width // n_shard
    share = own // n_rep
    mine = load(x_ref, buf.at[own_rows(pos, count)], lsem.at[0])
    w2 = load(wd_ref, wd, lsem.at[2])
    saved = Out(gu_ref, gu, isem, big)

    def fetch(q, _):
        saved.start(q)
        return 0

    lax.fori_loop(0, chips, fetch, 0)
    w1 = load(wg_ref, wg, lsem.at[1])
    in_r = load(resid_ref, resid, lsem.at[3])
    in_m = load(mixed_ref, mixed, lsem.at[4])
    greet_all(n_shard, n_rep)
    mine.wait()
    w2.wait()

    def on_chip(q, t):
        r = rows_of(q, big)
        saved.wait(q)

        def one(k, _):
            lo = pl.ds(pl.multiple_of(k * 256, 256), 256)
            hi = pl.ds(pl.multiple_of(ff + k * 256, 256), 256)
            d_mixed = mm_nt(buf[r, :], wd[lo, :])
            gate, up = gu[r, lo].astype(F32), gu[r, hi].astype(F32)
            sigma = jax.nn.sigmoid(gate)
            d_gate = d_mixed * up * sigma * (1.0 + gate * (1.0 - sigma))
            dgu[r, lo] = d_gate.astype(BF)
            dgu[r, hi] = (d_mixed * gate * sigma).astype(BF)
            return 0

        lax.fori_loop(0, ff // 256, one, 0)

    gather_loop(pos, count, buf, gsems, on_chip)
    w1.wait()
    in_r.wait()
    in_m.wait()

    def partial(q):
        r = rows_of(q, big)

        def one(k, _):
            lo = rows_of(k, 512)
            p[r, lo] = mm_nt(dgu[r, :], wg[lo, :]).astype(BF)
            return 0

        lax.fori_loop(0, width // 512, one, 0)

    shares = ShareSum(acc, got, (xs, xr), n_shard, n_rep)
    owners = 4
    most = owners * own
    parts = width // most

    def grad_rows(k):
        at = rows_of(k, most)

        def one(n, _):
            lo = rows_of(n, 256)
            acc[at, lo] = mm_tn(resid[:, at], dgu[:, lo]).astype(BF)
            return 0

        lax.fori_loop(0, 2 * ff // 256, one, 0)
        for d in range(owners):
            shares.start(k * owners + d)

    def grad_down():
        def rows(m, _):
            at = rows_of(m, most)

            def one(n, _):
                lo = rows_of(n, 256)
                down[at, lo] = mm_tn(mixed[:, at], buf[:, lo]).astype(BF)
                return 0

            lax.fori_loop(0, width // 256, one, 0)
            return 0

        lax.fori_loop(0, ff // most, rows, 0)
        load(down, down_ref, lsem.at[3])

    def chunk(t):
        def run():
            def one(k, _):
                grad_rows(k)
                return 0

            lax.fori_loop(parts * t // 4, parts * (t + 1) // 4, one, 0)

        return run

    scatter_loop(
        pos, count, bufs, ssems, partial, out_ref, [chunk(t) for t in range(4)] + [grad_down],
        "0ff1" + "f" * (na - 2) + "s2s3" + "s" * (na - 3) + "4",
    )

    gain_rows(aux_ref, 1, row)
    live_rows(aux_ref, pos, mask)
    sums[...] = jnp.zeros_like(sums)

    def close(at):
        d_resid = cot_ref[at, :].astype(F32) * mask[at, :1] + out_ref[at, :]
        out_ref[at, :] = d_resid
        hat = hat_ref[at, :]
        sums[...] += jnp.sum(d_resid * hat, axis=0, keepdims=True)
        d_ref[at, :] = norm_back(d_resid, hat, scale_ref[at, :1], row[...]).astype(BF)

    norm_rows(count, close)
    gain_ref[...] = jnp.zeros_like(gain_ref)
    for d in range(n_shard):
        cols = slice(d * own, (d + 1) * own)
        gain_ref[d, 0:1, :] = sums[:, cols]
        gain_ref[d, 1:2, :] = mlp_gain_ref[:, cols]

    def collect(d, _):
        shares.add(d)
        pltpu.make_async_copy(
            acc.at[shares.part(d, shares.r)], gsum_ref.at[rows_of(d, share)], osem.at[d]
        ).start()
        return 0

    lax.fori_loop(0, n_shard, collect, 0)

    def end(d, _):
        shares.sent(d)
        pltpu.make_async_copy(
            acc.at[shares.part(d, shares.r)], gsum_ref.at[rows_of(d, share)], osem.at[d]
        ).wait()
        return 0

    lax.fori_loop(0, n_shard, end, 0)
    pltpu.make_async_copy(down, down_ref, lsem.at[3]).wait()


def attn_back_kernel(
    n_shard, n_rep, heads,
    x_ref, tok_ref, wo_ref, wq_ref, hats_ref, rot_ref, prob_ref, ctx_ref, aux_ref, sums_ref,
    table_ref, gain_ref, gsum_ref, down_ref,
    gu_ref, dn_ref, go_ref, gq_ref, gains_ref, out_ref,
    buf, tok, wq, dctx, ups, dqkv, stats, inner, got, ggot, mine_g, rgot, lsem, xs, xr, gs, gr, rs, rr, *rest,
):
    rest = list(rest)

    def take(n):
        out = rest[:n]
        del rest[:n]
        return out

    pos = position(n_shard)
    na = pos[3]
    gsems, bufs, ssems = take(5), take(4), take(6)
    dacc, dgot, *dsems = take(4)
    oacc, ogot, *osems = take(4)
    qacc, qgot, *qsems = take(4)
    dgsems, ogsems, gusems, qksems = take(3), take(3), take(5), take(5)
    p = bufs[0]
    count, width = out_ref.shape
    big = 2 * count
    own = wo_ref.shape[0]
    hw = own // heads
    r_me = lax.axis_index("rep")
    mine = load(x_ref, buf.at[own_rows(pos, count)], lsem.at[0])
    in_d = load(down_ref, dacc, lsem.at[1])
    in_t = load(tok_ref, tok, lsem.at[2])
    in_w = load(wq_ref, wq, lsem.at[3])
    share = own // n_rep
    gu_rows = RowsBack(lambda d: gsum_ref.at[rows_of(d, share)], gu_ref, gusems, 2, n_shard, n_rep)
    down = ShareSum(dacc, dgot, dsems, 1, n_rep)
    down_all = ShareGather(dacc.at[down.part(0, r_me)], dn_ref, dgsems, n_rep)
    wout = ShareSum(oacc, ogot, osems, 1, n_rep)
    wout_all = ShareGather(oacc.at[wout.part(0, r_me)], go_ref, ogsems, n_rep)
    wqkv = ShareSum(qacc, qgot, qsems, n_shard, n_rep)
    wqkv_rows = RowsBack(
        lambda d: qacc.at[wqkv.part(d, r_me)], gq_ref, qksems, 3, n_shard, n_rep
    )
    greet_all(n_shard, n_rep)
    mine.wait()

    def hook(t):
        @pl.when(t == 0)
        def _():
            gu_rows.start_own()
            in_d.wait()
            down.start(0)

            def one(k, _):
                gain_desc(k).start()
                return 0

            lax.fori_loop(1, n_shard, one, 0)

        @pl.when(t == na - 2)
        def _():
            down.add(0)
            down_all.start()

        @pl.when(t == na - 1)
        def _():
            gu_rows.start(0, 1, half)
            gu_rows.forward_own()

    half = n_shard // 2

    def gain_desc(k):
        target = lax.rem(lax.axis_index("shard") + k, n_shard)
        return send(gain_ref.at[target], ggot.at[k - 1], gs.at[k - 1], gr.at[k - 1], shard=target)

    def gain_rep(m):
        target = lax.rem(r_me + m, n_rep)
        return send(mine_g, rgot.at[m - 1], rs.at[m - 1], rr.at[m - 1], rep=target)

    def on_chip(q, t):
        r = rows_of(q, big)
        dctx[r, :] = mm_nt(buf[r, :], wo_ref[...]).astype(BF)

    gather_loop(pos, count, buf, gsems, on_chip, hook)
    early = half * 5 // 8
    gu_rows.start(1, 0, early)
    root = hw ** (-0.5)
    me = lax.axis_index("shard")
    mine_g[...] = gain_ref[me]

    def scale_of(i):
        at = pl.ds(pl.multiple_of(i * count, count), count)
        return lax.rsqrt(sums_ref[:, at] / width + EPSILON)

    def attend(i, _):
        r = rows_of(i, count)
        at = pl.ds(pl.multiple_of(i * count, count), count)
        cos, sin = rope_of(spots_of(aux_ref[i, 0:1, :], count)[1], table_ref[...])
        totals = [jnp.zeros((1, count), F32), jnp.zeros((1, count), F32)]
        for h in range(heads):
            def part(g):
                lo = g * own + h * hw
                return slice(lo, lo + hw)

            cols = slice(h * hw, (h + 1) * hw)
            query, keys, values = rot_ref[r, part(0)], rot_ref[r, part(1)], rot_ref[r, part(2)]
            probs = prob_ref[r, h * count : (h + 1) * count]
            probs_b = probs.astype(BF)
            d_ctx = dctx[r, cols]
            d_values = mm_tn(probs_b, d_ctx)
            d_probs = mm_nt(d_ctx, values)
            delta = jnp.sum(probs_b.astype(F32) * d_probs, axis=-1, keepdims=True)
            d_scores = (probs * (d_probs - delta) * root).astype(BF)
            d_query = mm(d_scores, keys)
            d_keys = mm_tn(d_scores, query)
            dqkv[r, part(2)] = d_values.astype(BF)
            for g, x in enumerate((d_query, d_keys)):
                x = x * cos - swap_halves(x) * sin
                hat = hats_ref[r, part(g)]
                mine_g[2 + g : 3 + g, cols] += jnp.sum(x * hat, axis=0, keepdims=True)
                up = x * aux_ref[me, 3 + g : 4 + g, cols]
                ups[r, part(g)] = up
                totals[g] = totals[g] + row_sums(up * hat)
        for g in range(2):
            stats[pl.ds(g, 1), at] = totals[g]

        @pl.when((i > 0) & (i < half))
        def _():
            gu_rows.forward(0, i, i + 1)

        return 0

    lax.fori_loop(0, n_shard, attend, 0, unroll=UNROLL)
    exchange_start(n_shard, stats, got, xs, xr)
    gu_rows.start(1, early, half)

    def out_cols(n, _):
        lo = rows_of(n, 256)
        oacc[:, lo] = mm_tn(ctx_ref[...], buf[:, lo]).astype(BF)
        return 0

    lax.fori_loop(0, width // 256, out_cols, 0)
    wout.start(0)

    def gain_take(k, _):
        gain_desc(k).wait_recv()
        mine_g[...] += ggot[k - 1]
        return 0

    lax.fori_loop(1, n_shard, gain_take, 0)
    for m in range(1, n_rep):
        gain_rep(m).start()
    exchange_finish(n_shard, stats, got, xs, xr, inner)

    def settle(i, _):
        r = rows_of(i, count)
        at = pl.ds(pl.multiple_of(i * count, count), count)
        scale = scale_of(i)
        mean = inner[:, at] / width
        for g in range(2):
            lo = slice(g * own, (g + 1) * own)
            column = turned(scale[g : g + 1], count)[:, :1]
            down_by = turned(mean[g : g + 1], count)[:, :1]
            dqkv[r, lo] = (column * (ups[r, lo] - hats_ref[r, lo] * down_by)).astype(BF)
        return 0

    lax.fori_loop(0, n_shard, settle, 0)
    in_w.wait()
    in_t.wait()

    def partial(q):
        r = rows_of(q, big)

        def one(k, _):
            lo = rows_of(k, 512)
            p[r, lo] = mm_nt(dqkv[r, :], wq[lo, :]).astype(BF)
            return 0

        lax.fori_loop(0, width // 512, one, 0)

    most = 4 * own

    def grad_rows(k, _):
        at = rows_of(k, most)
        qacc[at, :] = mm_tn(tok[:, at], dqkv[...]).astype(BF)
        return 0

    def near_far(do, flip):
        def one(k, _):
            do(peer(k, flip, 1))
            return 0

        lax.fori_loop(0, half, one, 0)

    def work0():
        lax.fori_loop(0, width // most, grad_rows, 0)
        near_far(wqkv.start, 0)
        near_far(wqkv.start, 1)

    def work1():
        gu_rows.forward(1, 0, half)

    def work2():
        wout.add(0)
        wout_all.start()

    def work3():
        near_far(wqkv.add, 0)
        wqkv_rows.start_own()
        wqkv_rows.start(0, 1, half)

    def work4():
        near_far(wqkv.add, 1)
        wqkv_rows.start(1, 0, half)

    def work5():
        wqkv_rows.forward_own()
        wqkv_rows.forward(0, 1, half)

    def work6():
        wqkv_rows.forward(1, 0, half)

    scatter_loop(
        pos, count, bufs, ssems, partial, out_ref, [work0, work1, work2, work3, work4, work5, work6],
        "0" + "f" * na + "12s3s45" + "s" * (na - 3) + "6",
    )

    def end(d, _):
        wqkv.sent(d)
        return 0

    lax.fori_loop(0, n_shard, end, 0)
    down.sent(0)
    wout.sent(0)

    def gain_sent(k, _):
        gain_desc(k).wait_send()
        return 0

    lax.fori_loop(1, n_shard, gain_sent, 0)
    gains_ref[...] = mine_g[...]
    for m in range(1, n_rep):
        gain_rep(m).wait_recv()
        gains_ref[...] += rgot[m - 1]
    for m in range(1, n_rep):
        gain_rep(m).wait_send()
    wqkv_rows.finish()
    gu_rows.finish()
    down_all.finish()
    wout_all.finish()


def rope_table(count, head_width):
    half_width = head_width // 2
    inverse = np.float32(THETA) ** (-(np.float32(2.0) * np.arange(half_width, dtype=np.float32)) / np.float32(head_width))
    angle = np.arange(count, dtype=np.float32)[:, None] * inverse[None, :].astype(np.float32)
    cosine, sine = np.cos(angle), np.sin(angle)
    return np.concatenate([cosine, cosine, -sine, sine], axis=1).astype(np.float32)


def make(n_rep, n_shard):
    chips = n_shard // 2

    def shards(
        tokens, segment_ids, cotangent, w_qkv, w_out, w_gate_up, w_down,
        q_gain, k_gain, attn_gain, mlp_gain,
    ):
        count, width = tokens.shape
        heads = H // n_shard
        hw = width // H
        own = width // n_shard
        ff = w_down.shape[0]
        total = count * n_shard
        gathered = pltpu.VMEM((total, width), BF)

        assert own == count
        aux = jnp.stack(
            [x.astype(F32) for x in (segment_ids, attn_gain, mlp_gain, q_gain, k_gain)]
            + [jnp.zeros((count,), F32)] * 3
        )
        table = jnp.asarray(rope_table(count, hw))
        chunk = n_shard - 1
        (
            tokens_g, wq, wg, auxg, squares, hats, rots, probs, context_b,
            attn_hat, attn_scale, resid, resid_b,
        ) = call(
            functools.partial(attn_kernel, n_shard, n_rep, heads), "attn", 1,
            [
                ((total, width), BF, ANY), ((width, 3 * own), BF, ANY), ((width, 2 * ff), BF, ANY),
                ((n_shard, 8, count), F32, VM), ((2, total), F32, VM), ((total, 2 * own), F32, VM),
                ((total, 3 * own), BF, VM), ((total, heads * count), F32, VM),
                ((total, own), BF, VM), ((count, width), F32, VM), ((count, 128), F32, VM),
                ((count, width), F32, VM), ((count, width), BF, VM),
            ],
            [ANY, VM, ANY, VM, ANY, VM],
            [
                pltpu.VMEM((1, width), F32), gathered, pltpu.VMEM((width, 3 * own), BF), pltpu.VMEM((own, 2 * ff), BF),
                pltpu.VMEM((total, 3 * own), F32), pltpu.VMEM((2, total), F32),
                pltpu.VMEM((chunk, 2, total), F32),
                DMA((2,)), DMA((chips,)), DMA((chunk,)), DMA((chunk,)), DMA((chunk,)), DMA((chunk,)),
            ] + gather_sems(n_shard) + columns_sems(n_shard, n_rep, 3)
            + columns_sems(n_shard, n_rep, 2)
            + scatter_bufs(n_shard, count, width) + scatter_sems(n_shard),
            tokens, aux, w_qkv, w_out, w_gate_up, table,
        )
        resid_g, gate_up, mixed_b, output, d_down, grad_mlp = call(
            functools.partial(mlp_kernel, n_shard), "mlp", 3,
            [
                ((total, width), BF, ANY), ((total, 2 * ff), BF, ANY),
                ((total, ff), BF, ANY), ((count, width), BF, VM), ((count, width), BF, VM),
                ((1, width), F32, VM),
            ],
            [ANY, ANY, ANY, VM, VM, VM],
            [
                pltpu.VMEM((count, width), F32), pltpu.VMEM((1, width), F32),
                pltpu.VMEM((count, count), F32), gathered, pltpu.VMEM((width, 2 * ff), BF), pltpu.VMEM((ff, width), BF),
                pltpu.VMEM((total, 2 * ff), BF), pltpu.VMEM((total, ff), BF),
                DMA((3,)), DMA((chips,)), DMA((chips,)), DMA((chips,)),
            ] + scatter_bufs(n_shard, count, width) + scatter_sems(n_shard) + gather_sems(n_shard),
            resid_b, wg, w_down, auxg, resid, cotangent,
        )
        gu_sum, down_acc, d_resid, d_attn, norm_gains = call(
            functools.partial(mlp_back_kernel, n_shard, n_rep), "mlp_back", 4,
            [
                ((width // n_rep, 2 * ff), BF, ANY), ((ff, width), BF, ANY),
                ((count, width), F32, VM), ((count, width), BF, VM), ((n_shard, 8, own), F32, VM),
            ],
            [ANY] * 6 + [VM] * 5,
            [
                pltpu.VMEM((1, width), F32), pltpu.VMEM((1, width), F32),
                pltpu.VMEM((count, count), F32), gathered, pltpu.VMEM((width, 2 * ff), BF), pltpu.VMEM((ff, width), BF),
                pltpu.VMEM((total, 2 * ff), BF), pltpu.VMEM((total, 2 * ff), BF),
                gathered, pltpu.VMEM((total, ff), BF),
                pltpu.VMEM((ff, width), BF), DMA((5,)), DMA((chips,)), DMA((n_shard,)),
            ] + share_scratch(width, 2 * ff, n_shard, n_rep)
            + scatter_bufs(n_shard, count, width) + scatter_sems(n_shard) + gather_sems(n_shard),
            d_down, gate_up, wg, w_down, resid_g, mixed_b,
            auxg, cotangent, attn_hat, attn_scale, grad_mlp,
        )
        gu_rows, down_rows, out_rows, qkv_rows, gains, d_tokens_sum = call(
            functools.partial(attn_back_kernel, n_shard, n_rep, heads), "attn_back", 5,
            [
                ((own, n_shard * 2 * ff), BF, ANY), ((ff, width), BF, ANY), ((own, width), BF, ANY),
                ((own, 3 * width), BF, ANY), ((8, own), F32, VM), ((count, width), F32, VM),
            ],
            [ANY, ANY, VM, ANY, VM, VM, VM, VM, VM, VM, VM, VM, ANY, ANY],
            [
                gathered, gathered, pltpu.VMEM((width, 3 * own), BF), pltpu.VMEM((total, own), BF),
                pltpu.VMEM((total, 2 * own), F32), pltpu.VMEM((total, 3 * own), BF),
                pltpu.VMEM((2, total), F32),
                pltpu.VMEM((2, total), F32), pltpu.VMEM((chunk, 2, total), F32),
                pltpu.VMEM((chunk, 8, own), F32), pltpu.VMEM((8, own), F32),
                pltpu.VMEM((n_rep - 1, 8, own), F32),
                DMA((4,)), DMA((chunk,)), DMA((chunk,)), DMA((chunk,)), DMA((chunk,)),
                DMA((n_rep - 1,)), DMA((n_rep - 1,)),
            ] + gather_sems(n_shard) + scatter_bufs(n_shard, count, width) + scatter_sems(n_shard)
            + share_scratch(ff, width, 1, n_rep) + share_scratch(own, width, 1, n_rep)
            + share_scratch(width, 3 * own, n_shard, n_rep)
            + share_gather_sems(n_rep) * 2
            + rows_back_sems(n_shard, n_rep, 2) + rows_back_sems(n_shard, n_rep, 3),
            d_attn, tokens_g, w_out, wq, hats, rots, probs, context_b, auxg, squares,
            table, norm_gains, gu_sum, down_acc,
        )
        grad_tokens = d_resid + d_tokens_sum
        return (
            output, grad_tokens, qkv_rows.astype(F32), out_rows.astype(F32), gu_rows.astype(F32),
            down_rows.astype(F32), gains[2], gains[3], gains[0], gains[1],
        )

    return shards


def solution(mesh):
    rows = P(("rep", "shard"), None)
    return jax.shard_map(
        make(mesh.shape["rep"], mesh.shape["shard"]),
        mesh=mesh,
        in_specs=(rows, P(("rep", "shard")), rows)
        + (P("shard", None),) * 4
        + (P("shard"),) * 4,
        out_specs=(rows, rows) + (P("shard", None),) * 4 + (P("shard"),) * 4,
        check_vma=False,
    )
```

```python
import functools

import jax
import jax.numpy as jnp
import numpy as np
from jax import lax
from jax.experimental import pallas as pl
from jax.experimental.pallas import tpu as pltpu
from jax.sharding import PartitionSpec as P

H = 16
EPSILON = 1e-06
THETA = 500000.0
BF = jnp.bfloat16
F32 = jnp.float32
MESH = pl.DeviceIdType.MESH
DMA = pltpu.SemaphoreType.DMA
ANY = pl.BlockSpec(memory_space=pl.ANY)
VM = pl.BlockSpec(memory_space=pltpu.VMEM)
CHUNKS = 2
UNROLL = 2
VMEM_LIMIT = 62 << 20


def position(n_shard):
    s = lax.axis_index("shard")
    return s // 4, (s // 2) % 2, s % 2, n_shard // 4


def index(a, b, c):
    return (a * 2 + b) * 2 + c


def line_order(t, a, na):
    m = jnp.minimum(a, na - 1 - a)
    near = jnp.where(t % 2 == 1, a - (t + 1) // 2, a + (t + 1) // 2)
    far = jnp.where(m == a, t, na - 1 - t)
    return jnp.where(t <= 2 * m, near, far)


def peer(k, flip, sign):
    s = lax.axis_index("shard")
    na = lax.axis_size("shard") // 4
    a, b, c = s // 4, (s // 2) % 2, s % 2
    return index(lax.rem(a + na + sign * (k // 2), na), (b + flip) % 2, (c + k) % 2)


def rows_of(i, size):
    return pl.ds(pl.multiple_of(i * size, size), size)


def send(src, dst, ssem, rsem, **target):
    return pltpu.make_async_remote_copy(
        src_ref=src, dst_ref=dst, send_sem=ssem, recv_sem=rsem,
        device_id=target, device_id_type=MESH,
    )


def signal(sem, **target):
    pl.semaphore_signal(sem, inc=1, device_id=target, device_id_type=MESH)


def greet(pos):
    barrier = pltpu.get_barrier_semaphore()
    a, b, c, na = pos

    @pl.when(a > 0)
    def _():
        signal(barrier, shard=index(a - 1, b, c))

    @pl.when(a < na - 1)
    def _():
        signal(barrier, shard=index(a + 1, b, c))

    signal(barrier, shard=index(a, 1 - b, c))
    signal(barrier, shard=index(a, b, 1 - c))
    pl.semaphore_wait(barrier, 2 + (a > 0).astype(jnp.int32) + (a < na - 1).astype(jnp.int32))


def greet_all(n_shard, n_rep):
    barrier = pltpu.get_barrier_semaphore()
    s, r = lax.axis_index("shard"), lax.axis_index("rep")

    def one(k, _):
        signal(barrier, shard=lax.rem(s + k, n_shard))
        return 0

    lax.fori_loop(1, n_shard, one, 0)
    for k in range(1, n_rep):
        signal(barrier, rep=lax.rem(r + k, n_rep))
    pl.semaphore_wait(barrier, n_shard - 1 + n_rep - 1)


def gather_sems(n_shard):
    na = n_shard // 4
    return [
        DMA((n_shard * CHUNKS,)), DMA((na * CHUNKS,)), DMA((na * CHUNKS,)),
        DMA((na * CHUNKS,)), DMA((2 * na * CHUNKS,)),
    ]


def gather_loop(pos, count, buf, sems, on_chip, hook=None):
    recv, up, down, ysend, csend = sems
    a, b, c, na = pos
    rows = count // CHUNKS

    def desc(i, ch, ssem, target):
        piece = buf.at[pl.ds(pl.multiple_of(i * count + ch * rows, rows), rows)]
        return send(piece, piece, ssem, recv.at[i * CHUNKS + ch], shard=target)

    def sends(j, ch):
        i = index(j, b, c)

        @pl.when((j <= a) & (a < na - 1))
        def _():
            desc(i, ch, up.at[j * CHUNKS + ch], index(a + 1, b, c)).start()

        @pl.when((j >= a) & (a > 0))
        def _():
            desc(i, ch, down.at[j * CHUNKS + ch], index(a - 1, b, c)).start()

        desc(i, ch, ysend.at[j * CHUNKS + ch], index(a, 1 - b, c)).start()
        desc(i, ch, csend.at[(j * 2 + b) * CHUNKS + ch], index(a, b, 1 - c)).start()

    def arrived(i, ch):
        desc(i, ch, csend.at[0], index(a, b, 1 - c)).wait_recv()

    def pair_step(j, t):
        i = index(j, 1 - b, c)
        for ch in range(CHUNKS):
            arrived(i, ch)
            desc(i, ch, csend.at[(j * 2 + 1 - b) * CHUNKS + ch], index(a, b, 1 - c)).start()
        for ch in range(CHUNKS):
            arrived(index(j, 1 - b, 1 - c), ch)
        on_chip(j * 2 + 1 - b, t)

    def step(t, _):
        j = line_order(t, a, na)
        for ch in range(CHUNKS):

            @pl.when(t > 0)
            def _():
                arrived(index(j, b, c), ch)

            sends(j, ch)
        if hook is not None:
            hook(t)
        for ch in range(CHUNKS):
            arrived(index(j, b, 1 - c), ch)
        on_chip(j * 2 + b, t)

        @pl.when(t > 0)
        def _():
            pair_step(line_order(t - 1, a, na), t)

        return 0

    lax.fori_loop(0, na, step, 0)
    pair_step(line_order(na - 1, a, na), na)

    def finish(j, _):
        i = index(j, b, c)
        for ch in range(CHUNKS):

            @pl.when((j <= a) & (a < na - 1))
            def _():
                desc(i, ch, up.at[j * CHUNKS + ch], index(a, b, 1 - c)).wait_send()

            @pl.when((j >= a) & (a > 0))
            def _():
                desc(i, ch, down.at[j * CHUNKS + ch], index(a, b, 1 - c)).wait_send()

            desc(i, ch, ysend.at[j * CHUNKS + ch], index(a, 1 - b, c)).wait_send()
            for bb in range(2):
                slot = (j * 2 + bb) * CHUNKS + ch
                desc(index(j, bb, c), ch, csend.at[slot], index(a, b, 1 - c)).wait_send()
        return 0

    lax.fori_loop(0, na, finish, 0)


def scatter_sems(n_shard):
    na = n_shard // 4
    return [DMA((2 * na,)), DMA((2 * na,)), DMA((na,)), DMA((na,)), DMA((na,)), DMA((na + 1,))]


def scatter_bufs(n_shard, count, width):
    na = n_shard // 4
    return [
        pltpu.VMEM((n_shard * count, width), BF), pltpu.VMEM((2 * na * count, width), BF),
        pltpu.VMEM((na * count, width), BF), pltpu.VMEM(((na + 1) * count, width), BF),
    ]


def scatter_loop(pos, count, bufs, sems, partial, out, works=(), order=None):
    p, cgot, ygot, zgot = bufs
    csend, crecv, ysend, yrecv, zsend, zrecv = sems
    a, b, c, na = pos
    tile = 32

    def to_core(q):
        return send(
            p.at[rows_of(q * 2 + 1 - c, count)], cgot.at[rows_of(q, count)],
            csend.at[q], crecv.at[q], shard=index(a, b, 1 - c),
        )

    def to_pair(j):
        return send(
            p.at[rows_of(index(j, 1 - b, c), count)], ygot.at[rows_of(j, count)],
            ysend.at[j], yrecv.at[j], shard=index(a, 1 - b, c),
        )

    def along(j, slot, target):
        return send(
            p.at[rows_of(index(j, b, c), count)], zgot.at[rows_of(slot, count)],
            zsend.at[j], zrecv.at[slot], shard=target,
        )

    def add(i, others, into=None):
        def one(k, _):
            def at(slot):
                return pl.ds(pl.multiple_of(slot * count + k * tile, tile), tile)

            total = p[at(i), :].astype(F32)
            for ref, slot in others:
                total = total + ref[at(slot), :].astype(F32)
            if into is None:
                p[at(i), :] = total.astype(BF)
            else:
                into[at(0), :] = total
            return 0

        lax.fori_loop(0, count // tile, one, 0)

    def first(t, _):
        j = line_order(na - 1 - t, a, na)
        far, near = j * 2 + 1 - b, j * 2 + b
        partial(far)
        to_core(far).start()
        partial(near)
        to_core(near).start()
        to_core(far).wait_recv()
        add(index(j, 1 - b, c), [(cgot, far)])
        to_pair(j).start()
        return 0

    def second(t, _):
        j = line_order(na - 1 - t, a, na)
        near = j * 2 + b
        i = index(j, b, c)
        to_core(near).wait_recv()
        to_pair(j).wait_recv()
        inner = ((j < a) & (a < na - 1)) | ((j > a) & (a > 0))

        @pl.when(inner)
        def _():
            along(j, j, index(a, b, 1 - c)).wait_recv()
            add(i, [(cgot, near), (ygot, j), (zgot, j)])

        @pl.when(jnp.logical_not(inner))
        def _():
            add(i, [(cgot, near), (ygot, j)])

        @pl.when(j > a)
        def _():
            along(j, j, index(a + 1, b, c)).start()

        @pl.when(j < a)
        def _():
            along(j, jnp.where(j == a - 1, na, j), index(a - 1, b, c)).start()

        return 0

    if order is None:
        lax.fori_loop(0, na, first, 0)
        lax.fori_loop(0, na - 1, second, 0)
    else:
        done_first = done_second = 0
        for token in order:
            if token == "f":
                first(done_first, 0)
                done_first += 1
            elif token == "s":
                second(done_second, 0)
                done_second += 1
            else:
                works[int(token)]()
        assert done_first == na and done_second == na - 1
    near = a * 2 + b
    to_core(near).wait_recv()
    to_pair(a).wait_recv()
    add(index(a, b, c), [(cgot, near), (ygot, a)], out)

    def more(slot):
        along(a, slot, index(a, b, 1 - c)).wait_recv()

        def one(k, _):
            got = zgot[pl.ds(pl.multiple_of(slot * count + k * tile, tile), tile), :]
            out[rows_of(k, tile), :] += got.astype(F32)
            return 0

        lax.fori_loop(0, count // tile, one, 0)

    @pl.when(a > 0)
    def _():
        more(a)

    @pl.when(a < na - 1)
    def _():
        more(na)

    def finish(j, _):
        for bb in range(2):
            to_core(j * 2 + bb).wait_send()
        to_pair(j).wait_send()

        @pl.when(j != a)
        def _():
            along(j, j, index(a, b, 1 - c)).wait_send()

        return 0

    lax.fori_loop(0, na, finish, 0)


def columns_sems(n_shard, n_rep, groups):
    return [
        DMA((n_shard * groups,)), DMA((n_shard * groups,)),
        DMA((n_shard * n_rep,)), DMA((n_shard * n_rep,)), DMA((groups + 1,)),
    ]


class Columns:
    def __init__(self, w, out, stage, sems, groups, n_shard, n_rep):
        self.w, self.out, self.stage, self.groups = w, out, stage, groups
        self.ssem, self.rsem, self.fsend, self.frecv, self.lsem = sems
        self.n_shard, self.n_rep = n_shard, n_rep
        self.own = w.shape[0]
        self.share = self.own // n_rep
        self.total = w.shape[1] // groups
        self.width = self.total // n_shard
        self.s, self.r = lax.axis_index("shard"), lax.axis_index("rep")

    def move(self, source, target, g):
        cols = pl.ds(pl.multiple_of(g * self.total + target * self.width, 128), self.width)
        src = self.w.at[rows_of(self.r, self.share), cols]
        at = pl.ds(pl.multiple_of(source * self.own + self.r * self.share, self.share), self.share)
        dst = self.out.at[at, pl.ds(g * self.width, self.width)]
        return send(
            src, dst, self.ssem.at[target * self.groups + g],
            self.rsem.at[source * self.groups + g], shard=target,
        )

    def pass_on(self, source, k, replica):
        at = pl.ds(
            pl.multiple_of(source * self.own + replica * self.share, self.share), self.share
        )
        piece = self.out.at[at]
        return send(
            piece, piece, self.fsend.at[source * self.n_rep + k],
            self.frecv.at[source * self.n_rep + replica],
            rep=lax.rem(self.r + k, self.n_rep),
        )

    def local_in(self, g):
        cols = pl.ds(pl.multiple_of(g * self.total + self.s * self.width, 128), self.width)
        into = pl.ds(g * self.width, self.width)
        if self.stage is None:
            dst = self.out.at[rows_of(self.s, self.own), into]
        else:
            dst = self.stage.at[:, into]
        return pltpu.make_async_copy(self.w.at[:, cols], dst, self.lsem.at[g])

    def local_out(self):
        return pltpu.make_async_copy(
            self.stage, self.out.at[rows_of(self.s, self.own)], self.lsem.at[self.groups]
        )

    def start(self, flip, low, high):
        def one(k, _):
            for g in range(self.groups):
                self.move(self.s, peer(k, flip, 1), g).start()
            return 0

        lax.fori_loop(low, high, one, 0)

    def start_own(self):
        for g in range(self.groups):
            self.local_in(g).start()
        if self.stage is not None:
            for g in range(self.groups):
                self.local_in(g).wait()
            self.local_out().start()

    def forward(self, flip, low, high):
        def one(k, _):
            source = peer(k, flip, -1)
            for g in range(self.groups):
                self.move(source, self.s, g).wait_recv()
            for m in range(1, self.n_rep):
                self.pass_on(source, m, self.r).start()
            return 0

        lax.fori_loop(low, high, one, 0)

    def finish(self):
        def one(k, _):
            source = lax.rem(self.s + self.n_shard - k, self.n_shard)
            for g in range(self.groups):
                self.move(self.s, source, g).wait_send()
            for m in range(1, self.n_rep):
                self.pass_on(source, m, self.r).wait_send()
                self.pass_on(source, m, lax.rem(self.r + m, self.n_rep)).wait_recv()
            return 0

        lax.fori_loop(1, self.n_shard, one, 0)
        if self.stage is not None:
            self.local_out().wait()
        else:
            for g in range(self.groups):
                self.local_in(g).wait()


class ShareSum:
    def __init__(self, acc, got, sems, blocks, n_rep):
        self.acc, self.got, self.blocks, self.n_rep = acc, got, blocks, n_rep
        self.ssem, self.rsem = sems
        self.share = acc.shape[0] // (blocks * n_rep)
        self.r = lax.axis_index("rep")

    def part(self, block, replica):
        return rows_of(block * self.n_rep + replica, self.share)

    def desc(self, block, m):
        target = lax.rem(self.r + m, self.n_rep)
        slot = (m - 1) * self.blocks + block
        return send(
            self.acc.at[self.part(block, target)], self.got.at[rows_of(slot, self.share)],
            self.ssem.at[slot], self.rsem.at[slot], rep=target,
        )

    def start(self, block):
        for m in range(1, self.n_rep):
            self.desc(block, m).start()

    def add(self, block):
        for m in range(1, self.n_rep):
            self.desc(block, m).wait_recv()
        tile = min(self.share, 32)

        def one(k, _):
            at = pl.ds(
                pl.multiple_of((block * self.n_rep + self.r) * self.share + k * tile, tile), tile
            )
            total = self.acc[at, :].astype(F32)
            for m in range(1, self.n_rep):
                slot = (m - 1) * self.blocks + block
                total = total + self.got[
                    pl.ds(pl.multiple_of(slot * self.share + k * tile, tile), tile), :
                ].astype(F32)
            self.acc[at, :] = total.astype(BF)
            return 0

        lax.fori_loop(0, self.share // tile, one, 0)

    def sent(self, block):
        for m in range(1, self.n_rep):
            self.desc(block, m).wait_send()


def share_scratch(rows, cols, blocks, n_rep):
    return [
        pltpu.VMEM((rows, cols), BF), pltpu.VMEM(((n_rep - 1) * rows // n_rep, cols), BF),
        DMA(((n_rep - 1) * blocks,)), DMA(((n_rep - 1) * blocks,)),
    ]


class ShareGather:
    def __init__(self, src, out, sems, n_rep):
        self.src, self.out, self.n_rep = src, out, n_rep
        self.ssem, self.rsem, self.lsem = sems
        self.r = lax.axis_index("rep")
        self.share = out.shape[0] // n_rep

    def local(self):
        return pltpu.make_async_copy(self.src, self.out.at[rows_of(self.r, self.share)], self.lsem)

    def desc(self, m, replica):
        return send(
            self.src, self.out.at[rows_of(replica, self.share)],
            self.ssem.at[m - 1], self.rsem.at[replica], rep=lax.rem(self.r + m, self.n_rep),
        )

    def start(self):
        self.local().start()
        for m in range(1, self.n_rep):
            self.desc(m, self.r).start()

    def finish(self):
        self.local().wait()
        for m in range(1, self.n_rep):
            self.desc(m, self.r).wait_send()
            self.desc(m, lax.rem(self.r + m, self.n_rep)).wait_recv()


def share_gather_sems(n_rep):
    return [DMA((n_rep - 1,)), DMA((n_rep,)), DMA(())]


class RowsBack:
    def __init__(self, src, out, sems, groups, n_shard, n_rep):
        self.src, self.out, self.groups = src, out, groups
        self.ssem, self.rsem, self.fsend, self.frecv, self.lsem = sems
        self.n_shard, self.n_rep = n_shard, n_rep
        self.share = out.shape[0] // n_rep
        self.total = out.shape[1] // groups
        self.width = self.total // n_shard
        self.s, self.r = lax.axis_index("shard"), lax.axis_index("rep")

    def place(self, source, replica, g):
        cols = pl.ds(pl.multiple_of(g * self.total + source * self.width, 128), self.width)
        return self.out.at[rows_of(replica, self.share), cols]

    def piece(self, target, g):
        return self.src(target).at[:, pl.ds(g * self.width, self.width)]

    def move(self, source, target, g):
        return send(
            self.piece(target, g), self.place(source, self.r, g),
            self.ssem.at[target * self.groups + g], self.rsem.at[source * self.groups + g],
            shard=target,
        )

    def local(self, g):
        return pltpu.make_async_copy(
            self.piece(self.s, g), self.place(self.s, self.r, g), self.lsem.at[g]
        )

    def pass_on(self, source, m, replica, g):
        at = self.place(source, replica, g)
        return send(
            at, at, self.fsend.at[(source * self.n_rep + m) * self.groups + g],
            self.frecv.at[(source * self.n_rep + replica) * self.groups + g],
            rep=lax.rem(self.r + m, self.n_rep),
        )

    def start(self, flip, low, high):
        def one(k, _):
            for g in range(self.groups):
                self.move(self.s, peer(k, flip, 1), g).start()
            return 0

        lax.fori_loop(low, high, one, 0)

    def start_own(self):
        for g in range(self.groups):
            self.local(g).start()

    def relay(self, source):
        for g in range(self.groups):
            for m in range(1, self.n_rep):
                self.pass_on(source, m, self.r, g).start()

    def forward_own(self):
        for g in range(self.groups):
            self.local(g).wait()
        self.relay(self.s)

    def forward(self, flip, low, high):
        def one(k, _):
            source = peer(k, flip, -1)
            for g in range(self.groups):
                self.move(source, self.s, g).wait_recv()
            self.relay(source)
            return 0

        lax.fori_loop(low, high, one, 0)

    def finish(self):
        def one(k, _):
            source = lax.rem(self.s + self.n_shard - k, self.n_shard)
            for g in range(self.groups):

                @pl.when(k > 0)
                def _():
                    self.move(self.s, source, g).wait_send()

                for m in range(1, self.n_rep):
                    self.pass_on(source, m, self.r, g).wait_send()
                    self.pass_on(source, m, lax.rem(self.r + m, self.n_rep), g).wait_recv()
            return 0

        lax.fori_loop(0, self.n_shard, one, 0)


def rows_back_sems(n_shard, n_rep, groups):
    return [
        DMA((n_shard * groups,)), DMA((n_shard * groups,)),
        DMA((n_shard * n_rep * groups,)), DMA((n_shard * n_rep * groups,)), DMA((groups,)),
    ]


def mm(left, right):
    return jnp.dot(left, right, preferred_element_type=F32)


def mm_nt(left, right):
    return lax.dot_general(left, right, (((1,), (1,)), ((), ())), preferred_element_type=F32)


def mm_tn(left, right):
    return lax.dot_general(left, right, (((0,), (0,)), ((), ())), preferred_element_type=F32)


def call(kernel, name, cid, outs, ins, scratch, *args, flops=0, moved=0):
    return pl.pallas_call(
        kernel,
        name=name,
        out_shape=[jax.ShapeDtypeStruct(shape, dtype) for shape, dtype, _ in outs],
        in_specs=ins,
        out_specs=[spec for _, _, spec in outs],
        scratch_shapes=scratch,
        compiler_params=pltpu.CompilerParams(
            collective_id=cid, has_side_effects=True, vmem_limit_bytes=VMEM_LIMIT
        ),
        cost_estimate=pl.CostEstimate(flops=flops, bytes_accessed=moved, transcendentals=0),
    )(*args)


def load(src, dst, sem):
    cp = pltpu.make_async_copy(src, dst, sem)
    cp.start()
    return cp


def own_rows(pos, count):
    a, b, c, _ = pos
    return rows_of(index(a, b, c), count)


class Out:
    def __init__(self, src, dst, sem, size):
        self.src, self.dst, self.sem, self.size = src, dst, sem, size

    def desc(self, q):
        r = rows_of(q, self.size)
        return pltpu.make_async_copy(self.src.at[r], self.dst.at[r], self.sem.at[q])

    def start(self, q):
        self.desc(q).start()

    def wait(self, q):
        self.desc(q).wait()


def wait_all(outs, chips):
    def one(q, _):
        for o in outs:
            o.wait(q)
        return 0

    lax.fori_loop(0, chips, one, 0)


def turned(row, count):
    return jnp.transpose(jnp.broadcast_to(row, (count, count)))


def spots_of(seg_row, count):
    lane = lax.broadcasted_iota(jnp.int32, (count, count), 1).astype(F32)
    slot = lax.broadcasted_iota(jnp.int32, (count, count), 0).astype(F32)
    same = turned(seg_row, count) == seg_row
    first = jnp.min(jnp.where(same, lane, float(count)), axis=-1, keepdims=True)
    return same & (lane <= slot), slot[:, :1] - first


def swap_halves(x):
    return pltpu.roll(x, x.shape[1] // 2, 1)


def rope_of(spots, table):
    count = spots.shape[0]
    lane = lax.broadcasted_iota(jnp.int32, (count, count), 1)
    pick = jnp.where(lane.astype(F32) == spots, 1.0, 0.0).astype(BF)
    parts = mm(pick, table)
    n = parts.shape[1] // 3
    both = parts[:, :n] + parts[:, n : 2 * n] + parts[:, 2 * n :]
    return both[:, : n // 2], both[:, n // 2 :]


def row_sums(x):
    ones = jnp.ones((8, x.shape[1]), F32)
    return lax.dot_general(
        ones, x, (((1,), (1,)), ((), ())),
        preferred_element_type=F32, precision=lax.Precision.HIGHEST,
    )[:1]


def gain_rows(aux_ref, k, row):
    own = aux_ref.shape[2]
    for d in range(aux_ref.shape[0]):
        row[:, d * own : (d + 1) * own] = aux_ref[d, k : k + 1, :]


def norm_rows(rows, do):
    tile = 32

    def one(k, _):
        do(rows_of(k, tile))
        return 0

    lax.fori_loop(0, rows // tile, one, 0)


def row_scale(v):
    return lax.rsqrt(jnp.mean(v * v, axis=-1, keepdims=True) + EPSILON)


def norm_back(upstream, normed, rscale, gain):
    scaled = upstream * gain
    inner = jnp.mean(scaled * normed, axis=-1, keepdims=True)
    return rscale * (scaled - normed * inner)


def attn_kernel(
    n_shard, n_rep, heads,
    x_ref, aux_ref, wqkv_ref, wo_ref, wgu_ref, table_ref,
    g_ref, wq_ref, wg_ref, auxg_ref, sums_ref, hats_out, rot_out, prob_out, ctx_out,
    out_ref, scale_ref, resid_ref, residb_ref,
    hats_ref, rot_ref, prob_ref, ctx_ref, row, buf, wq, stage, qkv, stats, got, packed, lsem, osem, xs, xr, as_, ar, *rest,
):
    pos = position(n_shard)
    gsems, c3, c2, bufs, ssems = rest[:5], rest[5:10], rest[10:15], rest[15:19], rest[19:]
    p = bufs[0]
    count, width = out_ref.shape
    chips = n_shard // 2
    big = 2 * count
    own = wo_ref.shape[0]
    hw = own // heads
    na = pos[3]
    s = lax.axis_index("shard")
    mine = load(x_ref, buf.at[own_rows(pos, count)], lsem.at[0])
    qkv_w = Columns(wqkv_ref, wq, None, c3, 3, n_shard, n_rep)
    gu_w = Columns(wgu_ref, wg_ref, stage, c2, 2, n_shard, n_rep)
    auxg_ref[s] = aux_ref[...]
    greet_all(n_shard, n_rep)
    mine.wait()
    out_x = Out(buf, g_ref, osem, big)

    def aux_desc(k):
        target = lax.rem(s + k, n_shard)
        return send(aux_ref, auxg_ref.at[s], as_.at[k - 1], ar.at[k - 1], shard=target)

    def hook(t):
        @pl.when(t == 0)
        def _():
            qkv_w.start_own()
            gu_w.start_own()
            qkv_w.start(0, 1, half)
            qkv_w.start(1, 0, half)

            def one(k, _):
                aux_desc(k).start()
                return 0

            lax.fori_loop(1, n_shard, one, 0)

        @pl.when(t == na - 1)
        def _():
            gu_w.start(0, 1, half)
            qkv_w.forward(0, 1, half)
            qkv_w.forward(1, 0, half)

    half = n_shard // 2

    def project(q, _):
        r = rows_of(q, big)
        v = mm(buf[r, :], wq[...])
        qkv[r, :] = v
        for g in range(2):
            x = v[:, g * own : (g + 1) * own]
            stats[pl.ds(g, 1), pl.ds(pl.multiple_of(q * big, big), big)] = row_sums(x * x)

        @pl.when(q > 0)
        def _():
            gu_w.forward(0, q, q + 1)

        return 0

    gather_loop(pos, count, buf, gsems, lambda q, t: out_x.start(q), hook)
    qkv_w.finish()
    keep = load(wq, wq_ref, lsem.at[1])
    lax.fori_loop(0, chips, project, 0)
    packed[...] = stats[...].astype(BF)
    exchange_start(n_shard, packed, got, xs, xr)
    gu_w.start(1, 0, half)
    exchange_finish(n_shard, stats, packed, got, xs, xr, sums_ref)

    def aux_done(k, _):
        aux_desc(k).wait_recv()
        aux_desc(k).wait_send()
        return 0

    lax.fori_loop(1, n_shard, aux_done, 0)
    root = hw ** (-0.5)

    def attend(i, _):
        r = rows_of(i, count)
        at = pl.ds(pl.multiple_of(i * count, count), count)
        ok, spots = spots_of(auxg_ref[i, 0:1, :], count)
        cos, sin = rope_of(spots, table_ref[...])
        scale = lax.rsqrt(sums_ref[:, at] / width + EPSILON)
        q_scale = turned(scale[0:1], count)[:, :1]
        k_scale = turned(scale[1:2], count)[:, :1]
        for h in range(heads):
            def part(g):
                lo = g * own + h * hw
                return slice(lo, lo + hw)

            cols = slice(h * hw, (h + 1) * hw)

            def turn(g, scale, gain):
                hat = qkv[r, part(g)] * scale
                hats_ref[r, part(g)] = hat
                x = hat * gain
                x = (x * cos + swap_halves(x) * sin).astype(BF)
                rot_ref[r, part(g)] = x
                return x

            query = turn(0, q_scale, aux_ref[3:4, cols])
            keys = turn(1, k_scale, aux_ref[4:5, cols])
            values = qkv[r, part(2)].astype(BF)
            rot_ref[r, part(2)] = values
            scores = jnp.where(ok, mm_nt(query, keys) * root, -1e30)
            e = jnp.exp(scores - jnp.max(scores, axis=-1, keepdims=True))
            probs = e / jnp.sum(e, axis=-1, keepdims=True)
            prob_ref[r, h * count : (h + 1) * count] = probs
            ctx_ref[r, cols] = mm(probs.astype(BF), values).astype(BF)

        return 0

    lax.fori_loop(0, n_shard, attend, 0, unroll=UNROLL)
    kept = [
        load(hats_ref, hats_out, lsem.at[2]), load(rot_ref, rot_out, lsem.at[3]),
        load(prob_ref, prob_out, lsem.at[4]), load(ctx_ref, ctx_out, lsem.at[5]),
    ]

    def partial(q):
        r = rows_of(q, big)
        p[r, :] = mm(ctx_ref[r, :], wo_ref[...]).astype(BF)

    def pass_far(t):
        return lambda: gu_w.forward(1, half * t // 3, half * (t + 1) // 3)

    scatter_loop(
        pos, count, bufs, ssems, partial, out_ref, [pass_far(t) for t in range(3)],
        "f" * na + "0s1s2" + "s" * (na - 3),
    )
    gain_rows(auxg_ref, 1, row)

    def close(at):
        v = out_ref[at, :]
        scale = row_scale(v)
        hat = v * scale
        out_ref[at, :] = hat
        scale_ref[at, :] = jnp.broadcast_to(scale, (scale.shape[0], scale_ref.shape[1]))
        mine_at = pl.ds(pl.multiple_of(s * count + at.start, at.size), at.size)
        resid = buf[mine_at, :].astype(F32) + hat * row[...]
        resid_ref[at, :] = resid
        residb_ref[at, :] = resid.astype(BF)

    norm_rows(count, close)
    gu_w.finish()
    keep.wait()
    for cp in kept:
        cp.wait()
    wait_all([out_x], chips)


def exchange_desc(n_shard, stats, got, xs, xr, k):
    target = lax.rem(lax.axis_index("shard") + k, n_shard)
    return send(stats, got.at[k - 1], xs.at[k - 1], xr.at[k - 1], shard=target)


def exchange_start(n_shard, stats, got, xs, xr):
    def start(k, _):
        exchange_desc(n_shard, stats, got, xs, xr, k).start()
        return 0

    lax.fori_loop(1, n_shard, start, 0)


def exchange_finish(n_shard, stats, packed, got, xs, xr, sums):
    sums[...] = stats[...]

    def take(k, _):
        exchange_desc(n_shard, packed, got, xs, xr, k).wait_recv()
        sums[...] += got[k - 1].astype(F32)
        return 0

    lax.fori_loop(1, n_shard, take, 0)

    def done(k, _):
        exchange_desc(n_shard, packed, got, xs, xr, k).wait_send()
        return 0

    lax.fori_loop(1, n_shard, done, 0)


def live_rows(aux_ref, pos, mask):
    a, b, c, _ = pos
    segs = turned(aux_ref[index(a, b, c), 0:1, :], mask.shape[0])
    mask[...] = jnp.where(segs >= 0.0, 1.0, 0.0).astype(F32)


def mlp_kernel(
    n_shard, x_ref, wg_ref, wd_ref, aux_ref, resid_ref, cot_ref,
    g_ref, gu_ref, mixed_ref, y_ref, d_ref, gain_ref,
    out_ref, row, mask, buf, wg, wd, gu, mixed, lsem, osem, gsem, msem, *rest,
):
    pos = position(n_shard)
    bufs, ssems, gsems = rest[:4], rest[4:10], rest[10:]
    p = bufs[0]
    count, width = out_ref.shape
    big = 2 * count
    chips = n_shard // 2
    ff = wd.shape[0]
    mine = load(x_ref, buf.at[own_rows(pos, count)], lsem.at[0])
    w1 = load(wg_ref, wg, lsem.at[1])
    w2 = load(wd_ref, wd, lsem.at[2])
    greet(pos)
    mine.wait()
    out_x, out_g = Out(buf, g_ref, osem, big), Out(gu, gu_ref, gsem, big)
    out_m = Out(mixed, mixed_ref, msem, big)
    w1.wait()

    def on_chip(q, t):
        r = rows_of(q, big)
        out_x.start(q)

        def one(k, _):
            lo = pl.ds(pl.multiple_of(k * 256, 256), 256)
            hi = pl.ds(pl.multiple_of(ff + k * 256, 256), 256)
            gate = mm(buf[r, :], wg[:, lo])
            up = mm(buf[r, :], wg[:, hi])
            gu[r, lo] = gate.astype(BF)
            gu[r, hi] = up.astype(BF)
            mixed[r, lo] = (gate * jax.nn.sigmoid(gate) * up).astype(BF)
            return 0

        lax.fori_loop(0, ff // 256, one, 0)
        out_g.start(q)
        out_m.start(q)

    gather_loop(pos, count, buf, gsems, on_chip)
    w2.wait()

    def partial(q):
        r = rows_of(q, big)

        def one(k, _):
            lo = rows_of(k, 512)
            p[r, lo] = mm(mixed[r, :], wd[:, lo]).astype(BF)
            return 0

        lax.fori_loop(0, width // 512, one, 0)

    gain_rows(aux_ref, 2, row)
    live_rows(aux_ref, pos, mask)
    scatter_loop(pos, count, bufs, ssems, partial, out_ref)
    gain_ref[...] = jnp.zeros_like(gain_ref)

    def close(at):
        v = out_ref[at, :]
        scale = row_scale(v)
        hat = v * scale
        y_ref[at, :] = (resid_ref[at, :] + hat * row[...]).astype(BF)
        d_out = cot_ref[at, :].astype(F32) * mask[at, :1]
        gain_ref[...] += jnp.sum(d_out * hat, axis=0, keepdims=True)
        d_ref[at, :] = norm_back(d_out, hat, scale, row[...]).astype(BF)

    norm_rows(count, close)
    wait_all([out_x, out_g, out_m], chips)


def mlp_back_kernel(
    n_shard, n_rep, x_ref, gu_ref, wg_ref, wd_ref, resid_ref, mixed_ref,
    aux_ref, cot_ref, hat_ref, scale_ref, mlp_gain_ref,
    gsum_ref, down_ref, out_ref, d_ref, gain_ref,
    row, sums, mask, buf, wg, wd, gu, dgu, resid, mixed, down, lsem, isem, osem, acc, got, xs, xr, *rest,
):
    pos = position(n_shard)
    na = pos[3]
    bufs, ssems, gsems = rest[:4], rest[4:10], rest[10:]
    p = bufs[0]
    count, width = out_ref.shape
    big = 2 * count
    chips = n_shard // 2
    ff = wd.shape[0]
    own = width // n_shard
    share = own // n_rep
    mine = load(x_ref, buf.at[own_rows(pos, count)], lsem.at[0])
    w2 = load(wd_ref, wd, lsem.at[2])
    saved = Out(gu_ref, gu, isem, big)

    def fetch(q, _):
        saved.start(q)
        return 0

    lax.fori_loop(0, chips, fetch, 0)
    w1 = load(wg_ref, wg, lsem.at[1])
    in_r = load(resid_ref, resid, lsem.at[3])
    in_m = load(mixed_ref, mixed, lsem.at[4])
    greet_all(n_shard, n_rep)
    mine.wait()
    w2.wait()

    def on_chip(q, t):
        r = rows_of(q, big)
        saved.wait(q)

        def one(k, _):
            lo = pl.ds(pl.multiple_of(k * 256, 256), 256)
            hi = pl.ds(pl.multiple_of(ff + k * 256, 256), 256)
            d_mixed = mm_nt(buf[r, :], wd[lo, :])
            gate, up = gu[r, lo].astype(F32), gu[r, hi].astype(F32)
            sigma = jax.nn.sigmoid(gate)
            d_gate = d_mixed * up * sigma * (1.0 + gate * (1.0 - sigma))
            dgu[r, lo] = d_gate.astype(BF)
            dgu[r, hi] = (d_mixed * gate * sigma).astype(BF)
            return 0

        lax.fori_loop(0, ff // 256, one, 0)

    gather_loop(pos, count, buf, gsems, on_chip)
    w1.wait()
    in_r.wait()
    in_m.wait()

    def partial(q):
        r = rows_of(q, big)

        def one(k, _):
            lo = rows_of(k, 512)
            p[r, lo] = mm_nt(dgu[r, :], wg[lo, :]).astype(BF)
            return 0

        lax.fori_loop(0, width // 512, one, 0)

    shares = ShareSum(acc, got, (xs, xr), n_shard, n_rep)
    owners = 4
    most = owners * own
    parts = width // most

    def grad_rows(k):
        at = rows_of(k, most)

        def one(n, _):
            lo = rows_of(n, 256)
            acc[at, lo] = mm_tn(resid[:, at], dgu[:, lo]).astype(BF)
            return 0

        lax.fori_loop(0, 2 * ff // 256, one, 0)
        for d in range(owners):
            shares.start(k * owners + d)

    def grad_down():
        def rows(m, _):
            at = rows_of(m, most)

            def one(n, _):
                lo = rows_of(n, 256)
                down[at, lo] = mm_tn(mixed[:, at], buf[:, lo]).astype(BF)
                return 0

            lax.fori_loop(0, width // 256, one, 0)
            return 0

        lax.fori_loop(0, ff // most, rows, 0)
        load(down, down_ref, lsem.at[3])

    def chunk(t):
        def run():
            def one(k, _):
                grad_rows(k)
                return 0

            lax.fori_loop(parts * t // 4, parts * (t + 1) // 4, one, 0)

        return run

    scatter_loop(
        pos, count, bufs, ssems, partial, out_ref, [chunk(t) for t in range(4)] + [grad_down],
        "0ff1" + "f" * (na - 2) + "s2s3" + "s" * (na - 3) + "4",
    )

    gain_rows(aux_ref, 1, row)
    live_rows(aux_ref, pos, mask)
    sums[...] = jnp.zeros_like(sums)

    def close(at):
        d_resid = cot_ref[at, :].astype(F32) * mask[at, :1] + out_ref[at, :]
        out_ref[at, :] = d_resid
        hat = hat_ref[at, :]
        sums[...] += jnp.sum(d_resid * hat, axis=0, keepdims=True)
        d_ref[at, :] = norm_back(d_resid, hat, scale_ref[at, :1], row[...]).astype(BF)

    norm_rows(count, close)
    gain_ref[...] = jnp.zeros_like(gain_ref)
    for d in range(n_shard):
        cols = slice(d * own, (d + 1) * own)
        gain_ref[d, 0:1, :] = sums[:, cols]
        gain_ref[d, 1:2, :] = mlp_gain_ref[:, cols]

    def collect(d, _):
        shares.add(d)
        pltpu.make_async_copy(
            acc.at[shares.part(d, shares.r)], gsum_ref.at[rows_of(d, share)], osem.at[d]
        ).start()
        return 0

    lax.fori_loop(0, n_shard, collect, 0)

    def end(d, _):
        shares.sent(d)
        pltpu.make_async_copy(
            acc.at[shares.part(d, shares.r)], gsum_ref.at[rows_of(d, share)], osem.at[d]
        ).wait()
        return 0

    lax.fori_loop(0, n_shard, end, 0)
    pltpu.make_async_copy(down, down_ref, lsem.at[3]).wait()


def attn_back_kernel(
    n_shard, n_rep, heads,
    x_ref, tok_ref, wo_ref, wq_ref, hats_in, rot_in, prob_in, ctx_in, aux_ref, sums_ref,
    table_ref, gain_ref, gsum_ref, down_ref,
    gu_ref, dn_ref, go_ref, gq_ref, gains_ref, out_ref,
    hats_ref, rot_ref, prob_ref, ctx_ref, buf, tok, wq, dctx, ups, dqkv, stats, inner, got, packed, ggot, mine_g, rgot, lsem, xs, xr, gs, gr, rs, rr, *rest,
):
    rest = list(rest)

    def take(n):
        out = rest[:n]
        del rest[:n]
        return out

    pos = position(n_shard)
    na = pos[3]
    gsems, bufs, ssems = take(5), take(4), take(6)
    dacc, dgot, *dsems = take(4)
    oacc, ogot, *osems = take(4)
    qacc, qgot, *qsems = take(4)
    dgsems, ogsems, gusems, qksems = take(3), take(3), take(5), take(5)
    p = bufs[0]
    count, width = out_ref.shape
    big = 2 * count
    own = wo_ref.shape[0]
    hw = own // heads
    r_me = lax.axis_index("rep")
    mine = load(x_ref, buf.at[own_rows(pos, count)], lsem.at[0])
    in_d = load(down_ref, dacc, lsem.at[1])
    kept = [
        load(hats_in, hats_ref, lsem.at[4]), load(rot_in, rot_ref, lsem.at[5]),
        load(prob_in, prob_ref, lsem.at[6]), load(ctx_in, ctx_ref, lsem.at[7]),
    ]
    in_t = load(tok_ref, tok, lsem.at[2])
    in_w = load(wq_ref, wq, lsem.at[3])
    share = own // n_rep
    gu_rows = RowsBack(lambda d: gsum_ref.at[rows_of(d, share)], gu_ref, gusems, 2, n_shard, n_rep)
    down = ShareSum(dacc, dgot, dsems, 1, n_rep)
    down_all = ShareGather(dacc.at[down.part(0, r_me)], dn_ref, dgsems, n_rep)
    wout = ShareSum(oacc, ogot, osems, 1, n_rep)
    wout_all = ShareGather(oacc.at[wout.part(0, r_me)], go_ref, ogsems, n_rep)
    wqkv = ShareSum(qacc, qgot, qsems, n_shard, n_rep)
    wqkv_rows = RowsBack(
        lambda d: qacc.at[wqkv.part(d, r_me)], gq_ref, qksems, 3, n_shard, n_rep
    )
    greet_all(n_shard, n_rep)
    mine.wait()

    def hook(t):
        @pl.when(t == 0)
        def _():
            gu_rows.start_own()
            in_d.wait()
            down.start(0)

            def one(k, _):
                gain_desc(k).start()
                return 0

            lax.fori_loop(1, n_shard, one, 0)

        @pl.when(t == na - 2)
        def _():
            down.add(0)
            down_all.start()

        @pl.when(t == na - 1)
        def _():
            gu_rows.start(0, 1, half)
            gu_rows.forward_own()

    half = n_shard // 2

    def gain_desc(k):
        target = lax.rem(lax.axis_index("shard") + k, n_shard)
        return send(gain_ref.at[target], ggot.at[k - 1], gs.at[k - 1], gr.at[k - 1], shard=target)

    def gain_rep(m):
        target = lax.rem(r_me + m, n_rep)
        return send(mine_g, rgot.at[m - 1], rs.at[m - 1], rr.at[m - 1], rep=target)

    def on_chip(q, t):
        r = rows_of(q, big)
        dctx[r, :] = mm_nt(buf[r, :], wo_ref[...]).astype(BF)

    gather_loop(pos, count, buf, gsems, on_chip, hook)
    early = half * 5 // 8
    gu_rows.start(1, 0, early)
    root = hw ** (-0.5)
    me = lax.axis_index("shard")
    mine_g[...] = gain_ref[me]
    for cp in kept:
        cp.wait()

    def scale_of(i):
        at = pl.ds(pl.multiple_of(i * count, count), count)
        return lax.rsqrt(sums_ref[:, at] / width + EPSILON)

    def attend(i, _):
        r = rows_of(i, count)
        at = pl.ds(pl.multiple_of(i * count, count), count)
        cos, sin = rope_of(spots_of(aux_ref[i, 0:1, :], count)[1], table_ref[...])
        totals = [jnp.zeros((1, count), F32), jnp.zeros((1, count), F32)]
        for h in range(heads):
            def part(g):
                lo = g * own + h * hw
                return slice(lo, lo + hw)

            cols = slice(h * hw, (h + 1) * hw)
            query, keys, values = rot_ref[r, part(0)], rot_ref[r, part(1)], rot_ref[r, part(2)]
            probs = prob_ref[r, h * count : (h + 1) * count]
            probs_b = probs.astype(BF)
            d_ctx = dctx[r, cols]
            d_values = mm_tn(probs_b, d_ctx)
            d_probs = mm_nt(d_ctx, values)
            delta = jnp.sum(probs_b.astype(F32) * d_probs, axis=-1, keepdims=True)
            d_scores = (probs * (d_probs - delta) * root).astype(BF)
            d_query = mm(d_scores, keys)
            d_keys = mm_tn(d_scores, query)
            dqkv[r, part(2)] = d_values.astype(BF)
            for g, x in enumerate((d_query, d_keys)):
                x = x * cos - swap_halves(x) * sin
                hat = hats_ref[r, part(g)]
                mine_g[2 + g : 3 + g, cols] += jnp.sum(x * hat, axis=0, keepdims=True)
                up = x * aux_ref[me, 3 + g : 4 + g, cols]
                ups[r, part(g)] = up
                totals[g] = totals[g] + row_sums(up * hat)
        for g in range(2):
            stats[pl.ds(g, 1), at] = totals[g]

        @pl.when((i > 0) & (i < half))
        def _():
            gu_rows.forward(0, i, i + 1)

        return 0

    lax.fori_loop(0, n_shard, attend, 0, unroll=UNROLL)
    packed[...] = stats[...].astype(BF)
    exchange_start(n_shard, packed, got, xs, xr)
    gu_rows.start(1, early, half)

    def out_cols(n, _):
        lo = rows_of(n, 256)
        oacc[:, lo] = mm_tn(ctx_ref[...], buf[:, lo]).astype(BF)
        return 0

    lax.fori_loop(0, width // 256, out_cols, 0)
    wout.start(0)

    def gain_take(k, _):
        gain_desc(k).wait_recv()
        mine_g[...] += ggot[k - 1]
        return 0

    lax.fori_loop(1, n_shard, gain_take, 0)
    for m in range(1, n_rep):
        gain_rep(m).start()
    exchange_finish(n_shard, stats, packed, got, xs, xr, inner)

    def settle(i, _):
        r = rows_of(i, count)
        at = pl.ds(pl.multiple_of(i * count, count), count)
        scale = scale_of(i)
        mean = inner[:, at] / width
        for g in range(2):
            lo = slice(g * own, (g + 1) * own)
            column = turned(scale[g : g + 1], count)[:, :1]
            down_by = turned(mean[g : g + 1], count)[:, :1]
            dqkv[r, lo] = (column * (ups[r, lo] - hats_ref[r, lo] * down_by)).astype(BF)
        return 0

    lax.fori_loop(0, n_shard, settle, 0)
    in_w.wait()
    in_t.wait()

    def partial(q):
        r = rows_of(q, big)

        def one(k, _):
            lo = rows_of(k, 512)
            p[r, lo] = mm_nt(dqkv[r, :], wq[lo, :]).astype(BF)
            return 0

        lax.fori_loop(0, width // 512, one, 0)

    most = 4 * own

    def grad_rows(k, _):
        at = rows_of(k, most)
        qacc[at, :] = mm_tn(tok[:, at], dqkv[...]).astype(BF)
        return 0

    def near_far(do, flip):
        def one(k, _):
            do(peer(k, flip, 1))
            return 0

        lax.fori_loop(0, half, one, 0)

    def work0():
        lax.fori_loop(0, width // most, grad_rows, 0)
        near_far(wqkv.start, 0)
        near_far(wqkv.start, 1)

    def work1():
        gu_rows.forward(1, 0, half)

    def work2():
        wout.add(0)
        wout_all.start()

    def work3():
        near_far(wqkv.add, 0)
        wqkv_rows.start_own()
        wqkv_rows.start(0, 1, half)

    def work4():
        near_far(wqkv.add, 1)
        wqkv_rows.start(1, 0, half)

    def work5():
        wqkv_rows.forward_own()
        wqkv_rows.forward(0, 1, half)

    def work6():
        wqkv_rows.forward(1, 0, half)

    scatter_loop(
        pos, count, bufs, ssems, partial, out_ref, [work0, work1, work2, work3, work4, work5, work6],
        "ff0" + "f" * (na - 2) + "12s3s45" + "s" * (na - 3) + "6",
    )

    def end(d, _):
        wqkv.sent(d)
        return 0

    lax.fori_loop(0, n_shard, end, 0)
    down.sent(0)
    wout.sent(0)

    def gain_sent(k, _):
        gain_desc(k).wait_send()
        return 0

    lax.fori_loop(1, n_shard, gain_sent, 0)
    gains_ref[...] = mine_g[...]
    for m in range(1, n_rep):
        gain_rep(m).wait_recv()
        gains_ref[...] += rgot[m - 1]
    for m in range(1, n_rep):
        gain_rep(m).wait_send()
    wqkv_rows.finish()
    gu_rows.finish()
    down_all.finish()
    wout_all.finish()


def rope_table(count, head_width):
    half_width = head_width // 2
    inverse = np.float32(THETA) ** (-(np.float32(2.0) * np.arange(half_width, dtype=np.float32)) / np.float32(head_width))
    angle = np.arange(count, dtype=np.float32)[:, None] * inverse[None, :].astype(np.float32)
    cosine, sine = np.cos(angle), np.sin(angle)
    rest = np.concatenate([cosine, cosine, -sine, sine], axis=1).astype(np.float32)
    parts = []
    for _ in range(3):
        parts.append(rest.astype(BF))
        rest = rest - parts[-1].astype(np.float32)
    return np.concatenate(parts, axis=1)


def make(n_rep, n_shard):
    chips = n_shard // 2

    def shards(
        tokens, segment_ids, cotangent, w_qkv, w_out, w_gate_up, w_down,
        q_gain, k_gain, attn_gain, mlp_gain,
    ):
        count, width = tokens.shape
        heads = H // n_shard
        hw = width // H
        own = width // n_shard
        ff = w_down.shape[0]
        total = count * n_shard
        gathered = pltpu.VMEM((total, width), BF)

        assert own == count
        aux = jnp.stack(
            [x.astype(F32) for x in (segment_ids, attn_gain, mlp_gain, q_gain, k_gain)]
            + [jnp.zeros((count,), F32)] * 3
        )
        table = jnp.asarray(rope_table(count, hw))
        chunk = n_shard - 1
        saved = [
            pltpu.VMEM((total, 2 * own), F32), pltpu.VMEM((total, 3 * own), BF),
            pltpu.VMEM((total, heads * count), F32), pltpu.VMEM((total, own), BF),
        ]
        (
            tokens_g, wq, wg, auxg, squares, hats, rots, probs, context_b,
            attn_hat, attn_scale, resid, resid_b,
        ) = call(
            functools.partial(attn_kernel, n_shard, n_rep, heads), "attn", 1,
            [
                ((total, width), BF, ANY), ((width, 3 * own), BF, ANY), ((width, 2 * ff), BF, ANY),
                ((n_shard, 8, count), F32, VM), ((2, total), F32, VM), ((total, 2 * own), F32, ANY),
                ((total, 3 * own), BF, ANY), ((total, heads * count), F32, ANY),
                ((total, own), BF, ANY), ((count, width), F32, VM), ((count, 128), F32, VM),
                ((count, width), F32, VM), ((count, width), BF, VM),
            ],
            [ANY, VM, ANY, VM, ANY, VM],
            saved + [
                pltpu.VMEM((1, width), F32), gathered, pltpu.VMEM((width, 3 * own), BF), pltpu.VMEM((own, 2 * ff), BF),
                pltpu.VMEM((total, 3 * own), F32), pltpu.VMEM((2, total), F32),
                pltpu.VMEM((chunk, 2, total), BF), pltpu.VMEM((2, total), BF),
                DMA((6,)), DMA((chips,)), DMA((chunk,)), DMA((chunk,)), DMA((chunk,)), DMA((chunk,)),
            ] + gather_sems(n_shard) + columns_sems(n_shard, n_rep, 3)
            + columns_sems(n_shard, n_rep, 2)
            + scatter_bufs(n_shard, count, width) + scatter_sems(n_shard),
            tokens, aux, w_qkv, w_out, w_gate_up, table,
        )
        resid_g, gate_up, mixed_b, output, d_down, grad_mlp = call(
            functools.partial(mlp_kernel, n_shard), "mlp", 3,
            [
                ((total, width), BF, ANY), ((total, 2 * ff), BF, ANY),
                ((total, ff), BF, ANY), ((count, width), BF, VM), ((count, width), BF, VM),
                ((1, width), F32, VM),
            ],
            [ANY, ANY, ANY, VM, VM, VM],
            [
                pltpu.VMEM((count, width), F32), pltpu.VMEM((1, width), F32),
                pltpu.VMEM((count, count), F32), gathered, pltpu.VMEM((width, 2 * ff), BF), pltpu.VMEM((ff, width), BF),
                pltpu.VMEM((total, 2 * ff), BF), pltpu.VMEM((total, ff), BF),
                DMA((3,)), DMA((chips,)), DMA((chips,)), DMA((chips,)),
            ] + scatter_bufs(n_shard, count, width) + scatter_sems(n_shard) + gather_sems(n_shard),
            resid_b, wg, w_down, auxg, resid, cotangent,
        )
        gu_sum, down_acc, d_resid, d_attn, norm_gains = call(
            functools.partial(mlp_back_kernel, n_shard, n_rep), "mlp_back", 4,
            [
                ((width // n_rep, 2 * ff), BF, ANY), ((ff, width), BF, ANY),
                ((count, width), F32, VM), ((count, width), BF, VM), ((n_shard, 8, own), F32, VM),
            ],
            [ANY] * 6 + [VM] * 5,
            [
                pltpu.VMEM((1, width), F32), pltpu.VMEM((1, width), F32),
                pltpu.VMEM((count, count), F32), gathered, pltpu.VMEM((width, 2 * ff), BF), pltpu.VMEM((ff, width), BF),
                pltpu.VMEM((total, 2 * ff), BF), pltpu.VMEM((total, 2 * ff), BF),
                gathered, pltpu.VMEM((total, ff), BF),
                pltpu.VMEM((ff, width), BF), DMA((5,)), DMA((chips,)), DMA((n_shard,)),
            ] + share_scratch(width, 2 * ff, n_shard, n_rep)
            + scatter_bufs(n_shard, count, width) + scatter_sems(n_shard) + gather_sems(n_shard),
            d_down, gate_up, wg, w_down, resid_g, mixed_b,
            auxg, cotangent, attn_hat, attn_scale, grad_mlp,
        )
        gu_rows, down_rows, out_rows, qkv_rows, gains, d_tokens_sum = call(
            functools.partial(attn_back_kernel, n_shard, n_rep, heads), "attn_back", 5,
            [
                ((own, n_shard * 2 * ff), BF, ANY), ((ff, width), BF, ANY), ((own, width), BF, ANY),
                ((own, 3 * width), BF, ANY), ((8, own), F32, VM), ((count, width), F32, VM),
            ],
            [ANY, ANY, VM, ANY, ANY, ANY, ANY, ANY, VM, VM, VM, VM, ANY, ANY],
            saved + [
                gathered, gathered, pltpu.VMEM((width, 3 * own), BF), pltpu.VMEM((total, own), BF),
                pltpu.VMEM((total, 2 * own), F32), pltpu.VMEM((total, 3 * own), BF),
                pltpu.VMEM((2, total), F32),
                pltpu.VMEM((2, total), F32), pltpu.VMEM((chunk, 2, total), BF),
                pltpu.VMEM((2, total), BF), pltpu.VMEM((chunk, 8, own), F32), pltpu.VMEM((8, own), F32),
                pltpu.VMEM((n_rep - 1, 8, own), F32),
                DMA((8,)), DMA((chunk,)), DMA((chunk,)), DMA((chunk,)), DMA((chunk,)),
                DMA((n_rep - 1,)), DMA((n_rep - 1,)),
            ] + gather_sems(n_shard) + scatter_bufs(n_shard, count, width) + scatter_sems(n_shard)
            + share_scratch(ff, width, 1, n_rep) + share_scratch(own, width, 1, n_rep)
            + share_scratch(width, 3 * own, n_shard, n_rep)
            + share_gather_sems(n_rep) * 2
            + rows_back_sems(n_shard, n_rep, 2) + rows_back_sems(n_shard, n_rep, 3),
            d_attn, tokens_g, w_out, wq, hats, rots, probs, context_b, auxg, squares,
            table, norm_gains, gu_sum, down_acc,
        )
        grad_tokens = d_resid + d_tokens_sum
        return (
            output, grad_tokens, qkv_rows.astype(F32), out_rows.astype(F32), gu_rows.astype(F32),
            down_rows.astype(F32), gains[2], gains[3], gains[0], gains[1],
        )

    return shards


def solution(mesh):
    rows = P(("rep", "shard"), None)
    return jax.shard_map(
        make(mesh.shape["rep"], mesh.shape["shard"]),
        mesh=mesh,
        in_specs=(rows, P(("rep", "shard")), rows)
        + (P("shard", None),) * 4
        + (P("shard"),) * 4,
        out_specs=(rows, rows) + (P("shard", None),) * 4 + (P("shard"),) * 4,
        check_vma=False,
    )
```

```python
import functools

import jax
import jax.numpy as jnp
import numpy as np
from jax import lax
from jax.experimental import pallas as pl
from jax.experimental.pallas import tpu as pltpu
from jax.sharding import PartitionSpec as P

H = 16
EPSILON = 1e-06
THETA = 500000.0
BF = jnp.bfloat16
F32 = jnp.float32
MESH = pl.DeviceIdType.MESH
DMA = pltpu.SemaphoreType.DMA
ANY = pl.BlockSpec(memory_space=pl.ANY)
VM = pl.BlockSpec(memory_space=pltpu.VMEM)
CHUNKS = 2
UNROLL = 2
VMEM_LIMIT = 62 << 20


def position(n_shard):
    s = lax.axis_index("shard")
    return s // 4, (s // 2) % 2, s % 2, n_shard // 4


def index(a, b, c):
    return (a * 2 + b) * 2 + c


def line_order(t, a, na):
    m = jnp.minimum(a, na - 1 - a)
    near = jnp.where(t % 2 == 1, a - (t + 1) // 2, a + (t + 1) // 2)
    far = jnp.where(m == a, t, na - 1 - t)
    return jnp.where(t <= 2 * m, near, far)


def peer(k, flip, sign):
    s = lax.axis_index("shard")
    na = lax.axis_size("shard") // 4
    a, b, c = s // 4, (s // 2) % 2, s % 2
    return index(lax.rem(a + na + sign * (k // 2), na), (b + flip) % 2, (c + k) % 2)


def rows_of(i, size):
    return pl.ds(pl.multiple_of(i * size, size), size)


def send(src, dst, ssem, rsem, **target):
    return pltpu.make_async_remote_copy(
        src_ref=src, dst_ref=dst, send_sem=ssem, recv_sem=rsem,
        device_id=target, device_id_type=MESH,
    )


def signal(sem, **target):
    pl.semaphore_signal(sem, inc=1, device_id=target, device_id_type=MESH)


def greet(pos):
    barrier = pltpu.get_barrier_semaphore()
    a, b, c, na = pos

    @pl.when(a > 0)
    def _():
        signal(barrier, shard=index(a - 1, b, c))

    @pl.when(a < na - 1)
    def _():
        signal(barrier, shard=index(a + 1, b, c))

    signal(barrier, shard=index(a, 1 - b, c))
    signal(barrier, shard=index(a, b, 1 - c))
    pl.semaphore_wait(barrier, 2 + (a > 0).astype(jnp.int32) + (a < na - 1).astype(jnp.int32))


def greet_all(n_shard, n_rep):
    barrier = pltpu.get_barrier_semaphore()
    s, r = lax.axis_index("shard"), lax.axis_index("rep")

    def one(k, _):
        signal(barrier, shard=lax.rem(s + k, n_shard))
        return 0

    lax.fori_loop(1, n_shard, one, 0)
    for k in range(1, n_rep):
        signal(barrier, rep=lax.rem(r + k, n_rep))
    pl.semaphore_wait(barrier, n_shard - 1 + n_rep - 1)


def gather_sems(n_shard):
    na = n_shard // 4
    return [
        DMA((n_shard * CHUNKS,)), DMA((na * CHUNKS,)), DMA((na * CHUNKS,)),
        DMA((na * CHUNKS,)), DMA((2 * na * CHUNKS,)),
    ]


def gather_loop(pos, count, buf, sems, on_chip, hook=None, late=None):
    recv, up, down, ysend, csend = sems
    a, b, c, na = pos
    rows = count // CHUNKS

    def desc(i, ch, ssem, target):
        piece = buf.at[pl.ds(pl.multiple_of(i * count + ch * rows, rows), rows)]
        return send(piece, piece, ssem, recv.at[i * CHUNKS + ch], shard=target)

    def sends(j, ch):
        i = index(j, b, c)

        @pl.when((j <= a) & (a < na - 1))
        def _():
            desc(i, ch, up.at[j * CHUNKS + ch], index(a + 1, b, c)).start()

        @pl.when((j >= a) & (a > 0))
        def _():
            desc(i, ch, down.at[j * CHUNKS + ch], index(a - 1, b, c)).start()

        desc(i, ch, ysend.at[j * CHUNKS + ch], index(a, 1 - b, c)).start()
        desc(i, ch, csend.at[(j * 2 + b) * CHUNKS + ch], index(a, b, 1 - c)).start()

    def arrived(i, ch):
        desc(i, ch, csend.at[0], index(a, b, 1 - c)).wait_recv()

    def pair_step(j, t):
        i = index(j, 1 - b, c)
        for ch in range(CHUNKS):
            arrived(i, ch)
            desc(i, ch, csend.at[(j * 2 + 1 - b) * CHUNKS + ch], index(a, b, 1 - c)).start()
        for ch in range(CHUNKS):
            arrived(index(j, 1 - b, 1 - c), ch)
        on_chip(j * 2 + 1 - b, t)

    def step(t, _):
        j = line_order(t, a, na)
        for ch in range(CHUNKS):

            @pl.when(t > 0)
            def _():
                arrived(index(j, b, c), ch)

            sends(j, ch)
        if hook is not None:
            hook(t)
        for ch in range(CHUNKS):
            arrived(index(j, b, 1 - c), ch)
        on_chip(j * 2 + b, t)

        @pl.when(t > 0)
        def _():
            pair_step(line_order(t - 1, a, na), t)

        return 0

    lax.fori_loop(0, na, step, 0)
    if late is not None:
        late()
    pair_step(line_order(na - 1, a, na), na)

    def finish(j, _):
        i = index(j, b, c)
        for ch in range(CHUNKS):

            @pl.when((j <= a) & (a < na - 1))
            def _():
                desc(i, ch, up.at[j * CHUNKS + ch], index(a, b, 1 - c)).wait_send()

            @pl.when((j >= a) & (a > 0))
            def _():
                desc(i, ch, down.at[j * CHUNKS + ch], index(a, b, 1 - c)).wait_send()

            desc(i, ch, ysend.at[j * CHUNKS + ch], index(a, 1 - b, c)).wait_send()
            for bb in range(2):
                slot = (j * 2 + bb) * CHUNKS + ch
                desc(index(j, bb, c), ch, csend.at[slot], index(a, b, 1 - c)).wait_send()
        return 0

    lax.fori_loop(0, na, finish, 0)


def scatter_sems(n_shard):
    na = n_shard // 4
    return [DMA((2 * na,)), DMA((2 * na,)), DMA((na,)), DMA((na,)), DMA((na,)), DMA((na + 1,))]


def scatter_bufs(n_shard, count, width):
    na = n_shard // 4
    return [
        pltpu.VMEM((n_shard * count, width), BF), pltpu.VMEM((2 * na * count, width), BF),
        pltpu.VMEM((na * count, width), BF), pltpu.VMEM(((na + 1) * count, width), BF),
    ]


def scatter_loop(pos, count, bufs, sems, partial, out, works=(), order=None):
    p, cgot, ygot, zgot = bufs
    csend, crecv, ysend, yrecv, zsend, zrecv = sems
    a, b, c, na = pos
    tile = 32

    def to_core(q):
        return send(
            p.at[rows_of(q * 2 + 1 - c, count)], cgot.at[rows_of(q, count)],
            csend.at[q], crecv.at[q], shard=index(a, b, 1 - c),
        )

    def to_pair(j):
        return send(
            p.at[rows_of(index(j, 1 - b, c), count)], ygot.at[rows_of(j, count)],
            ysend.at[j], yrecv.at[j], shard=index(a, 1 - b, c),
        )

    def along(j, slot, target):
        return send(
            p.at[rows_of(index(j, b, c), count)], zgot.at[rows_of(slot, count)],
            zsend.at[j], zrecv.at[slot], shard=target,
        )

    def add(i, others, into=None):
        def one(k, _):
            def at(slot):
                return pl.ds(pl.multiple_of(slot * count + k * tile, tile), tile)

            total = p[at(i), :].astype(F32)
            for ref, slot in others:
                total = total + ref[at(slot), :].astype(F32)
            if into is None:
                p[at(i), :] = total.astype(BF)
            else:
                into[at(0), :] = total
            return 0

        lax.fori_loop(0, count // tile, one, 0)

    def first(t, _):
        j = line_order(na - 1 - t, a, na)
        far, near = j * 2 + 1 - b, j * 2 + b
        partial(far)
        to_core(far).start()
        partial(near)
        to_core(near).start()
        to_core(far).wait_recv()
        add(index(j, 1 - b, c), [(cgot, far)])
        to_pair(j).start()
        return 0

    def second(t, _):
        j = line_order(na - 1 - t, a, na)
        near = j * 2 + b
        i = index(j, b, c)
        to_core(near).wait_recv()
        to_pair(j).wait_recv()
        inner = ((j < a) & (a < na - 1)) | ((j > a) & (a > 0))

        @pl.when(inner)
        def _():
            along(j, j, index(a, b, 1 - c)).wait_recv()
            add(i, [(cgot, near), (ygot, j), (zgot, j)])

        @pl.when(jnp.logical_not(inner))
        def _():
            add(i, [(cgot, near), (ygot, j)])

        @pl.when(j > a)
        def _():
            along(j, j, index(a + 1, b, c)).start()

        @pl.when(j < a)
        def _():
            along(j, jnp.where(j == a - 1, na, j), index(a - 1, b, c)).start()

        return 0

    if order is None:
        lax.fori_loop(0, na, first, 0)
        lax.fori_loop(0, na - 1, second, 0)
    else:
        done_first = done_second = 0
        for token in order:
            if token == "f":
                first(done_first, 0)
                done_first += 1
            elif token == "s":
                second(done_second, 0)
                done_second += 1
            else:
                works[int(token)]()
        assert done_first == na and done_second == na - 1
    near = a * 2 + b
    to_core(near).wait_recv()
    to_pair(a).wait_recv()
    add(index(a, b, c), [(cgot, near), (ygot, a)], out)

    def more(slot):
        along(a, slot, index(a, b, 1 - c)).wait_recv()

        def one(k, _):
            got = zgot[pl.ds(pl.multiple_of(slot * count + k * tile, tile), tile), :]
            out[rows_of(k, tile), :] += got.astype(F32)
            return 0

        lax.fori_loop(0, count // tile, one, 0)

    @pl.when(a > 0)
    def _():
        more(a)

    @pl.when(a < na - 1)
    def _():
        more(na)

    def finish(j, _):
        for bb in range(2):
            to_core(j * 2 + bb).wait_send()
        to_pair(j).wait_send()

        @pl.when(j != a)
        def _():
            along(j, j, index(a, b, 1 - c)).wait_send()

        return 0

    lax.fori_loop(0, na, finish, 0)


def columns_sems(n_shard, n_rep, groups):
    return [
        DMA((n_shard * groups,)), DMA((n_shard * groups,)),
        DMA((n_shard * n_rep,)), DMA((n_shard * n_rep,)), DMA((groups + 1,)),
    ]


class Columns:
    def __init__(self, w, out, stage, sems, groups, n_shard, n_rep):
        self.w, self.out, self.stage, self.groups = w, out, stage, groups
        self.ssem, self.rsem, self.fsend, self.frecv, self.lsem = sems
        self.n_shard, self.n_rep = n_shard, n_rep
        self.own = w.shape[0]
        self.share = self.own // n_rep
        self.total = w.shape[1] // groups
        self.width = self.total // n_shard
        self.s, self.r = lax.axis_index("shard"), lax.axis_index("rep")

    def move(self, source, target, g):
        cols = pl.ds(pl.multiple_of(g * self.total + target * self.width, 128), self.width)
        src = self.w.at[rows_of(self.r, self.share), cols]
        at = pl.ds(pl.multiple_of(source * self.own + self.r * self.share, self.share), self.share)
        dst = self.out.at[at, pl.ds(g * self.width, self.width)]
        return send(
            src, dst, self.ssem.at[target * self.groups + g],
            self.rsem.at[source * self.groups + g], shard=target,
        )

    def pass_on(self, source, k, replica):
        at = pl.ds(
            pl.multiple_of(source * self.own + replica * self.share, self.share), self.share
        )
        piece = self.out.at[at]
        return send(
            piece, piece, self.fsend.at[source * self.n_rep + k],
            self.frecv.at[source * self.n_rep + replica],
            rep=lax.rem(self.r + k, self.n_rep),
        )

    def local_in(self, g):
        cols = pl.ds(pl.multiple_of(g * self.total + self.s * self.width, 128), self.width)
        into = pl.ds(g * self.width, self.width)
        if self.stage is None:
            dst = self.out.at[rows_of(self.s, self.own), into]
        else:
            dst = self.stage.at[:, into]
        return pltpu.make_async_copy(self.w.at[:, cols], dst, self.lsem.at[g])

    def local_out(self):
        return pltpu.make_async_copy(
            self.stage, self.out.at[rows_of(self.s, self.own)], self.lsem.at[self.groups]
        )

    def start(self, flip, low, high):
        def one(k, _):
            for g in range(self.groups):
                self.move(self.s, peer(k, flip, 1), g).start()
            return 0

        lax.fori_loop(low, high, one, 0)

    def start_own(self):
        for g in range(self.groups):
            self.local_in(g).start()
        if self.stage is not None:
            for g in range(self.groups):
                self.local_in(g).wait()
            self.local_out().start()

    def forward(self, flip, low, high):
        def one(k, _):
            source = peer(k, flip, -1)
            for g in range(self.groups):
                self.move(source, self.s, g).wait_recv()
            for m in range(1, self.n_rep):
                self.pass_on(source, m, self.r).start()
            return 0

        lax.fori_loop(low, high, one, 0)

    def finish(self):
        def one(k, _):
            source = lax.rem(self.s + self.n_shard - k, self.n_shard)
            for g in range(self.groups):
                self.move(self.s, source, g).wait_send()
            for m in range(1, self.n_rep):
                self.pass_on(source, m, self.r).wait_send()
                self.pass_on(source, m, lax.rem(self.r + m, self.n_rep)).wait_recv()
            return 0

        lax.fori_loop(1, self.n_shard, one, 0)
        if self.stage is not None:
            self.local_out().wait()
        else:
            for g in range(self.groups):
                self.local_in(g).wait()


class ShareSum:
    def __init__(self, acc, got, sems, blocks, n_rep):
        self.acc, self.got, self.blocks, self.n_rep = acc, got, blocks, n_rep
        self.ssem, self.rsem = sems
        self.share = acc.shape[0] // (blocks * n_rep)
        self.r = lax.axis_index("rep")

    def part(self, block, replica):
        return rows_of(block * self.n_rep + replica, self.share)

    def desc(self, block, m):
        target = lax.rem(self.r + m, self.n_rep)
        slot = (m - 1) * self.blocks + block
        return send(
            self.acc.at[self.part(block, target)], self.got.at[rows_of(slot, self.share)],
            self.ssem.at[slot], self.rsem.at[slot], rep=target,
        )

    def start(self, block):
        for m in range(1, self.n_rep):
            self.desc(block, m).start()

    def add(self, block):
        for m in range(1, self.n_rep):
            self.desc(block, m).wait_recv()
        tile = min(self.share, 32)

        def one(k, _):
            at = pl.ds(
                pl.multiple_of((block * self.n_rep + self.r) * self.share + k * tile, tile), tile
            )
            total = self.acc[at, :].astype(F32)
            for m in range(1, self.n_rep):
                slot = (m - 1) * self.blocks + block
                total = total + self.got[
                    pl.ds(pl.multiple_of(slot * self.share + k * tile, tile), tile), :
                ].astype(F32)
            self.acc[at, :] = total.astype(BF)
            return 0

        lax.fori_loop(0, self.share // tile, one, 0)

    def sent(self, block):
        for m in range(1, self.n_rep):
            self.desc(block, m).wait_send()


def share_scratch(rows, cols, blocks, n_rep):
    return [
        pltpu.VMEM((rows, cols), BF), pltpu.VMEM(((n_rep - 1) * rows // n_rep, cols), BF),
        DMA(((n_rep - 1) * blocks,)), DMA(((n_rep - 1) * blocks,)),
    ]


class ShareGather:
    def __init__(self, src, out, sems, n_rep):
        self.src, self.out, self.n_rep = src, out, n_rep
        self.ssem, self.rsem, self.lsem = sems
        self.r = lax.axis_index("rep")
        self.share = out.shape[0] // n_rep

    def local(self):
        return pltpu.make_async_copy(self.src, self.out.at[rows_of(self.r, self.share)], self.lsem)

    def desc(self, m, replica):
        return send(
            self.src, self.out.at[rows_of(replica, self.share)],
            self.ssem.at[m - 1], self.rsem.at[replica], rep=lax.rem(self.r + m, self.n_rep),
        )

    def start(self):
        self.local().start()
        for m in range(1, self.n_rep):
            self.desc(m, self.r).start()

    def finish(self):
        self.local().wait()
        for m in range(1, self.n_rep):
            self.desc(m, self.r).wait_send()
            self.desc(m, lax.rem(self.r + m, self.n_rep)).wait_recv()


def share_gather_sems(n_rep):
    return [DMA((n_rep - 1,)), DMA((n_rep,)), DMA(())]


class RowsBack:
    def __init__(self, src, out, sems, groups, n_shard, n_rep):
        self.src, self.out, self.groups = src, out, groups
        self.ssem, self.rsem, self.fsend, self.frecv, self.lsem = sems
        self.n_shard, self.n_rep = n_shard, n_rep
        self.share = out.shape[0] // n_rep
        self.total = out.shape[1] // groups
        self.width = self.total // n_shard
        self.s, self.r = lax.axis_index("shard"), lax.axis_index("rep")

    def place(self, source, replica, g):
        cols = pl.ds(pl.multiple_of(g * self.total + source * self.width, 128), self.width)
        return self.out.at[rows_of(replica, self.share), cols]

    def piece(self, target, g):
        return self.src(target).at[:, pl.ds(g * self.width, self.width)]

    def move(self, source, target, g):
        return send(
            self.piece(target, g), self.place(source, self.r, g),
            self.ssem.at[target * self.groups + g], self.rsem.at[source * self.groups + g],
            shard=target,
        )

    def local(self, g):
        return pltpu.make_async_copy(
            self.piece(self.s, g), self.place(self.s, self.r, g), self.lsem.at[g]
        )

    def pass_on(self, source, m, replica, g):
        at = self.place(source, replica, g)
        return send(
            at, at, self.fsend.at[(source * self.n_rep + m) * self.groups + g],
            self.frecv.at[(source * self.n_rep + replica) * self.groups + g],
            rep=lax.rem(self.r + m, self.n_rep),
        )

    def start(self, flip, low, high):
        def one(k, _):
            for g in range(self.groups):
                self.move(self.s, peer(k, flip, 1), g).start()
            return 0

        lax.fori_loop(low, high, one, 0)

    def start_own(self):
        for g in range(self.groups):
            self.local(g).start()

    def relay(self, source):
        for g in range(self.groups):
            for m in range(1, self.n_rep):
                self.pass_on(source, m, self.r, g).start()

    def forward_own(self):
        for g in range(self.groups):
            self.local(g).wait()
        self.relay(self.s)

    def forward(self, flip, low, high):
        def one(k, _):
            source = peer(k, flip, -1)
            for g in range(self.groups):
                self.move(source, self.s, g).wait_recv()
            self.relay(source)
            return 0

        lax.fori_loop(low, high, one, 0)

    def finish(self):
        def one(k, _):
            source = lax.rem(self.s + self.n_shard - k, self.n_shard)
            for g in range(self.groups):

                @pl.when(k > 0)
                def _():
                    self.move(self.s, source, g).wait_send()

                for m in range(1, self.n_rep):
                    self.pass_on(source, m, self.r, g).wait_send()
                    self.pass_on(source, m, lax.rem(self.r + m, self.n_rep), g).wait_recv()
            return 0

        lax.fori_loop(0, self.n_shard, one, 0)


def rows_back_sems(n_shard, n_rep, groups):
    return [
        DMA((n_shard * groups,)), DMA((n_shard * groups,)),
        DMA((n_shard * n_rep * groups,)), DMA((n_shard * n_rep * groups,)), DMA((groups,)),
    ]


def mm(left, right):
    return jnp.dot(left, right, preferred_element_type=F32)


def mm_nt(left, right):
    return lax.dot_general(left, right, (((1,), (1,)), ((), ())), preferred_element_type=F32)


def mm_tn(left, right):
    return lax.dot_general(left, right, (((0,), (0,)), ((), ())), preferred_element_type=F32)


def call(kernel, name, cid, outs, ins, scratch, *args, flops=0, moved=0):
    return pl.pallas_call(
        kernel,
        name=name,
        out_shape=[jax.ShapeDtypeStruct(shape, dtype) for shape, dtype, _ in outs],
        in_specs=ins,
        out_specs=[spec for _, _, spec in outs],
        scratch_shapes=scratch,
        compiler_params=pltpu.CompilerParams(
            collective_id=cid, has_side_effects=True, vmem_limit_bytes=VMEM_LIMIT
        ),
        cost_estimate=pl.CostEstimate(flops=flops, bytes_accessed=moved, transcendentals=0),
    )(*args)


def load(src, dst, sem):
    cp = pltpu.make_async_copy(src, dst, sem)
    cp.start()
    return cp


def own_rows(pos, count):
    a, b, c, _ = pos
    return rows_of(index(a, b, c), count)


class Out:
    def __init__(self, src, dst, sem, size):
        self.src, self.dst, self.sem, self.size = src, dst, sem, size

    def desc(self, q):
        r = rows_of(q, self.size)
        return pltpu.make_async_copy(self.src.at[r], self.dst.at[r], self.sem.at[q])

    def start(self, q):
        self.desc(q).start()

    def wait(self, q):
        self.desc(q).wait()


def wait_all(outs, chips):
    def one(q, _):
        for o in outs:
            o.wait(q)
        return 0

    lax.fori_loop(0, chips, one, 0)


def turned(row, count):
    return jnp.transpose(jnp.broadcast_to(row, (count, count)))


def spots_of(seg_row, count):
    lane = lax.broadcasted_iota(jnp.int32, (count, count), 1).astype(F32)
    slot = lax.broadcasted_iota(jnp.int32, (count, count), 0).astype(F32)
    same = turned(seg_row, count) == seg_row
    first = jnp.min(jnp.where(same, lane, float(count)), axis=-1, keepdims=True)
    return same & (lane <= slot), slot[:, :1] - first


def swap_halves(x):
    return pltpu.roll(x, x.shape[1] // 2, 1)


def rope_of(spots, table):
    count = spots.shape[0]
    lane = lax.broadcasted_iota(jnp.int32, (count, count), 1)
    pick = jnp.where(lane.astype(F32) == spots, 1.0, 0.0).astype(BF)
    parts = mm(pick, table)
    n = parts.shape[1] // 3
    both = parts[:, :n] + parts[:, n : 2 * n] + parts[:, 2 * n :]
    return both[:, : n // 2], both[:, n // 2 :]


def row_sums(x):
    ones = jnp.ones((8, x.shape[1]), F32)
    return lax.dot_general(
        ones, x, (((1,), (1,)), ((), ())),
        preferred_element_type=F32, precision=lax.Precision.HIGHEST,
    )[:1]


def gain_rows(aux_ref, k, row):
    own = aux_ref.shape[2]
    for d in range(aux_ref.shape[0]):
        row[:, d * own : (d + 1) * own] = aux_ref[d, k : k + 1, :]


def norm_rows(rows, do):
    tile = 32

    def one(k, _):
        do(rows_of(k, tile))
        return 0

    lax.fori_loop(0, rows // tile, one, 0)


def row_scale(v):
    return lax.rsqrt(jnp.mean(v * v, axis=-1, keepdims=True) + EPSILON)


def norm_back(upstream, normed, rscale, gain):
    scaled = upstream * gain
    inner = jnp.mean(scaled * normed, axis=-1, keepdims=True)
    return rscale * (scaled - normed * inner)


def attn_kernel(
    n_shard, n_rep, heads,
    x_ref, aux_ref, wqkv_ref, wo_ref, wgu_ref, table_ref,
    g_ref, wq_ref, wg_ref, auxg_ref, sums_ref, hats_out, rot_out, prob_out, ctx_out,
    out_ref, scale_ref, resid_ref, residb_ref,
    hats_ref, rot_ref, prob_ref, ctx_ref, row, buf, wq, stage, qkv, stats, got, packed, lsem, osem, xs, xr, as_, ar, *rest,
):
    pos = position(n_shard)
    gsems, c3, c2, bufs, ssems = rest[:5], rest[5:10], rest[10:15], rest[15:19], rest[19:]
    p = bufs[0]
    count, width = out_ref.shape
    chips = n_shard // 2
    big = 2 * count
    own = wo_ref.shape[0]
    hw = own // heads
    na = pos[3]
    s = lax.axis_index("shard")
    mine = load(x_ref, buf.at[own_rows(pos, count)], lsem.at[0])
    qkv_w = Columns(wqkv_ref, wq, None, c3, 3, n_shard, n_rep)
    gu_w = Columns(wgu_ref, wg_ref, stage, c2, 2, n_shard, n_rep)
    auxg_ref[s] = aux_ref[...]
    greet_all(n_shard, n_rep)
    mine.wait()
    out_x = Out(buf, g_ref, osem, big)

    def aux_desc(k):
        target = lax.rem(s + k, n_shard)
        return send(aux_ref, auxg_ref.at[s], as_.at[k - 1], ar.at[k - 1], shard=target)

    def hook(t):
        @pl.when(t == 0)
        def _():
            qkv_w.start_own()
            gu_w.start_own()
            qkv_w.start(0, 1, half)
            qkv_w.start(1, 0, half)

            def one(k, _):
                aux_desc(k).start()
                return 0

            lax.fori_loop(1, n_shard, one, 0)

        @pl.when(t == na - 2)
        def _():
            qkv_w.forward(0, 1, half)
            qkv_w.forward(1, 0, half)

        @pl.when(t == na - 1)
        def _():
            gu_w.start(0, 1, half)

    half = n_shard // 2

    def project(q):
        r = rows_of(q, big)
        v = mm(buf[r, :], wq[...])
        qkv[r, :] = v
        for g in range(2):
            x = v[:, g * own : (g + 1) * own]
            stats[pl.ds(g, 1), pl.ds(pl.multiple_of(q * big, big), big)] = row_sums(x * x)


    a, b = pos[:2]

    def late():
        qkv_w.finish()

        def there(u, _):
            project(line_order(u, a, na) * 2 + b)

            @pl.when(u < na - 1)
            def _():
                project(line_order(u, a, na) * 2 + 1 - b)

            return 0

        lax.fori_loop(0, na, there, 0)

    gather_loop(pos, count, buf, gsems, lambda q, t: out_x.start(q), hook, late)
    keep = load(wq, wq_ref, lsem.at[1])
    project(line_order(na - 1, a, na) * 2 + 1 - b)
    packed[...] = stats[...].astype(BF)
    exchange_start(n_shard, packed, got, xs, xr)
    gu_w.start(1, 0, half)
    gu_w.forward(0, 1, half)
    exchange_finish(n_shard, stats, packed, got, xs, xr, sums_ref)

    def aux_done(k, _):
        aux_desc(k).wait_recv()
        aux_desc(k).wait_send()
        return 0

    lax.fori_loop(1, n_shard, aux_done, 0)
    root = hw ** (-0.5)

    def attend(i, _):
        r = rows_of(i, count)
        at = pl.ds(pl.multiple_of(i * count, count), count)
        ok, spots = spots_of(auxg_ref[i, 0:1, :], count)
        cos, sin = rope_of(spots, table_ref[...])
        scale = lax.rsqrt(sums_ref[:, at] / width + EPSILON)
        q_scale = turned(scale[0:1], count)[:, :1]
        k_scale = turned(scale[1:2], count)[:, :1]
        for h in range(heads):
            def part(g):
                lo = g * own + h * hw
                return slice(lo, lo + hw)

            cols = slice(h * hw, (h + 1) * hw)

            def turn(g, scale, gain):
                hat = qkv[r, part(g)] * scale
                hats_ref[r, part(g)] = hat
                x = hat * gain
                x = (x * cos + swap_halves(x) * sin).astype(BF)
                rot_ref[r, part(g)] = x
                return x

            query = turn(0, q_scale, aux_ref[3:4, cols])
            keys = turn(1, k_scale, aux_ref[4:5, cols])
            values = qkv[r, part(2)].astype(BF)
            rot_ref[r, part(2)] = values
            scores = jnp.where(ok, mm_nt(query, keys) * root, -1e30)
            e = jnp.exp(scores - jnp.max(scores, axis=-1, keepdims=True))
            probs = e / jnp.sum(e, axis=-1, keepdims=True)
            prob_ref[r, h * count : (h + 1) * count] = probs
            ctx_ref[r, cols] = mm(probs.astype(BF), values).astype(BF)

        return 0

    lax.fori_loop(0, n_shard, attend, 0, unroll=UNROLL)
    kept = [
        load(hats_ref, hats_out, lsem.at[2]), load(rot_ref, rot_out, lsem.at[3]),
        load(prob_ref, prob_out, lsem.at[4]), load(ctx_ref, ctx_out, lsem.at[5]),
    ]

    def partial(q):
        r = rows_of(q, big)
        p[r, :] = mm(ctx_ref[r, :], wo_ref[...]).astype(BF)

    def pass_far(t):
        return lambda: gu_w.forward(1, half * t // 3, half * (t + 1) // 3)

    scatter_loop(
        pos, count, bufs, ssems, partial, out_ref, [pass_far(t) for t in range(3)],
        "f" * na + "0s1s2" + "s" * (na - 3),
    )
    gain_rows(auxg_ref, 1, row)

    def close(at):
        v = out_ref[at, :]
        scale = row_scale(v)
        hat = v * scale
        out_ref[at, :] = hat
        scale_ref[at, :] = jnp.broadcast_to(scale, (scale.shape[0], scale_ref.shape[1]))
        mine_at = pl.ds(pl.multiple_of(s * count + at.start, at.size), at.size)
        resid = buf[mine_at, :].astype(F32) + hat * row[...]
        resid_ref[at, :] = resid
        residb_ref[at, :] = resid.astype(BF)

    norm_rows(count, close)
    gu_w.finish()
    keep.wait()
    for cp in kept:
        cp.wait()
    wait_all([out_x], chips)


def exchange_desc(n_shard, stats, got, xs, xr, k):
    target = lax.rem(lax.axis_index("shard") + k, n_shard)
    return send(stats, got.at[k - 1], xs.at[k - 1], xr.at[k - 1], shard=target)


def exchange_start(n_shard, stats, got, xs, xr):
    def start(k, _):
        exchange_desc(n_shard, stats, got, xs, xr, k).start()
        return 0

    lax.fori_loop(1, n_shard, start, 0)


def exchange_finish(n_shard, stats, packed, got, xs, xr, sums):
    sums[...] = stats[...]

    def take(k, _):
        exchange_desc(n_shard, packed, got, xs, xr, k).wait_recv()
        sums[...] += got[k - 1].astype(F32)
        return 0

    lax.fori_loop(1, n_shard, take, 0)

    def done(k, _):
        exchange_desc(n_shard, packed, got, xs, xr, k).wait_send()
        return 0

    lax.fori_loop(1, n_shard, done, 0)


def live_rows(aux_ref, pos, mask):
    a, b, c, _ = pos
    segs = turned(aux_ref[index(a, b, c), 0:1, :], mask.shape[0])
    mask[...] = jnp.where(segs >= 0.0, 1.0, 0.0).astype(F32)


def mlp_kernel(
    n_shard, x_ref, wg_ref, wd_ref, aux_ref, resid_ref, cot_ref,
    g_ref, gu_ref, mixed_ref, y_ref, d_ref, gain_ref,
    out_ref, row, mask, buf, wg, wd, gu, mixed, lsem, osem, gsem, msem, *rest,
):
    pos = position(n_shard)
    bufs, ssems, gsems = rest[:4], rest[4:10], rest[10:]
    p = bufs[0]
    count, width = out_ref.shape
    big = 2 * count
    chips = n_shard // 2
    ff = wd.shape[0]
    mine = load(x_ref, buf.at[own_rows(pos, count)], lsem.at[0])
    w1 = load(wg_ref, wg, lsem.at[1])
    w2 = load(wd_ref, wd, lsem.at[2])
    greet(pos)
    mine.wait()
    out_x, out_g = Out(buf, g_ref, osem, big), Out(gu, gu_ref, gsem, big)
    out_m = Out(mixed, mixed_ref, msem, big)
    w1.wait()

    def on_chip(q, t):
        r = rows_of(q, big)
        out_x.start(q)

        def one(k, _):
            lo = pl.ds(pl.multiple_of(k * 256, 256), 256)
            hi = pl.ds(pl.multiple_of(ff + k * 256, 256), 256)
            gate = mm(buf[r, :], wg[:, lo])
            up = mm(buf[r, :], wg[:, hi])
            gu[r, lo] = gate.astype(BF)
            gu[r, hi] = up.astype(BF)
            mixed[r, lo] = (gate * jax.nn.sigmoid(gate) * up).astype(BF)
            return 0

        lax.fori_loop(0, ff // 256, one, 0)
        out_g.start(q)
        out_m.start(q)

    gather_loop(pos, count, buf, gsems, on_chip)
    w2.wait()

    def partial(q):
        r = rows_of(q, big)

        def one(k, _):
            lo = rows_of(k, 512)
            p[r, lo] = mm(mixed[r, :], wd[:, lo]).astype(BF)
            return 0

        lax.fori_loop(0, width // 512, one, 0)

    gain_rows(aux_ref, 2, row)
    live_rows(aux_ref, pos, mask)
    scatter_loop(pos, count, bufs, ssems, partial, out_ref)
    gain_ref[...] = jnp.zeros_like(gain_ref)

    def close(at):
        v = out_ref[at, :]
        scale = row_scale(v)
        hat = v * scale
        y_ref[at, :] = (resid_ref[at, :] + hat * row[...]).astype(BF)
        d_out = cot_ref[at, :].astype(F32) * mask[at, :1]
        gain_ref[...] += jnp.sum(d_out * hat, axis=0, keepdims=True)
        d_ref[at, :] = norm_back(d_out, hat, scale, row[...]).astype(BF)

    norm_rows(count, close)
    wait_all([out_x, out_g, out_m], chips)


def mlp_back_kernel(
    n_shard, n_rep, x_ref, gu_ref, wg_ref, wd_ref, resid_ref, mixed_ref,
    aux_ref, cot_ref, hat_ref, scale_ref, mlp_gain_ref,
    gsum_ref, down_ref, out_ref, d_ref, gain_ref,
    row, sums, mask, buf, wg, wd, gu, dgu, resid, mixed, down, lsem, isem, osem, acc, got, xs, xr, *rest,
):
    pos = position(n_shard)
    na = pos[3]
    bufs, ssems, gsems = rest[:4], rest[4:10], rest[10:]
    p = bufs[0]
    count, width = out_ref.shape
    big = 2 * count
    chips = n_shard // 2
    ff = wd.shape[0]
    own = width // n_shard
    share = own // n_rep
    mine = load(x_ref, buf.at[own_rows(pos, count)], lsem.at[0])
    w2 = load(wd_ref, wd, lsem.at[2])
    saved = Out(gu_ref, gu, isem, big)

    def fetch(q, _):
        saved.start(q)
        return 0

    lax.fori_loop(0, chips, fetch, 0)
    w1 = load(wg_ref, wg, lsem.at[1])
    in_r = load(resid_ref, resid, lsem.at[3])
    in_m = load(mixed_ref, mixed, lsem.at[4])
    greet_all(n_shard, n_rep)
    mine.wait()
    w2.wait()

    def on_chip(q, t):
        r = rows_of(q, big)
        saved.wait(q)

        def one(k, _):
            lo = pl.ds(pl.multiple_of(k * 256, 256), 256)
            hi = pl.ds(pl.multiple_of(ff + k * 256, 256), 256)
            d_mixed = mm_nt(buf[r, :], wd[lo, :])
            gate, up = gu[r, lo].astype(F32), gu[r, hi].astype(F32)
            sigma = jax.nn.sigmoid(gate)
            d_gate = d_mixed * up * sigma * (1.0 + gate * (1.0 - sigma))
            dgu[r, lo] = d_gate.astype(BF)
            dgu[r, hi] = (d_mixed * gate * sigma).astype(BF)
            return 0

        lax.fori_loop(0, ff // 256, one, 0)

    gather_loop(pos, count, buf, gsems, on_chip)
    w1.wait()
    in_r.wait()
    in_m.wait()

    def partial(q):
        r = rows_of(q, big)

        def one(k, _):
            lo = rows_of(k, 512)
            p[r, lo] = mm_nt(dgu[r, :], wg[lo, :]).astype(BF)
            return 0

        lax.fori_loop(0, width // 512, one, 0)

    shares = ShareSum(acc, got, (xs, xr), n_shard, n_rep)
    owners = 4
    most = owners * own
    parts = width // most

    def grad_rows(k):
        at = rows_of(k, most)

        def one(n, _):
            lo = rows_of(n, 256)
            acc[at, lo] = mm_tn(resid[:, at], dgu[:, lo]).astype(BF)
            return 0

        lax.fori_loop(0, 2 * ff // 256, one, 0)
        for d in range(owners):
            shares.start(k * owners + d)

    def grad_down():
        def rows(m, _):
            at = rows_of(m, most)

            def one(n, _):
                lo = rows_of(n, 256)
                down[at, lo] = mm_tn(mixed[:, at], buf[:, lo]).astype(BF)
                return 0

            lax.fori_loop(0, width // 256, one, 0)
            return 0

        lax.fori_loop(0, ff // most, rows, 0)
        load(down, down_ref, lsem.at[3])

    def chunk(t):
        def run():
            def one(k, _):
                grad_rows(k)
                return 0

            lax.fori_loop(parts * t // 4, parts * (t + 1) // 4, one, 0)

        return run

    scatter_loop(
        pos, count, bufs, ssems, partial, out_ref, [chunk(t) for t in range(4)] + [grad_down],
        "0ff1" + "f" * (na - 2) + "s2s3" + "s" * (na - 3) + "4",
    )

    gain_rows(aux_ref, 1, row)
    live_rows(aux_ref, pos, mask)
    sums[...] = jnp.zeros_like(sums)

    def close(at):
        d_resid = cot_ref[at, :].astype(F32) * mask[at, :1] + out_ref[at, :]
        out_ref[at, :] = d_resid
        hat = hat_ref[at, :]
        sums[...] += jnp.sum(d_resid * hat, axis=0, keepdims=True)
        d_ref[at, :] = norm_back(d_resid, hat, scale_ref[at, :1], row[...]).astype(BF)

    norm_rows(count, close)
    gain_ref[...] = jnp.zeros_like(gain_ref)
    for d in range(n_shard):
        cols = slice(d * own, (d + 1) * own)
        gain_ref[d, 0:1, :] = sums[:, cols]
        gain_ref[d, 1:2, :] = mlp_gain_ref[:, cols]

    def collect(d, _):
        shares.add(d)
        pltpu.make_async_copy(
            acc.at[shares.part(d, shares.r)], gsum_ref.at[rows_of(d, share)], osem.at[d]
        ).start()
        return 0

    lax.fori_loop(0, n_shard, collect, 0)

    def end(d, _):
        shares.sent(d)
        pltpu.make_async_copy(
            acc.at[shares.part(d, shares.r)], gsum_ref.at[rows_of(d, share)], osem.at[d]
        ).wait()
        return 0

    lax.fori_loop(0, n_shard, end, 0)
    pltpu.make_async_copy(down, down_ref, lsem.at[3]).wait()


def attn_back_kernel(
    n_shard, n_rep, heads,
    x_ref, tok_ref, wo_ref, wq_ref, hats_in, rot_in, prob_in, ctx_in, aux_ref, sums_ref,
    table_ref, gain_ref, gsum_ref, down_ref,
    gu_ref, dn_ref, go_ref, gq_ref, gains_ref, out_ref,
    hats_ref, rot_ref, prob_ref, ctx_ref, buf, tok, wq, dctx, ups, dqkv, stats, inner, got, packed, ggot, mine_g, rgot, lsem, xs, xr, gs, gr, rs, rr, *rest,
):
    rest = list(rest)

    def take(n):
        out = rest[:n]
        del rest[:n]
        return out

    pos = position(n_shard)
    na = pos[3]
    gsems, bufs, ssems = take(5), take(4), take(6)
    dacc, dgot, *dsems = take(4)
    oacc, ogot, *osems = take(4)
    qacc, qgot, *qsems = take(4)
    dgsems, ogsems, gusems, qksems = take(3), take(3), take(5), take(5)
    p = bufs[0]
    count, width = out_ref.shape
    big = 2 * count
    own = wo_ref.shape[0]
    hw = own // heads
    r_me = lax.axis_index("rep")
    mine = load(x_ref, buf.at[own_rows(pos, count)], lsem.at[0])
    in_d = load(down_ref, dacc, lsem.at[1])
    kept = [
        load(hats_in, hats_ref, lsem.at[4]), load(rot_in, rot_ref, lsem.at[5]),
        load(prob_in, prob_ref, lsem.at[6]), load(ctx_in, ctx_ref, lsem.at[7]),
    ]
    in_t = load(tok_ref, tok, lsem.at[2])
    in_w = load(wq_ref, wq, lsem.at[3])
    share = own // n_rep
    gu_rows = RowsBack(lambda d: gsum_ref.at[rows_of(d, share)], gu_ref, gusems, 2, n_shard, n_rep)
    down = ShareSum(dacc, dgot, dsems, 1, n_rep)
    down_all = ShareGather(dacc.at[down.part(0, r_me)], dn_ref, dgsems, n_rep)
    wout = ShareSum(oacc, ogot, osems, 1, n_rep)
    wout_all = ShareGather(oacc.at[wout.part(0, r_me)], go_ref, ogsems, n_rep)
    wqkv = ShareSum(qacc, qgot, qsems, n_shard, n_rep)
    wqkv_rows = RowsBack(
        lambda d: qacc.at[wqkv.part(d, r_me)], gq_ref, qksems, 3, n_shard, n_rep
    )
    greet_all(n_shard, n_rep)
    mine.wait()

    def hook(t):
        @pl.when(t == 0)
        def _():
            gu_rows.start_own()
            in_d.wait()
            down.start(0)

            def one(k, _):
                gain_desc(k).start()
                return 0

            lax.fori_loop(1, n_shard, one, 0)

        @pl.when(t == na - 2)
        def _():
            down.add(0)
            down_all.start()

        @pl.when(t == na - 1)
        def _():
            gu_rows.start(0, 1, half)
            gu_rows.forward_own()

    half = n_shard // 2

    def gain_desc(k):
        target = lax.rem(lax.axis_index("shard") + k, n_shard)
        return send(gain_ref.at[target], ggot.at[k - 1], gs.at[k - 1], gr.at[k - 1], shard=target)

    def gain_rep(m):
        target = lax.rem(r_me + m, n_rep)
        return send(mine_g, rgot.at[m - 1], rs.at[m - 1], rr.at[m - 1], rep=target)

    def on_chip(q, t):
        r = rows_of(q, big)
        dctx[r, :] = mm_nt(buf[r, :], wo_ref[...]).astype(BF)

    gather_loop(pos, count, buf, gsems, on_chip, hook)
    early = half * 5 // 8
    gu_rows.start(1, 0, early)
    root = hw ** (-0.5)
    me = lax.axis_index("shard")
    mine_g[...] = gain_ref[me]
    for cp in kept:
        cp.wait()

    def scale_of(i):
        at = pl.ds(pl.multiple_of(i * count, count), count)
        return lax.rsqrt(sums_ref[:, at] / width + EPSILON)

    def attend(i, _):
        r = rows_of(i, count)
        at = pl.ds(pl.multiple_of(i * count, count), count)
        cos, sin = rope_of(spots_of(aux_ref[i, 0:1, :], count)[1], table_ref[...])
        totals = [jnp.zeros((1, count), F32), jnp.zeros((1, count), F32)]
        for h in range(heads):
            def part(g):
                lo = g * own + h * hw
                return slice(lo, lo + hw)

            cols = slice(h * hw, (h + 1) * hw)
            query, keys, values = rot_ref[r, part(0)], rot_ref[r, part(1)], rot_ref[r, part(2)]
            probs = prob_ref[r, h * count : (h + 1) * count]
            probs_b = probs.astype(BF)
            d_ctx = dctx[r, cols]
            d_values = mm_tn(probs_b, d_ctx)
            d_probs = mm_nt(d_ctx, values)
            delta = jnp.sum(probs_b.astype(F32) * d_probs, axis=-1, keepdims=True)
            d_scores = (probs * (d_probs - delta) * root).astype(BF)
            d_query = mm(d_scores, keys)
            d_keys = mm_tn(d_scores, query)
            dqkv[r, part(2)] = d_values.astype(BF)
            for g, x in enumerate((d_query, d_keys)):
                x = x * cos - swap_halves(x) * sin
                hat = hats_ref[r, part(g)]
                mine_g[2 + g : 3 + g, cols] += jnp.sum(x * hat, axis=0, keepdims=True)
                up = x * aux_ref[me, 3 + g : 4 + g, cols]
                ups[r, part(g)] = up
                totals[g] = totals[g] + row_sums(up * hat)
        for g in range(2):
            stats[pl.ds(g, 1), at] = totals[g]

        @pl.when((i > 0) & (i < half))
        def _():
            gu_rows.forward(0, i, i + 1)

        return 0

    lax.fori_loop(0, n_shard, attend, 0, unroll=UNROLL)
    packed[...] = stats[...].astype(BF)
    exchange_start(n_shard, packed, got, xs, xr)
    gu_rows.start(1, early, half)

    def out_cols(n, _):
        lo = rows_of(n, 256)
        oacc[:, lo] = mm_tn(ctx_ref[...], buf[:, lo]).astype(BF)
        return 0

    lax.fori_loop(0, width // 256, out_cols, 0)
    wout.start(0)

    def gain_take(k, _):
        gain_desc(k).wait_recv()
        mine_g[...] += ggot[k - 1]
        return 0

    lax.fori_loop(1, n_shard, gain_take, 0)
    for m in range(1, n_rep):
        gain_rep(m).start()
    exchange_finish(n_shard, stats, packed, got, xs, xr, inner)

    def settle(i, _):
        r = rows_of(i, count)
        at = pl.ds(pl.multiple_of(i * count, count), count)
        scale = scale_of(i)
        mean = inner[:, at] / width
        for g in range(2):
            lo = slice(g * own, (g + 1) * own)
            column = turned(scale[g : g + 1], count)[:, :1]
            down_by = turned(mean[g : g + 1], count)[:, :1]
            dqkv[r, lo] = (column * (ups[r, lo] - hats_ref[r, lo] * down_by)).astype(BF)
        return 0

    lax.fori_loop(0, n_shard, settle, 0)
    in_w.wait()
    in_t.wait()

    def partial(q):
        r = rows_of(q, big)

        def one(k, _):
            lo = rows_of(k, 512)
            p[r, lo] = mm_nt(dqkv[r, :], wq[lo, :]).astype(BF)
            return 0

        lax.fori_loop(0, width // 512, one, 0)

    most = 4 * own

    def grad_rows(k, _):
        at = rows_of(k, most)
        qacc[at, :] = mm_tn(tok[:, at], dqkv[...]).astype(BF)
        return 0

    def near_far(do, flip):
        def one(k, _):
            do(peer(k, flip, 1))
            return 0

        lax.fori_loop(0, half, one, 0)

    def work0():
        lax.fori_loop(0, width // most, grad_rows, 0)
        near_far(wqkv.start, 0)
        near_far(wqkv.start, 1)

    def work1():
        gu_rows.forward(1, 0, half)

    def work2():
        wout.add(0)
        wout_all.start()

    def work3():
        near_far(wqkv.add, 0)
        wqkv_rows.start_own()
        wqkv_rows.start(0, 1, half)

    def work4():
        near_far(wqkv.add, 1)
        wqkv_rows.start(1, 0, half)

    def work5():
        wqkv_rows.forward_own()
        wqkv_rows.forward(0, 1, half)

    def work6():
        wqkv_rows.forward(1, 0, half)

    scatter_loop(
        pos, count, bufs, ssems, partial, out_ref, [work0, work1, work2, work3, work4, work5, work6],
        "ff0" + "f" * (na - 2) + "12s3s45" + "s" * (na - 3) + "6",
    )

    def end(d, _):
        wqkv.sent(d)
        return 0

    lax.fori_loop(0, n_shard, end, 0)
    down.sent(0)
    wout.sent(0)

    def gain_sent(k, _):
        gain_desc(k).wait_send()
        return 0

    lax.fori_loop(1, n_shard, gain_sent, 0)
    gains_ref[...] = mine_g[...]
    for m in range(1, n_rep):
        gain_rep(m).wait_recv()
        gains_ref[...] += rgot[m - 1]
    for m in range(1, n_rep):
        gain_rep(m).wait_send()
    wqkv_rows.finish()
    gu_rows.finish()
    down_all.finish()
    wout_all.finish()


def rope_table(count, head_width):
    half_width = head_width // 2
    inverse = np.float32(THETA) ** (-(np.float32(2.0) * np.arange(half_width, dtype=np.float32)) / np.float32(head_width))
    angle = np.arange(count, dtype=np.float32)[:, None] * inverse[None, :].astype(np.float32)
    cosine, sine = np.cos(angle), np.sin(angle)
    rest = np.concatenate([cosine, cosine, -sine, sine], axis=1).astype(np.float32)
    parts = []
    for _ in range(3):
        parts.append(rest.astype(BF))
        rest = rest - parts[-1].astype(np.float32)
    return np.concatenate(parts, axis=1)


def make(n_rep, n_shard):
    chips = n_shard // 2

    def shards(
        tokens, segment_ids, cotangent, w_qkv, w_out, w_gate_up, w_down,
        q_gain, k_gain, attn_gain, mlp_gain,
    ):
        count, width = tokens.shape
        heads = H // n_shard
        hw = width // H
        own = width // n_shard
        ff = w_down.shape[0]
        total = count * n_shard
        gathered = pltpu.VMEM((total, width), BF)

        assert own == count
        aux = jnp.stack(
            [x.astype(F32) for x in (segment_ids, attn_gain, mlp_gain, q_gain, k_gain)]
            + [jnp.zeros((count,), F32)] * 3
        )
        table = jnp.asarray(rope_table(count, hw))
        chunk = n_shard - 1
        saved = [
            pltpu.VMEM((total, 2 * own), F32), pltpu.VMEM((total, 3 * own), BF),
            pltpu.VMEM((total, heads * count), F32), pltpu.VMEM((total, own), BF),
        ]
        (
            tokens_g, wq, wg, auxg, squares, hats, rots, probs, context_b,
            attn_hat, attn_scale, resid, resid_b,
        ) = call(
            functools.partial(attn_kernel, n_shard, n_rep, heads), "attn", 1,
            [
                ((total, width), BF, ANY), ((width, 3 * own), BF, ANY), ((width, 2 * ff), BF, ANY),
                ((n_shard, 8, count), F32, VM), ((2, total), F32, VM), ((total, 2 * own), F32, ANY),
                ((total, 3 * own), BF, ANY), ((total, heads * count), F32, ANY),
                ((total, own), BF, ANY), ((count, width), F32, VM), ((count, 128), F32, VM),
                ((count, width), F32, VM), ((count, width), BF, VM),
            ],
            [ANY, VM, ANY, VM, ANY, VM],
            saved + [
                pltpu.VMEM((1, width), F32), gathered, pltpu.VMEM((width, 3 * own), BF), pltpu.VMEM((own, 2 * ff), BF),
                pltpu.VMEM((total, 3 * own), F32), pltpu.VMEM((2, total), F32),
                pltpu.VMEM((chunk, 2, total), BF), pltpu.VMEM((2, total), BF),
                DMA((6,)), DMA((chips,)), DMA((chunk,)), DMA((chunk,)), DMA((chunk,)), DMA((chunk,)),
            ] + gather_sems(n_shard) + columns_sems(n_shard, n_rep, 3)
            + columns_sems(n_shard, n_rep, 2)
            + scatter_bufs(n_shard, count, width) + scatter_sems(n_shard),
            tokens, aux, w_qkv, w_out, w_gate_up, table,
        )
        resid_g, gate_up, mixed_b, output, d_down, grad_mlp = call(
            functools.partial(mlp_kernel, n_shard), "mlp", 3,
            [
                ((total, width), BF, ANY), ((total, 2 * ff), BF, ANY),
                ((total, ff), BF, ANY), ((count, width), BF, VM), ((count, width), BF, VM),
                ((1, width), F32, VM),
            ],
            [ANY, ANY, ANY, VM, VM, VM],
            [
                pltpu.VMEM((count, width), F32), pltpu.VMEM((1, width), F32),
                pltpu.VMEM((count, count), F32), gathered, pltpu.VMEM((width, 2 * ff), BF), pltpu.VMEM((ff, width), BF),
                pltpu.VMEM((total, 2 * ff), BF), pltpu.VMEM((total, ff), BF),
                DMA((3,)), DMA((chips,)), DMA((chips,)), DMA((chips,)),
            ] + scatter_bufs(n_shard, count, width) + scatter_sems(n_shard) + gather_sems(n_shard),
            resid_b, wg, w_down, auxg, resid, cotangent,
        )
        gu_sum, down_acc, d_resid, d_attn, norm_gains = call(
            functools.partial(mlp_back_kernel, n_shard, n_rep), "mlp_back", 4,
            [
                ((width // n_rep, 2 * ff), BF, ANY), ((ff, width), BF, ANY),
                ((count, width), F32, VM), ((count, width), BF, VM), ((n_shard, 8, own), F32, VM),
            ],
            [ANY] * 6 + [VM] * 5,
            [
                pltpu.VMEM((1, width), F32), pltpu.VMEM((1, width), F32),
                pltpu.VMEM((count, count), F32), gathered, pltpu.VMEM((width, 2 * ff), BF), pltpu.VMEM((ff, width), BF),
                pltpu.VMEM((total, 2 * ff), BF), pltpu.VMEM((total, 2 * ff), BF),
                gathered, pltpu.VMEM((total, ff), BF),
                pltpu.VMEM((ff, width), BF), DMA((5,)), DMA((chips,)), DMA((n_shard,)),
            ] + share_scratch(width, 2 * ff, n_shard, n_rep)
            + scatter_bufs(n_shard, count, width) + scatter_sems(n_shard) + gather_sems(n_shard),
            d_down, gate_up, wg, w_down, resid_g, mixed_b,
            auxg, cotangent, attn_hat, attn_scale, grad_mlp,
        )
        gu_rows, down_rows, out_rows, qkv_rows, gains, d_tokens_sum = call(
            functools.partial(attn_back_kernel, n_shard, n_rep, heads), "attn_back", 5,
            [
                ((own, n_shard * 2 * ff), BF, ANY), ((ff, width), BF, ANY), ((own, width), BF, ANY),
                ((own, 3 * width), BF, ANY), ((8, own), F32, VM), ((count, width), F32, VM),
            ],
            [ANY, ANY, VM, ANY, ANY, ANY, ANY, ANY, VM, VM, VM, VM, ANY, ANY],
            saved + [
                gathered, gathered, pltpu.VMEM((width, 3 * own), BF), pltpu.VMEM((total, own), BF),
                pltpu.VMEM((total, 2 * own), F32), pltpu.VMEM((total, 3 * own), BF),
                pltpu.VMEM((2, total), F32),
                pltpu.VMEM((2, total), F32), pltpu.VMEM((chunk, 2, total), BF),
                pltpu.VMEM((2, total), BF), pltpu.VMEM((chunk, 8, own), F32), pltpu.VMEM((8, own), F32),
                pltpu.VMEM((n_rep - 1, 8, own), F32),
                DMA((8,)), DMA((chunk,)), DMA((chunk,)), DMA((chunk,)), DMA((chunk,)),
                DMA((n_rep - 1,)), DMA((n_rep - 1,)),
            ] + gather_sems(n_shard) + scatter_bufs(n_shard, count, width) + scatter_sems(n_shard)
            + share_scratch(ff, width, 1, n_rep) + share_scratch(own, width, 1, n_rep)
            + share_scratch(width, 3 * own, n_shard, n_rep)
            + share_gather_sems(n_rep) * 2
            + rows_back_sems(n_shard, n_rep, 2) + rows_back_sems(n_shard, n_rep, 3),
            d_attn, tokens_g, w_out, wq, hats, rots, probs, context_b, auxg, squares,
            table, norm_gains, gu_sum, down_acc,
        )
        grad_tokens = d_resid + d_tokens_sum
        return (
            output, grad_tokens, qkv_rows.astype(F32), out_rows.astype(F32), gu_rows.astype(F32),
            down_rows.astype(F32), gains[2], gains[3], gains[0], gains[1],
        )

    return shards


def solution(mesh):
    rows = P(("rep", "shard"), None)
    return jax.shard_map(
        make(mesh.shape["rep"], mesh.shape["shard"]),
        mesh=mesh,
        in_specs=(rows, P(("rep", "shard")), rows)
        + (P("shard", None),) * 4
        + (P("shard"),) * 4,
        out_specs=(rows, rows) + (P("shard", None),) * 4 + (P("shard"),) * 4,
        check_vma=False,
    )
```

```python
import functools

import jax
import jax.numpy as jnp
import numpy as np
from jax import lax
from jax.experimental import pallas as pl
from jax.experimental.pallas import tpu as pltpu
from jax.sharding import PartitionSpec as P

H = 16
EPSILON = 1e-06
THETA = 500000.0
BF = jnp.bfloat16
F32 = jnp.float32
MESH = pl.DeviceIdType.MESH
DMA = pltpu.SemaphoreType.DMA
ANY = pl.BlockSpec(memory_space=pl.ANY)
VM = pl.BlockSpec(memory_space=pltpu.VMEM)
CHUNKS = 2
UNROLL = 2
VMEM_LIMIT = 62 << 20


def position(n_shard):
    s = lax.axis_index("shard")
    return s // 4, (s // 2) % 2, s % 2, n_shard // 4


def index(a, b, c):
    return (a * 2 + b) * 2 + c


def line_order(t, a, na):
    m = jnp.minimum(a, na - 1 - a)
    near = jnp.where(t % 2 == 1, a - (t + 1) // 2, a + (t + 1) // 2)
    far = jnp.where(m == a, t, na - 1 - t)
    return jnp.where(t <= 2 * m, near, far)


def peer(k, flip, sign):
    s = lax.axis_index("shard")
    na = lax.axis_size("shard") // 4
    a, b, c = s // 4, (s // 2) % 2, s % 2
    return index(lax.rem(a + na + sign * (k // 2), na), (b + flip) % 2, (c + k) % 2)


def rows_of(i, size):
    return pl.ds(pl.multiple_of(i * size, size), size)


def send(src, dst, ssem, rsem, **target):
    return pltpu.make_async_remote_copy(
        src_ref=src, dst_ref=dst, send_sem=ssem, recv_sem=rsem,
        device_id=target, device_id_type=MESH,
    )


def signal(sem, **target):
    pl.semaphore_signal(sem, inc=1, device_id=target, device_id_type=MESH)


def greet(pos):
    barrier = pltpu.get_barrier_semaphore()
    a, b, c, na = pos

    @pl.when(a > 0)
    def _():
        signal(barrier, shard=index(a - 1, b, c))

    @pl.when(a < na - 1)
    def _():
        signal(barrier, shard=index(a + 1, b, c))

    signal(barrier, shard=index(a, 1 - b, c))
    signal(barrier, shard=index(a, b, 1 - c))
    pl.semaphore_wait(barrier, 2 + (a > 0).astype(jnp.int32) + (a < na - 1).astype(jnp.int32))


def greet_all(n_shard, n_rep):
    barrier = pltpu.get_barrier_semaphore()
    s, r = lax.axis_index("shard"), lax.axis_index("rep")

    def one(k, _):
        signal(barrier, shard=lax.rem(s + k, n_shard))
        return 0

    lax.fori_loop(1, n_shard, one, 0)
    for k in range(1, n_rep):
        signal(barrier, rep=lax.rem(r + k, n_rep))
    pl.semaphore_wait(barrier, n_shard - 1 + n_rep - 1)


def gather_sems(n_shard):
    na = n_shard // 4
    return [
        DMA((n_shard * CHUNKS,)), DMA((na * CHUNKS,)), DMA((na * CHUNKS,)),
        DMA((na * CHUNKS,)), DMA((2 * na * CHUNKS,)),
    ]


def gather_loop(pos, count, buf, sems, on_chip, hook=None, late=None):
    recv, up, down, ysend, csend = sems
    a, b, c, na = pos
    rows = count // CHUNKS

    def desc(i, ch, ssem, target):
        piece = buf.at[pl.ds(pl.multiple_of(i * count + ch * rows, rows), rows)]
        return send(piece, piece, ssem, recv.at[i * CHUNKS + ch], shard=target)

    def sends(j, ch):
        i = index(j, b, c)

        @pl.when((j <= a) & (a < na - 1))
        def _():
            desc(i, ch, up.at[j * CHUNKS + ch], index(a + 1, b, c)).start()

        @pl.when((j >= a) & (a > 0))
        def _():
            desc(i, ch, down.at[j * CHUNKS + ch], index(a - 1, b, c)).start()

        desc(i, ch, ysend.at[j * CHUNKS + ch], index(a, 1 - b, c)).start()
        desc(i, ch, csend.at[(j * 2 + b) * CHUNKS + ch], index(a, b, 1 - c)).start()

    def arrived(i, ch):
        desc(i, ch, csend.at[0], index(a, b, 1 - c)).wait_recv()

    def pair_step(j, t):
        i = index(j, 1 - b, c)
        for ch in range(CHUNKS):
            arrived(i, ch)
            desc(i, ch, csend.at[(j * 2 + 1 - b) * CHUNKS + ch], index(a, b, 1 - c)).start()
        for ch in range(CHUNKS):
            arrived(index(j, 1 - b, 1 - c), ch)
        on_chip(j * 2 + 1 - b, t)

    def step(t, _):
        j = line_order(t, a, na)
        for ch in range(CHUNKS):

            @pl.when(t > 0)
            def _():
                arrived(index(j, b, c), ch)

            sends(j, ch)
        if hook is not None:
            hook(t)
        for ch in range(CHUNKS):
            arrived(index(j, b, 1 - c), ch)
        on_chip(j * 2 + b, t)

        @pl.when(t > 0)
        def _():
            pair_step(line_order(t - 1, a, na), t)

        return 0

    lax.fori_loop(0, na, step, 0)
    if late is not None:
        late()
    pair_step(line_order(na - 1, a, na), na)

    def finish(j, _):
        i = index(j, b, c)
        for ch in range(CHUNKS):

            @pl.when((j <= a) & (a < na - 1))
            def _():
                desc(i, ch, up.at[j * CHUNKS + ch], index(a, b, 1 - c)).wait_send()

            @pl.when((j >= a) & (a > 0))
            def _():
                desc(i, ch, down.at[j * CHUNKS + ch], index(a, b, 1 - c)).wait_send()

            desc(i, ch, ysend.at[j * CHUNKS + ch], index(a, 1 - b, c)).wait_send()
            for bb in range(2):
                slot = (j * 2 + bb) * CHUNKS + ch
                desc(index(j, bb, c), ch, csend.at[slot], index(a, b, 1 - c)).wait_send()
        return 0

    lax.fori_loop(0, na, finish, 0)


def scatter_sems(n_shard):
    na = n_shard // 4
    return [DMA((2 * na,)), DMA((2 * na,)), DMA((na,)), DMA((na,)), DMA((na,)), DMA((na + 1,))]


def scatter_bufs(n_shard, count, width):
    na = n_shard // 4
    return [
        pltpu.VMEM((n_shard * count, width), BF), pltpu.VMEM((2 * na * count, width), BF),
        pltpu.VMEM((na * count, width), BF), pltpu.VMEM(((na + 1) * count, width), BF),
    ]


def scatter_loop(pos, count, bufs, sems, partial, out, works=(), order=None):
    p, cgot, ygot, zgot = bufs
    csend, crecv, ysend, yrecv, zsend, zrecv = sems
    a, b, c, na = pos
    tile = 32

    def to_core(q):
        return send(
            p.at[rows_of(q * 2 + 1 - c, count)], cgot.at[rows_of(q, count)],
            csend.at[q], crecv.at[q], shard=index(a, b, 1 - c),
        )

    def to_pair(j):
        return send(
            p.at[rows_of(index(j, 1 - b, c), count)], ygot.at[rows_of(j, count)],
            ysend.at[j], yrecv.at[j], shard=index(a, 1 - b, c),
        )

    def along(j, slot, target):
        return send(
            p.at[rows_of(index(j, b, c), count)], zgot.at[rows_of(slot, count)],
            zsend.at[j], zrecv.at[slot], shard=target,
        )

    def add(i, others, into=None):
        def one(k, _):
            def at(slot):
                return pl.ds(pl.multiple_of(slot * count + k * tile, tile), tile)

            total = p[at(i), :].astype(F32)
            for ref, slot in others:
                total = total + ref[at(slot), :].astype(F32)
            if into is None:
                p[at(i), :] = total.astype(BF)
            else:
                into[at(0), :] = total
            return 0

        lax.fori_loop(0, count // tile, one, 0)

    def first(t, _):
        j = line_order(na - 1 - t, a, na)
        far, near = j * 2 + 1 - b, j * 2 + b
        partial(far)
        to_core(far).start()
        partial(near)
        to_core(near).start()
        to_core(far).wait_recv()
        add(index(j, 1 - b, c), [(cgot, far)])
        to_pair(j).start()
        return 0

    def second(t, _):
        j = line_order(na - 1 - t, a, na)
        near = j * 2 + b
        i = index(j, b, c)
        to_core(near).wait_recv()
        to_pair(j).wait_recv()
        inner = ((j < a) & (a < na - 1)) | ((j > a) & (a > 0))

        @pl.when(inner)
        def _():
            along(j, j, index(a, b, 1 - c)).wait_recv()
            add(i, [(cgot, near), (ygot, j), (zgot, j)])

        @pl.when(jnp.logical_not(inner))
        def _():
            add(i, [(cgot, near), (ygot, j)])

        @pl.when(j > a)
        def _():
            along(j, j, index(a + 1, b, c)).start()

        @pl.when(j < a)
        def _():
            along(j, jnp.where(j == a - 1, na, j), index(a - 1, b, c)).start()

        return 0

    if order is None:
        lax.fori_loop(0, na, first, 0)
        lax.fori_loop(0, na - 1, second, 0)
    else:
        done_first = done_second = 0
        for token in order:
            if token == "f":
                first(done_first, 0)
                done_first += 1
            elif token == "s":
                second(done_second, 0)
                done_second += 1
            else:
                works[int(token)]()
        assert done_first == na and done_second == na - 1
    near = a * 2 + b
    to_core(near).wait_recv()
    to_pair(a).wait_recv()
    add(index(a, b, c), [(cgot, near), (ygot, a)], out)

    def more(slot):
        along(a, slot, index(a, b, 1 - c)).wait_recv()

        def one(k, _):
            got = zgot[pl.ds(pl.multiple_of(slot * count + k * tile, tile), tile), :]
            out[rows_of(k, tile), :] += got.astype(F32)
            return 0

        lax.fori_loop(0, count // tile, one, 0)

    @pl.when(a > 0)
    def _():
        more(a)

    @pl.when(a < na - 1)
    def _():
        more(na)

    def finish(j, _):
        for bb in range(2):
            to_core(j * 2 + bb).wait_send()
        to_pair(j).wait_send()

        @pl.when(j != a)
        def _():
            along(j, j, index(a, b, 1 - c)).wait_send()

        return 0

    lax.fori_loop(0, na, finish, 0)


def columns_sems(n_shard, n_rep, groups):
    return [
        DMA((n_shard * groups,)), DMA((n_shard * groups,)),
        DMA((n_shard * n_rep,)), DMA((n_shard * n_rep,)), DMA((groups + 1,)),
    ]


class Columns:
    def __init__(self, w, out, stage, sems, groups, n_shard, n_rep):
        self.w, self.out, self.stage, self.groups = w, out, stage, groups
        self.ssem, self.rsem, self.fsend, self.frecv, self.lsem = sems
        self.n_shard, self.n_rep = n_shard, n_rep
        self.own = w.shape[0]
        self.share = self.own // n_rep
        self.total = w.shape[1] // groups
        self.width = self.total // n_shard
        self.s, self.r = lax.axis_index("shard"), lax.axis_index("rep")

    def move(self, source, target, g):
        cols = pl.ds(pl.multiple_of(g * self.total + target * self.width, 128), self.width)
        src = self.w.at[rows_of(self.r, self.share), cols]
        at = pl.ds(pl.multiple_of(source * self.own + self.r * self.share, self.share), self.share)
        dst = self.out.at[at, pl.ds(g * self.width, self.width)]
        return send(
            src, dst, self.ssem.at[target * self.groups + g],
            self.rsem.at[source * self.groups + g], shard=target,
        )

    def pass_on(self, source, k, replica):
        at = pl.ds(
            pl.multiple_of(source * self.own + replica * self.share, self.share), self.share
        )
        piece = self.out.at[at]
        return send(
            piece, piece, self.fsend.at[source * self.n_rep + k],
            self.frecv.at[source * self.n_rep + replica],
            rep=lax.rem(self.r + k, self.n_rep),
        )

    def local_in(self, g):
        cols = pl.ds(pl.multiple_of(g * self.total + self.s * self.width, 128), self.width)
        into = pl.ds(g * self.width, self.width)
        if self.stage is None:
            dst = self.out.at[rows_of(self.s, self.own), into]
        else:
            dst = self.stage.at[:, into]
        return pltpu.make_async_copy(self.w.at[:, cols], dst, self.lsem.at[g])

    def local_out(self):
        return pltpu.make_async_copy(
            self.stage, self.out.at[rows_of(self.s, self.own)], self.lsem.at[self.groups]
        )

    def start(self, flip, low, high):
        def one(k, _):
            for g in range(self.groups):
                self.move(self.s, peer(k, flip, 1), g).start()
            return 0

        lax.fori_loop(low, high, one, 0)

    def start_own(self):
        for g in range(self.groups):
            self.local_in(g).start()
        if self.stage is not None:
            for g in range(self.groups):
                self.local_in(g).wait()
            self.local_out().start()

    def forward(self, flip, low, high):
        def one(k, _):
            source = peer(k, flip, -1)
            for g in range(self.groups):
                self.move(source, self.s, g).wait_recv()
            for m in range(1, self.n_rep):
                self.pass_on(source, m, self.r).start()
            return 0

        lax.fori_loop(low, high, one, 0)

    def finish(self):
        def one(k, _):
            source = lax.rem(self.s + self.n_shard - k, self.n_shard)
            for g in range(self.groups):
                self.move(self.s, source, g).wait_send()
            for m in range(1, self.n_rep):
                self.pass_on(source, m, self.r).wait_send()
                self.pass_on(source, m, lax.rem(self.r + m, self.n_rep)).wait_recv()
            return 0

        lax.fori_loop(1, self.n_shard, one, 0)
        if self.stage is not None:
            self.local_out().wait()
        else:
            for g in range(self.groups):
                self.local_in(g).wait()


class ShareSum:
    def __init__(self, acc, got, sems, blocks, n_rep):
        self.acc, self.got, self.blocks, self.n_rep = acc, got, blocks, n_rep
        self.ssem, self.rsem = sems
        self.share = acc.shape[0] // (blocks * n_rep)
        self.r = lax.axis_index("rep")

    def part(self, block, replica):
        return rows_of(block * self.n_rep + replica, self.share)

    def desc(self, block, m):
        target = lax.rem(self.r + m, self.n_rep)
        slot = (m - 1) * self.blocks + block
        return send(
            self.acc.at[self.part(block, target)], self.got.at[rows_of(slot, self.share)],
            self.ssem.at[slot], self.rsem.at[slot], rep=target,
        )

    def start(self, block):
        for m in range(1, self.n_rep):
            self.desc(block, m).start()

    def add(self, block):
        for m in range(1, self.n_rep):
            self.desc(block, m).wait_recv()
        tile = min(self.share, 32)

        def one(k, _):
            at = pl.ds(
                pl.multiple_of((block * self.n_rep + self.r) * self.share + k * tile, tile), tile
            )
            total = self.acc[at, :].astype(F32)
            for m in range(1, self.n_rep):
                slot = (m - 1) * self.blocks + block
                total = total + self.got[
                    pl.ds(pl.multiple_of(slot * self.share + k * tile, tile), tile), :
                ].astype(F32)
            self.acc[at, :] = total.astype(BF)
            return 0

        lax.fori_loop(0, self.share // tile, one, 0)

    def sent(self, block):
        for m in range(1, self.n_rep):
            self.desc(block, m).wait_send()


def share_scratch(rows, cols, blocks, n_rep):
    return [
        pltpu.VMEM((rows, cols), BF), pltpu.VMEM(((n_rep - 1) * rows // n_rep, cols), BF),
        DMA(((n_rep - 1) * blocks,)), DMA(((n_rep - 1) * blocks,)),
    ]


class ShareGather:
    def __init__(self, src, out, sems, n_rep):
        self.src, self.out, self.n_rep = src, out, n_rep
        self.ssem, self.rsem, self.lsem = sems
        self.r = lax.axis_index("rep")
        self.share = out.shape[0] // n_rep

    def local(self):
        return pltpu.make_async_copy(self.src, self.out.at[rows_of(self.r, self.share)], self.lsem)

    def desc(self, m, replica):
        return send(
            self.src, self.out.at[rows_of(replica, self.share)],
            self.ssem.at[m - 1], self.rsem.at[replica], rep=lax.rem(self.r + m, self.n_rep),
        )

    def start(self):
        self.local().start()
        for m in range(1, self.n_rep):
            self.desc(m, self.r).start()

    def finish(self):
        self.local().wait()
        for m in range(1, self.n_rep):
            self.desc(m, self.r).wait_send()
            self.desc(m, lax.rem(self.r + m, self.n_rep)).wait_recv()


def share_gather_sems(n_rep):
    return [DMA((n_rep - 1,)), DMA((n_rep,)), DMA(())]


class RowsBack:
    def __init__(self, src, out, sems, groups, n_shard, n_rep):
        self.src, self.out, self.groups = src, out, groups
        self.ssem, self.rsem, self.fsend, self.frecv, self.lsem = sems
        self.n_shard, self.n_rep = n_shard, n_rep
        self.share = out.shape[0] // n_rep
        self.total = out.shape[1] // groups
        self.width = self.total // n_shard
        self.s, self.r = lax.axis_index("shard"), lax.axis_index("rep")

    def place(self, source, replica, g):
        cols = pl.ds(pl.multiple_of(g * self.total + source * self.width, 128), self.width)
        return self.out.at[rows_of(replica, self.share), cols]

    def piece(self, target, g):
        return self.src(target).at[:, pl.ds(g * self.width, self.width)]

    def move(self, source, target, g):
        return send(
            self.piece(target, g), self.place(source, self.r, g),
            self.ssem.at[target * self.groups + g], self.rsem.at[source * self.groups + g],
            shard=target,
        )

    def local(self, g):
        return pltpu.make_async_copy(
            self.piece(self.s, g), self.place(self.s, self.r, g), self.lsem.at[g]
        )

    def pass_on(self, source, m, replica, g):
        at = self.place(source, replica, g)
        return send(
            at, at, self.fsend.at[(source * self.n_rep + m) * self.groups + g],
            self.frecv.at[(source * self.n_rep + replica) * self.groups + g],
            rep=lax.rem(self.r + m, self.n_rep),
        )

    def start(self, flip, low, high):
        def one(k, _):
            for g in range(self.groups):
                self.move(self.s, peer(k, flip, 1), g).start()
            return 0

        lax.fori_loop(low, high, one, 0)

    def start_own(self):
        for g in range(self.groups):
            self.local(g).start()

    def relay(self, source):
        for g in range(self.groups):
            for m in range(1, self.n_rep):
                self.pass_on(source, m, self.r, g).start()

    def forward_own(self):
        for g in range(self.groups):
            self.local(g).wait()
        self.relay(self.s)

    def forward(self, flip, low, high):
        def one(k, _):
            source = peer(k, flip, -1)
            for g in range(self.groups):
                self.move(source, self.s, g).wait_recv()
            self.relay(source)
            return 0

        lax.fori_loop(low, high, one, 0)

    def finish(self):
        def one(k, _):
            source = lax.rem(self.s + self.n_shard - k, self.n_shard)
            for g in range(self.groups):

                @pl.when(k > 0)
                def _():
                    self.move(self.s, source, g).wait_send()

                for m in range(1, self.n_rep):
                    self.pass_on(source, m, self.r, g).wait_send()
                    self.pass_on(source, m, lax.rem(self.r + m, self.n_rep), g).wait_recv()
            return 0

        lax.fori_loop(0, self.n_shard, one, 0)


def rows_back_sems(n_shard, n_rep, groups):
    return [
        DMA((n_shard * groups,)), DMA((n_shard * groups,)),
        DMA((n_shard * n_rep * groups,)), DMA((n_shard * n_rep * groups,)), DMA((groups,)),
    ]


def mm(left, right):
    return jnp.dot(left, right, preferred_element_type=F32)


def mm_nt(left, right):
    return lax.dot_general(left, right, (((1,), (1,)), ((), ())), preferred_element_type=F32)


def mm_tn(left, right):
    return lax.dot_general(left, right, (((0,), (0,)), ((), ())), preferred_element_type=F32)


def call(kernel, name, cid, outs, ins, scratch, *args, flops=0, moved=0):
    return pl.pallas_call(
        kernel,
        name=name,
        out_shape=[jax.ShapeDtypeStruct(shape, dtype) for shape, dtype, _ in outs],
        in_specs=ins,
        out_specs=[spec for _, _, spec in outs],
        scratch_shapes=scratch,
        compiler_params=pltpu.CompilerParams(
            collective_id=cid, has_side_effects=True, vmem_limit_bytes=VMEM_LIMIT
        ),
        cost_estimate=pl.CostEstimate(flops=flops, bytes_accessed=moved, transcendentals=0),
    )(*args)


def load(src, dst, sem):
    cp = pltpu.make_async_copy(src, dst, sem)
    cp.start()
    return cp


def own_rows(pos, count):
    a, b, c, _ = pos
    return rows_of(index(a, b, c), count)


class Out:
    def __init__(self, src, dst, sem, size):
        self.src, self.dst, self.sem, self.size = src, dst, sem, size

    def desc(self, q):
        r = rows_of(q, self.size)
        return pltpu.make_async_copy(self.src.at[r], self.dst.at[r], self.sem.at[q])

    def start(self, q):
        self.desc(q).start()

    def wait(self, q):
        self.desc(q).wait()


def wait_all(outs, chips):
    def one(q, _):
        for o in outs:
            o.wait(q)
        return 0

    lax.fori_loop(0, chips, one, 0)


def turned(row, count):
    return jnp.transpose(jnp.broadcast_to(row, (count, count)))


def spots_of(seg_row, count):
    lane = lax.broadcasted_iota(jnp.int32, (count, count), 1).astype(F32)
    slot = lax.broadcasted_iota(jnp.int32, (count, count), 0).astype(F32)
    same = turned(seg_row, count) == seg_row
    first = jnp.min(jnp.where(same, lane, float(count)), axis=-1, keepdims=True)
    return same & (lane <= slot), slot[:, :1] - first


def swap_halves(x):
    return pltpu.roll(x, x.shape[1] // 2, 1)


def rope_of(spots, table):
    count = spots.shape[0]
    lane = lax.broadcasted_iota(jnp.int32, (count, count), 1)
    pick = jnp.where(lane.astype(F32) == spots, 1.0, 0.0).astype(BF)
    parts = mm(pick, table)
    n = parts.shape[1] // 3
    both = parts[:, :n] + parts[:, n : 2 * n] + parts[:, 2 * n :]
    return both[:, : n // 2], both[:, n // 2 :]


def row_sums(x):
    ones = jnp.ones((8, x.shape[1]), F32)
    return lax.dot_general(
        ones, x, (((1,), (1,)), ((), ())),
        preferred_element_type=F32, precision=lax.Precision.HIGHEST,
    )[:1]


def gain_rows(aux_ref, k, row):
    own = aux_ref.shape[2]
    for d in range(aux_ref.shape[0]):
        row[:, d * own : (d + 1) * own] = aux_ref[d, k : k + 1, :]


def norm_rows(rows, do):
    tile = 32

    def one(k, _):
        do(rows_of(k, tile))
        return 0

    lax.fori_loop(0, rows // tile, one, 0)


def row_scale(v):
    return lax.rsqrt(jnp.mean(v * v, axis=-1, keepdims=True) + EPSILON)


def norm_back(upstream, normed, rscale, gain):
    scaled = upstream * gain
    inner = jnp.mean(scaled * normed, axis=-1, keepdims=True)
    return rscale * (scaled - normed * inner)


def attn_kernel(
    n_shard, n_rep, heads,
    x_ref, aux_ref, wqkv_ref, wo_ref, wgu_ref, table_ref,
    g_ref, wq_ref, wg_ref, auxg_ref, sums_ref, hats_out, rot_out, prob_out, ctx_out,
    out_ref, scale_ref, resid_ref, residb_ref,
    hats_ref, rot_ref, prob_ref, ctx_ref, row, buf, wq, stage, qkv, stats, got, packed, lsem, osem, xs, xr, as_, ar, *rest,
):
    pos = position(n_shard)
    gsems, c3, c2, bufs, ssems = rest[:5], rest[5:10], rest[10:15], rest[15:19], rest[19:]
    p = bufs[0]
    count, width = out_ref.shape
    chips = n_shard // 2
    big = 2 * count
    own = wo_ref.shape[0]
    hw = own // heads
    na = pos[3]
    s = lax.axis_index("shard")
    mine = load(x_ref, buf.at[own_rows(pos, count)], lsem.at[0])
    qkv_w = Columns(wqkv_ref, wq, None, c3, 3, n_shard, n_rep)
    gu_w = Columns(wgu_ref, wg_ref, stage, c2, 2, n_shard, n_rep)
    auxg_ref[s] = aux_ref[...]
    greet_all(n_shard, n_rep)
    mine.wait()
    out_x = Out(buf, g_ref, osem, big)

    def aux_desc(k):
        target = lax.rem(s + k, n_shard)
        return send(aux_ref, auxg_ref.at[s], as_.at[k - 1], ar.at[k - 1], shard=target)

    def hook(t):
        @pl.when(t == 0)
        def _():
            qkv_w.start_own()
            gu_w.start_own()
            qkv_w.start(0, 1, half)
            qkv_w.start(1, 0, half)

            def one(k, _):
                aux_desc(k).start()
                return 0

            lax.fori_loop(1, n_shard, one, 0)

        @pl.when(t == na - 2)
        def _():
            qkv_w.forward(0, 1, half)
            qkv_w.forward(1, 0, half)

        @pl.when(t == na - 1)
        def _():
            gu_w.start(0, 1, half)

    half = n_shard // 2

    def project(q):
        r = rows_of(q, big)
        v = mm(buf[r, :], wq[...])
        qkv[r, :] = v
        for g in range(2):
            x = v[:, g * own : (g + 1) * own]
            stats[pl.ds(g, 1), pl.ds(pl.multiple_of(q * big, big), big)] = row_sums(x * x)


    a, b = pos[:2]

    def late():
        qkv_w.finish()

        def there(u, _):
            project(line_order(u, a, na) * 2 + b)

            @pl.when(u < na - 1)
            def _():
                project(line_order(u, a, na) * 2 + 1 - b)

            return 0

        lax.fori_loop(0, na, there, 0)

    gather_loop(pos, count, buf, gsems, lambda q, t: out_x.start(q), hook, late)
    keep = load(wq, wq_ref, lsem.at[1])
    project(line_order(na - 1, a, na) * 2 + 1 - b)
    packed[...] = stats[...].astype(BF)
    exchange_start(n_shard, packed, got, xs, xr)
    gu_w.start(1, 0, half)
    gu_w.forward(0, 1, half)
    exchange_finish(n_shard, stats, packed, got, xs, xr, sums_ref)

    def aux_done(k, _):
        aux_desc(k).wait_recv()
        aux_desc(k).wait_send()
        return 0

    lax.fori_loop(1, n_shard, aux_done, 0)
    root = hw ** (-0.5)

    def attend(i, _):
        r = rows_of(i, count)
        at = pl.ds(pl.multiple_of(i * count, count), count)
        ok, spots = spots_of(auxg_ref[i, 0:1, :], count)
        cos, sin = rope_of(spots, table_ref[...])
        scale = lax.rsqrt(sums_ref[:, at] / width + EPSILON)
        q_scale = turned(scale[0:1], count)[:, :1]
        k_scale = turned(scale[1:2], count)[:, :1]
        for h in range(heads):
            def part(g):
                lo = g * own + h * hw
                return slice(lo, lo + hw)

            cols = slice(h * hw, (h + 1) * hw)

            def turn(g, scale, gain):
                hat = qkv[r, part(g)] * scale
                hats_ref[r, part(g)] = hat
                x = hat * gain
                x = (x * cos + swap_halves(x) * sin).astype(BF)
                rot_ref[r, part(g)] = x
                return x

            query = turn(0, q_scale, aux_ref[3:4, cols])
            keys = turn(1, k_scale, aux_ref[4:5, cols])
            values = qkv[r, part(2)].astype(BF)
            rot_ref[r, part(2)] = values
            scores = jnp.where(ok, mm_nt(query, keys) * root, -1e30)
            e = jnp.exp(scores - jnp.max(scores, axis=-1, keepdims=True))
            probs = e / jnp.sum(e, axis=-1, keepdims=True)
            prob_ref[r, h * count : (h + 1) * count] = probs
            ctx_ref[r, cols] = mm(probs.astype(BF), values).astype(BF)

        return 0

    lax.fori_loop(0, n_shard, attend, 0, unroll=UNROLL)
    kept = [
        load(hats_ref, hats_out, lsem.at[2]), load(rot_ref, rot_out, lsem.at[3]),
        load(prob_ref, prob_out, lsem.at[4]), load(ctx_ref, ctx_out, lsem.at[5]),
    ]

    def partial(q):
        r = rows_of(q, big)
        p[r, :] = mm(ctx_ref[r, :], wo_ref[...]).astype(BF)

    def pass_far(t):
        return lambda: gu_w.forward(1, half * t // 3, half * (t + 1) // 3)

    scatter_loop(
        pos, count, bufs, ssems, partial, out_ref, [pass_far(t) for t in range(3)],
        "f" * na + "0s1s2" + "s" * (na - 3),
    )
    gain_rows(auxg_ref, 1, row)

    def close(at):
        v = out_ref[at, :]
        scale = row_scale(v)
        hat = v * scale
        out_ref[at, :] = hat
        scale_ref[at, :] = jnp.broadcast_to(scale, (scale.shape[0], scale_ref.shape[1]))
        mine_at = pl.ds(pl.multiple_of(s * count + at.start, at.size), at.size)
        resid = buf[mine_at, :].astype(F32) + hat * row[...]
        resid_ref[at, :] = resid
        residb_ref[at, :] = resid.astype(BF)

    norm_rows(count, close)
    gu_w.finish()
    keep.wait()
    for cp in kept:
        cp.wait()
    wait_all([out_x], chips)


def exchange_desc(n_shard, stats, got, xs, xr, k):
    target = lax.rem(lax.axis_index("shard") + k, n_shard)
    return send(stats, got.at[k - 1], xs.at[k - 1], xr.at[k - 1], shard=target)


def exchange_start(n_shard, stats, got, xs, xr):
    def start(k, _):
        exchange_desc(n_shard, stats, got, xs, xr, k).start()
        return 0

    lax.fori_loop(1, n_shard, start, 0)


def exchange_finish(n_shard, stats, packed, got, xs, xr, sums):
    sums[...] = stats[...]

    def take(k, _):
        exchange_desc(n_shard, packed, got, xs, xr, k).wait_recv()
        sums[...] += got[k - 1].astype(F32)
        return 0

    lax.fori_loop(1, n_shard, take, 0)

    def done(k, _):
        exchange_desc(n_shard, packed, got, xs, xr, k).wait_send()
        return 0

    lax.fori_loop(1, n_shard, done, 0)


def live_rows(aux_ref, pos, mask):
    a, b, c, _ = pos
    segs = turned(aux_ref[index(a, b, c), 0:1, :], mask.shape[0])
    mask[...] = jnp.where(segs >= 0.0, 1.0, 0.0).astype(F32)


def mlp_kernel(
    n_shard, x_ref, wg_ref, wd_ref, aux_ref, resid_ref, cot_ref,
    g_ref, gu_ref, mixed_ref, y_ref, d_ref, gain_ref,
    out_ref, row, mask, buf, wg, wd, gu, mixed, lsem, osem, gsem, msem, *rest,
):
    pos = position(n_shard)
    bufs, ssems, gsems = rest[:4], rest[4:10], rest[10:]
    p = bufs[0]
    count, width = out_ref.shape
    big = 2 * count
    chips = n_shard // 2
    ff = wd.shape[0]
    mine = load(x_ref, buf.at[own_rows(pos, count)], lsem.at[0])
    w1 = load(wg_ref, wg, lsem.at[1])
    w2 = load(wd_ref, wd, lsem.at[2])
    greet(pos)
    mine.wait()
    out_x, out_g = Out(buf, g_ref, osem, big), Out(gu, gu_ref, gsem, big)
    out_m = Out(mixed, mixed_ref, msem, big)
    w1.wait()

    def on_chip(q, t):
        r = rows_of(q, big)
        out_x.start(q)

        def one(k, _):
            lo = pl.ds(pl.multiple_of(k * 256, 256), 256)
            hi = pl.ds(pl.multiple_of(ff + k * 256, 256), 256)
            gate = mm(buf[r, :], wg[:, lo])
            up = mm(buf[r, :], wg[:, hi])
            gu[r, lo] = gate.astype(BF)
            gu[r, hi] = up.astype(BF)
            mixed[r, lo] = (gate * jax.nn.sigmoid(gate) * up).astype(BF)
            return 0

        lax.fori_loop(0, ff // 256, one, 0)
        out_g.start(q)
        out_m.start(q)

    gather_loop(pos, count, buf, gsems, on_chip)
    w2.wait()

    def partial(q):
        r = rows_of(q, big)

        def one(k, _):
            lo = rows_of(k, 512)
            p[r, lo] = mm(mixed[r, :], wd[:, lo]).astype(BF)
            return 0

        lax.fori_loop(0, width // 512, one, 0)

    gain_rows(aux_ref, 2, row)
    live_rows(aux_ref, pos, mask)
    scatter_loop(pos, count, bufs, ssems, partial, out_ref)
    gain_ref[...] = jnp.zeros_like(gain_ref)

    def close(at):
        v = out_ref[at, :]
        scale = row_scale(v)
        hat = v * scale
        y_ref[at, :] = (resid_ref[at, :] + hat * row[...]).astype(BF)
        d_out = cot_ref[at, :].astype(F32) * mask[at, :1]
        gain_ref[...] += jnp.sum(d_out * hat, axis=0, keepdims=True)
        d_ref[at, :] = norm_back(d_out, hat, scale, row[...]).astype(BF)

    norm_rows(count, close)
    wait_all([out_x, out_g, out_m], chips)


def mlp_back_kernel(
    n_shard, n_rep, x_ref, gu_ref, wg_ref, wd_ref, resid_ref, mixed_ref,
    aux_ref, cot_ref, hat_ref, scale_ref, mlp_gain_ref,
    gsum_ref, down_ref, out_ref, d_ref, gain_ref,
    row, sums, mask, buf, wg, wd, gu, dgu, resid, mixed, down, lsem, isem, osem, acc, got, xs, xr, *rest,
):
    pos = position(n_shard)
    na = pos[3]
    bufs, ssems, gsems = rest[:4], rest[4:10], rest[10:]
    p = bufs[0]
    count, width = out_ref.shape
    big = 2 * count
    chips = n_shard // 2
    ff = wd.shape[0]
    own = width // n_shard
    share = own // n_rep
    mine = load(x_ref, buf.at[own_rows(pos, count)], lsem.at[0])
    w2 = load(wd_ref, wd, lsem.at[2])
    saved = Out(gu_ref, gu, isem, big)

    def fetch(q, _):
        saved.start(q)
        return 0

    lax.fori_loop(0, chips, fetch, 0)
    w1 = load(wg_ref, wg, lsem.at[1])
    in_r = load(resid_ref, resid, lsem.at[3])
    in_m = load(mixed_ref, mixed, lsem.at[4])
    greet_all(n_shard, n_rep)
    mine.wait()
    w2.wait()

    def on_chip(q, t):
        r = rows_of(q, big)
        saved.wait(q)

        def one(k, _):
            lo = pl.ds(pl.multiple_of(k * 256, 256), 256)
            hi = pl.ds(pl.multiple_of(ff + k * 256, 256), 256)
            d_mixed = mm_nt(buf[r, :], wd[lo, :])
            gate, up = gu[r, lo].astype(F32), gu[r, hi].astype(F32)
            sigma = jax.nn.sigmoid(gate)
            d_gate = d_mixed * up * sigma * (1.0 + gate * (1.0 - sigma))
            dgu[r, lo] = d_gate.astype(BF)
            dgu[r, hi] = (d_mixed * gate * sigma).astype(BF)
            return 0

        lax.fori_loop(0, ff // 256, one, 0)

    gather_loop(pos, count, buf, gsems, on_chip)
    w1.wait()
    in_r.wait()
    in_m.wait()

    def partial(q):
        r = rows_of(q, big)

        def one(k, _):
            lo = rows_of(k, 512)
            p[r, lo] = mm_nt(dgu[r, :], wg[lo, :]).astype(BF)
            return 0

        lax.fori_loop(0, width // 512, one, 0)

    shares = ShareSum(acc, got, (xs, xr), n_shard, n_rep)
    owners = 4
    most = owners * own
    parts = width // most

    def grad_rows(k):
        at = rows_of(k, most)

        def one(n, _):
            lo = rows_of(n, 256)
            acc[at, lo] = mm_tn(resid[:, at], dgu[:, lo]).astype(BF)
            return 0

        lax.fori_loop(0, 2 * ff // 256, one, 0)
        for d in range(owners):
            shares.start(k * owners + d)

    def grad_down():
        def rows(m, _):
            at = rows_of(m, most)

            def one(n, _):
                lo = rows_of(n, 256)
                down[at, lo] = mm_tn(mixed[:, at], buf[:, lo]).astype(BF)
                return 0

            lax.fori_loop(0, width // 256, one, 0)
            return 0

        lax.fori_loop(0, ff // most, rows, 0)
        load(down, down_ref, lsem.at[3])

    def chunk(t):
        def run():
            def one(k, _):
                grad_rows(k)
                return 0

            lax.fori_loop(parts * t // 4, parts * (t + 1) // 4, one, 0)

        return run

    scatter_loop(
        pos, count, bufs, ssems, partial, out_ref, [chunk(t) for t in range(4)] + [grad_down],
        "0ff1" + "f" * (na - 2) + "s2s3" + "s" * (na - 3) + "4",
    )

    gain_rows(aux_ref, 1, row)
    live_rows(aux_ref, pos, mask)
    sums[...] = jnp.zeros_like(sums)

    def close(at):
        d_resid = cot_ref[at, :].astype(F32) * mask[at, :1] + out_ref[at, :]
        out_ref[at, :] = d_resid
        hat = hat_ref[at, :]
        sums[...] += jnp.sum(d_resid * hat, axis=0, keepdims=True)
        d_ref[at, :] = norm_back(d_resid, hat, scale_ref[at, :1], row[...]).astype(BF)

    norm_rows(count, close)
    gain_ref[...] = jnp.zeros_like(gain_ref)
    for d in range(n_shard):
        cols = slice(d * own, (d + 1) * own)
        gain_ref[d, 0:1, :] = sums[:, cols]
        gain_ref[d, 1:2, :] = mlp_gain_ref[:, cols]

    def collect(d, _):
        shares.add(d)
        pltpu.make_async_copy(
            acc.at[shares.part(d, shares.r)], gsum_ref.at[rows_of(d, share)], osem.at[d]
        ).start()
        return 0

    lax.fori_loop(0, n_shard, collect, 0)

    def end(d, _):
        shares.sent(d)
        pltpu.make_async_copy(
            acc.at[shares.part(d, shares.r)], gsum_ref.at[rows_of(d, share)], osem.at[d]
        ).wait()
        return 0

    lax.fori_loop(0, n_shard, end, 0)
    pltpu.make_async_copy(down, down_ref, lsem.at[3]).wait()


def attn_back_kernel(
    n_shard, n_rep, heads,
    x_ref, tok_ref, wo_ref, wq_ref, hats_in, rot_in, prob_in, ctx_in, aux_ref, sums_ref,
    table_ref, gain_ref, gsum_ref, down_ref,
    gu_ref, dn_ref, go_ref, gq_ref, gains_ref, out_ref,
    hats_ref, rot_ref, prob_ref, ctx_ref, buf, tok, wq, dctx, ups, dqkv, stats, inner, got, packed, ggot, mine_g, rgot, lsem, xs, xr, gs, gr, rs, rr, *rest,
):
    rest = list(rest)

    def take(n):
        out = rest[:n]
        del rest[:n]
        return out

    pos = position(n_shard)
    na = pos[3]
    gsems, bufs, ssems = take(5), take(4), take(6)
    dacc, dgot, *dsems = take(4)
    oacc, ogot, *osems = take(4)
    qacc, qgot, *qsems = take(4)
    dgsems, ogsems, gusems, qksems = take(3), take(3), take(5), take(5)
    p = bufs[0]
    count, width = out_ref.shape
    big = 2 * count
    own = wo_ref.shape[0]
    hw = own // heads
    r_me = lax.axis_index("rep")
    mine = load(x_ref, buf.at[own_rows(pos, count)], lsem.at[0])
    in_d = load(down_ref, dacc, lsem.at[1])
    kept = [
        load(hats_in, hats_ref, lsem.at[4]), load(rot_in, rot_ref, lsem.at[5]),
        load(prob_in, prob_ref, lsem.at[6]), load(ctx_in, ctx_ref, lsem.at[7]),
    ]
    in_t = load(tok_ref, tok, lsem.at[2])
    in_w = load(wq_ref, wq, lsem.at[3])
    share = own // n_rep
    gu_rows = RowsBack(lambda d: gsum_ref.at[rows_of(d, share)], gu_ref, gusems, 2, n_shard, n_rep)
    down = ShareSum(dacc, dgot, dsems, 1, n_rep)
    down_all = ShareGather(dacc.at[down.part(0, r_me)], dn_ref, dgsems, n_rep)
    wout = ShareSum(oacc, ogot, osems, 1, n_rep)
    wout_all = ShareGather(oacc.at[wout.part(0, r_me)], go_ref, ogsems, n_rep)
    wqkv = ShareSum(qacc, qgot, qsems, n_shard, n_rep)
    wqkv_rows = RowsBack(
        lambda d: qacc.at[wqkv.part(d, r_me)], gq_ref, qksems, 3, n_shard, n_rep
    )
    greet_all(n_shard, n_rep)
    mine.wait()

    def hook(t):
        @pl.when(t == 0)
        def _():
            gu_rows.start_own()
            in_d.wait()
            down.start(0)

            def one(k, _):
                gain_desc(k).start()
                return 0

            lax.fori_loop(1, n_shard, one, 0)

        @pl.when(t == na - 2)
        def _():
            down.add(0)
            down_all.start()

        @pl.when(t == na - 1)
        def _():
            gu_rows.start(0, 1, half)
            gu_rows.forward_own()

    half = n_shard // 2

    def gain_desc(k):
        target = lax.rem(lax.axis_index("shard") + k, n_shard)
        return send(gain_ref.at[target], ggot.at[k - 1], gs.at[k - 1], gr.at[k - 1], shard=target)

    def gain_rep(m):
        target = lax.rem(r_me + m, n_rep)
        return send(mine_g, rgot.at[m - 1], rs.at[m - 1], rr.at[m - 1], rep=target)

    def on_chip(q, t):
        r = rows_of(q, big)
        dctx[r, :] = mm_nt(buf[r, :], wo_ref[...]).astype(BF)

    root = hw ** (-0.5)
    me = lax.axis_index("shard")
    mine_g[...] = gain_ref[me]
    for cp in kept:
        cp.wait()

    def scale_of(i):
        at = pl.ds(pl.multiple_of(i * count, count), count)
        return lax.rsqrt(sums_ref[:, at] / width + EPSILON)

    def attend(i):
        r = rows_of(i, count)
        at = pl.ds(pl.multiple_of(i * count, count), count)
        cos, sin = rope_of(spots_of(aux_ref[i, 0:1, :], count)[1], table_ref[...])
        totals = [jnp.zeros((1, count), F32), jnp.zeros((1, count), F32)]
        for h in range(heads):
            def part(g):
                lo = g * own + h * hw
                return slice(lo, lo + hw)

            cols = slice(h * hw, (h + 1) * hw)
            query, keys, values = rot_ref[r, part(0)], rot_ref[r, part(1)], rot_ref[r, part(2)]
            probs = prob_ref[r, h * count : (h + 1) * count]
            probs_b = probs.astype(BF)
            d_ctx = dctx[r, cols]
            d_values = mm_tn(probs_b, d_ctx)
            d_probs = mm_nt(d_ctx, values)
            delta = jnp.sum(probs_b.astype(F32) * d_probs, axis=-1, keepdims=True)
            d_scores = (probs * (d_probs - delta) * root).astype(BF)
            d_query = mm(d_scores, keys)
            d_keys = mm_tn(d_scores, query)
            dqkv[r, part(2)] = d_values.astype(BF)
            for g, x in enumerate((d_query, d_keys)):
                x = x * cos - swap_halves(x) * sin
                hat = hats_ref[r, part(g)]
                mine_g[2 + g : 3 + g, cols] += jnp.sum(x * hat, axis=0, keepdims=True)
                up = x * aux_ref[me, 3 + g : 4 + g, cols]
                ups[r, part(g)] = up
                totals[g] = totals[g] + row_sums(up * hat)
        for g in range(2):
            stats[pl.ds(g, 1), at] = totals[g]

    def attend_chip(q):
        attend(q * 2)
        attend(q * 2 + 1)

    a, b = pos[:2]

    def late():
        def there(u, _):
            attend_chip(line_order(u, a, na) * 2 + b)

            @pl.when(u < na - 1)
            def _():
                attend_chip(line_order(u, a, na) * 2 + 1 - b)

            return 0

        lax.fori_loop(0, na, there, 0)

    gather_loop(pos, count, buf, gsems, on_chip, hook, late)
    early = half * 5 // 8
    gu_rows.start(1, 0, early)
    attend_chip(line_order(na - 1, a, na) * 2 + 1 - b)
    packed[...] = stats[...].astype(BF)
    exchange_start(n_shard, packed, got, xs, xr)
    gu_rows.start(1, early, half)
    gu_rows.forward(0, 1, half)

    def out_cols(n, _):
        lo = rows_of(n, 256)
        oacc[:, lo] = mm_tn(ctx_ref[...], buf[:, lo]).astype(BF)
        return 0

    lax.fori_loop(0, width // 256, out_cols, 0)
    wout.start(0)

    def gain_take(k, _):
        gain_desc(k).wait_recv()
        mine_g[...] += ggot[k - 1]
        return 0

    lax.fori_loop(1, n_shard, gain_take, 0)
    for m in range(1, n_rep):
        gain_rep(m).start()
    exchange_finish(n_shard, stats, packed, got, xs, xr, inner)

    def settle(i, _):
        r = rows_of(i, count)
        at = pl.ds(pl.multiple_of(i * count, count), count)
        scale = scale_of(i)
        mean = inner[:, at] / width
        for g in range(2):
            lo = slice(g * own, (g + 1) * own)
            column = turned(scale[g : g + 1], count)[:, :1]
            down_by = turned(mean[g : g + 1], count)[:, :1]
            dqkv[r, lo] = (column * (ups[r, lo] - hats_ref[r, lo] * down_by)).astype(BF)
        return 0

    lax.fori_loop(0, n_shard, settle, 0)
    in_w.wait()
    in_t.wait()

    def partial(q):
        r = rows_of(q, big)

        def one(k, _):
            lo = rows_of(k, 512)
            p[r, lo] = mm_nt(dqkv[r, :], wq[lo, :]).astype(BF)
            return 0

        lax.fori_loop(0, width // 512, one, 0)

    most = 4 * own

    def grad_rows(k, _):
        at = rows_of(k, most)
        qacc[at, :] = mm_tn(tok[:, at], dqkv[...]).astype(BF)
        return 0

    def near_far(do, flip):
        def one(k, _):
            do(peer(k, flip, 1))
            return 0

        lax.fori_loop(0, half, one, 0)

    def work0():
        lax.fori_loop(0, width // most, grad_rows, 0)
        near_far(wqkv.start, 0)
        near_far(wqkv.start, 1)

    def work1():
        gu_rows.forward(1, 0, half)

    def work2():
        wout.add(0)
        wout_all.start()

    def work3():
        near_far(wqkv.add, 0)
        wqkv_rows.start_own()
        wqkv_rows.start(0, 1, half)

    def work4():
        near_far(wqkv.add, 1)
        wqkv_rows.start(1, 0, half)

    def work5():
        wqkv_rows.forward_own()
        wqkv_rows.forward(0, 1, half)

    def work6():
        wqkv_rows.forward(1, 0, half)

    scatter_loop(
        pos, count, bufs, ssems, partial, out_ref, [work0, work1, work2, work3, work4, work5, work6],
        "ff0" + "f" * (na - 2) + "12s3s45" + "s" * (na - 3) + "6",
    )

    def end(d, _):
        wqkv.sent(d)
        return 0

    lax.fori_loop(0, n_shard, end, 0)
    down.sent(0)
    wout.sent(0)

    def gain_sent(k, _):
        gain_desc(k).wait_send()
        return 0

    lax.fori_loop(1, n_shard, gain_sent, 0)
    gains_ref[...] = mine_g[...]
    for m in range(1, n_rep):
        gain_rep(m).wait_recv()
        gains_ref[...] += rgot[m - 1]
    for m in range(1, n_rep):
        gain_rep(m).wait_send()
    wqkv_rows.finish()
    gu_rows.finish()
    down_all.finish()
    wout_all.finish()


def rope_table(count, head_width):
    half_width = head_width // 2
    inverse = np.float32(THETA) ** (-(np.float32(2.0) * np.arange(half_width, dtype=np.float32)) / np.float32(head_width))
    angle = np.arange(count, dtype=np.float32)[:, None] * inverse[None, :].astype(np.float32)
    cosine, sine = np.cos(angle), np.sin(angle)
    rest = np.concatenate([cosine, cosine, -sine, sine], axis=1).astype(np.float32)
    parts = []
    for _ in range(3):
        parts.append(rest.astype(BF))
        rest = rest - parts[-1].astype(np.float32)
    return np.concatenate(parts, axis=1)


def make(n_rep, n_shard):
    chips = n_shard // 2

    def shards(
        tokens, segment_ids, cotangent, w_qkv, w_out, w_gate_up, w_down,
        q_gain, k_gain, attn_gain, mlp_gain,
    ):
        count, width = tokens.shape
        heads = H // n_shard
        hw = width // H
        own = width // n_shard
        ff = w_down.shape[0]
        total = count * n_shard
        gathered = pltpu.VMEM((total, width), BF)

        assert own == count
        aux = jnp.stack(
            [x.astype(F32) for x in (segment_ids, attn_gain, mlp_gain, q_gain, k_gain)]
            + [jnp.zeros((count,), F32)] * 3
        )
        table = jnp.asarray(rope_table(count, hw))
        chunk = n_shard - 1
        saved = [
            pltpu.VMEM((total, 2 * own), F32), pltpu.VMEM((total, 3 * own), BF),
            pltpu.VMEM((total, heads * count), F32), pltpu.VMEM((total, own), BF),
        ]
        (
            tokens_g, wq, wg, auxg, squares, hats, rots, probs, context_b,
            attn_hat, attn_scale, resid, resid_b,
        ) = call(
            functools.partial(attn_kernel, n_shard, n_rep, heads), "attn", 1,
            [
                ((total, width), BF, ANY), ((width, 3 * own), BF, ANY), ((width, 2 * ff), BF, ANY),
                ((n_shard, 8, count), F32, VM), ((2, total), F32, VM), ((total, 2 * own), F32, ANY),
                ((total, 3 * own), BF, ANY), ((total, heads * count), F32, ANY),
                ((total, own), BF, ANY), ((count, width), F32, VM), ((count, 128), F32, VM),
                ((count, width), F32, VM), ((count, width), BF, VM),
            ],
            [ANY, VM, ANY, VM, ANY, VM],
            saved + [
                pltpu.VMEM((1, width), F32), gathered, pltpu.VMEM((width, 3 * own), BF), pltpu.VMEM((own, 2 * ff), BF),
                pltpu.VMEM((total, 3 * own), F32), pltpu.VMEM((2, total), F32),
                pltpu.VMEM((chunk, 2, total), BF), pltpu.VMEM((2, total), BF),
                DMA((6,)), DMA((chips,)), DMA((chunk,)), DMA((chunk,)), DMA((chunk,)), DMA((chunk,)),
            ] + gather_sems(n_shard) + columns_sems(n_shard, n_rep, 3)
            + columns_sems(n_shard, n_rep, 2)
            + scatter_bufs(n_shard, count, width) + scatter_sems(n_shard),
            tokens, aux, w_qkv, w_out, w_gate_up, table,
        )
        resid_g, gate_up, mixed_b, output, d_down, grad_mlp = call(
            functools.partial(mlp_kernel, n_shard), "mlp", 3,
            [
                ((total, width), BF, ANY), ((total, 2 * ff), BF, ANY),
                ((total, ff), BF, ANY), ((count, width), BF, VM), ((count, width), BF, VM),
                ((1, width), F32, VM),
            ],
            [ANY, ANY, ANY, VM, VM, VM],
            [
                pltpu.VMEM((count, width), F32), pltpu.VMEM((1, width), F32),
                pltpu.VMEM((count, count), F32), gathered, pltpu.VMEM((width, 2 * ff), BF), pltpu.VMEM((ff, width), BF),
                pltpu.VMEM((total, 2 * ff), BF), pltpu.VMEM((total, ff), BF),
                DMA((3,)), DMA((chips,)), DMA((chips,)), DMA((chips,)),
            ] + scatter_bufs(n_shard, count, width) + scatter_sems(n_shard) + gather_sems(n_shard),
            resid_b, wg, w_down, auxg, resid, cotangent,
        )
        gu_sum, down_acc, d_resid, d_attn, norm_gains = call(
            functools.partial(mlp_back_kernel, n_shard, n_rep), "mlp_back", 4,
            [
                ((width // n_rep, 2 * ff), BF, ANY), ((ff, width), BF, ANY),
                ((count, width), F32, VM), ((count, width), BF, VM), ((n_shard, 8, own), F32, VM),
            ],
            [ANY] * 6 + [VM] * 5,
            [
                pltpu.VMEM((1, width), F32), pltpu.VMEM((1, width), F32),
                pltpu.VMEM((count, count), F32), gathered, pltpu.VMEM((width, 2 * ff), BF), pltpu.VMEM((ff, width), BF),
                pltpu.VMEM((total, 2 * ff), BF), pltpu.VMEM((total, 2 * ff), BF),
                gathered, pltpu.VMEM((total, ff), BF),
                pltpu.VMEM((ff, width), BF), DMA((5,)), DMA((chips,)), DMA((n_shard,)),
            ] + share_scratch(width, 2 * ff, n_shard, n_rep)
            + scatter_bufs(n_shard, count, width) + scatter_sems(n_shard) + gather_sems(n_shard),
            d_down, gate_up, wg, w_down, resid_g, mixed_b,
            auxg, cotangent, attn_hat, attn_scale, grad_mlp,
        )
        gu_rows, down_rows, out_rows, qkv_rows, gains, d_tokens_sum = call(
            functools.partial(attn_back_kernel, n_shard, n_rep, heads), "attn_back", 5,
            [
                ((own, n_shard * 2 * ff), BF, ANY), ((ff, width), BF, ANY), ((own, width), BF, ANY),
                ((own, 3 * width), BF, ANY), ((8, own), F32, VM), ((count, width), F32, VM),
            ],
            [ANY, ANY, VM, ANY, ANY, ANY, ANY, ANY, VM, VM, VM, VM, ANY, ANY],
            saved + [
                gathered, gathered, pltpu.VMEM((width, 3 * own), BF), pltpu.VMEM((total, own), BF),
                pltpu.VMEM((total, 2 * own), F32), pltpu.VMEM((total, 3 * own), BF),
                pltpu.VMEM((2, total), F32),
                pltpu.VMEM((2, total), F32), pltpu.VMEM((chunk, 2, total), BF),
                pltpu.VMEM((2, total), BF), pltpu.VMEM((chunk, 8, own), F32), pltpu.VMEM((8, own), F32),
                pltpu.VMEM((n_rep - 1, 8, own), F32),
                DMA((8,)), DMA((chunk,)), DMA((chunk,)), DMA((chunk,)), DMA((chunk,)),
                DMA((n_rep - 1,)), DMA((n_rep - 1,)),
            ] + gather_sems(n_shard) + scatter_bufs(n_shard, count, width) + scatter_sems(n_shard)
            + share_scratch(ff, width, 1, n_rep) + share_scratch(own, width, 1, n_rep)
            + share_scratch(width, 3 * own, n_shard, n_rep)
            + share_gather_sems(n_rep) * 2
            + rows_back_sems(n_shard, n_rep, 2) + rows_back_sems(n_shard, n_rep, 3),
            d_attn, tokens_g, w_out, wq, hats, rots, probs, context_b, auxg, squares,
            table, norm_gains, gu_sum, down_acc,
        )
        grad_tokens = d_resid + d_tokens_sum
        return (
            output, grad_tokens, qkv_rows.astype(F32), out_rows.astype(F32), gu_rows.astype(F32),
            down_rows.astype(F32), gains[2], gains[3], gains[0], gains[1],
        )

    return shards


def solution(mesh):
    rows = P(("rep", "shard"), None)
    return jax.shard_map(
        make(mesh.shape["rep"], mesh.shape["shard"]),
        mesh=mesh,
        in_specs=(rows, P(("rep", "shard")), rows)
        + (P("shard", None),) * 4
        + (P("shard"),) * 4,
        out_specs=(rows, rows) + (P("shard", None),) * 4 + (P("shard"),) * 4,
        check_vma=False,
    )
```
